32 devices in a mesh: ctx: 8 (over z, y), wt: 4 (over x, core).
Axes of the slice: x: 2, y: 2, z: 4, core: 2. Of those that a mesh axis runs over, the one named last changes fastest.
Arguments:
- tokens: bfloat16 [4, 2048, 2048], P('wt', 'ctx'), may hold values from -6 to 6
- out_grad: bfloat16 [4, 2048, 2048], P('wt', 'ctx'), may hold values from -6 to 6
- segments: int32 [4, 2048], P('wt', 'ctx'), may hold values from 0 to 7, never falling along the last dimension, each value on 1 to 1024 neighbouring positions
- adapter_index: int32 [4], P('wt'), may hold values from 0 to 7
- first_gain: float32 [2048], replicated, may hold values from 0.1 to 1.9
- first_bias: float32 [2048], replicated, may hold values from -3 to 3
- second_gain: float32 [2048], replicated, may hold values from 0.1 to 1.9
- second_bias: float32 [2048], replicated, may hold values from -3 to 3
- qkv_weight: bfloat16 [2048, 2304], P('wt'), may hold values from -0.125 to 0.125
- out_weight: bfloat16 [2048, 2048], P('wt'), may hold values from -0.5 to 0.5
- expand_weight: bfloat16 [2048, 8192], P('wt'), may hold values from -0.125 to 0.125
- shrink_weight: bfloat16 [8192, 2048], P('wt'), may hold values from -0.0625 to 0.0625
- query_first: bfloat16 [8, 2048, 16], replicated, may hold values from -0.125 to 0.125
- query_second: bfloat16 [8, 16, 2048], replicated, may hold values from -1.5 to 1.5
- key_first: bfloat16 [8, 2048, 16], replicated, may hold values from -0.125 to 0.125
- key_second: bfloat16 [8, 16, 128], replicated, may hold values from -1.5 to 1.5
- value_first: bfloat16 [8, 2048, 16], replicated, may hold values from -0.125 to 0.125
- value_second: bfloat16 [8, 16, 128], replicated, may hold values from -1.5 to 1.5
- output_first: bfloat16 [8, 2048, 16], replicated, may hold values from -0.5 to 0.5
- output_second: bfloat16 [8, 16, 2048], replicated, may hold values from -1.5 to 1.5
- expand_first: bfloat16 [8, 2048, 16], replicated, may hold values from -0.125 to 0.125
- expand_second: bfloat16 [8, 16, 8192], replicated, may hold values from -1.5 to 1.5
- shrink_first: bfloat16 [8, 8192, 16], replicated, may hold values from -0.0625 to 0.0625
- shrink_second: bfloat16 [8, 16, 2048], replicated, may hold values from -1.5 to 1.5
Outputs:
- layer_out: bfloat16 [4, 2048, 2048], P('wt', 'ctx')
- tokens_grad: bfloat16 [4, 2048, 2048], P('wt', 'ctx')
- grad_query_first: float32 [8, 2048, 16], P(None, 'wt')
- grad_query_second: float32 [8, 16, 2048], P(None, None, 'wt')
- grad_key_first: float32 [8, 2048, 16], P(None, 'wt')
- grad_key_second: float32 [8, 16, 128], P(None, None, 'wt')
- grad_value_first: float32 [8, 2048, 16], P(None, 'wt')
- grad_value_second: float32 [8, 16, 128], P(None, None, 'wt')
- grad_output_first: float32 [8, 2048, 16], P(None, 'wt')
- grad_output_second: float32 [8, 16, 2048], P(None, None, 'wt')
- grad_expand_first: float32 [8, 2048, 16], P(None, 'wt')
- grad_expand_second: float32 [8, 16, 8192], P(None, None, 'wt')
- grad_shrink_first: float32 [8, 8192, 16], P(None, 'wt')
- grad_shrink_second: float32 [8, 16, 2048], P(None, None, 'wt')
The draws below stay inside these ranges and needn't reach their ends.
Inputs may be any that keep to these rules, and one draw needn't show every extreme that they name: `segments`: within each sequence the numbers never fall; a document is a run of equal numbers of at most 1024 positions.
All inputs are finite; a program needn't handle non-finite values.
Results may differ from the reference program's by a relative error of at most 0.02.
Values may be sent and summed in bfloat16 or wider, within the bound.
A program may use at most 320 MiB of HBM per device.

```python
import math
import jax
import jax.numpy as jnp
import numpy as np
from jax import lax

D = 2048
HEADS = 16
HEAD = 128
FF = 8192
RANK = 16
ADAPTERS = 8
KEY_BLOCK = 512
SEQ = 2048
SEQS = 4
DOCS = 8
DOC_MOST = 1024


def place_ends(entries, own_key, low, largest):
    longest = entries.shape.index(max(entries.shape))
    spots = []
    for shift in (0, 1):
        where = [jax.random.randint(jax.random.fold_in(own_key, axis), (), 0, length) for axis, length in enumerate(entries.shape)]
        where[longest] = (where[longest] + shift) % entries.shape[longest]
        spots.append(tuple(where))
    return entries.at[spots[0]].set(low).at[spots[1]].set(largest)


def level_of(own_key, dims, pieces, smallest, high):
    def one(dim, shards_of):
        steps = jax.random.uniform(jax.random.fold_in(jax.random.fold_in(own_key, 6), dim), (shards_of,), jnp.float32, smallest / len(pieces), high / len(pieces))
        return jnp.repeat(jnp.exp(steps), dims[dim] // shards_of).reshape((-1,) + (1,) * (len(dims) - dim - 1))

    level = one(*pieces[0])
    for cut in pieces[1:]:
        level = level * one(*cut)
    return level


def length_profile(number_of, total, reach, slope):
    loads = [(1 << 20) // math.isqrt(grade ** slope) + 1 for grade in range(2, number_of + 1)]
    spare, given = total - reach - (number_of - 1), [1] * (number_of - 1)
    while spare > 0:
        movable = [i for i in range(number_of - 1) if given[i] < reach]
        pool, left = sum([loads[i] for i in movable]), spare
        for i in movable:
            extra = min(reach - given[i], max(1, left * loads[i] // pool), spare)
            given[i] = given[i] + extra
            spare = spare - extra
    return np.array([reach] + given)


def ragged(stream_key, count, total, limit, slope):
    if count == 2:
        one = jax.random.randint(stream_key, (), max(1, total - limit), min(limit, total - 1) + 1)
        return jnp.stack([one, total - one])
    lengths = jnp.asarray(length_profile(count, total, limit, slope), jnp.int32)
    couples = (count - 1) // 2
    source_of, receiver = lengths[1:1 + 2 * couples:2], lengths[2:2 + 2 * couples:2]
    room = jnp.minimum(source_of - 1, limit - receiver)
    moved = jax.random.randint(jax.random.fold_in(stream_key, 1), (couples,), 0, 1 << 20) % (room + 1)
    lengths = lengths.at[1:1 + 2 * couples:2].set(source_of - moved).at[2:2 + 2 * couples:2].set(receiver + moved)
    return lengths[jax.random.permutation(jax.random.fold_in(stream_key, 2), count)]


def centred(key, dims, scale, bound, pieces=(), kind=jnp.bfloat16):
    values = scale * jax.random.normal(key, dims, jnp.float32)
    if pieces:
        values = values * level_of(key, dims, pieces, -0.22, 0.18)
    return jnp.clip(values, -bound, bound).astype(kind)


def setup_inputs(seed: int = 0) -> dict:
    key_list = jax.random.split(jax.random.key(seed), 25)
    return {
        "tokens": centred(key_list[0], (SEQS, SEQ, D), 1.0, 6.0, ((0, 4), (1, 8))),
        "out_grad": centred(key_list[1], (SEQS, SEQ, D), 1.0, 6.0, ((0, 4), (1, 8))),
        "segments": jax.vmap(lambda own: jnp.searchsorted(jnp.cumsum(ragged(own, DOCS, SEQ, DOC_MOST, 2)), jnp.arange(SEQ), side="right"))(jax.random.split(key_list[2], SEQS)).reshape((SEQS, SEQ)).astype(jnp.int32),
        "adapter_index": place_ends(jax.random.randint(key_list[3], (SEQS,), 0, ADAPTERS), jax.random.fold_in(key_list[3], 1), 0, ADAPTERS - 1).astype(jnp.int32),
        "first_gain": jnp.clip(1.0 + 0.18 * jax.random.normal(key_list[4], (D,), jnp.float32), 0.1, 1.9),
        "first_bias": centred(key_list[5], (D,), 0.5, 3.0, (), jnp.float32),
        "second_gain": jnp.clip(1.0 + 0.18 * jax.random.normal(key_list[6], (D,), jnp.float32), 0.1, 1.9),
        "second_bias": centred(key_list[7], (D,), 0.5, 3.0, (), jnp.float32),
        "qkv_weight": centred(key_list[8], (D, D + 2 * HEAD), D ** -0.5, 0.125, ((0, 4),)),
        "out_weight": centred(key_list[9], (D, D), (D // HEADS) ** -0.5, 0.5, ((0, 4),)),
        "expand_weight": centred(key_list[10], (D, FF), D ** -0.5, 0.125, ((0, 4),)),
        "shrink_weight": centred(key_list[11], (FF, D), FF ** -0.5, 0.0625, ((0, 4),)),
        "query_first": centred(key_list[12], (ADAPTERS, D, RANK), D ** -0.5, 0.125),
        "query_second": centred(key_list[13], (ADAPTERS, RANK, D), RANK ** -0.5, 1.5),
        "key_first": centred(key_list[14], (ADAPTERS, D, RANK), D ** -0.5, 0.125),
        "key_second": centred(key_list[15], (ADAPTERS, RANK, HEAD), RANK ** -0.5, 1.5),
        "value_first": centred(key_list[16], (ADAPTERS, D, RANK), D ** -0.5, 0.125),
        "value_second": centred(key_list[17], (ADAPTERS, RANK, HEAD), RANK ** -0.5, 1.5),
        "output_first": centred(key_list[18], (ADAPTERS, D, RANK), (D // HEADS) ** -0.5, 0.5),
        "output_second": centred(key_list[19], (ADAPTERS, RANK, D), RANK ** -0.5, 1.5),
        "expand_first": centred(key_list[20], (ADAPTERS, D, RANK), D ** -0.5, 0.125),
        "expand_second": centred(key_list[21], (ADAPTERS, RANK, FF), RANK ** -0.5, 1.5),
        "shrink_first": centred(key_list[22], (ADAPTERS, FF, RANK), FF ** -0.5, 0.0625),
        "shrink_second": centred(key_list[23], (ADAPTERS, RANK, D), RANK ** -0.5, 1.5),
    }


@jax.custom_vjp
def low(v):
    return lax.optimization_barrier(v.astype(jnp.bfloat16)).astype(jnp.float32)

@jax.custom_vjp
def low_back(v):
    return v

def low_keep(v):
    return (low(v), None)

def low_pass(kept, grad):
    return (grad,)

def back_keep(v):
    return (v, None)

def back_low(kept, grad):
    return (low(grad),)
low.defvjp(low_keep, low_pass)
low_back.defvjp(back_keep, back_low)
LOWEST = -1e+30

def product(left, right):
    return jnp.dot(left, right, precision=lax.Precision.HIGHEST, preferred_element_type=jnp.float32)

def layer_norm(values, gain, offset):
    centre = values - lax.optimization_barrier(jnp.mean(values, -1, keepdims=True))
    scale_inv = lax.rsqrt(lax.optimization_barrier(jnp.mean(centre * centre, -1, keepdims=True)) + 1e-05)
    return centre * scale_inv * gain + offset

def attend(query, keys, values, seg):
    length = keys.shape[0]
    heads = query.shape[1]
    head_size = query.shape[2]
    place = jnp.arange(length, dtype=jnp.int32)
    blocks = length // KEY_BLOCK
    score_scale = 1.0 / math.sqrt(head_size)

    def one_block(item):
        query_block, seg_block, place_block = item
        raw = jnp.einsum('thd,kd->thk', query_block, keys, precision=lax.Precision.HIGHEST, preferred_element_type=jnp.float32)
        scores = low_back(raw * score_scale)
        allowed = (seg_block[:, None] == seg[None, :]) & (place_block[:, None] >= place[None, :])
        scores = jnp.where(allowed[:, None, :], scores, LOWEST)
        highest = lax.optimization_barrier(jnp.max(scores, -1, keepdims=True))
        weights = jnp.exp(scores - highest)
        probs = weights / lax.optimization_barrier(jnp.sum(weights, -1, keepdims=True))
        return jnp.einsum('thk,kd->thd', low(probs), values, precision=lax.Precision.HIGHEST, preferred_element_type=jnp.float32)
    outputs = lax.map(jax.checkpoint(one_block), (query.reshape(blocks, KEY_BLOCK, heads, head_size), seg.reshape(blocks, KEY_BLOCK), place.reshape(blocks, KEY_BLOCK)))
    return outputs.reshape(length, heads * head_size)

def forward(hidden, adapt, which, seg, frozen):
    gain_one, bias_one, gain_two, bias_two, qkv_weight, out_weight, expand_weight, shrink_weight = frozen
    chosen = [lax.dynamic_index_in_dim(table, which, 0, keepdims=False) for table in adapt]
    query_a, query_b, key_a, key_b, value_a, value_b, output_a, output_b, expand_a, expand_b, shrink_a, shrink_b = chosen
    width = hidden.shape[1]
    head_size = key_b.shape[1]
    heads = width // head_size
    first = low(layer_norm(hidden, gain_one, bias_one))
    base = product(first, qkv_weight)
    query_low = low(low_back(product(first, query_a)))
    key_low = low(low_back(product(first, key_a)))
    value_low = low(low_back(product(first, value_a)))
    query = low(low_back(base[:, :width] + product(query_low, query_b)))
    keys = low(low_back(base[:, width:width + head_size] + product(key_low, key_b)))
    values = low(low_back(base[:, width + head_size:] + product(value_low, value_b)))
    attended = low(low_back(attend(query.reshape(-1, heads, head_size), keys, values, seg)))
    output_low = low(low_back(product(attended, output_a)))
    middle = hidden + low_back(product(attended, out_weight) + product(output_low, output_b))
    second = low(layer_norm(middle, gain_two, bias_two))
    expand_low = low(low_back(product(second, expand_a)))
    upward = low_back(product(second, expand_weight) + product(expand_low, expand_b))
    active = low(low_back(jax.nn.gelu(upward, approximate=True)))
    shrink_low = low(low_back(product(active, shrink_a)))
    return middle + low_back(product(active, shrink_weight) + product(shrink_low, shrink_b))

def reference(tokens, out_grad, segments, adapter_index, first_gain, first_bias, second_gain, second_bias, qkv_weight, out_weight, expand_weight, shrink_weight, query_first, query_second, key_first, key_second, value_first, value_second, output_first, output_second, expand_first, expand_second, shrink_first, shrink_second):
    frozen = (first_gain.astype(jnp.float32), first_bias.astype(jnp.float32), second_gain.astype(jnp.float32), second_bias.astype(jnp.float32), qkv_weight.astype(jnp.float32), out_weight.astype(jnp.float32), expand_weight.astype(jnp.float32), shrink_weight.astype(jnp.float32))
    adapters = (query_first.astype(jnp.float32), query_second.astype(jnp.float32), key_first.astype(jnp.float32), key_second.astype(jnp.float32), value_first.astype(jnp.float32), value_second.astype(jnp.float32), output_first.astype(jnp.float32), output_second.astype(jnp.float32), expand_first.astype(jnp.float32), expand_second.astype(jnp.float32), shrink_first.astype(jnp.float32), shrink_second.astype(jnp.float32))

    def one_sequence(totals, item):
        hidden, grad_out, seg, which = item

        def layer(hidden_in, adapt):
            return forward(hidden_in, adapt, which, seg, frozen)
        result, pull = jax.vjp(layer, hidden, adapters)
        grad_in, grad_adapt = pull(grad_out)
        totals = jax.tree.map(lambda left, right: left + right, totals, grad_adapt)
        return (totals, (result.astype(jnp.bfloat16), grad_in.astype(jnp.bfloat16)))
    zeros = jax.tree.map(jnp.zeros_like, adapters)
    totals, (results, grads) = lax.scan(one_sequence, zeros, (tokens.astype(jnp.float32), out_grad.astype(jnp.float32), segments, adapter_index))
    return (results, grads, totals[0], totals[1], totals[2], totals[3], totals[4], totals[5], totals[6], totals[7], totals[8], totals[9], totals[10], totals[11])
```

```python
import functools
import math

import jax
import jax.numpy as jnp
from jax import lax
from jax.experimental import pallas as pl
from jax.experimental.pallas import tpu as pltpu
from jax.sharding import PartitionSpec as P

HEADS = 16
HEAD = 128
ADAPTERS = 8
KEY_BLOCK = 512


EPSILON = 1e-05
LOWEST = -1e30


def matmul(left, right):
    return jnp.dot(left, right, preferred_element_type=jnp.float32)


def matmul_right_t(left, right):
    return lax.dot_general(
        left, right, (((1,), (1,)), ((), ())), preferred_element_type=jnp.float32
    )


def matmul_left_t(left, right):
    return lax.dot_general(
        left, right, (((0,), (0,)), ((), ())), preferred_element_type=jnp.float32
    )


def layer_norm(values, gain, offset):
    centre = values - jnp.mean(values, -1, keepdims=True)
    scale_inv = lax.rsqrt(jnp.mean(centre * centre, -1, keepdims=True) + EPSILON)
    normed = centre * scale_inv
    return (normed * gain + offset, normed, scale_inv)


def norm_back(grad_out, gain, normed, scale_inv):
    grad_norm = grad_out * gain
    return scale_inv * (
        grad_norm
        - jnp.mean(grad_norm, -1, keepdims=True)
        - normed * jnp.mean(grad_norm * normed, -1, keepdims=True)
    )


def gelu_tanh(values):
    return jax.nn.gelu(values, approximate=True)


def fold_rows(left, piece):
    return matmul(left, piece)


def project_back(grad_low, piece):
    return matmul_right_t(grad_low, piece)


def spread_table(onehot, table):
    return onehot[:, None, None] * table[None]


MESH = pl.DeviceIdType.MESH
GELU_SCALE = 0.7978845608


def dot_nn(left, right):
    return lax.dot_general(
        left, right, (((1,), (0,)), ((), ())), preferred_element_type=jnp.float32
    )


def dot_nt(left, right):
    return lax.dot_general(
        left, right, (((1,), (1,)), ((), ())), preferred_element_type=jnp.float32
    )


def dot_tn(left, right):
    return lax.dot_general(
        left, right, (((0,), (0,)), ((), ())), preferred_element_type=jnp.float32
    )


def mlp_kernel(
    dims,
    h2_ref,
    dy_ref,
    low_ref,
    ext_ref,
    we_own,
    we_one,
    we_two,
    we_three,
    ws_hbm,
    out_ref,
    dh_ref,
    lows_ref,
    gexp_ref,
    gshr_ref,
    ids_ref,
    h2_all,
    dy_all,
    low_all,
    ext_all,
    we,
    ws,
    act,
    dup,
    sis_send,
    sis_recv,
    own_recv,
    far_part,
    far_send,
    far_recv,
    low_send,
    low_recv,
    in_send_sem,
    in_recv_sem,
    sis_send_sem,
    sis_recv_sem,
    own_send_sem,
    own_recv_sem,
    far_send_sem,
    far_recv_sem,
    low_send_sem,
    low_recv_sem,
    local_sem,
):
    tok, width, units, rank, rows = dims
    me = lax.axis_index("wt")
    core = lax.rem(me, 2)
    side = lax.div(me, 2)
    sister = me + 1 - 2 * core
    across = me + 2 - 4 * side
    diagonal = sister + 2 - 4 * side
    tile_a = 256
    tile_b = 512
    tiles_a = units // tile_a
    tiles_b = width // tile_b

    local = [
        pltpu.make_async_copy(
            we_own.at[:, pl.ds(pl.multiple_of(me * units, units), units)],
            we.at[pl.ds(pl.multiple_of(me * rows, rows), rows)],
            local_sem.at[0],
        ),
        pltpu.make_async_copy(
            we_one, we.at[pl.ds(pl.multiple_of(sister * rows, rows), rows)], local_sem.at[1]
        ),
        pltpu.make_async_copy(
            we_two, we.at[pl.ds(pl.multiple_of(across * rows, rows), rows)], local_sem.at[2]
        ),
        pltpu.make_async_copy(
            we_three, we.at[pl.ds(pl.multiple_of(diagonal * rows, rows), rows)], local_sem.at[3]
        ),
        pltpu.make_async_copy(ws_hbm, ws, local_sem.at[4]),
        pltpu.make_async_copy(h2_ref, h2_all.at[pl.ds(0, tok)], local_sem.at[5]),
        pltpu.make_async_copy(dy_ref, dy_all.at[pl.ds(0, tok)], local_sem.at[6]),
        pltpu.make_async_copy(low_ref, low_all.at[0], local_sem.at[7]),
        pltpu.make_async_copy(ext_ref.at[me], ext_all.at[0], local_sem.at[8]),
    ]
    for copy in local:
        copy.start()

    barrier = pltpu.get_barrier_semaphore()
    for peer in (sister, across, diagonal):
        pl.semaphore_signal(barrier, inc=1, device_id={"wt": peer}, device_id_type=MESH)
    pl.semaphore_wait(barrier, 3)

    def remote(src, dst, send, recv, peer):
        return pltpu.make_async_remote_copy(
            src_ref=src,
            dst_ref=dst,
            send_sem=send,
            recv_sem=recv,
            device_id={"wt": peer},
            device_id_type=MESH,
        )

    def entry(number, src, dst, peer):
        return remote(src, dst, in_send_sem.at[number], in_recv_sem.at[number], peer)

    half = tok // 2
    tops = [pl.ds(0, half), pl.ds(half, half)]

    def slot_rows(slot, piece):
        return pl.ds(slot * tok + piece * half, half)

    near = [
        entry(0, low_ref, low_all.at[1], sister),
        entry(1, ext_ref.at[sister], ext_all.at[1], sister),
        entry(2, h2_ref, h2_all.at[pl.ds(tok, tok)], sister),
        entry(3, dy_ref, dy_all.at[pl.ds(tok, tok)], sister),
    ]
    direct = [
        entry(4, low_ref, low_all.at[2], across),
        entry(5, ext_ref.at[across], ext_all.at[2], across),
        entry(6, low_ref, low_all.at[3], diagonal),
        entry(7, ext_ref.at[diagonal], ext_all.at[3], diagonal),
    ]
    far = [entry(8 + i, h2_ref.at[tops[i]], h2_all.at[slot_rows(2, i)], across) for i in range(2)]
    far += [entry(10 + i, dy_ref.at[tops[i]], dy_all.at[slot_rows(2, i)], across) for i in range(2)]
    relay = [
        entry(12 + i, h2_all.at[slot_rows(2, i)], h2_all.at[slot_rows(3, i)], sister)
        for i in range(2)
    ]
    relay += [
        entry(14 + i, dy_all.at[slot_rows(2, i)], dy_all.at[slot_rows(3, i)], sister)
        for i in range(2)
    ]
    for copy in near + direct + far:
        copy.start()

    def front(pair):
        pair_rows = pl.ds(pair * 2 * tok, 2 * tok)

        def step(number, carry):
            cols = pl.ds(pl.multiple_of(number * tile_a, tile_a), tile_a)

            def with_low(kind):
                parts = []
                for own in range(2):
                    slot = 2 * pair + own
                    small = low_all[slot, :, kind * 128 : kind * 128 + rank]
                    parts.append(dot_nn(small, ext_all[slot, kind, :, cols]))
                return jnp.concatenate(parts, 0)

            upward = dot_nn(h2_all[pair_rows, :], we[:, cols]) + with_low(0)
            square = upward * upward
            bend = jnp.tanh(GELU_SCALE * (upward + 0.044715 * (square * upward)))
            active = (0.5 * upward * (1.0 + bend)).astype(jnp.bfloat16)
            slope = 0.5 * (1.0 + bend) + 0.5 * upward * (1.0 - bend * bend) * GELU_SCALE * (
                1.0 + 3.0 * 0.044715 * square
            )
            grad = (dot_nt(dy_all[pair_rows, :], ws[cols, :]) + with_low(1)).astype(jnp.bfloat16)
            grad_up = (grad.astype(jnp.float32) * slope).astype(jnp.bfloat16)
            act[:, cols] = active
            dup[:, cols] = grad_up
            for own in range(2):
                slot = 2 * pair + own
                picked = slice(own * tok, (own + 1) * tok)
                gexp_ref[slot, :, cols] = dot_tn(low_all[slot, :, 0:rank], grad_up[picked])
                gshr_ref[slot, :, cols] = dot_tn(low_all[slot, :, 128 : 128 + rank], active[picked])
            return carry

        lax.fori_loop(0, tiles_a, step, 0)

    def low_parts(pair):
        parts = []
        for own in range(2):
            slot = 2 * pair + own
            picked = pl.ds(own * tok, tok)
            grad_low = dot_nt(dup[picked, :], ext_all[slot, 0])
            act_low = dot_nt(act[picked, :], ext_all[slot, 1])
            parts.append((grad_low, act_low))
        return parts

    def back_tile(kind, number):
        cols = pl.ds(pl.multiple_of(number * tile_b, tile_b), tile_b)
        if kind == 0:
            return dot_nt(dup[...], we[cols, :])
        return dot_nn(act[...], ws[:, cols])

    def sis_copy(kind, number):
        return remote(
            sis_send.at[1, kind, number],
            sis_recv.at[kind, number],
            sis_send_sem.at[kind, number],
            sis_recv_sem.at[kind, number],
            sister,
        )

    def own_copy(kind, number):
        return remote(
            sis_send.at[0, kind, number],
            own_recv.at[kind, number],
            own_send_sem.at[kind, number],
            own_recv_sem.at[kind, number],
            sister,
        )

    def far_copy(kind, number):
        return remote(
            far_send.at[kind, number],
            far_recv.at[kind, number],
            far_send_sem.at[kind, number],
            far_recv_sem.at[kind, number],
            across,
        )

    for copy in local:
        copy.wait()
    for copy in near:
        copy.wait_recv()
    front(0)
    for index in range(4):
        far[index].wait_recv()
        relay[index].start()

    low_send[...] = jnp.zeros_like(low_send)
    lows_ref[...] = jnp.zeros_like(lows_ref)
    parts = low_parts(0)
    lows_ref[:, 0:rank] = parts[0][0]
    lows_ref[:, 128 : 128 + rank] = parts[0][1]
    low_send[0, :, 0:rank] = parts[1][0].astype(jnp.bfloat16)
    low_send[0, :, 128 : 128 + rank] = parts[1][1].astype(jnp.bfloat16)
    low_own = remote(
        low_send.at[0], low_recv.at[0], low_send_sem.at[0], low_recv_sem.at[0], sister
    )
    low_own.start()
    for kind, target in ((0, dh_ref), (1, out_ref)):

        def near_step(number, carry, kind=kind, target=target):
            cols = pl.ds(pl.multiple_of(number * tile_b, tile_b), tile_b)
            both = back_tile(kind, number)
            target[:, cols] = both[:tok]
            sis_send[0, kind, number] = both[tok:].astype(jnp.bfloat16)
            own_copy(kind, number).start()
            return carry

        lax.fori_loop(0, tiles_b, near_step, 0)

    for copy in direct:
        copy.wait_recv()
    for copy in relay:
        copy.wait_recv()
    front(1)
    parts = low_parts(1)
    low_send[1, :, 0:rank] = parts[1][0].astype(jnp.bfloat16)
    low_send[1, :, 128 : 128 + rank] = parts[1][1].astype(jnp.bfloat16)
    low_sis = remote(
        low_send.at[1], low_recv.at[1], low_send_sem.at[1], low_recv_sem.at[1], sister
    )
    low_sis.start()
    for kind in range(2):

        def far_step(number, carry, kind=kind):
            both = back_tile(kind, number)
            far_part[number] = both[:tok]
            sis_send[1, kind, number] = both[tok:].astype(jnp.bfloat16)
            sis_copy(kind, number).start()
            return carry

        def join_step(number, carry, kind=kind):
            sis_copy(kind, number).wait_recv()
            far_send[kind, number] = (
                far_part[number] + sis_recv[kind, number].astype(jnp.float32)
            ).astype(jnp.bfloat16)
            far_copy(kind, number).start()
            return carry

        lax.fori_loop(0, tiles_b, far_step, 0)
        lax.fori_loop(0, tiles_b, join_step, 0)
    low_sis.wait_recv()
    low_send[2, :, 0:rank] = (
        parts[0][0] + low_recv[1, :, 0:rank].astype(jnp.float32)
    ).astype(jnp.bfloat16)
    low_send[2, :, 128 : 128 + rank] = (
        parts[0][1] + low_recv[1, :, 128 : 128 + rank].astype(jnp.float32)
    ).astype(jnp.bfloat16)
    low_far = remote(
        low_send.at[2], low_recv.at[2], low_send_sem.at[2], low_recv_sem.at[2], across
    )
    low_far.start()
    for slot in range(4):
        ids_ref[slot] = low_all[slot, 0:16, 128:256].astype(jnp.float32)

    for kind, target in ((0, dh_ref), (1, out_ref)):

        def end_step(number, carry, kind=kind, target=target):
            cols = pl.ds(pl.multiple_of(number * tile_b, tile_b), tile_b)
            own_copy(kind, number).wait_recv()
            far_copy(kind, number).wait_recv()
            target[:, cols] = (
                target[:, cols]
                + own_recv[kind, number].astype(jnp.float32)
                + far_recv[kind, number].astype(jnp.float32)
            )
            own_copy(kind, number).wait_send()
            sis_copy(kind, number).wait_send()
            far_copy(kind, number).wait_send()
            return carry

        lax.fori_loop(0, tiles_b, end_step, 0)
    low_own.wait_recv()
    low_far.wait_recv()
    lows_ref[...] = (
        lows_ref[...] + low_recv[0].astype(jnp.float32) + low_recv[2].astype(jnp.float32)
    )
    for copy in near + direct + far + relay + [low_own, low_sis, low_far]:
        copy.wait_send()


def mlp_call(normed, grad_top, low, ext, pieces, shrink_weight, rank):
    tok, width = normed.shape
    units = shrink_weight.shape[0]
    rows = pieces[0].shape[0]
    tiles = width // 512
    bf = jnp.bfloat16
    full = lambda: pl.BlockSpec(memory_space=pltpu.VMEM)
    hbm = lambda: pl.BlockSpec(memory_space=pl.ANY)
    dma = pltpu.SemaphoreType.DMA
    return pl.pallas_call(
        functools.partial(mlp_kernel, (tok, width, units, rank, rows)),
        out_shape=(
            jax.ShapeDtypeStruct((tok, width), jnp.float32),
            jax.ShapeDtypeStruct((tok, width), jnp.float32),
            jax.ShapeDtypeStruct((tok, 256), jnp.float32),
            jax.ShapeDtypeStruct((4, rank, units), jnp.float32),
            jax.ShapeDtypeStruct((4, rank, units), jnp.float32),
            jax.ShapeDtypeStruct((4, 16, 128), jnp.float32),
        ),
        in_specs=[full(), full(), full(), full(), hbm(), hbm(), hbm(), hbm(), hbm()],
        out_specs=(full(), full(), full(), full(), full(), full()),
        scratch_shapes=[
            pltpu.VMEM((4 * tok, width), bf),
            pltpu.VMEM((4 * tok, width), bf),
            pltpu.VMEM((4, tok, 256), bf),
            pltpu.VMEM((4, 2, rank, units), bf),
            pltpu.VMEM((width, units), bf),
            pltpu.VMEM((units, width), bf),
            pltpu.VMEM((2 * tok, units), bf),
            pltpu.VMEM((2 * tok, units), bf),
            pltpu.VMEM((2, 2, tiles, tok, 512), bf),
            pltpu.VMEM((2, tiles, tok, 512), bf),
            pltpu.VMEM((2, tiles, tok, 512), bf),
            pltpu.VMEM((tiles, tok, 512), jnp.float32),
            pltpu.VMEM((2, tiles, tok, 512), bf),
            pltpu.VMEM((2, tiles, tok, 512), bf),
            pltpu.VMEM((3, tok, 256), bf),
            pltpu.VMEM((3, tok, 256), bf),
            dma((16,)),
            dma((16,)),
            dma((2, tiles)),
            dma((2, tiles)),
            dma((2, tiles)),
            dma((2, tiles)),
            dma((2, tiles)),
            dma((2, tiles)),
            dma((3,)),
            dma((3,)),
            dma((9,)),
        ],
        compiler_params=pltpu.CompilerParams(
            collective_id=1, has_side_effects=True, vmem_limit_bytes=63 * 1024 * 1024
        ),
        name="mlp",
    )(normed, grad_top, low, ext, *pieces, shrink_weight)


def body(
    tokens,
    out_grad,
    segments,
    adapter_index,
    first_gain,
    first_bias,
    second_gain,
    second_bias,
    qkv_weight,
    out_weight,
    expand_weight,
    shrink_weight,
    query_first,
    query_second,
    key_first,
    key_second,
    value_first,
    value_second,
    output_first,
    output_second,
    expand_first,
    expand_second,
    shrink_first,
    shrink_second,
):
    hidden = tokens[0].astype(jnp.float32)
    tok_count = hidden.shape[0]
    model_width = hidden.shape[1]
    chosen = adapter_index[0]

    def select(table):
        return lax.dynamic_index_in_dim(table, chosen, 0, keepdims=False)

    own_query_first = select(query_first)
    own_query_second = select(query_second)
    own_key_first = select(key_first)
    own_key_second = select(key_second)
    own_value_first = select(value_first)
    own_value_second = select(value_second)
    own_output_first = select(output_first)
    own_output_second = select(output_second)
    own_expand_first = select(expand_first)
    own_expand_second = select(expand_second)
    own_shrink_first = select(shrink_first)
    own_shrink_second = select(shrink_second)
    rank_width = own_query_first.shape[1]
    score_scale = 1.0 / math.sqrt(HEAD)
    normed_one, plain_one, inverse_one = layer_norm(hidden, first_gain, first_bias)
    first_low = normed_one.astype(jnp.bfloat16)
    attn_first = jnp.concatenate([own_query_first, own_key_first, own_value_first], 1)
    low_rank = matmul(first_low, attn_first).astype(jnp.bfloat16)
    base = fold_rows(first_low, lax.all_gather(qkv_weight, "wt", axis=0, tiled=True))
    query = (
        (base[:, :model_width] + matmul(low_rank[:, :rank_width], own_query_second))
        .astype(jnp.bfloat16)
        .reshape(tok_count, HEADS, HEAD)
    )
    keys_own = (
        base[:, model_width : model_width + HEAD]
        + matmul(low_rank[:, rank_width : 2 * rank_width], own_key_second)
    ).astype(jnp.bfloat16)
    values_own = (
        base[:, model_width + HEAD :] + matmul(low_rank[:, 2 * rank_width :], own_value_second)
    ).astype(jnp.bfloat16)
    keys_all, values_all, segs_all = (
        lax.all_gather(keys_own, "ctx", axis=0, tiled=True),
        lax.all_gather(values_own, "ctx", axis=0, tiled=True),
        lax.all_gather(segments[0], "ctx", axis=0, tiled=True),
    )
    query_segs = segments[0]
    position = lax.axis_index("ctx") * tok_count + jnp.arange(tok_count, dtype=jnp.int32)
    first_block = jnp.sum((segs_all < query_segs[0]).astype(jnp.int32)) // KEY_BLOCK
    stop_block = position[tok_count - 1] // KEY_BLOCK + 1
    offsets = jnp.arange(KEY_BLOCK, dtype=jnp.int32)

    def block_scores(start):
        key_block = lax.dynamic_slice_in_dim(keys_all, start, KEY_BLOCK, 0)
        value_block = lax.dynamic_slice_in_dim(values_all, start, KEY_BLOCK, 0)
        seg_block = lax.dynamic_slice_in_dim(segs_all, start, KEY_BLOCK, 0)
        allowed = (query_segs[:, None] == seg_block[None, :]) & (
            position[:, None] >= start + offsets[None, :]
        )
        raw = (
            jnp.einsum("thd,kd->thk", query, key_block, preferred_element_type=jnp.float32)
            * score_scale
        )
        return (jnp.where(allowed[:, None, :], raw, LOWEST), allowed, key_block, value_block)

    def stats_step(index, carry):
        highest, total = carry
        scores, allowed, key_block, value_block = block_scores(index * KEY_BLOCK)
        new_high = jnp.maximum(highest, jnp.max(scores, -1))
        weights = jnp.where(allowed[:, None, :], jnp.exp(scores - new_high[..., None]), 0.0)
        return (new_high, total * jnp.exp(highest - new_high) + jnp.sum(weights, -1))

    highest, total = lax.fori_loop(
        first_block,
        stop_block,
        stats_step,
        (
            jnp.full((tok_count, HEADS), LOWEST, jnp.float32),
            jnp.zeros((tok_count, HEADS), jnp.float32),
        ),
    )
    log_total = highest + jnp.log(total)

    def value_step(index, gathered):
        scores, allowed, key_block, value_block = block_scores(index * KEY_BLOCK)
        probs = jnp.where(allowed[:, None, :], jnp.exp(scores - log_total[..., None]), 0.0).astype(
            jnp.bfloat16
        )
        return gathered + jnp.einsum(
            "thk,kd->thd", probs, value_block, preferred_element_type=jnp.float32
        )

    attended = lax.fori_loop(
        first_block, stop_block, value_step, jnp.zeros((tok_count, HEADS, HEAD), jnp.float32)
    )
    attended_low = attended.reshape(tok_count, model_width).astype(jnp.bfloat16)
    output_low = matmul(attended_low, own_output_first).astype(jnp.bfloat16)
    branch = fold_rows(attended_low, lax.all_gather(out_weight, "wt", axis=0, tiled=True))
    middle = hidden + branch + matmul(output_low, own_output_second)
    normed_two, plain_two, inverse_two = layer_norm(middle, second_gain, second_bias)
    second_low = normed_two.astype(jnp.bfloat16)
    expand_low = matmul(second_low, own_expand_first).astype(jnp.bfloat16)
    grad_low = out_grad[0]
    grad_top = grad_low.astype(jnp.float32)
    grad_shrink_low = matmul_right_t(grad_low, own_shrink_second).astype(jnp.bfloat16)
    blank = jnp.zeros((tok_count, 128 - rank_width), jnp.bfloat16)
    mark = jnp.zeros((tok_count, 128 - rank_width), jnp.bfloat16) + chosen.astype(jnp.bfloat16)
    low_pack = jnp.concatenate([expand_low, blank, grad_shrink_low, mark], 1)
    members = lax.axis_size("wt")
    units = shrink_weight.shape[0]
    ext = jnp.stack(
        [
            own_expand_second.reshape(rank_width, members, units).transpose(1, 0, 2),
            own_shrink_first.T.reshape(rank_width, members, units).transpose(1, 0, 2),
        ],
        1,
    )
    member = lax.axis_index("wt")
    pieces = [expand_weight]
    for hop in (1, 2, 3):
        part = lax.dynamic_slice_in_dim(expand_weight, (member ^ hop) * units, units, 1)
        pieces.append(lax.ppermute(part, "wt", [(i, i ^ hop) for i in range(members)]))
    shrunk, grad_second, low_sums, expand_grads, shrink_grads, marks = mlp_call(
        second_low, grad_low, low_pack, ext, pieces, shrink_weight, rank_width
    )
    grad_expand_low = low_sums[:, :rank_width].astype(jnp.bfloat16)
    shrink_low = low_sums[:, 128 : 128 + rank_width].astype(jnp.bfloat16)
    layer_out = (middle + shrunk + matmul(shrink_low, own_shrink_second)).astype(jnp.bfloat16)[None]
    grad_second = grad_second + matmul_right_t(grad_expand_low, own_expand_first)
    shrink_second_grad = matmul_left_t(shrink_low, grad_low)
    expand_first_grad = matmul_left_t(second_low, grad_expand_low)
    grad_middle = grad_top + norm_back(grad_second, second_gain, plain_two, inverse_two)
    grad_branch = grad_middle.astype(jnp.bfloat16)
    grad_output_low = matmul_right_t(grad_branch, own_output_second).astype(jnp.bfloat16)
    grad_attended = project_back(
        grad_branch, lax.all_gather(out_weight, "wt", axis=0, tiled=True)
    ) + matmul_right_t(grad_output_low, own_output_first)
    output_second_grad = matmul_left_t(output_low, grad_branch)
    output_first_grad = matmul_left_t(attended_low, grad_output_low)
    grad_attn_low = grad_attended.astype(jnp.bfloat16).reshape(tok_count, HEADS, HEAD)
    delta = jnp.sum(grad_attn_low.astype(jnp.float32) * attended, -1)
    seq_length = keys_all.shape[0]

    def back_step(index, carry):
        grad_query, grad_keys, grad_values = carry
        start = index * KEY_BLOCK
        scores, allowed, key_block, value_block = block_scores(start)
        probs = jnp.where(allowed[:, None, :], jnp.exp(scores - log_total[..., None]), 0.0)
        probs_low = probs.astype(jnp.bfloat16)
        grad_probs = jnp.einsum(
            "thd,kd->thk", grad_attn_low, value_block, preferred_element_type=jnp.float32
        )
        grad_scores = (probs * (grad_probs - delta[..., None])).astype(jnp.bfloat16)
        grad_query = grad_query + jnp.einsum(
            "thk,kd->thd", grad_scores, key_block, preferred_element_type=jnp.float32
        )
        key_part = jnp.einsum("thk,thd->kd", grad_scores, query, preferred_element_type=jnp.float32)
        value_part = jnp.einsum(
            "thk,thd->kd", probs_low, grad_attn_low, preferred_element_type=jnp.float32
        )
        grad_keys = lax.dynamic_update_slice_in_dim(grad_keys, key_part, start, 0)
        grad_values = lax.dynamic_update_slice_in_dim(grad_values, value_part, start, 0)
        return (grad_query, grad_keys, grad_values)

    start_carry = (
        jnp.zeros((tok_count, HEADS, HEAD), jnp.float32),
        jnp.zeros((seq_length, HEAD), jnp.float32),
        jnp.zeros((seq_length, HEAD), jnp.float32),
    )
    grad_query, grad_keys, grad_values = lax.fori_loop(
        first_block, stop_block, back_step, start_carry
    )
    own_key_grad, own_value_grad = (
        lax.psum_scatter(
            (grad_keys * score_scale).astype(jnp.bfloat16), "ctx", scatter_dimension=0, tiled=True
        ).astype(jnp.float32),
        lax.psum_scatter(
            grad_values.astype(jnp.bfloat16), "ctx", scatter_dimension=0, tiled=True
        ).astype(jnp.float32),
    )
    grad_query_low = (grad_query * score_scale).reshape(tok_count, model_width).astype(jnp.bfloat16)
    own_key_low = own_key_grad.astype(jnp.bfloat16)
    own_value_low = own_value_grad.astype(jnp.bfloat16)
    grad_qkv_low = jnp.concatenate([grad_query_low, own_key_low, own_value_low], 1)
    grad_rank = jnp.concatenate(
        [
            matmul_right_t(grad_query_low, own_query_second),
            matmul_right_t(own_key_low, own_key_second),
            matmul_right_t(own_value_low, own_value_second),
        ],
        1,
    ).astype(jnp.bfloat16)
    grad_first = project_back(
        grad_qkv_low, lax.all_gather(qkv_weight, "wt", axis=0, tiled=True)
    ) + matmul_right_t(grad_rank, attn_first)
    query_second_grad = matmul_left_t(low_rank[:, :rank_width], grad_query_low)
    key_second_grad = matmul_left_t(low_rank[:, rank_width : 2 * rank_width], own_key_low)
    value_second_grad = matmul_left_t(low_rank[:, 2 * rank_width :], own_value_low)
    attn_first_grad = matmul_left_t(first_low, grad_rank)
    query_first_grad = attn_first_grad[:, :rank_width]
    key_first_grad = attn_first_grad[:, rank_width : 2 * rank_width]
    value_first_grad = attn_first_grad[:, 2 * rank_width :]
    tokens_grad = (grad_middle + norm_back(grad_first, first_gain, plain_one, inverse_one)).astype(
        jnp.bfloat16
    )[None]
    wide = [
        query_first_grad.T,
        query_second_grad,
        key_first_grad.T,
        value_first_grad.T,
        output_first_grad.T,
        output_second_grad,
        expand_first_grad.T,
        shrink_second_grad,
    ]
    share = model_width // members
    small = HEAD // members
    table = jnp.concatenate(wide, 0).reshape(8 * rank_width, members, share).transpose(1, 0, 2)
    small_table = jnp.concatenate([key_second_grad, value_second_grad], 0)
    small_table = small_table.reshape(2 * rank_width, members, small).transpose(1, 0, 2)
    small_table = jnp.pad(small_table, ((0, 0), (0, 0), (0, share - small)))
    table = lax.psum(jnp.concatenate([table, small_table], 1), "ctx")
    table = lax.all_to_all(table, "wt", 0, 0, tiled=True)
    mlp_sums = lax.psum(jnp.stack([expand_grads, shrink_grads], 1), "ctx")
    ids = marks[:, 0, 64]
    steps = jnp.arange(ADAPTERS, dtype=jnp.float32)
    relative = (ids[None, :] == steps[:, None]).astype(jnp.float32)
    absolute = jnp.concatenate(
        [relative[:, i : i + 1] for i in range(members)], 1
    )
    order = jnp.arange(members) ^ member
    absolute = jnp.take(absolute, order, axis=1)

    def spread(hot, part):
        total = 0.0
        for index in range(members):
            total = total + hot[:, index][:, None, None] * part[index][None]
        return total

    outs = []
    for number in range(8):
        outs.append(spread(absolute, table[:, number * rank_width : (number + 1) * rank_width]))
    for number in range(2):
        start = (8 + number) * rank_width
        outs.append(spread(absolute, table[:, start : start + rank_width, :small]))
    expand_second_out = spread(relative, mlp_sums[:, 0])
    shrink_first_out = spread(relative, mlp_sums[:, 1]).transpose(0, 2, 1)
    flip = lambda value: value.transpose(0, 2, 1)
    return (
        layer_out,
        tokens_grad,
        flip(outs[0]),
        outs[1],
        flip(outs[2]),
        outs[8],
        flip(outs[3]),
        outs[9],
        flip(outs[4]),
        outs[5],
        flip(outs[6]),
        expand_second_out,
        shrink_first_out,
        outs[7],
    )


def solution(mesh):
    placed = (
        P("wt", "ctx", None),
        P("wt", "ctx", None),
        P("wt", "ctx"),
        P("wt"),
        P(),
        P(),
        P(),
        P(),
        P("wt", None),
        P("wt", None),
        P("wt", None),
        P("wt", None),
        P(),
        P(),
        P(),
        P(),
        P(),
        P(),
        P(),
        P(),
        P(),
        P(),
        P(),
        P(),
    )
    return jax.shard_map(
        body,
        mesh=mesh,
        in_specs=placed,
        out_specs=(
            P("wt", "ctx", None),
            P("wt", "ctx", None),
            P(None, "wt", None),
            P(None, None, "wt"),
            P(None, "wt", None),
            P(None, None, "wt"),
            P(None, "wt", None),
            P(None, None, "wt"),
            P(None, "wt", None),
            P(None, None, "wt"),
            P(None, "wt", None),
            P(None, None, "wt"),
            P(None, "wt", None),
            P(None, None, "wt"),
        ),
        check_vma=False,
    )
```

```python
import functools
import math

import jax
import jax.numpy as jnp
from jax import lax
from jax.experimental import pallas as pl
from jax.experimental.pallas import tpu as pltpu
from jax.sharding import PartitionSpec as P

EPSILON = 1e-05
LOWEST = -1e30

MESH = pl.DeviceIdType.MESH
GELU_SCALE = 0.7978845608


def dot_nn(left, right):
    return lax.dot_general(
        left, right, (((1,), (0,)), ((), ())), preferred_element_type=jnp.float32
    )


def dot_nt(left, right):
    return lax.dot_general(
        left, right, (((1,), (1,)), ((), ())), preferred_element_type=jnp.float32
    )


def dot_tn(left, right):
    return lax.dot_general(
        left, right, (((0,), (0,)), ((), ())), preferred_element_type=jnp.float32
    )


def mlp_kernel(
    dims,
    h2_ref,
    dy_ref,
    low_ref,
    ext_ref,
    we_hbm,
    ws_hbm,
    out_ref,
    dh_ref,
    lows_ref,
    gexp_ref,
    gshr_ref,
    ids_ref,
    h2_all,
    dy_all,
    low_all,
    ext_all,
    we,
    ws,
    act,
    dup,
    sis_send,
    sis_recv,
    own_recv,
    far_part,
    far_send,
    far_recv,
    low_send,
    low_recv,
    in_send_sem,
    in_recv_sem,
    sis_send_sem,
    sis_recv_sem,
    own_send_sem,
    own_recv_sem,
    far_send_sem,
    far_recv_sem,
    low_send_sem,
    low_recv_sem,
    local_sem,
):
    tok, width, units, rank = dims
    me = lax.axis_index("wt")
    core = lax.rem(me, 2)
    side = lax.div(me, 2)
    sister = me + 1 - 2 * core
    across = me + 2 - 4 * side
    diagonal = sister + 2 - 4 * side
    tile_a = 256
    tile_b = 512
    tiles_a = units // tile_a
    tiles_b = width // tile_b

    local = [
        pltpu.make_async_copy(we_hbm, we, local_sem.at[0]),
        pltpu.make_async_copy(ws_hbm, ws, local_sem.at[1]),
        pltpu.make_async_copy(h2_ref, h2_all.at[pl.ds(0, tok)], local_sem.at[2]),
        pltpu.make_async_copy(dy_ref, dy_all.at[pl.ds(0, tok)], local_sem.at[3]),
        pltpu.make_async_copy(low_ref, low_all.at[0], local_sem.at[4]),
        pltpu.make_async_copy(ext_ref.at[me], ext_all.at[0], local_sem.at[5]),
    ]
    for copy in local:
        copy.start()

    barrier = pltpu.get_barrier_semaphore()
    for peer in (sister, across, diagonal):
        pl.semaphore_signal(barrier, inc=1, device_id={"wt": peer}, device_id_type=MESH)
    pl.semaphore_wait(barrier, 3)

    def remote(src, dst, send, recv, peer):
        return pltpu.make_async_remote_copy(
            src_ref=src,
            dst_ref=dst,
            send_sem=send,
            recv_sem=recv,
            device_id={"wt": peer},
            device_id_type=MESH,
        )

    def entry(number, src, dst, peer):
        return remote(src, dst, in_send_sem.at[number], in_recv_sem.at[number], peer)

    half = tok // 2
    tops = [pl.ds(0, half), pl.ds(half, half)]

    def slot_rows(slot, piece):
        return pl.ds(slot * tok + piece * half, half)

    near = [
        entry(0, low_ref, low_all.at[1], sister),
        entry(1, ext_ref.at[sister], ext_all.at[1], sister),
        entry(2, h2_ref, h2_all.at[pl.ds(tok, tok)], sister),
        entry(3, dy_ref, dy_all.at[pl.ds(tok, tok)], sister),
    ]
    direct = [
        entry(4, low_ref, low_all.at[2], across),
        entry(5, ext_ref.at[across], ext_all.at[2], across),
        entry(6, low_ref, low_all.at[3], diagonal),
        entry(7, ext_ref.at[diagonal], ext_all.at[3], diagonal),
    ]
    far = [entry(8 + i, h2_ref.at[tops[i]], h2_all.at[slot_rows(2, i)], across) for i in range(2)]
    far += [entry(10 + i, dy_ref.at[tops[i]], dy_all.at[slot_rows(2, i)], across) for i in range(2)]
    relay = [
        entry(12 + i, h2_all.at[slot_rows(2, i)], h2_all.at[slot_rows(3, i)], sister)
        for i in range(2)
    ]
    relay += [
        entry(14 + i, dy_all.at[slot_rows(2, i)], dy_all.at[slot_rows(3, i)], sister)
        for i in range(2)
    ]
    for copy in near + direct + far:
        copy.start()

    def front(pair):
        pair_rows = pl.ds(pair * 2 * tok, 2 * tok)

        def step(number, carry):
            cols = pl.ds(pl.multiple_of(number * tile_a, tile_a), tile_a)

            def with_low(kind):
                parts = []
                for own in range(2):
                    slot = 2 * pair + own
                    small = low_all[slot, :, kind * 128 : kind * 128 + rank]
                    parts.append(dot_nn(small, ext_all[slot, kind, :, cols]))
                return jnp.concatenate(parts, 0)

            upward = dot_nn(h2_all[pair_rows, :], we[:, cols]) + with_low(0)
            square = upward * upward
            bend = jnp.tanh(GELU_SCALE * (upward + 0.044715 * (square * upward)))
            active = (0.5 * upward * (1.0 + bend)).astype(jnp.bfloat16)
            slope = 0.5 * (1.0 + bend) + 0.5 * upward * (1.0 - bend * bend) * GELU_SCALE * (
                1.0 + 3.0 * 0.044715 * square
            )
            grad = (dot_nt(dy_all[pair_rows, :], ws[cols, :]) + with_low(1)).astype(jnp.bfloat16)
            grad_up = (grad.astype(jnp.float32) * slope).astype(jnp.bfloat16)
            act[:, cols] = active
            dup[:, cols] = grad_up
            for own in range(2):
                slot = 2 * pair + own
                picked = slice(own * tok, (own + 1) * tok)
                gexp_ref[slot, :, cols] = dot_tn(low_all[slot, :, 0:rank], grad_up[picked])
                gshr_ref[slot, :, cols] = dot_tn(low_all[slot, :, 128 : 128 + rank], active[picked])
            return carry

        lax.fori_loop(0, tiles_a, step, 0)

    def low_parts(pair):
        parts = []
        for own in range(2):
            slot = 2 * pair + own
            picked = pl.ds(own * tok, tok)
            grad_low = dot_nt(dup[picked, :], ext_all[slot, 0])
            act_low = dot_nt(act[picked, :], ext_all[slot, 1])
            parts.append((grad_low, act_low))
        return parts

    def back_tile(kind, number):
        cols = pl.ds(pl.multiple_of(number * tile_b, tile_b), tile_b)
        if kind == 0:
            return dot_nt(dup[...], we[cols, :])
        return dot_nn(act[...], ws[:, cols])

    def sis_copy(kind, number):
        return remote(
            sis_send.at[1, kind, number],
            sis_recv.at[kind, number],
            sis_send_sem.at[kind, number],
            sis_recv_sem.at[kind, number],
            sister,
        )

    def own_copy(kind, number):
        return remote(
            sis_send.at[0, kind, number],
            own_recv.at[kind, number],
            own_send_sem.at[kind, number],
            own_recv_sem.at[kind, number],
            sister,
        )

    def far_copy(kind, number):
        return remote(
            far_send.at[kind, number],
            far_recv.at[kind, number],
            far_send_sem.at[kind, number],
            far_recv_sem.at[kind, number],
            across,
        )

    for copy in local:
        copy.wait()
    for copy in near:
        copy.wait_recv()
    front(0)
    for index in range(4):
        far[index].wait_recv()
        relay[index].start()

    low_send[...] = jnp.zeros_like(low_send)
    lows_ref[...] = jnp.zeros_like(lows_ref)
    parts = low_parts(0)
    lows_ref[:, 0:rank] = parts[0][0]
    lows_ref[:, 128 : 128 + rank] = parts[0][1]
    low_send[0, :, 0:rank] = parts[1][0].astype(jnp.bfloat16)
    low_send[0, :, 128 : 128 + rank] = parts[1][1].astype(jnp.bfloat16)
    low_own = remote(
        low_send.at[0], low_recv.at[0], low_send_sem.at[0], low_recv_sem.at[0], sister
    )
    low_own.start()
    for kind, target in ((0, dh_ref), (1, out_ref)):

        def near_step(number, carry, kind=kind, target=target):
            cols = pl.ds(pl.multiple_of(number * tile_b, tile_b), tile_b)
            both = back_tile(kind, number)
            target[:, cols] = both[:tok]
            sis_send[0, kind, number] = both[tok:].astype(jnp.bfloat16)
            own_copy(kind, number).start()
            return carry

        lax.fori_loop(0, tiles_b, near_step, 0)

    for copy in direct:
        copy.wait_recv()
    for copy in relay:
        copy.wait_recv()
    front(1)
    parts = low_parts(1)
    low_send[1, :, 0:rank] = parts[1][0].astype(jnp.bfloat16)
    low_send[1, :, 128 : 128 + rank] = parts[1][1].astype(jnp.bfloat16)
    low_sis = remote(
        low_send.at[1], low_recv.at[1], low_send_sem.at[1], low_recv_sem.at[1], sister
    )
    low_sis.start()
    for kind in range(2):

        def far_step(number, carry, kind=kind):
            both = back_tile(kind, number)
            far_part[number] = both[:tok]
            sis_send[1, kind, number] = both[tok:].astype(jnp.bfloat16)
            sis_copy(kind, number).start()
            return carry

        def join_step(number, carry, kind=kind):
            sis_copy(kind, number).wait_recv()
            far_send[kind, number] = (
                far_part[number] + sis_recv[kind, number].astype(jnp.float32)
            ).astype(jnp.bfloat16)
            far_copy(kind, number).start()
            return carry

        lax.fori_loop(0, tiles_b, far_step, 0)
        lax.fori_loop(0, tiles_b, join_step, 0)
    low_sis.wait_recv()
    low_send[2, :, 0:rank] = (
        parts[0][0] + low_recv[1, :, 0:rank].astype(jnp.float32)
    ).astype(jnp.bfloat16)
    low_send[2, :, 128 : 128 + rank] = (
        parts[0][1] + low_recv[1, :, 128 : 128 + rank].astype(jnp.float32)
    ).astype(jnp.bfloat16)
    low_far = remote(
        low_send.at[2], low_recv.at[2], low_send_sem.at[2], low_recv_sem.at[2], across
    )
    low_far.start()
    for slot in range(4):
        ids_ref[slot] = low_all[slot, 0:16, 128:256].astype(jnp.float32)

    for kind, target in ((0, dh_ref), (1, out_ref)):

        def end_step(number, carry, kind=kind, target=target):
            cols = pl.ds(pl.multiple_of(number * tile_b, tile_b), tile_b)
            own_copy(kind, number).wait_recv()
            far_copy(kind, number).wait_recv()
            target[:, cols] = (
                target[:, cols]
                + own_recv[kind, number].astype(jnp.float32)
                + far_recv[kind, number].astype(jnp.float32)
            )
            own_copy(kind, number).wait_send()
            sis_copy(kind, number).wait_send()
            far_copy(kind, number).wait_send()
            return carry

        lax.fori_loop(0, tiles_b, end_step, 0)
    low_own.wait_recv()
    low_far.wait_recv()
    lows_ref[...] = (
        lows_ref[...] + low_recv[0].astype(jnp.float32) + low_recv[2].astype(jnp.float32)
    )
    for copy in near + direct + far + relay + [low_own, low_sis, low_far]:
        copy.wait_send()


def mlp_call(normed, grad_top, low, ext, expand_part, shrink_weight, rank):
    tok, width = normed.shape
    units = shrink_weight.shape[0]
    tiles = width // 512
    bf = jnp.bfloat16
    full = lambda: pl.BlockSpec(memory_space=pltpu.VMEM)
    hbm = lambda: pl.BlockSpec(memory_space=pl.ANY)
    dma = pltpu.SemaphoreType.DMA
    return pl.pallas_call(
        functools.partial(mlp_kernel, (tok, width, units, rank)),
        out_shape=(
            jax.ShapeDtypeStruct((tok, width), jnp.float32),
            jax.ShapeDtypeStruct((tok, width), jnp.float32),
            jax.ShapeDtypeStruct((tok, 256), jnp.float32),
            jax.ShapeDtypeStruct((4, rank, units), jnp.float32),
            jax.ShapeDtypeStruct((4, rank, units), jnp.float32),
            jax.ShapeDtypeStruct((4, 16, 128), jnp.float32),
        ),
        in_specs=[full(), full(), full(), full(), hbm(), hbm()],
        out_specs=(full(), full(), full(), full(), full(), full()),
        scratch_shapes=[
            pltpu.VMEM((4 * tok, width), bf),
            pltpu.VMEM((4 * tok, width), bf),
            pltpu.VMEM((4, tok, 256), bf),
            pltpu.VMEM((4, 2, rank, units), bf),
            pltpu.VMEM((width, units), bf),
            pltpu.VMEM((units, width), bf),
            pltpu.VMEM((2 * tok, units), bf),
            pltpu.VMEM((2 * tok, units), bf),
            pltpu.VMEM((2, 2, tiles, tok, 512), bf),
            pltpu.VMEM((2, tiles, tok, 512), bf),
            pltpu.VMEM((2, tiles, tok, 512), bf),
            pltpu.VMEM((tiles, tok, 512), jnp.float32),
            pltpu.VMEM((2, tiles, tok, 512), bf),
            pltpu.VMEM((2, tiles, tok, 512), bf),
            pltpu.VMEM((3, tok, 256), bf),
            pltpu.VMEM((3, tok, 256), bf),
            dma((16,)),
            dma((16,)),
            dma((2, tiles)),
            dma((2, tiles)),
            dma((2, tiles)),
            dma((2, tiles)),
            dma((2, tiles)),
            dma((2, tiles)),
            dma((3,)),
            dma((3,)),
            dma((6,)),
        ],
        compiler_params=pltpu.CompilerParams(
            collective_id=1, has_side_effects=True, vmem_limit_bytes=63 * 1024 * 1024
        ),
        name="mlp",
    )(normed, grad_top, low, ext, expand_part, shrink_weight)


NORM_ROWS = 32


def norm_rows(values, gain, offset):
    mean = jnp.mean(values, -1, keepdims=True)
    centre = values - mean
    scale_inv = lax.rsqrt(jnp.mean(centre * centre, -1, keepdims=True) + EPSILON)
    normed = centre * scale_inv
    return normed * gain + offset, normed, scale_inv


def mask_fill(bias, seg_win, seg_own, window, tok):
    keys_at = lax.broadcasted_iota(jnp.int32, (tok, tok), 0)
    tokens_at = lax.broadcasted_iota(jnp.int32, (tok, tok), 1)
    own = seg_own[0:1, :].astype(jnp.float32)
    for block in range(window):
        same = seg_win[block].astype(jnp.float32).T[:, 0:1] == own
        if block == window - 1:
            same = same & (keys_at <= tokens_at)
        bias[block * tok : (block + 1) * tok, :] = jnp.where(
            same, 0.0, LOWEST
        ).astype(bias.dtype)


def turned(values):
    return values.astype(jnp.float32).T.astype(jnp.bfloat16)


def pick_kernel(
    index_ref,
    q_a,
    q_b,
    k_a,
    k_b,
    v_a,
    v_b,
    o_a,
    o_b,
    e_a,
    e_b,
    s_a,
    s_b,
    attn_a,
    attn_b,
    out_a,
    out_b,
    exp_a,
    shr_b,
    ext,
    mark,
):
    rank, width = q_a.shape[1:]
    head = k_b.shape[2]
    units = ext.shape[3]
    for table in (attn_a, attn_b, out_a, out_b, exp_a, shr_b):
        table[...] = jnp.zeros_like(table)
    attn_a[0:rank, :] = q_a[0]
    attn_a[rank : 2 * rank, :] = k_a[0]
    attn_a[2 * rank : 3 * rank, :] = v_a[0]
    attn_b[0:rank, 0:width] = q_b[0]
    attn_b[rank : 2 * rank, width : width + head] = k_b[0]
    attn_b[2 * rank : 3 * rank, width + head : width + 2 * head] = v_b[0]
    out_a[0:rank, :] = o_a[0]
    out_b[0:rank, :] = o_b[0]
    exp_a[0:rank, :] = e_a[0]
    shr_b[0:rank, :] = s_b[0]
    for part in range(ext.shape[0]):
        span = slice(part * units, (part + 1) * units)
        ext[part, 0] = e_b[0, :, span]
        ext[part, 1] = s_a[0, :, span]
    lane = lax.broadcasted_iota(jnp.int32, mark.shape, 1)
    mark[...] = jnp.where(lane < 64, 0.0, index_ref[0].astype(jnp.float32))


def pick_call(adapter_index, tables, members):
    adapters, rank, width = tables[0].shape
    head = tables[3].shape[2]
    units = tables[10].shape[2] // members
    bf = jnp.bfloat16
    shapes = [
        ((128, width), bf),
        ((128, width + 2 * head), bf),
        ((128, width), bf),
        ((128, width), bf),
        ((128, width), bf),
        ((128, width), bf),
        ((members, 2, rank, units), bf),
        ((8, 128), jnp.float32),
    ]
    return pl.pallas_call(
        pick_kernel,
        grid_spec=pltpu.PrefetchScalarGridSpec(
            num_scalar_prefetch=1,
            grid=(1,),
            in_specs=[
                pl.BlockSpec((1,) + table.shape[1:], lambda i, index: (index[0], 0, 0))
                for table in tables
            ],
            out_specs=[
                pl.BlockSpec(shape, lambda i, index, r=len(shape): (0,) * r) for shape, _ in shapes
            ],
        ),
        out_shape=[jax.ShapeDtypeStruct(shape, kind) for shape, kind in shapes],
        name="pick",
    )(adapter_index, *tables)


def front_kernel(
    dims,
    tokens_ref,
    grad_ref,
    seg_ref,
    gain1,
    bias1,
    gain2,
    bias2,
    attn_a,
    attn_b,
    out_a,
    out_b,
    exp_a,
    shr_b,
    mark,
    qkv_hbm,
    out_hbm,
    exp_hbm,
    q_ref,
    kv_win,
    seg_win,
    lse_ref,
    o_ref,
    mid_ref,
    h2_ref,
    low1_ref,
    low_o_ref,
    pack_ref,
    wq_out,
    wo_out,
    we_out,
    h1,
    bias,
    flipped,
    wq,
    wo,
    we,
    land,
    link_send,
    link_recv,
    sis_send,
    sis_recv,
    own_send,
    own_recv,
    kv_send,
    kv_recv,
    seg_send,
    seg_recv,
    local_sem,
    spill_sem,
):
    tok, width, units, rows, count, window, heads, head = dims
    me = lax.axis_index("wt")
    ctx = lax.axis_index("ctx")
    core = lax.rem(me, 2)
    side = lax.div(me, 2)
    sister = me + 1 - 2 * core
    across = me + 2 - 4 * side
    stride = count // 4
    bit_y = lax.rem(ctx, 2)
    bit_z = lax.rem(lax.div(ctx, stride), 2)
    next_y = ctx + 1 - 2 * bit_y
    next_z = ctx + stride - 2 * stride * bit_z
    reach = window - 1
    own_block = window - 1

    def remote(src, dst, send, recv, peer):
        return pltpu.make_async_remote_copy(
            src_ref=src, dst_ref=dst, send_sem=send, recv_sem=recv, device_id=peer,
            device_id_type=MESH,
        )

    my_rows = pl.ds(pl.multiple_of(me * rows, rows), rows)
    quarter = pl.ds(pl.multiple_of(me * units, units), units)
    local = [
        pltpu.make_async_copy(qkv_hbm, wq.at[my_rows], local_sem.at[0]),
        pltpu.make_async_copy(out_hbm, wo.at[my_rows], local_sem.at[1]),
        pltpu.make_async_copy(exp_hbm.at[:, quarter], we.at[my_rows], local_sem.at[2]),
        pltpu.make_async_copy(seg_ref, seg_win.at[own_block], local_sem.at[3]),
    ]
    for copy in local:
        copy.start()
    for step in range(1, window):

        @pl.when(ctx < step)
        def _(step=step):
            slot = own_block - step
            kv_win[slot * tok : (slot + 1) * tok, :] = jnp.zeros((tok, 2 * head), jnp.bfloat16)
            seg_win[slot] = jnp.full(seg_ref.shape, -1, jnp.int32)

    barrier = pltpu.get_barrier_semaphore()
    for peer in (sister, across):
        pl.semaphore_signal(barrier, inc=1, device_id={"wt": peer}, device_id_type=MESH)
    for other in range(count):

        @pl.when(ctx != other)
        def _(other=other):
            pl.semaphore_signal(barrier, inc=1, device_id={"ctx": other}, device_id_type=MESH)

    pl.semaphore_wait(barrier, 2 + count - 1)

    def part_rows(first, flip_y, flip_z, skip, length):
        turn_y = 1 - bit_y if flip_y else bit_y
        turn_z = 1 - bit_z if flip_z else bit_z
        start = first + (turn_y + 2 * turn_z) * (rows // 4) + skip
        return pl.ds(pl.multiple_of(start, 16), length)

    piece = rows // 4
    cut_x = 48 * piece // 128
    cut_y = 48 * piece // 128
    cut_z = piece - cut_x - cut_y
    wide = width // 2
    chunks = [
        (0, width, 2 * head),
        (0, 0, wide),
        (0, wide, wide),
        (1, 0, wide),
        (1, wide, wide),
        (2, 0, units // 2),
        (2, units // 2, units // 2),
        (3, 0, units // 2),
        (3, units // 2, units // 2),
    ]

    def chunk_copies(number):
        kind, start, span = chunks[number]
        cols = pl.ds(start, span)
        if kind < 2:
            source = (qkv_hbm, out_hbm)[kind]
            source_cols = cols
        else:
            source = exp_hbm
            target = across if kind == 2 else sister + 2 - 4 * side
            source_cols = pl.ds(pl.multiple_of(target * units + start, 128), span)
        home = (wq, wo, we, land)[kind]
        base = 0 if kind == 3 else across * rows
        home_base = 0 if kind == 3 else me * rows
        full = (False, False)
        diag = (True, True)
        sems = lambda way: (link_send.at[number, way], link_recv.at[number, way])

        def from_source(parity, skip, length):
            return (
                source.at[part_rows(0, *parity, skip, length), source_cols],
                home.at[part_rows(home_base, *parity, skip, length), cols],
            )

        def passing(parity, skip, length):
            at = home.at[part_rows(base, *parity, skip, length), cols]
            return (at, at)

        return [
            remote(*from_source(full, 0, piece), *sems(0), {"wt": across}),
            remote(*from_source(diag, 0, cut_x), *sems(1), {"wt": across}),
            remote(*passing(full, 0, piece), *sems(2), {"ctx": next_y}),
            remote(*passing(full, 0, piece), *sems(3), {"ctx": next_z}),
            remote(*passing((False, True), cut_x, cut_y), *sems(4), {"ctx": next_y}),
            remote(*passing((True, False), cut_x + cut_y, cut_z), *sems(5), {"ctx": next_z}),
        ]

    def sister_copy(number):
        kind, start, span = chunks[number]
        cols = pl.ds(start, span)
        far_rows = pl.ds(pl.multiple_of(across * rows, rows), rows)
        if kind == 3:
            src, dst = land.at[:, cols], we.at[far_rows, cols]
        else:
            home = (wq, wo)[kind]
            src = home.at[far_rows, cols]
            dst = src
        return remote(src, dst, sis_send.at[number], sis_recv.at[number], {"wt": sister})

    links = [chunk_copies(number) for number in range(len(chunks))]
    forwards = [None if chunks[n][0] == 2 else sister_copy(n) for n in range(len(chunks))]
    sister_quarter = pl.ds(pl.multiple_of(sister * units, units), units)
    own = [
        remote(qkv_hbm, wq.at[my_rows], own_send.at[0], own_recv.at[0], {"wt": sister}),
        remote(out_hbm, wo.at[my_rows], own_send.at[1], own_recv.at[1], {"wt": sister}),
        remote(
            exp_hbm.at[:, sister_quarter], we.at[my_rows], own_send.at[2], own_recv.at[2],
            {"wt": sister},
        ),
    ]

    def arrive(number):
        links[number][0].wait_recv()
        links[number][2].start()
        links[number][3].start()

    def turn(number):
        links[number][2].wait_recv()
        links[number][5].start()
        links[number][3].wait_recv()
        links[number][4].start()

    def finish(number):
        for way in (1, 4, 5):
            links[number][way].wait_recv()
        if forwards[number] is not None:
            forwards[number].start()

    def ready(number):
        if forwards[number] is not None:
            forwards[number].wait_recv()

    for number in range(len(chunks)):
        links[number][0].start()
        links[number][1].start()
        if number == 0:
            own[0].start()
    own[1].start()
    own[2].start()

    def seg_copy(step):
        return remote(
            seg_ref, seg_win.at[own_block - step], seg_send.at[step - 1], seg_recv.at[step - 1],
            {"ctx": ctx + step},
        )

    def kv_copy(step):
        slot = own_block - step
        return remote(
            kv_win.at[pl.ds(own_block * tok, tok)],
            kv_win.at[pl.ds(slot * tok, tok)],
            kv_send.at[step - 1],
            kv_recv.at[step - 1],
            {"ctx": ctx + step},
        )

    def each_sent(make, act):
        for step in range(1, window):

            @pl.when(ctx + step < count)
            def _(step=step):
                act(make(step))

    def each_received(make):
        for step in range(1, window):

            @pl.when(ctx >= step)
            def _(step=step):
                make(step).wait_recv()

    each_sent(seg_copy, lambda copy: copy.start())

    def first_norm(number, carry):
        at = pl.ds(pl.multiple_of(number * NORM_ROWS, NORM_ROWS), NORM_ROWS)
        out, _, _ = norm_rows(tokens_ref[at, :].astype(jnp.float32), gain1[...], bias1[...])
        h1[at, :] = out.astype(jnp.bfloat16)
        return carry

    lax.fori_loop(0, tok // NORM_ROWS, first_norm, 0)
    low1_ref[...] = dot_nt(h1[...], attn_a[...]).astype(jnp.bfloat16)
    pack_ref[:, 128:256] = (
        dot_nt(grad_ref[...], shr_b[...]) + mark[0:1, :]
    ).astype(jnp.bfloat16)

    arrive(0)
    turn(0)
    finish(0)
    local[0].wait()
    own[0].wait_recv()
    ready(0)
    last = pl.ds(width, 2 * head)
    kv_win[own_block * tok : (own_block + 1) * tok, :] = (
        dot_nn(h1[...], wq[:, last]) + dot_nn(low1_ref[...], attn_b[:, last])
    ).astype(jnp.bfloat16)
    each_sent(kv_copy, lambda copy: copy.start())
    arrive(1)
    turn(1)
    arrive(2)
    finish(1)
    turn(2)
    arrive(3)
    finish(2)
    local[3].wait()
    each_received(seg_copy)
    mask_fill(bias, seg_win, seg_ref, window, tok)
    ready(1)
    ready(2)

    def query_tile(number, carry):
        cols = pl.ds(pl.multiple_of(number * 256, 256), 256)
        q_ref[:, cols] = (
            dot_nn(h1[...], wq[:, cols]) + dot_nn(low1_ref[...], attn_b[:, cols])
        ).astype(jnp.bfloat16)
        return carry

    lax.fori_loop(0, width // 256, query_tile, 0)
    spill_q = pltpu.make_async_copy(wq, wq_out, spill_sem.at[0])
    spill_q.start()
    turn(3)
    arrive(4)
    finish(3)
    each_received(kv_copy)
    scale = 1.0 / math.sqrt(head)

    for block in range(window):
        span = slice(block * tok, (block + 1) * tok)
        flipped[:, span] = turned(kv_win[span, head : 2 * head])
    span_q = tok if window * tok <= 2048 else 128

    def one_head(number, carry):
        cols = pl.ds(pl.multiple_of(number * head, head), head)
        for first in range(0, tok, span_q):
            at = slice(first, first + span_q)
            scores = dot_nt(kv_win[:, 0:head], q_ref[at, cols]) * scale + bias[:, at]
            highest = jnp.max(scores, 0, keepdims=True)
            weights = jnp.exp(scores - highest)
            total = jnp.sum(weights, 0, keepdims=True)
            probs = (weights * (1.0 / total)).astype(jnp.bfloat16)
            o_ref[at, cols] = dot_nn(flipped[...], probs).T.astype(jnp.bfloat16)
            lse_ref[number, :, at] = jnp.broadcast_to(highest + jnp.log(total), (8, span_q))
        return carry

    group = heads // 4
    between = {0: (4, 5, None), 1: (5, 6, 4), 2: (6, 7, 5), 3: (7, 8, 6)}
    for index in range(4):
        lax.fori_loop(index * group, (index + 1) * group, one_head, 0)
        turning, coming, ending = between[index]
        turn(turning)
        arrive(coming)
        if ending is not None:
            finish(ending)
    local[1].wait()
    own[1].wait_recv()
    ready(3)
    ready(4)
    low_o_ref[...] = dot_nt(o_ref[...], out_a[...]).astype(jnp.bfloat16)

    def out_tile(number, carry):
        cols = pl.ds(pl.multiple_of(number * 256, 256), 256)
        mid_ref[:, cols] = (
            tokens_ref[:, cols].astype(jnp.float32)
            + dot_nn(o_ref[...], wo[:, cols])
            + dot_nn(low_o_ref[...], out_b[:, cols])
        )
        return carry

    lax.fori_loop(0, width // 256, out_tile, 0)
    spill_o = pltpu.make_async_copy(wo, wo_out, spill_sem.at[1])
    spill_o.start()
    turn(8)
    finish(7)

    def second_norm(number, carry):
        at = pl.ds(pl.multiple_of(number * NORM_ROWS, NORM_ROWS), NORM_ROWS)
        out, _, _ = norm_rows(mid_ref[at, :], gain2[...], bias2[...])
        h2_ref[at, :] = out.astype(jnp.bfloat16)
        return carry

    lax.fori_loop(0, tok // NORM_ROWS, second_norm, 0)
    pack_ref[:, 0:128] = dot_nt(h2_ref[...], exp_a[...]).astype(jnp.bfloat16)
    finish(8)
    local[2].wait()
    own[2].wait_recv()
    ready(7)
    ready(8)
    spill_e = pltpu.make_async_copy(we, we_out, spill_sem.at[2])
    spill_e.start()
    for number in range(len(chunks)):
        for copy in links[number]:
            copy.wait_send()
        if forwards[number] is not None:
            forwards[number].wait_send()
    for copy in own:
        copy.wait_send()
    each_sent(seg_copy, lambda copy: copy.wait_send())
    each_sent(kv_copy, lambda copy: copy.wait_send())
    spill_q.wait()
    spill_o.wait()
    spill_e.wait()


def front_call(tokens, grad_top, segments, vectors, picked, weights, count):
    tok, width = tokens.shape
    qkv_weight, out_weight, expand_weight = weights
    rows = qkv_weight.shape[0]
    head = (qkv_weight.shape[1] - width) // 2
    heads = width // head
    units = expand_weight.shape[1] // (width // rows)
    window = count // 2 + 1
    bf = jnp.bfloat16
    seg_rows = jnp.broadcast_to(segments[None, :], (8, tok))
    attn_a, attn_b, out_a, out_b, exp_a, shr_b, _, mark = picked
    vmem = lambda: pl.BlockSpec(memory_space=pltpu.VMEM)
    hbm = lambda: pl.BlockSpec(memory_space=pl.ANY)
    dma = pltpu.SemaphoreType.DMA
    dims = (tok, width, units, rows, count, window, heads, head)
    shape = jax.ShapeDtypeStruct
    return pl.pallas_call(
        functools.partial(front_kernel, dims),
        out_shape=(
            shape((tok, width), bf),
            shape((window * tok, 2 * head), bf),
            shape((window, 8, tok), jnp.int32),
            shape((heads, 8, tok), jnp.float32),
            shape((tok, width), bf),
            shape((tok, width), jnp.float32),
            shape((tok, width), bf),
            shape((tok, 128), bf),
            shape((tok, 128), bf),
            shape((tok, 256), bf),
            shape((width, width + 2 * head), bf),
            shape((width, width), bf),
            shape((width, units), bf),
        ),
        in_specs=[vmem() for _ in range(14)] + [hbm() for _ in range(3)],
        out_specs=tuple([vmem() for _ in range(10)] + [hbm() for _ in range(3)]),
        scratch_shapes=[
            pltpu.VMEM((tok, width), bf),
            pltpu.VMEM((window * tok, tok), jnp.float32),
            pltpu.VMEM((head, window * tok), bf),
            pltpu.VMEM((width, width + 2 * head), bf),
            pltpu.VMEM((width, width), bf),
            pltpu.VMEM((width, units), bf),
            pltpu.VMEM((rows, units), bf),
            dma((9, 6)),
            dma((9, 6)),
            dma((9,)),
            dma((9,)),
            dma((3,)),
            dma((3,)),
            dma((window - 1,)),
            dma((window - 1,)),
            dma((window - 1,)),
            dma((window - 1,)),
            dma((4,)),
            dma((3,)),
        ],
        compiler_params=pltpu.CompilerParams(
            collective_id=2, has_side_effects=True, vmem_limit_bytes=63 * 1024 * 1024
        ),
        name="front",
    )(
        tokens, grad_top, seg_rows, *vectors, attn_a, attn_b, out_a, out_b, exp_a,
        shr_b, mark, qkv_weight, out_weight, expand_weight,
    )


def norm_pull(grad_out, gain, normed, scale_inv):
    grad_norm = grad_out * gain
    return scale_inv * (
        grad_norm
        - jnp.mean(grad_norm, -1, keepdims=True)
        - normed * jnp.mean(grad_norm * normed, -1, keepdims=True)
    )


def back_kernel(
    dims,
    tokens_ref,
    grad_ref,
    seg_ref,
    gain1,
    bias1,
    gain2,
    bias2,
    attn_a,
    attn_b,
    out_a,
    out_b,
    exp_a,
    shr_b,
    q_ref,
    kv_win,
    seg_win,
    lse_ref,
    o_ref,
    mid_ref,
    h2_ref,
    low1_ref,
    low_o_ref,
    shrunk_ref,
    dh_ref,
    lows_ref,
    gexp_ref,
    gshr_ref,
    ids_ref,
    wq_hbm,
    wo_hbm,
    layer_ref,
    tgrad_ref,
    q_a,
    q_b,
    k_a,
    v_a,
    o_a,
    o_b,
    e_a,
    s_b,
    k_b,
    v_b,
    e_b,
    s_a,
    wq,
    bias,
    flipped,
    dmid,
    dacc,
    db,
    dout,
    dqkv,
    h1,
    dkv,
    dkv_send,
    dkv_recv,
    share,
    land,
    rs_a,
    ag_a,
    mlp_tab,
    rs_b,
    ag_b,
    local_sem,
    kv_ssem,
    kv_rsem,
    share_ssem,
    share_rsem,
    red_ssem,
    red_rsem,
):
    tok, width, rank, count, members, window, heads, head = dims
    me = lax.axis_index("wt")
    ctx = lax.axis_index("ctx")
    core = lax.rem(me, 2)
    side = lax.div(me, 2)
    sister = me + 1 - 2 * core
    across = me + 2 - 4 * side
    diagonal = sister + 2 - 4 * side
    own_block = window - 1
    part = width // members
    bf = jnp.bfloat16

    wo = wq.at[:, 0:width]
    local = [
        pltpu.make_async_copy(wo_hbm, wo, local_sem.at[0]),
        pltpu.make_async_copy(wq_hbm, wq, local_sem.at[1]),
    ]
    local[0].start()

    barrier = pltpu.get_barrier_semaphore()
    for peer in (sister, across, diagonal):
        pl.semaphore_signal(barrier, inc=1, device_id={"wt": peer}, device_id_type=MESH)
    for other in range(count):

        @pl.when(ctx != other)
        def _(other=other):
            pl.semaphore_signal(barrier, inc=1, device_id={"ctx": other}, device_id_type=MESH)

    def remote(src, dst, send, recv, peer):
        return pltpu.make_async_remote_copy(
            src_ref=src, dst_ref=dst, send_sem=send, recv_sem=recv, device_id=peer,
            device_id_type=MESH,
        )

    def each_other(act):
        for other in range(count):

            @pl.when(ctx != other)
            def _(other=other):
                act(other)

    def scatter_copy(lane, table, piece, landing, other):
        return remote(
            table.at[piece(other)],
            landing.at[ctx],
            red_ssem.at[lane, 0, other],
            red_rsem.at[lane, 0, ctx],
            {"ctx": other},
        )

    def scatter_wait(lane, table, piece, landing, other):
        remote(
            table.at[piece(other)],
            landing.at[other],
            red_ssem.at[lane, 0, other],
            red_rsem.at[lane, 0, other],
            {"ctx": other},
        ).wait_recv()

    def gather_copy(lane, result, other):
        return remote(
            result.at[ctx],
            result.at[ctx],
            red_ssem.at[lane, 1, other],
            red_rsem.at[lane, 1, ctx],
            {"ctx": other},
        )

    def gather_wait(lane, result, other):
        remote(
            result.at[other],
            result.at[other],
            red_ssem.at[lane, 1, other],
            red_rsem.at[lane, 1, other],
            {"ctx": other},
        ).wait_recv()

    def scatter_start(lane, table, piece, landing):
        each_other(lambda other: scatter_copy(lane, table, piece, landing, other).start())
        mine = pltpu.make_async_copy(
            table.at[piece(ctx)], landing.at[ctx], local_sem.at[2 + lane]
        )
        mine.start()
        return mine

    def reduce_gather(lane, table, piece, landing, result, mine):
        mine.wait()
        each_other(lambda other: scatter_wait(lane, table, piece, landing, other))
        total = landing[0].astype(jnp.float32)
        for other in range(1, count):
            total = total + landing[other].astype(jnp.float32)
        result[ctx] = total.astype(bf)
        each_other(lambda other: gather_copy(lane, result, other).start())

    def reduce_end(lane, table, piece, landing, result):
        each_other(lambda other: gather_wait(lane, result, other))
        each_other(lambda other: scatter_copy(lane, table, piece, landing, other).wait_send())
        each_other(lambda other: gather_copy(lane, result, other).wait_send())

    lanes_b = min(16, count)
    rows_b = count // lanes_b
    high_b, wide_b = rs_b.shape[1:]
    high_a, wide_a = rs_a.shape[1:]

    def piece_b(other):
        down = lax.div(other, lanes_b) if not isinstance(other, int) else other // lanes_b
        along = lax.rem(other, lanes_b) if not isinstance(other, int) else other % lanes_b
        return (
            pl.ds(pl.multiple_of(down * high_b, 16), high_b),
            pl.ds(pl.multiple_of(along * wide_b, 128), wide_b),
        )

    def piece_a(other):
        down = lax.div(other, 4) if not isinstance(other, int) else other // 4
        along = lax.rem(other, 4) if not isinstance(other, int) else other % 4
        return (
            pl.ds(pl.multiple_of(down * high_a, 16), high_a),
            pl.ds(pl.multiple_of(along * wide_a, 128), wide_a),
        )

    for slot in range(members):
        mlp_tab[2 * slot * rank : (2 * slot + 1) * rank, :] = gexp_ref[slot].astype(bf)
        mlp_tab[(2 * slot + 1) * rank : (2 * slot + 2) * rank, :] = gshr_ref[slot].astype(bf)
    pl.semaphore_wait(barrier, 3 + count - 1)
    mine_b = scatter_start(1, mlp_tab, piece_b, rs_b)

    grad_low = lows_ref[:, 0:128].astype(bf)
    shrink_low = lows_ref[:, 128:256].astype(bf)
    lows_tile = 512

    def low_step(number, carry):
        cols = pl.ds(pl.multiple_of(number * lows_tile, lows_tile), lows_tile)
        layer_ref[:, cols] = (
            mid_ref[:, cols] + shrunk_ref[:, cols] + dot_nn(shrink_low, shr_b[:, cols])
        ).astype(bf)
        dmid[:, cols] = dh_ref[:, cols] + dot_nn(grad_low, exp_a[:, cols])
        return carry

    lax.fori_loop(0, width // lows_tile, low_step, 0)

    def second_pull(number, carry):
        at = pl.ds(pl.multiple_of(number * NORM_ROWS, NORM_ROWS), NORM_ROWS)
        _, normed, scale_inv = norm_rows(mid_ref[at, :], gain2[...], bias2[...])
        value = grad_ref[at, :].astype(jnp.float32) + norm_pull(
            dmid[at, :], gain2[...], normed, scale_inv
        )
        dmid[at, :] = value
        db[at, :] = value.astype(bf)
        return carry

    lax.fori_loop(0, tok // NORM_ROWS, second_pull, 0)
    grad_out_low = dot_nt(db[...], out_b[...]).astype(bf)
    local[0].wait()

    def out_pull(number, carry):
        cols = pl.ds(pl.multiple_of(number * 256, 256), 256)
        dout[:, cols] = (
            dot_nt(db[...], wq[cols, 0:width]) + dot_nn(grad_out_low, out_a[:, cols])
        ).astype(bf)
        return carry

    lax.fori_loop(0, width // 256, out_pull, 0)
    local[1].start()
    reduce_gather(1, mlp_tab, piece_b, rs_b, ag_b, mine_b)

    mask_fill(bias, seg_win, seg_ref, window, tok)
    for block in range(window):
        span = slice(block * tok, (block + 1) * tok)
        flipped[:, span] = turned(kv_win[span, 0:head])
    dkv[...] = jnp.zeros_like(dkv)
    scale = 1.0 / math.sqrt(head)
    span_q = tok if window * tok <= 2048 else 128

    def one_head(number, carry):
        cols = pl.ds(pl.multiple_of(number * head, head), head)
        for first in range(0, tok, span_q):
            at = slice(first, first + span_q)
            query = q_ref[at, cols]
            grad = dout[at, cols]
            scores = dot_nt(kv_win[:, 0:head], query) * scale + bias[:, at]
            probs = jnp.exp(scores - lse_ref[number, 0:1, at])
            grad_probs = dot_nt(kv_win[:, head : 2 * head], grad)
            delta = jnp.sum(probs * grad_probs, 0, keepdims=True)
            grad_scores = (probs * (grad_probs - delta)).astype(bf)
            dqkv[at, cols] = (dot_nn(flipped[...], grad_scores).T * scale).astype(bf)
            dkv[:, 0:head] = dkv[:, 0:head] + dot_nn(grad_scores, query)
            dkv[:, head : 2 * head] = dkv[:, head : 2 * head] + dot_nn(probs.astype(bf), grad)
        return carry

    lax.fori_loop(0, heads, one_head, 0)

    def kv_copy(step):
        return remote(
            dkv_send.at[step - 1],
            dkv_recv.at[step - 1],
            kv_ssem.at[step - 1],
            kv_rsem.at[step - 1],
            {"ctx": ctx - step},
        )

    for step in range(1, window):

        @pl.when(ctx >= step)
        def _(step=step):
            at = slice((own_block - step) * tok, (own_block - step + 1) * tok)
            dkv_send[step - 1, :, 0:head] = (dkv[at, 0:head] * scale).astype(bf)
            dkv_send[step - 1, :, head : 2 * head] = dkv[at, head : 2 * head].astype(bf)
            kv_copy(step).start()

    local[1].wait()

    def first_norm(number, carry):
        at = pl.ds(pl.multiple_of(number * NORM_ROWS, NORM_ROWS), NORM_ROWS)
        out, _, _ = norm_rows(tokens_ref[at, :].astype(jnp.float32), gain1[...], bias1[...])
        h1[at, :] = out.astype(bf)
        return carry

    lax.fori_loop(0, tok // NORM_ROWS, first_norm, 0)

    def put(group, value):
        for other in range(members):
            span = slice(other * part, (other + 1) * part)
            share[other, group * rank : (group + 1) * rank, :] = value[:, span].astype(bf)

    query_grad = dqkv[:, 0:width]
    put(1, dot_tn(low1_ref[:, 0:rank], query_grad))
    put(4, dot_tn(grad_out_low[:, 0:rank], o_ref[...]))
    put(5, dot_tn(low_o_ref[:, 0:rank], db[...]))
    put(6, dot_tn(grad_low[:, 0:rank], h2_ref[...]))
    put(7, dot_tn(shrink_low[:, 0:rank], grad_ref[...]))

    def first_half(number, carry):
        cols = pl.ds(pl.multiple_of(number * 256, 256), 256)
        dacc[:, cols] = dot_nt(dqkv[:, 0:width], wq[cols, 0:width])
        return carry

    lax.fori_loop(0, width // 256, first_half, 0)

    own_at = slice(own_block * tok, (own_block + 1) * tok)
    dkv[own_at, 0:head] = dkv[own_at, 0:head] * scale
    for step in range(1, window):

        @pl.when(ctx + step < count)
        def _(step=step):
            kv_copy(step).wait_recv()
            dkv[own_at, :] = dkv[own_at, :] + dkv_recv[step - 1].astype(jnp.float32)

    last = slice(width, width + 2 * head)
    dqkv[:, last] = dkv[own_at, :].astype(bf)
    grad_rank = dot_nt(dqkv[...], attn_b[...]).astype(bf)
    first_grads = dot_tn(grad_rank[:, 0 : 3 * rank], h1[...])
    put(0, first_grads[0:rank])
    put(2, first_grads[rank : 2 * rank])
    put(3, first_grads[2 * rank : 3 * rank])
    small = dot_tn(low1_ref[...], dqkv[:, last])
    thin = head // members
    share[:, 8 * rank : 10 * rank, :] = jnp.zeros((members, 2 * rank, part), bf)
    for other in range(members):
        span = slice(other * thin, (other + 1) * thin)
        share[other, 8 * rank : 9 * rank, 0:thin] = small[rank : 2 * rank, span].astype(bf)
        span = slice(head + other * thin, head + (other + 1) * thin)
        share[other, 9 * rank : 10 * rank, 0:thin] = small[2 * rank : 3 * rank, span].astype(bf)

    deep = 10 * rank

    def slot_rows(slot):
        return pl.ds(slot * deep, deep)

    exchange = [
        remote(
            share.at[peer],
            land.at[slot_rows(slot)],
            share_ssem.at[slot - 1],
            share_rsem.at[slot - 1],
            {"wt": peer},
        )
        for slot, peer in ((1, sister), (2, across), (3, diagonal))
    ]
    for copy in exchange:
        copy.start()
    mine_share = pltpu.make_async_copy(share.at[me], land.at[slot_rows(0)], local_sem.at[4])
    mine_share.start()

    def second_half(number, carry):
        cols = pl.ds(pl.multiple_of(number * 256, 256), 256)
        dacc[:, cols] = (
            dacc[:, cols]
            + dot_nt(dqkv[:, last], wq[cols, last])
            + dot_nn(grad_rank, attn_a[:, cols])
        )
        return carry

    lax.fori_loop(0, width // 256, second_half, 0)

    mine_share.wait()
    for copy in exchange:
        copy.wait_recv()
    mine_a = scatter_start(0, land, piece_a, rs_a)

    def first_pull(number, carry):
        at = pl.ds(pl.multiple_of(number * NORM_ROWS, NORM_ROWS), NORM_ROWS)
        _, normed, scale_inv = norm_rows(
            tokens_ref[at, :].astype(jnp.float32), gain1[...], bias1[...]
        )
        tgrad_ref[at, :] = (
            dmid[at, :] + norm_pull(dacc[at, :], gain1[...], normed, scale_inv)
        ).astype(bf)
        return carry

    lax.fori_loop(0, tok // NORM_ROWS, first_pull, 0)
    reduce_gather(0, land, piece_a, rs_a, ag_a, mine_a)
    reduce_end(1, mlp_tab, piece_b, rs_b, ag_b)

    adapters = q_a.shape[0]
    marks = [ids_ref[slot, 0:1, 64:65] for slot in range(members)]

    def spread(targets, sources):
        for number in range(adapters):
            total = 0.0
            for slot in range(members):
                hot = jnp.where(marks[slot] == float(number), 1.0, 0.0)
                total = total + hot * sources[slot]
            targets(number, total)

    for group, target in ((0, e_b), (1, s_a)):
        for other in range(count):
            along = (other % lanes_b) * wide_b
            down = other // lanes_b
            sources = []
            for slot in range(members):
                top = (2 * slot + group) * rank - down * high_b
                if 0 <= top < high_b:
                    sources.append((slot, ag_b[other, top : top + rank, :].astype(jnp.float32)))
            for number in range(adapters):
                total = None
                for slot, value in sources:
                    hot = jnp.where(marks[slot] == float(number), 1.0, 0.0) * value
                    total = hot if total is None else total + hot
                at = (number, slice(None), slice(along, along + wide_b))
                if down == 0:
                    target[at] = total
                else:
                    target[at] = target[at] + total

    reduce_end(0, land, piece_a, rs_a, ag_a)
    for group, target in enumerate((q_a, q_b, k_a, v_a, o_a, o_b, e_a, s_b, k_b, v_b)):
        for along in range(4):
            sources = []
            for slot in range(members):
                top = slot * deep + group * rank
                down = top // high_a
                low = top - down * high_a
                sources.append(ag_a[down * 4 + along, low : low + rank, :].astype(jnp.float32))
            for number in range(adapters):
                total = 0.0
                for slot in range(members):
                    hot = jnp.where(marks[slot] == float(number), 1.0, 0.0)
                    total = total + hot * sources[slot]
                if group < 8:
                    target[number, :, along * wide_a : (along + 1) * wide_a] = total
                elif along == 0:
                    target[number] = total[:, 0:thin]
    for copy in exchange:
        copy.wait_send()
    for step in range(1, window):

        @pl.when(ctx >= step)
        def _(step=step):
            kv_copy(step).wait_send()


def back_call(tokens, grad_top, segments, vectors, picked, front, middle, count, members):
    tok, width = tokens.shape
    shrunk, grad_second, lows, gexp, gshr, ids = middle
    q, kv_win, seg_win, lse, o, mid, h2, low1, low_o, _, wq, wo, _ = front
    attn_a, attn_b, out_a, out_b, exp_a, shr_b, _, _ = picked
    head = kv_win.shape[1] // 2
    heads = width // head
    rank, units = gexp.shape[1:]
    window = count // 2 + 1
    part = width // members
    adapters = 8
    lanes_b = min(16, count)
    high_b, wide_b = 2 * rank * members * lanes_b // count, units // lanes_b
    high_a, wide_a = 10 * rank * members * 4 // count, part // 4
    bf = jnp.bfloat16
    seg_rows = jnp.broadcast_to(segments[None, :], (8, tok))
    vmem = lambda: pl.BlockSpec(memory_space=pltpu.VMEM)
    hbm = lambda: pl.BlockSpec(memory_space=pl.ANY)
    dma = pltpu.SemaphoreType.DMA
    shape = jax.ShapeDtypeStruct
    dims = (tok, width, rank, count, members, window, heads, head)
    inputs = [
        tokens, grad_top, seg_rows, *vectors, attn_a, attn_b, out_a, out_b, exp_a, shr_b,
        q, kv_win, seg_win, lse, o, mid, h2, low1, low_o, shrunk, grad_second, lows, gexp,
        gshr, ids,
    ]
    outs = [shape((tok, width), bf), shape((tok, width), bf)]
    outs += [shape((adapters, rank, part), jnp.float32) for _ in range(8)]
    outs += [shape((adapters, rank, head // members), jnp.float32) for _ in range(2)]
    outs += [shape((adapters, rank, units), jnp.float32) for _ in range(2)]
    return pl.pallas_call(
        functools.partial(back_kernel, dims),
        out_shape=tuple(outs),
        in_specs=[vmem() for _ in inputs] + [hbm(), hbm()],
        out_specs=tuple(vmem() for _ in outs),
        scratch_shapes=[
            pltpu.VMEM((width, width + 2 * head), bf),
            pltpu.VMEM((window * tok, tok), jnp.float32 if window * tok <= 2048 else bf),
            pltpu.VMEM((head, window * tok), bf),
            pltpu.VMEM((tok, width), jnp.float32),
            pltpu.VMEM((tok, width), jnp.float32),
            pltpu.VMEM((tok, width), bf),
            pltpu.VMEM((tok, width), bf),
            pltpu.VMEM((tok, width + 2 * head), bf),
            pltpu.VMEM((tok, width), bf),
            pltpu.VMEM((window * tok, 2 * head), jnp.float32),
            pltpu.VMEM((window - 1, tok, 2 * head), bf),
            pltpu.VMEM((window - 1, tok, 2 * head), bf),
            pltpu.VMEM((members, 10 * rank, part), bf),
            pltpu.VMEM((members * 10 * rank, part), bf),
            pltpu.VMEM((count, high_a, wide_a), bf),
            pltpu.VMEM((count, high_a, wide_a), bf),
            pltpu.VMEM((2 * rank * members, units), bf),
            pltpu.VMEM((count, high_b, wide_b), bf),
            pltpu.VMEM((count, high_b, wide_b), bf),
            dma((5,)),
            dma((window - 1,)),
            dma((window - 1,)),
            dma((3,)),
            dma((3,)),
            dma((2, 2, count)),
            dma((2, 2, count)),
        ],
        compiler_params=pltpu.CompilerParams(
            collective_id=3, has_side_effects=True, vmem_limit_bytes=63 * 1024 * 1024
        ),
        name="back",
    )(*inputs, wq, wo)


def body(
    tokens,
    out_grad,
    segments,
    adapter_index,
    first_gain,
    first_bias,
    second_gain,
    second_bias,
    qkv_weight,
    out_weight,
    expand_weight,
    shrink_weight,
    query_first,
    query_second,
    key_first,
    key_second,
    value_first,
    value_second,
    output_first,
    output_second,
    expand_first,
    expand_second,
    shrink_first,
    shrink_second,
):
    count = lax.axis_size("ctx")
    members = lax.axis_size("wt")
    rank = query_second.shape[1]
    flip = lambda table: table.transpose(0, 2, 1)
    row = lambda vector: vector[None, :]
    tables = [
        flip(query_first),
        query_second,
        flip(key_first),
        key_second,
        flip(value_first),
        value_second,
        flip(output_first),
        output_second,
        flip(expand_first),
        expand_second,
        flip(shrink_first),
        shrink_second,
    ]
    picked = pick_call(adapter_index, tables, members)
    vectors = [row(first_gain), row(first_bias), row(second_gain), row(second_bias)]
    weights = (qkv_weight, out_weight, expand_weight)
    front = front_call(
        tokens[0], out_grad[0], segments[0], vectors, picked, weights, count
    )
    h2, pack, expand_part = front[6], front[9], front[12]
    middle = mlp_call(h2, out_grad[0], pack, picked[6], expand_part, shrink_weight, rank)
    results = back_call(
        tokens[0], out_grad[0], segments[0], vectors, picked, front, middle, count, members
    )
    layer_out, tokens_grad = results[0][None], results[1][None]
    q_a, q_b, k_a, v_a, o_a, o_b, e_a, s_b, k_b, v_b, e_b, s_a = results[2:]
    return (
        layer_out,
        tokens_grad,
        flip(q_a),
        q_b,
        flip(k_a),
        k_b,
        flip(v_a),
        v_b,
        flip(o_a),
        o_b,
        flip(e_a),
        e_b,
        flip(s_a),
        s_b,
    )


def solution(mesh):
    placed = (
        P("wt", "ctx", None),
        P("wt", "ctx", None),
        P("wt", "ctx"),
        P("wt"),
        P(),
        P(),
        P(),
        P(),
        P("wt", None),
        P("wt", None),
        P("wt", None),
        P("wt", None),
        P(),
        P(),
        P(),
        P(),
        P(),
        P(),
        P(),
        P(),
        P(),
        P(),
        P(),
        P(),
    )
    return jax.shard_map(
        body,
        mesh=mesh,
        in_specs=placed,
        out_specs=(
            P("wt", "ctx", None),
            P("wt", "ctx", None),
            P(None, "wt", None),
            P(None, None, "wt"),
            P(None, "wt", None),
            P(None, None, "wt"),
            P(None, "wt", None),
            P(None, None, "wt"),
            P(None, "wt", None),
            P(None, None, "wt"),
            P(None, "wt", None),
            P(None, None, "wt"),
            P(None, "wt", None),
            P(None, None, "wt"),
        ),
        check_vma=False,
    )
```

```python
import functools
import math

import jax
import jax.numpy as jnp
from jax import lax
from jax.experimental import pallas as pl
from jax.experimental.pallas import tpu as pltpu
from jax.sharding import PartitionSpec as P

EPSILON = 1e-05
LOWEST = -1e30

MESH = pl.DeviceIdType.MESH
GELU_SCALE = 0.7978845608


def dot_nn(left, right):
    return lax.dot_general(
        left, right, (((1,), (0,)), ((), ())), preferred_element_type=jnp.float32
    )


def dot_nt(left, right):
    return lax.dot_general(
        left, right, (((1,), (1,)), ((), ())), preferred_element_type=jnp.float32
    )


def dot_tn(left, right):
    return lax.dot_general(
        left, right, (((0,), (0,)), ((), ())), preferred_element_type=jnp.float32
    )


def mlp_kernel(
    dims,
    h2_ref,
    dy_ref,
    low_ref,
    ext_ref,
    dy_far,
    ext_far,
    we_hbm,
    ws_hbm,
    out_ref,
    dh_ref,
    lows_ref,
    table_ref,
    ids_ref,
    out_far,
    h2_all,
    dy_all,
    lowt_all,
    low_all,
    ext_all,
    we,
    ws,
    act,
    dup,
    sis_send,
    sis_recv,
    own_recv,
    far_part,
    far_send,
    far_recv,
    low_send,
    low_recv,
    in_send_sem,
    in_recv_sem,
    sis_send_sem,
    sis_recv_sem,
    own_send_sem,
    own_recv_sem,
    far_send_sem,
    far_recv_sem,
    low_send_sem,
    low_recv_sem,
    local_sem,
):
    tok, width, units, rank = dims
    bf = jnp.bfloat16
    me = lax.axis_index("wt")
    core = lax.rem(me, 2)
    side = lax.div(me, 2)
    sister = me + 1 - 2 * core
    across = me + 2 - 4 * side
    diagonal = sister + 2 - 4 * side
    tile_a = 256
    tile_b = 512
    tiles_a = units // tile_a
    tiles_b = width // tile_b

    early = [
        pltpu.make_async_copy(h2_ref, h2_all.at[pl.ds(0, tok)], local_sem.at[0]),
        pltpu.make_async_copy(dy_ref, dy_all.at[pl.ds(0, tok)], local_sem.at[1]),
        pltpu.make_async_copy(dy_far, dy_all.at[pl.ds(tok, 3 * tok)], local_sem.at[2]),
        pltpu.make_async_copy(low_ref, lowt_all.at[0], local_sem.at[3]),
        pltpu.make_async_copy(ext_ref.at[me], ext_all.at[0], local_sem.at[4]),
        pltpu.make_async_copy(ext_far, ext_all.at[pl.ds(1, 3)], local_sem.at[5]),
        pltpu.make_async_copy(we_hbm, we, local_sem.at[6]),
        pltpu.make_async_copy(ws_hbm, ws, local_sem.at[7]),
    ]
    for copy in early:
        copy.start()

    barrier = pltpu.get_barrier_semaphore()
    for peer in (sister, across, diagonal):
        pl.semaphore_signal(barrier, inc=1, device_id={"wt": peer}, device_id_type=MESH)
    pl.semaphore_wait(barrier, 3)

    def remote(src, dst, send, recv, peer):
        return pltpu.make_async_remote_copy(
            src_ref=src,
            dst_ref=dst,
            send_sem=send,
            recv_sem=recv,
            device_id={"wt": peer},
            device_id_type=MESH,
        )

    def entry(number, src, dst, peer):
        return remote(src, dst, in_send_sem.at[number], in_recv_sem.at[number], peer)

    quart = tok // 4

    def slot_rows(slot, piece):
        return pl.ds(slot * tok + piece * quart, quart)

    near = [
        entry(0, low_ref, lowt_all.at[1], sister),
        entry(1, h2_ref, h2_all.at[pl.ds(tok, tok)], sister),
    ]
    direct = [
        entry(2, low_ref, lowt_all.at[2], across),
        entry(3, low_ref, lowt_all.at[3], diagonal),
    ]
    far = [
        entry(4 + i, h2_ref.at[pl.ds(i * quart, quart)], h2_all.at[slot_rows(2, i)], across)
        for i in range(4)
    ]
    relay = [
        entry(8 + i, h2_all.at[slot_rows(2, i)], h2_all.at[slot_rows(3, i)], sister)
        for i in range(4)
    ]
    for copy in near + direct + far:
        copy.start()

    def front(pair):
        pair_rows = pl.ds(pair * 2 * tok, 2 * tok)
        for own in range(2):
            slot = 2 * pair + own
            low_all[slot, :, 0:rank] = turned(lowt_all[slot, 0:rank, :])
            low_all[slot, :, 128 : 128 + rank] = turned(lowt_all[slot, rank : 2 * rank, :])

        def step(number, carry):
            cols = pl.ds(pl.multiple_of(number * tile_a, tile_a), tile_a)

            def with_low(kind):
                parts = []
                for own in range(2):
                    slot = 2 * pair + own
                    small = low_all[slot, :, kind * 128 : kind * 128 + rank]
                    parts.append(dot_nn(small, ext_all[slot, kind, :, cols]))
                return jnp.concatenate(parts, 0)

            upward = dot_nn(h2_all[pair_rows, :], we[:, cols]) + with_low(0)
            square = upward * upward
            bend = jnp.tanh(GELU_SCALE * (upward + 0.044715 * (square * upward)))
            active = (0.5 * upward * (1.0 + bend)).astype(bf)
            slope = 0.5 * (1.0 + bend) + 0.5 * upward * (1.0 - bend * bend) * GELU_SCALE * (
                1.0 + 3.0 * 0.044715 * square
            )
            grad = (dot_nt(dy_all[pair_rows, :], ws[cols, :]) + with_low(1)).astype(bf)
            grad_up = (grad.astype(jnp.float32) * slope).astype(bf)
            act[pair_rows, cols] = active
            dup[pair_rows, cols] = grad_up
            for own in range(2):
                slot = 2 * pair + own
                picked = slice(own * tok, (own + 1) * tok)
                for kind, right in enumerate((grad_up, active)):
                    left = lowt_all[slot, kind * rank : (kind + 1) * rank, :]
                    at = pl.ds((2 * slot + kind) * rank, rank)
                    table_ref[at, cols] = dot_nn(left, right[picked]).astype(bf)
            return carry

        lax.fori_loop(0, tiles_a, step, 0)

    def low_parts(pair):
        parts = []
        for own in range(2):
            slot = 2 * pair + own
            picked = pl.ds(slot * tok, tok)
            grad_low = dot_nt(dup[picked, :], ext_all[slot, 0])
            act_low = dot_nt(act[picked, :], ext_all[slot, 1])
            parts.append((grad_low, act_low))
        return parts

    def back_tile(pair, kind, number):
        cols = pl.ds(pl.multiple_of(number * tile_b, tile_b), tile_b)
        pair_rows = pl.ds(pair * 2 * tok, 2 * tok)
        if kind == 0:
            return dot_nt(dup[pair_rows, :], we[cols, :])
        return dot_nn(act[pair_rows, :], ws[:, cols])

    def sis_copy(kind, number):
        return remote(
            sis_send.at[1, kind, number],
            sis_recv.at[kind, number],
            sis_send_sem.at[kind, number],
            sis_recv_sem.at[kind, number],
            sister,
        )

    def own_copy(kind, number):
        return remote(
            sis_send.at[0, kind, number],
            own_recv.at[kind, number],
            own_send_sem.at[kind, number],
            own_recv_sem.at[kind, number],
            sister,
        )

    def far_copy(number):
        return remote(
            far_send.at[number],
            far_recv.at[number],
            far_send_sem.at[number],
            far_recv_sem.at[number],
            across,
        )

    for copy in early:
        copy.wait()
    for copy in near:
        copy.wait_recv()
    front(0)
    for copy in direct:
        copy.wait_recv()
    for index in range(4):
        far[index].wait_recv()
        relay[index].start()
    for slot in range(4):
        ids_ref[slot] = lowt_all[slot, 2 * rank : 3 * rank, 0:128].astype(jnp.float32)
    low_send[...] = jnp.zeros_like(low_send)
    lows_ref[...] = jnp.zeros_like(lows_ref)
    parts = low_parts(0)
    lows_ref[:, 0:rank] = parts[0][0]
    lows_ref[:, 128 : 128 + rank] = parts[0][1]
    low_send[0, :, 0:rank] = parts[1][0].astype(bf)
    low_send[0, :, 128 : 128 + rank] = parts[1][1].astype(bf)
    low_own = remote(
        low_send.at[0], low_recv.at[0], low_send_sem.at[0], low_recv_sem.at[0], sister
    )
    low_own.start()
    for copy in relay:
        copy.wait_recv()
    front(1)

    def join(kind, number):
        sis_copy(kind, number).wait_recv()
        total = (
            far_part[lax.rem(number, 2)] + sis_recv[kind, number].astype(jnp.float32)
        ).astype(bf)
        if kind == 0:
            far_send[number] = total
            far_copy(number).start()
        else:
            cols = pl.ds(pl.multiple_of(number * tile_b, tile_b), tile_b)
            out_far[:, cols] = total

    for kind in range(2):

        def far_step(number, carry, kind=kind):
            both = back_tile(1, kind, number)
            sis_send[1, kind, number] = both[tok:].astype(bf)
            sis_copy(kind, number).start()

            @pl.when(number > 0)
            def _():
                join(kind, number - 1)

            far_part[lax.rem(number, 2)] = both[:tok]
            return carry

        lax.fori_loop(0, tiles_b, far_step, 0)
        join(kind, tiles_b - 1)
    parts = low_parts(1)
    low_send[1, :, 0:rank] = parts[1][0].astype(bf)
    low_send[1, :, 128 : 128 + rank] = parts[1][1].astype(bf)
    low_sis = remote(
        low_send.at[1], low_recv.at[1], low_send_sem.at[1], low_recv_sem.at[1], sister
    )
    low_sis.start()

    for kind, target in ((0, dh_ref), (1, out_ref)):

        def near_step(number, carry, kind=kind, target=target):
            cols = pl.ds(pl.multiple_of(number * tile_b, tile_b), tile_b)
            both = back_tile(0, kind, number)
            target[:, cols] = both[:tok]
            sis_send[0, kind, number] = both[tok:].astype(bf)
            own_copy(kind, number).start()
            return carry

        lax.fori_loop(0, tiles_b, near_step, 0)
        if kind == 0:
            low_sis.wait_recv()
            low_send[2, :, 0:rank] = (
                parts[0][0] + low_recv[1, :, 0:rank].astype(jnp.float32)
            ).astype(bf)
            low_send[2, :, 128 : 128 + rank] = (
                parts[0][1] + low_recv[1, :, 128 : 128 + rank].astype(jnp.float32)
            ).astype(bf)
            low_far = remote(
                low_send.at[2], low_recv.at[2], low_send_sem.at[2], low_recv_sem.at[2], across
            )
            low_far.start()

    def end_step(number, carry):
        cols = pl.ds(pl.multiple_of(number * tile_b, tile_b), tile_b)
        own_copy(0, number).wait_recv()
        own_copy(1, number).wait_recv()
        far_copy(number).wait_recv()
        dh_ref[:, cols] = (
            dh_ref[:, cols]
            + own_recv[0, number].astype(jnp.float32)
            + far_recv[number].astype(jnp.float32)
        )
        out_ref[:, cols] = out_ref[:, cols] + own_recv[1, number].astype(jnp.float32)
        for kind in range(2):
            own_copy(kind, number).wait_send()
            sis_copy(kind, number).wait_send()
        far_copy(number).wait_send()
        return carry

    lax.fori_loop(0, tiles_b, end_step, 0)
    low_own.wait_recv()
    low_far.wait_recv()
    lows_ref[...] = (
        lows_ref[...] + low_recv[0].astype(jnp.float32) + low_recv[2].astype(jnp.float32)
    )
    for copy in near + direct + far + relay + [low_own, low_sis, low_far]:
        copy.wait_send()


def mlp_call(normed, grad_top, low, ext, dy_far, ext_far, expand_part, shrink_weight, rank):
    tok, width = normed.shape
    units = shrink_weight.shape[0]
    tiles = width // 512
    bf = jnp.bfloat16
    full = lambda: pl.BlockSpec(memory_space=pltpu.VMEM)
    hbm = lambda: pl.BlockSpec(memory_space=pl.ANY)
    dma = pltpu.SemaphoreType.DMA
    return pl.pallas_call(
        functools.partial(mlp_kernel, (tok, width, units, rank)),
        out_shape=(
            jax.ShapeDtypeStruct((tok, width), jnp.float32),
            jax.ShapeDtypeStruct((tok, width), jnp.float32),
            jax.ShapeDtypeStruct((tok, 256), jnp.float32),
            jax.ShapeDtypeStruct((8 * rank, units), bf),
            jax.ShapeDtypeStruct((4, rank, 128), jnp.float32),
            jax.ShapeDtypeStruct((tok, width), bf),
        ),
        in_specs=[full(), full(), full(), hbm(), hbm(), hbm(), hbm(), hbm()],
        out_specs=tuple(full() for _ in range(6)),
        scratch_shapes=[
            pltpu.VMEM((4 * tok, width), bf),
            pltpu.VMEM((4 * tok, width), bf),
            pltpu.VMEM((4, 3 * rank, tok), bf),
            pltpu.VMEM((4, tok, 256), bf),
            pltpu.VMEM((4, 2, rank, units), bf),
            pltpu.VMEM((width, units), bf),
            pltpu.VMEM((units, width), bf),
            pltpu.VMEM((4 * tok, units), bf),
            pltpu.VMEM((4 * tok, units), bf),
            pltpu.VMEM((2, 2, tiles, tok, 512), bf),
            pltpu.VMEM((2, tiles, tok, 512), bf),
            pltpu.VMEM((2, tiles, tok, 512), bf),
            pltpu.VMEM((2, tok, 512), jnp.float32),
            pltpu.VMEM((tiles, tok, 512), bf),
            pltpu.VMEM((tiles, tok, 512), bf),
            pltpu.VMEM((3, tok, 256), bf),
            pltpu.VMEM((3, tok, 256), bf),
            dma((12,)),
            dma((12,)),
            dma((2, tiles)),
            dma((2, tiles)),
            dma((2, tiles)),
            dma((2, tiles)),
            dma((tiles,)),
            dma((tiles,)),
            dma((3,)),
            dma((3,)),
            dma((8,)),
        ],
        compiler_params=pltpu.CompilerParams(
            collective_id=1, has_side_effects=True, vmem_limit_bytes=63 * 1024 * 1024
        ),
        name="mlp",
    )(normed, grad_top, low, ext, dy_far, ext_far, expand_part, shrink_weight)


NORM_ROWS = 32


def norm_rows(values, gain, offset):
    mean = jnp.mean(values, -1, keepdims=True)
    centre = values - mean
    scale_inv = lax.rsqrt(jnp.mean(centre * centre, -1, keepdims=True) + EPSILON)
    normed = centre * scale_inv
    return normed * gain + offset, normed, scale_inv


def mask_fill(bias, seg_win, seg_own, window, tok):
    keys_at = lax.broadcasted_iota(jnp.int32, (tok, tok), 0)
    tokens_at = lax.broadcasted_iota(jnp.int32, (tok, tok), 1)
    own = seg_own[0:1, :].astype(jnp.float32)
    for block in range(window):
        same = seg_win[block].astype(jnp.float32).T[:, 0:1] == own
        if block == window - 1:
            same = same & (keys_at <= tokens_at)
        bias[block * tok : (block + 1) * tok, :] = jnp.where(
            same, 0.0, LOWEST
        ).astype(bias.dtype)


def turned(values):
    return values.astype(jnp.float32).T.astype(jnp.bfloat16)


def pick_kernel(
    index_ref,
    q_a,
    q_b,
    k_a,
    k_b,
    v_a,
    v_b,
    o_a,
    o_b,
    e_a,
    e_b,
    s_a,
    s_b,
    attn_a,
    attn_b,
    out_a,
    out_b,
    exp_a,
    shr_b,
    ext,
    mark,
):
    rank, width = q_a.shape[1:]
    head = k_b.shape[2]
    units = ext.shape[3]
    for table in (attn_a, attn_b, out_a, out_b, exp_a, shr_b):
        table[...] = jnp.zeros_like(table)
    attn_a[0:rank, :] = q_a[0]
    attn_a[rank : 2 * rank, :] = k_a[0]
    attn_a[2 * rank : 3 * rank, :] = v_a[0]
    attn_b[0:rank, 0:width] = q_b[0]
    attn_b[rank : 2 * rank, width : width + head] = k_b[0]
    attn_b[2 * rank : 3 * rank, width + head : width + 2 * head] = v_b[0]
    out_a[0:rank, :] = o_a[0]
    out_b[0:rank, :] = o_b[0]
    exp_a[0:rank, :] = e_a[0]
    shr_b[0:rank, :] = s_b[0]
    for part in range(ext.shape[0]):
        span = slice(part * units, (part + 1) * units)
        ext[part, 0] = e_b[0, :, span]
        ext[part, 1] = s_a[0, :, span]
    lane = lax.broadcasted_iota(jnp.int32, mark.shape, 1)
    mark[...] = jnp.where(lane < 64, 0.0, index_ref[0].astype(jnp.float32))


def pick_call(adapter_index, tables, members):
    adapters, rank, width = tables[0].shape
    head = tables[3].shape[2]
    units = tables[10].shape[2] // members
    bf = jnp.bfloat16
    shapes = [
        ((128, width), bf),
        ((128, width + 2 * head), bf),
        ((128, width), bf),
        ((128, width), bf),
        ((128, width), bf),
        ((128, width), bf),
        ((members, 2, rank, units), bf),
        ((8, 128), jnp.float32),
    ]
    return pl.pallas_call(
        pick_kernel,
        grid_spec=pltpu.PrefetchScalarGridSpec(
            num_scalar_prefetch=1,
            grid=(1,),
            in_specs=[
                pl.BlockSpec((1,) + table.shape[1:], lambda i, index: (index[0], 0, 0))
                for table in tables
            ],
            out_specs=[
                pl.BlockSpec(shape, lambda i, index, r=len(shape): (0,) * r) for shape, _ in shapes
            ],
        ),
        out_shape=[jax.ShapeDtypeStruct(shape, kind) for shape, kind in shapes],
        name="pick",
    )(adapter_index, *tables)


def front_kernel(
    dims,
    tokens_ref,
    grad_ref,
    seg_ref,
    gain1,
    bias1,
    gain2,
    bias2,
    attn_a,
    attn_b,
    out_a,
    out_b,
    exp_a,
    shr_b,
    mark,
    grad_hbm,
    ext_hbm,
    qkv_hbm,
    out_hbm,
    exp_hbm,
    q_ref,
    kv_win,
    seg_win,
    lse_ref,
    o_ref,
    mid_ref,
    h2_ref,
    low1_ref,
    low_o_ref,
    pack_ref,
    dy_far,
    ext_far,
    wq_out,
    wo_out,
    we_out,
    h1,
    bias,
    flipped,
    wq,
    wo,
    we,
    land,
    link_send,
    link_recv,
    sis_send,
    sis_recv,
    own_send,
    own_recv,
    kv_send,
    kv_recv,
    seg_send,
    seg_recv,
    side_send,
    side_recv,
    local_sem,
    spill_sem,
):
    tok, width, units, rows, count, window, heads, head = dims
    me = lax.axis_index("wt")
    ctx = lax.axis_index("ctx")
    core = lax.rem(me, 2)
    side = lax.div(me, 2)
    sister = me + 1 - 2 * core
    across = me + 2 - 4 * side
    diagonal = sister + 2 - 4 * side
    stride = count // 4
    bit_y = lax.rem(ctx, 2)
    bit_z = lax.rem(lax.div(ctx, stride), 2)
    next_y = ctx + 1 - 2 * bit_y
    next_z = ctx + stride - 2 * stride * bit_z
    reach = window - 1
    own_block = window - 1

    def remote(src, dst, send, recv, peer):
        return pltpu.make_async_remote_copy(
            src_ref=src, dst_ref=dst, send_sem=send, recv_sem=recv, device_id=peer,
            device_id_type=MESH,
        )

    my_rows = pl.ds(pl.multiple_of(me * rows, rows), rows)
    quarter = pl.ds(pl.multiple_of(me * units, units), units)
    local = [
        pltpu.make_async_copy(qkv_hbm, wq.at[my_rows], local_sem.at[0]),
        pltpu.make_async_copy(out_hbm, wo.at[my_rows], local_sem.at[1]),
        pltpu.make_async_copy(exp_hbm.at[:, quarter], we.at[my_rows], local_sem.at[2]),
        pltpu.make_async_copy(seg_ref, seg_win.at[own_block], local_sem.at[3]),
    ]
    for copy in local:
        copy.start()
    for step in range(1, window):

        @pl.when(ctx < step)
        def _(step=step):
            slot = own_block - step
            kv_win[slot * tok : (slot + 1) * tok, :] = jnp.zeros((tok, 2 * head), jnp.bfloat16)
            seg_win[slot] = jnp.full(seg_ref.shape, -1, jnp.int32)

    barrier = pltpu.get_barrier_semaphore()
    for peer in (sister, across, diagonal):
        pl.semaphore_signal(barrier, inc=1, device_id={"wt": peer}, device_id_type=MESH)
    for other in range(count):

        @pl.when(ctx != other)
        def _(other=other):
            pl.semaphore_signal(barrier, inc=1, device_id={"ctx": other}, device_id_type=MESH)

    pl.semaphore_wait(barrier, 3 + count - 1)

    def part_rows(first, flip_y, flip_z, skip, length):
        turn_y = 1 - bit_y if flip_y else bit_y
        turn_z = 1 - bit_z if flip_z else bit_z
        start = first + (turn_y + 2 * turn_z) * (rows // 4) + skip
        return pl.ds(pl.multiple_of(start, 16), length)

    piece = rows // 4
    cut_y = piece // 2
    cut_z = piece - cut_y
    wide = width // 2
    slim = width // 4
    chunks = [(0, width, 2 * head)]
    chunks += [(0, i * slim, slim) for i in range(4)]
    chunks += [(1, i * wide, wide) for i in range(2)]
    chunks += [(2, i * (units // 2), units // 2) for i in range(2)]
    chunks += [(3, i * (units // 2), units // 2) for i in range(2)]

    def chunk_copies(number):
        kind, start, span = chunks[number]
        cols = pl.ds(start, span)
        if kind < 2:
            source = (qkv_hbm, out_hbm)[kind]
            source_cols = cols
        else:
            source = exp_hbm
            target = across if kind == 2 else sister + 2 - 4 * side
            source_cols = pl.ds(pl.multiple_of(target * units + start, 128), span)
        home = (wq, wo, we, land)[kind]
        base = 0 if kind == 3 else across * rows
        home_base = 0 if kind == 3 else me * rows
        full = (False, False)
        sems = lambda way: (link_send.at[number, way], link_recv.at[number, way])

        def from_source(parity, skip, length):
            return (
                source.at[part_rows(0, *parity, skip, length), source_cols],
                home.at[part_rows(home_base, *parity, skip, length), cols],
            )

        def passing(parity, skip, length):
            at = home.at[part_rows(base, *parity, skip, length), cols]
            return (at, at)

        return [
            remote(*from_source(full, 0, piece), *sems(0), {"wt": across}),
            remote(*passing(full, 0, piece), *sems(1), {"ctx": next_y}),
            remote(*passing(full, 0, piece), *sems(2), {"ctx": next_z}),
            remote(*passing((False, True), 0, cut_y), *sems(3), {"ctx": next_y}),
            remote(*passing((True, False), cut_y, cut_z), *sems(4), {"ctx": next_z}),
        ]

    def sister_copy(number):
        kind, start, span = chunks[number]
        cols = pl.ds(start, span)
        far_rows = pl.ds(pl.multiple_of(across * rows, rows), rows)
        if kind == 3:
            src, dst = land.at[:, cols], we.at[far_rows, cols]
        else:
            home = (wq, wo)[kind]
            src = home.at[far_rows, cols]
            dst = src
        return remote(src, dst, sis_send.at[number], sis_recv.at[number], {"wt": sister})

    links = [chunk_copies(number) for number in range(len(chunks))]
    forwards = [None if chunks[n][0] == 2 else sister_copy(n) for n in range(len(chunks))]
    sister_quarter = pl.ds(pl.multiple_of(sister * units, units), units)
    own = [
        remote(qkv_hbm, wq.at[my_rows], own_send.at[0], own_recv.at[0], {"wt": sister}),
        remote(out_hbm, wo.at[my_rows], own_send.at[1], own_recv.at[1], {"wt": sister}),
        remote(
            exp_hbm.at[:, sister_quarter], we.at[my_rows], own_send.at[2], own_recv.at[2],
            {"wt": sister},
        ),
    ]

    def arrive(number):
        links[number][0].wait_recv()
        links[number][1].start()
        links[number][2].start()

    def turn(number):
        links[number][1].wait_recv()
        links[number][4].start()
        links[number][2].wait_recv()
        links[number][3].start()

    def finish(number):
        for way in (3, 4):
            links[number][way].wait_recv()
        if forwards[number] is not None:
            forwards[number].start()

    def ready(number):
        if forwards[number] is not None:
            forwards[number].wait_recv()

    def side_copy(number, src, dst, peer):
        return remote(src, dst, side_send.at[number], side_recv.at[number], {"wt": peer})

    half = tok // 2
    near = [
        side_copy(0, ext_hbm.at[sister], ext_far.at[0], sister),
        side_copy(1, grad_hbm, dy_far.at[pl.ds(0, tok)], sister),
    ]
    distant = [
        side_copy(2, ext_hbm.at[across], ext_far.at[1], across),
        side_copy(3, ext_hbm.at[diagonal], ext_far.at[2], diagonal),
    ]
    far_dy = [
        side_copy(
            4 + i,
            grad_hbm.at[pl.ds(i * half, half)],
            dy_far.at[pl.ds(tok + i * half, half)],
            across,
        )
        for i in range(2)
    ]
    relay_dy = [
        side_copy(
            6 + i,
            dy_far.at[pl.ds(tok + i * half, half)],
            dy_far.at[pl.ds(2 * tok + i * half, half)],
            sister,
        )
        for i in range(2)
    ]

    for number in range(len(chunks)):
        links[number][0].start()
        if number == 0:
            own[0].start()
    own[1].start()
    own[2].start()
    for copy in near + distant + far_dy:
        copy.start()

    def seg_copy(step):
        return remote(
            seg_ref, seg_win.at[own_block - step], seg_send.at[step - 1], seg_recv.at[step - 1],
            {"ctx": ctx + step},
        )

    def kv_copy(step):
        slot = own_block - step
        return remote(
            kv_win.at[pl.ds(own_block * tok, tok)],
            kv_win.at[pl.ds(slot * tok, tok)],
            kv_send.at[step - 1],
            kv_recv.at[step - 1],
            {"ctx": ctx + step},
        )

    def each_sent(make, act):
        for step in range(1, window):

            @pl.when(ctx + step < count)
            def _(step=step):
                act(make(step))

    def each_received(make):
        for step in range(1, window):

            @pl.when(ctx >= step)
            def _(step=step):
                make(step).wait_recv()

    each_sent(seg_copy, lambda copy: copy.start())

    def first_norm(number, carry):
        at = pl.ds(pl.multiple_of(number * NORM_ROWS, NORM_ROWS), NORM_ROWS)
        out, _, _ = norm_rows(tokens_ref[at, :].astype(jnp.float32), gain1[...], bias1[...])
        h1[at, :] = out.astype(jnp.bfloat16)
        return carry

    lax.fori_loop(0, tok // NORM_ROWS, first_norm, 0)
    low1_ref[...] = dot_nt(h1[...], attn_a[...]).astype(jnp.bfloat16)
    rank = pack_ref.shape[0] // 3
    pack_ref[rank : 2 * rank, :] = dot_nt(shr_b[0:rank, :], grad_ref[...]).astype(jnp.bfloat16)
    pack_ref[2 * rank : 3 * rank, :] = jnp.broadcast_to(
        mark[0:1, 64:65], (rank, tok)
    ).astype(jnp.bfloat16)

    arrive(0)
    turn(0)
    arrive(1)
    finish(0)
    local[0].wait()
    own[0].wait_recv()
    ready(0)
    last = pl.ds(width, 2 * head)
    kv_win[own_block * tok : (own_block + 1) * tok, :] = (
        dot_nn(h1[...], wq[:, last]) + dot_nn(low1_ref[...], attn_b[:, last])
    ).astype(jnp.bfloat16)
    each_sent(kv_copy, lambda copy: copy.start())
    turn(1)
    arrive(2)
    finish(1)
    turn(2)
    arrive(3)
    finish(2)
    turn(3)
    arrive(4)
    finish(3)
    local[3].wait()
    each_received(seg_copy)
    mask_fill(bias, seg_win, seg_ref, window, tok)
    turn(4)
    arrive(5)
    finish(4)
    for number in range(1, 5):
        ready(number)

    def query_tile(number, carry):
        cols = pl.ds(pl.multiple_of(number * 256, 256), 256)
        q_ref[:, cols] = (
            dot_nn(h1[...], wq[:, cols]) + dot_nn(low1_ref[...], attn_b[:, cols])
        ).astype(jnp.bfloat16)
        return carry

    lax.fori_loop(0, width // 256, query_tile, 0)
    spill_q = pltpu.make_async_copy(wq, wq_out, spill_sem.at[0])
    spill_q.start()
    turn(5)
    arrive(6)
    finish(5)
    each_received(kv_copy)
    scale = 1.0 / math.sqrt(head)

    for block in range(window):
        span = slice(block * tok, (block + 1) * tok)
        flipped[:, span] = turned(kv_win[span, head : 2 * head])
    span_q = tok if window * tok <= 2048 else 128

    def one_head(number, carry):
        cols = pl.ds(pl.multiple_of(number * head, head), head)
        for first in range(0, tok, span_q):
            at = slice(first, first + span_q)
            scores = dot_nt(kv_win[:, 0:head], q_ref[at, cols]) * scale + bias[:, at]
            highest = jnp.max(scores, 0, keepdims=True)
            weights = jnp.exp(scores - highest)
            total = jnp.sum(weights, 0, keepdims=True)
            probs = (weights * (1.0 / total)).astype(jnp.bfloat16)
            o_ref[at, cols] = dot_nn(flipped[...], probs).T.astype(jnp.bfloat16)
            lse_ref[number, :, at] = jnp.broadcast_to(highest + jnp.log(total), (8, span_q))
        return carry

    group = heads // 8
    for index in range(8):
        lax.fori_loop(index * group, (index + 1) * group, one_head, 0)
        if index % 2 == 0:
            turn(6 + index // 2)
        else:
            arrive(7 + index // 2)
            finish(6 + index // 2)
    local[1].wait()
    own[1].wait_recv()
    ready(5)
    ready(6)
    low_o_ref[...] = dot_nt(o_ref[...], out_a[...]).astype(jnp.bfloat16)

    def out_tile(number, carry):
        cols = pl.ds(pl.multiple_of(number * 256, 256), 256)
        mid_ref[:, cols] = (
            tokens_ref[:, cols].astype(jnp.float32)
            + dot_nn(o_ref[...], wo[:, cols])
            + dot_nn(low_o_ref[...], out_b[:, cols])
        )
        return carry

    lax.fori_loop(0, width // 256, out_tile, 0)
    spill_o = pltpu.make_async_copy(wo, wo_out, spill_sem.at[1])
    spill_o.start()
    turn(10)

    def second_norm(number, carry):
        at = pl.ds(pl.multiple_of(number * NORM_ROWS, NORM_ROWS), NORM_ROWS)
        out, _, _ = norm_rows(mid_ref[at, :], gain2[...], bias2[...])
        h2_ref[at, :] = out.astype(jnp.bfloat16)
        return carry

    lax.fori_loop(0, tok // NORM_ROWS, second_norm, 0)
    pack_ref[0:rank, :] = dot_nt(exp_a[0:rank, :], h2_ref[...]).astype(jnp.bfloat16)
    finish(10)
    for index in range(2):
        far_dy[index].wait_recv()
        relay_dy[index].start()
    local[2].wait()
    own[2].wait_recv()
    ready(9)
    ready(10)
    spill_e = pltpu.make_async_copy(we, we_out, spill_sem.at[2])
    spill_e.start()
    for number in range(len(chunks)):
        for copy in links[number]:
            copy.wait_send()
        if forwards[number] is not None:
            forwards[number].wait_send()
    for copy in near + distant + relay_dy:
        copy.wait_recv()
    for copy in own + near + distant + far_dy + relay_dy:
        copy.wait_send()
    each_sent(seg_copy, lambda copy: copy.wait_send())
    each_sent(kv_copy, lambda copy: copy.wait_send())
    spill_q.wait()
    spill_o.wait()
    spill_e.wait()


def front_call(tokens, grad_top, segments, vectors, picked, weights, count):
    tok, width = tokens.shape
    qkv_weight, out_weight, expand_weight = weights
    rows = qkv_weight.shape[0]
    head = (qkv_weight.shape[1] - width) // 2
    heads = width // head
    units = expand_weight.shape[1] // (width // rows)
    window = count // 2 + 1
    bf = jnp.bfloat16
    seg_rows = jnp.broadcast_to(segments[None, :], (8, tok))
    attn_a, attn_b, out_a, out_b, exp_a, shr_b, ext, mark = picked
    rank = ext.shape[2]
    vmem = lambda: pl.BlockSpec(memory_space=pltpu.VMEM)
    hbm = lambda: pl.BlockSpec(memory_space=pl.ANY)
    dma = pltpu.SemaphoreType.DMA
    dims = (tok, width, units, rows, count, window, heads, head)
    shape = jax.ShapeDtypeStruct
    return pl.pallas_call(
        functools.partial(front_kernel, dims),
        out_shape=(
            shape((tok, width), bf),
            shape((window * tok, 2 * head), bf),
            shape((window, 8, tok), jnp.int32),
            shape((heads, 8, tok), jnp.float32),
            shape((tok, width), bf),
            shape((tok, width), jnp.float32),
            shape((tok, width), bf),
            shape((tok, 128), bf),
            shape((tok, 128), bf),
            shape((3 * rank, tok), bf),
            shape((3 * tok, width), bf),
            shape((3,) + ext.shape[1:], bf),
            shape((width, width + 2 * head), bf),
            shape((width, width), bf),
            shape((width, units), bf),
        ),
        in_specs=[vmem() for _ in range(14)] + [hbm() for _ in range(5)],
        out_specs=tuple([vmem() for _ in range(10)] + [hbm() for _ in range(5)]),
        scratch_shapes=[
            pltpu.VMEM((tok, width), bf),
            pltpu.VMEM((window * tok, tok), jnp.float32),
            pltpu.VMEM((head, window * tok), bf),
            pltpu.VMEM((width, width + 2 * head), bf),
            pltpu.VMEM((width, width), bf),
            pltpu.VMEM((width, units), bf),
            pltpu.VMEM((rows, units), bf),
            dma((11, 5)),
            dma((11, 5)),
            dma((11,)),
            dma((11,)),
            dma((3,)),
            dma((3,)),
            dma((window - 1,)),
            dma((window - 1,)),
            dma((window - 1,)),
            dma((window - 1,)),
            dma((8,)),
            dma((8,)),
            dma((4,)),
            dma((3,)),
        ],
        compiler_params=pltpu.CompilerParams(
            collective_id=2, has_side_effects=True, vmem_limit_bytes=63 * 1024 * 1024
        ),
        name="front",
    )(
        tokens, grad_top, seg_rows, *vectors, attn_a, attn_b, out_a, out_b, exp_a,
        shr_b, mark, grad_top, ext, qkv_weight, out_weight, expand_weight,
    )


def norm_pull(grad_out, gain, normed, scale_inv):
    grad_norm = grad_out * gain
    return scale_inv * (
        grad_norm
        - jnp.mean(grad_norm, -1, keepdims=True)
        - normed * jnp.mean(grad_norm * normed, -1, keepdims=True)
    )


def back_kernel(
    dims,
    tokens_ref,
    grad_ref,
    seg_ref,
    gain1,
    bias1,
    gain2,
    bias2,
    attn_a,
    attn_b,
    out_a,
    out_b,
    exp_a,
    shr_b,
    q_ref,
    kv_win,
    seg_win,
    lse_ref,
    o_ref,
    mid_ref,
    h2_ref,
    low1_ref,
    low_o_ref,
    shrunk_ref,
    dh_ref,
    lows_ref,
    ids_ref,
    wq_hbm,
    wo_hbm,
    out_far,
    mlp_tab,
    layer_ref,
    tgrad_ref,
    q_a,
    q_b,
    k_a,
    v_a,
    o_a,
    o_b,
    e_a,
    s_b,
    k_b,
    v_b,
    e_b,
    s_a,
    wq,
    bias,
    flipped,
    dmid,
    dacc,
    db,
    dout,
    dqkv,
    h1,
    dkv,
    dkv_send,
    dkv_recv,
    share,
    land,
    rs_a,
    ag_a,
    rs_b,
    ag_b,
    out_recv,
    out_ssem,
    out_rsem,
    local_sem,
    kv_ssem,
    kv_rsem,
    share_ssem,
    share_rsem,
    red_ssem,
    red_rsem,
):
    tok, width, rank, count, members, window, heads, head = dims
    me = lax.axis_index("wt")
    ctx = lax.axis_index("ctx")
    core = lax.rem(me, 2)
    side = lax.div(me, 2)
    sister = me + 1 - 2 * core
    across = me + 2 - 4 * side
    diagonal = sister + 2 - 4 * side
    own_block = window - 1
    part = width // members
    bf = jnp.bfloat16

    wo = wq.at[:, 0:width]
    local = [
        pltpu.make_async_copy(wo_hbm, wo, local_sem.at[0]),
        pltpu.make_async_copy(wq_hbm, wq, local_sem.at[1]),
    ]
    local[0].start()

    barrier = pltpu.get_barrier_semaphore()
    for peer in (sister, across, diagonal):
        pl.semaphore_signal(barrier, inc=1, device_id={"wt": peer}, device_id_type=MESH)
    for other in range(count):

        @pl.when(ctx != other)
        def _(other=other):
            pl.semaphore_signal(barrier, inc=1, device_id={"ctx": other}, device_id_type=MESH)

    def remote(src, dst, send, recv, peer):
        return pltpu.make_async_remote_copy(
            src_ref=src, dst_ref=dst, send_sem=send, recv_sem=recv, device_id=peer,
            device_id_type=MESH,
        )

    def each_other(act):
        for other in range(count):

            @pl.when(ctx != other)
            def _(other=other):
                act(other)

    def scatter_copy(lane, table, piece, landing, other):
        return remote(
            table.at[piece(other)],
            landing.at[ctx],
            red_ssem.at[lane, 0, other],
            red_rsem.at[lane, 0, ctx],
            {"ctx": other},
        )

    def scatter_wait(lane, table, piece, landing, other):
        remote(
            table.at[piece(other)],
            landing.at[other],
            red_ssem.at[lane, 0, other],
            red_rsem.at[lane, 0, other],
            {"ctx": other},
        ).wait_recv()

    def gather_copy(lane, result, other):
        return remote(
            result.at[ctx],
            result.at[ctx],
            red_ssem.at[lane, 1, other],
            red_rsem.at[lane, 1, ctx],
            {"ctx": other},
        )

    def gather_wait(lane, result, other):
        remote(
            result.at[other],
            result.at[other],
            red_ssem.at[lane, 1, other],
            red_rsem.at[lane, 1, other],
            {"ctx": other},
        ).wait_recv()

    def scatter_start(lane, table, piece, landing):
        each_other(lambda other: scatter_copy(lane, table, piece, landing, other).start())
        mine = pltpu.make_async_copy(
            table.at[piece(ctx)], landing.at[ctx], local_sem.at[2 + lane]
        )
        mine.start()
        return mine

    def reduce_gather(lane, table, piece, landing, result, mine):
        mine.wait()
        each_other(lambda other: scatter_wait(lane, table, piece, landing, other))
        total = landing[0].astype(jnp.float32)
        for other in range(1, count):
            total = total + landing[other].astype(jnp.float32)
        result[ctx] = total.astype(bf)
        each_other(lambda other: gather_copy(lane, result, other).start())

    def reduce_end(lane, table, piece, landing, result):
        each_other(lambda other: gather_wait(lane, result, other))
        each_other(lambda other: scatter_copy(lane, table, piece, landing, other).wait_send())
        each_other(lambda other: gather_copy(lane, result, other).wait_send())

    lanes_b = min(16, count)
    rows_b = count // lanes_b
    high_b, wide_b = rs_b.shape[1:]
    high_a, wide_a = rs_a.shape[1:]

    def piece_b(other):
        down = lax.div(other, lanes_b) if not isinstance(other, int) else other // lanes_b
        along = lax.rem(other, lanes_b) if not isinstance(other, int) else other % lanes_b
        return (
            pl.ds(pl.multiple_of(down * high_b, 16), high_b),
            pl.ds(pl.multiple_of(along * wide_b, 128), wide_b),
        )

    def piece_a(other):
        down = lax.div(other, 4) if not isinstance(other, int) else other // 4
        along = lax.rem(other, 4) if not isinstance(other, int) else other % 4
        return (
            pl.ds(pl.multiple_of(down * high_a, 16), high_a),
            pl.ds(pl.multiple_of(along * wide_a, 128), wide_a),
        )

    pl.semaphore_wait(barrier, 3 + count - 1)
    mine_b = scatter_start(1, mlp_tab, piece_b, rs_b)
    out_copy = remote(out_far, out_recv, out_ssem.at[0], out_rsem.at[0], {"wt": across})
    out_copy.start()

    grad_low = lows_ref[:, 0:128].astype(bf)
    shrink_low = lows_ref[:, 128:256].astype(bf)
    lows_tile = 512

    def low_step(number, carry):
        cols = pl.ds(pl.multiple_of(number * lows_tile, lows_tile), lows_tile)
        dmid[:, cols] = dh_ref[:, cols] + dot_nn(grad_low, exp_a[:, cols])
        return carry

    lax.fori_loop(0, width // lows_tile, low_step, 0)

    def second_pull(number, carry):
        at = pl.ds(pl.multiple_of(number * NORM_ROWS, NORM_ROWS), NORM_ROWS)
        _, normed, scale_inv = norm_rows(mid_ref[at, :], gain2[...], bias2[...])
        value = grad_ref[at, :].astype(jnp.float32) + norm_pull(
            dmid[at, :], gain2[...], normed, scale_inv
        )
        dmid[at, :] = value
        db[at, :] = value.astype(bf)
        return carry

    lax.fori_loop(0, tok // NORM_ROWS, second_pull, 0)
    grad_out_low = dot_nt(db[...], out_b[...]).astype(bf)
    local[0].wait()

    def out_pull(number, carry):
        cols = pl.ds(pl.multiple_of(number * 256, 256), 256)
        dout[:, cols] = (
            dot_nt(db[...], wq[cols, 0:width]) + dot_nn(grad_out_low, out_a[:, cols])
        ).astype(bf)
        return carry

    lax.fori_loop(0, width // 256, out_pull, 0)
    local[1].start()
    reduce_gather(1, mlp_tab, piece_b, rs_b, ag_b, mine_b)

    mask_fill(bias, seg_win, seg_ref, window, tok)
    for block in range(window):
        span = slice(block * tok, (block + 1) * tok)
        flipped[:, span] = turned(kv_win[span, 0:head])
    dkv[...] = jnp.zeros_like(dkv)
    scale = 1.0 / math.sqrt(head)
    span_q = tok if window * tok <= 2048 else 128

    def one_head(number, carry):
        cols = pl.ds(pl.multiple_of(number * head, head), head)
        for first in range(0, tok, span_q):
            at = slice(first, first + span_q)
            query = q_ref[at, cols]
            grad = dout[at, cols]
            scores = dot_nt(kv_win[:, 0:head], query) * scale + bias[:, at]
            probs = jnp.exp(scores - lse_ref[number, 0:1, at])
            grad_probs = dot_nt(kv_win[:, head : 2 * head], grad)
            delta = jnp.sum(probs * grad_probs, 0, keepdims=True)
            grad_scores = (probs * (grad_probs - delta)).astype(bf)
            dqkv[at, cols] = (dot_nn(flipped[...], grad_scores).T * scale).astype(bf)
            dkv[:, 0:head] = dkv[:, 0:head] + dot_nn(grad_scores, query)
            dkv[:, head : 2 * head] = dkv[:, head : 2 * head] + dot_nn(probs.astype(bf), grad)
        return carry

    lax.fori_loop(0, heads, one_head, 0)

    out_copy.wait_recv()

    def layer_step(number, carry):
        cols = pl.ds(pl.multiple_of(number * lows_tile, lows_tile), lows_tile)
        layer_ref[:, cols] = (
            mid_ref[:, cols]
            + shrunk_ref[:, cols]
            + out_recv[:, cols].astype(jnp.float32)
            + dot_nn(shrink_low, shr_b[:, cols])
        ).astype(bf)
        return carry

    def kv_copy(step):
        return remote(
            dkv_send.at[step - 1],
            dkv_recv.at[step - 1],
            kv_ssem.at[step - 1],
            kv_rsem.at[step - 1],
            {"ctx": ctx - step},
        )

    for step in range(1, window):

        @pl.when(ctx >= step)
        def _(step=step):
            at = slice((own_block - step) * tok, (own_block - step + 1) * tok)
            dkv_send[step - 1, :, 0:head] = (dkv[at, 0:head] * scale).astype(bf)
            dkv_send[step - 1, :, head : 2 * head] = dkv[at, head : 2 * head].astype(bf)
            kv_copy(step).start()

    local[1].wait()

    def first_norm(number, carry):
        at = pl.ds(pl.multiple_of(number * NORM_ROWS, NORM_ROWS), NORM_ROWS)
        out, _, _ = norm_rows(tokens_ref[at, :].astype(jnp.float32), gain1[...], bias1[...])
        h1[at, :] = out.astype(bf)
        return carry

    lax.fori_loop(0, tok // NORM_ROWS, first_norm, 0)
    lax.fori_loop(0, width // lows_tile, layer_step, 0)

    def put(group, value):
        for other in range(members):
            span = slice(other * part, (other + 1) * part)
            share[other, group * rank : (group + 1) * rank, :] = value[:, span].astype(bf)

    query_grad = dqkv[:, 0:width]
    put(1, dot_tn(low1_ref[:, 0:rank], query_grad))
    put(4, dot_tn(grad_out_low[:, 0:rank], o_ref[...]))
    put(5, dot_tn(low_o_ref[:, 0:rank], db[...]))
    put(6, dot_tn(grad_low[:, 0:rank], h2_ref[...]))
    put(7, dot_tn(shrink_low[:, 0:rank], grad_ref[...]))

    def first_half(number, carry):
        cols = pl.ds(pl.multiple_of(number * 256, 256), 256)
        dacc[:, cols] = dot_nt(dqkv[:, 0:width], wq[cols, 0:width])
        return carry

    lax.fori_loop(0, width // 256, first_half, 0)

    own_at = slice(own_block * tok, (own_block + 1) * tok)
    dkv[own_at, 0:head] = dkv[own_at, 0:head] * scale
    for step in range(1, window):

        @pl.when(ctx + step < count)
        def _(step=step):
            kv_copy(step).wait_recv()
            dkv[own_at, :] = dkv[own_at, :] + dkv_recv[step - 1].astype(jnp.float32)

    last = slice(width, width + 2 * head)
    dqkv[:, last] = dkv[own_at, :].astype(bf)
    grad_rank = dot_nt(dqkv[...], attn_b[...]).astype(bf)
    first_grads = dot_tn(grad_rank[:, 0 : 3 * rank], h1[...])
    put(0, first_grads[0:rank])
    put(2, first_grads[rank : 2 * rank])
    put(3, first_grads[2 * rank : 3 * rank])
    small = dot_tn(low1_ref[...], dqkv[:, last])
    thin = head // members
    share[:, 8 * rank : 10 * rank, :] = jnp.zeros((members, 2 * rank, part), bf)
    for other in range(members):
        span = slice(other * thin, (other + 1) * thin)
        share[other, 8 * rank : 9 * rank, 0:thin] = small[rank : 2 * rank, span].astype(bf)
        span = slice(head + other * thin, head + (other + 1) * thin)
        share[other, 9 * rank : 10 * rank, 0:thin] = small[2 * rank : 3 * rank, span].astype(bf)

    deep = 10 * rank

    def slot_rows(slot):
        return pl.ds(slot * deep, deep)

    exchange = [
        remote(
            share.at[peer],
            land.at[slot_rows(slot)],
            share_ssem.at[slot - 1],
            share_rsem.at[slot - 1],
            {"wt": peer},
        )
        for slot, peer in ((1, sister), (2, across), (3, diagonal))
    ]
    for copy in exchange:
        copy.start()
    mine_share = pltpu.make_async_copy(share.at[me], land.at[slot_rows(0)], local_sem.at[4])
    mine_share.start()

    def second_half(number, carry):
        cols = pl.ds(pl.multiple_of(number * 256, 256), 256)
        dacc[:, cols] = (
            dacc[:, cols]
            + dot_nt(dqkv[:, last], wq[cols, last])
            + dot_nn(grad_rank, attn_a[:, cols])
        )
        return carry

    lax.fori_loop(0, width // 256, second_half, 0)

    mine_share.wait()
    for copy in exchange:
        copy.wait_recv()
    mine_a = scatter_start(0, land, piece_a, rs_a)

    def first_pull(number, carry):
        at = pl.ds(pl.multiple_of(number * NORM_ROWS, NORM_ROWS), NORM_ROWS)
        _, normed, scale_inv = norm_rows(
            tokens_ref[at, :].astype(jnp.float32), gain1[...], bias1[...]
        )
        tgrad_ref[at, :] = (
            dmid[at, :] + norm_pull(dacc[at, :], gain1[...], normed, scale_inv)
        ).astype(bf)
        return carry

    lax.fori_loop(0, tok // NORM_ROWS, first_pull, 0)
    reduce_gather(0, land, piece_a, rs_a, ag_a, mine_a)
    reduce_end(1, mlp_tab, piece_b, rs_b, ag_b)

    adapters = q_a.shape[0]
    marks = [ids_ref[slot, 0:1, 64:65] for slot in range(members)]

    def spread(targets, sources):
        for number in range(adapters):
            total = 0.0
            for slot in range(members):
                hot = jnp.where(marks[slot] == float(number), 1.0, 0.0)
                total = total + hot * sources[slot]
            targets(number, total)

    for group, target in ((0, e_b), (1, s_a)):
        for other in range(count):
            along = (other % lanes_b) * wide_b
            down = other // lanes_b
            sources = []
            for slot in range(members):
                top = (2 * slot + group) * rank - down * high_b
                if 0 <= top < high_b:
                    sources.append((slot, ag_b[other, top : top + rank, :].astype(jnp.float32)))
            for number in range(adapters):
                total = None
                for slot, value in sources:
                    hot = jnp.where(marks[slot] == float(number), 1.0, 0.0) * value
                    total = hot if total is None else total + hot
                at = (number, slice(None), slice(along, along + wide_b))
                if down == 0:
                    target[at] = total
                else:
                    target[at] = target[at] + total

    reduce_end(0, land, piece_a, rs_a, ag_a)
    for group, target in enumerate((q_a, q_b, k_a, v_a, o_a, o_b, e_a, s_b, k_b, v_b)):
        for along in range(4):
            sources = []
            for slot in range(members):
                top = slot * deep + group * rank
                down = top // high_a
                low = top - down * high_a
                sources.append(ag_a[down * 4 + along, low : low + rank, :].astype(jnp.float32))
            for number in range(adapters):
                total = 0.0
                for slot in range(members):
                    hot = jnp.where(marks[slot] == float(number), 1.0, 0.0)
                    total = total + hot * sources[slot]
                if group < 8:
                    target[number, :, along * wide_a : (along + 1) * wide_a] = total
                elif along == 0:
                    target[number] = total[:, 0:thin]
    for copy in exchange:
        copy.wait_send()
    out_copy.wait_send()
    for step in range(1, window):

        @pl.when(ctx >= step)
        def _(step=step):
            kv_copy(step).wait_send()


def back_call(tokens, grad_top, segments, vectors, picked, front, middle, count, members):
    tok, width = tokens.shape
    shrunk, grad_second, lows, mlp_tab, ids, out_far = middle
    q, kv_win, seg_win, lse, o, mid, h2, low1, low_o, _, _, _, wq, wo, _ = front
    attn_a, attn_b, out_a, out_b, exp_a, shr_b, _, _ = picked
    head = kv_win.shape[1] // 2
    heads = width // head
    rank, units = ids.shape[1], mlp_tab.shape[1]
    window = count // 2 + 1
    part = width // members
    adapters = 8
    lanes_b = min(16, count)
    high_b, wide_b = 2 * rank * members * lanes_b // count, units // lanes_b
    high_a, wide_a = 10 * rank * members * 4 // count, part // 4
    bf = jnp.bfloat16
    seg_rows = jnp.broadcast_to(segments[None, :], (8, tok))
    vmem = lambda: pl.BlockSpec(memory_space=pltpu.VMEM)
    hbm = lambda: pl.BlockSpec(memory_space=pl.ANY)
    dma = pltpu.SemaphoreType.DMA
    shape = jax.ShapeDtypeStruct
    dims = (tok, width, rank, count, members, window, heads, head)
    inputs = [
        tokens, grad_top, seg_rows, *vectors, attn_a, attn_b, out_a, out_b, exp_a, shr_b,
        q, kv_win, seg_win, lse, o, mid, h2, low1, low_o, shrunk, grad_second, lows, ids,
    ]
    outs = [shape((tok, width), bf), shape((tok, width), bf)]
    outs += [shape((adapters, rank, part), jnp.float32) for _ in range(8)]
    outs += [shape((adapters, rank, head // members), jnp.float32) for _ in range(2)]
    outs += [shape((adapters, rank, units), jnp.float32) for _ in range(2)]
    return pl.pallas_call(
        functools.partial(back_kernel, dims),
        out_shape=tuple(outs),
        in_specs=[vmem() for _ in inputs] + [hbm() for _ in range(4)],
        out_specs=tuple(vmem() for _ in outs),
        scratch_shapes=[
            pltpu.VMEM((width, width + 2 * head), bf),
            pltpu.VMEM((window * tok, tok), jnp.float32 if window * tok <= 2048 else bf),
            pltpu.VMEM((head, window * tok), bf),
            pltpu.VMEM((tok, width), jnp.float32),
            pltpu.VMEM((tok, width), jnp.float32),
            pltpu.VMEM((tok, width), bf),
            pltpu.VMEM((tok, width), bf),
            pltpu.VMEM((tok, width + 2 * head), bf),
            pltpu.VMEM((tok, width), bf),
            pltpu.VMEM((window * tok, 2 * head), jnp.float32),
            pltpu.VMEM((window - 1, tok, 2 * head), bf),
            pltpu.VMEM((window - 1, tok, 2 * head), bf),
            pltpu.VMEM((members, 10 * rank, part), bf),
            pltpu.VMEM((members * 10 * rank, part), bf),
            pltpu.VMEM((count, high_a, wide_a), bf),
            pltpu.VMEM((count, high_a, wide_a), bf),
            pltpu.VMEM((count, high_b, wide_b), bf),
            pltpu.VMEM((count, high_b, wide_b), bf),
            pltpu.VMEM((tok, width), bf),
            dma((1,)),
            dma((1,)),
            dma((5,)),
            dma((window - 1,)),
            dma((window - 1,)),
            dma((3,)),
            dma((3,)),
            dma((2, 2, count)),
            dma((2, 2, count)),
        ],
        compiler_params=pltpu.CompilerParams(
            collective_id=3, has_side_effects=True, vmem_limit_bytes=63 * 1024 * 1024
        ),
        name="back",
    )(*inputs, wq, wo, out_far, mlp_tab)


def body(
    tokens,
    out_grad,
    segments,
    adapter_index,
    first_gain,
    first_bias,
    second_gain,
    second_bias,
    qkv_weight,
    out_weight,
    expand_weight,
    shrink_weight,
    query_first,
    query_second,
    key_first,
    key_second,
    value_first,
    value_second,
    output_first,
    output_second,
    expand_first,
    expand_second,
    shrink_first,
    shrink_second,
):
    count = lax.axis_size("ctx")
    members = lax.axis_size("wt")
    rank = query_second.shape[1]
    flip = lambda table: table.transpose(0, 2, 1)
    row = lambda vector: vector[None, :]
    tables = [
        flip(query_first),
        query_second,
        flip(key_first),
        key_second,
        flip(value_first),
        value_second,
        flip(output_first),
        output_second,
        flip(expand_first),
        expand_second,
        flip(shrink_first),
        shrink_second,
    ]
    picked = pick_call(adapter_index, tables, members)
    vectors = [row(first_gain), row(first_bias), row(second_gain), row(second_bias)]
    weights = (qkv_weight, out_weight, expand_weight)
    front = front_call(
        tokens[0], out_grad[0], segments[0], vectors, picked, weights, count
    )
    h2, pack, dy_far, ext_far, expand_part = (front[i] for i in (6, 9, 10, 11, 14))
    middle = mlp_call(
        h2, out_grad[0], pack, picked[6], dy_far, ext_far, expand_part, shrink_weight, rank
    )
    results = back_call(
        tokens[0], out_grad[0], segments[0], vectors, picked, front, middle, count, members
    )
    layer_out, tokens_grad = results[0][None], results[1][None]
    q_a, q_b, k_a, v_a, o_a, o_b, e_a, s_b, k_b, v_b, e_b, s_a = results[2:]
    return (
        layer_out,
        tokens_grad,
        flip(q_a),
        q_b,
        flip(k_a),
        k_b,
        flip(v_a),
        v_b,
        flip(o_a),
        o_b,
        flip(e_a),
        e_b,
        flip(s_a),
        s_b,
    )


def solution(mesh):
    placed = (
        P("wt", "ctx", None),
        P("wt", "ctx", None),
        P("wt", "ctx"),
        P("wt"),
        P(),
        P(),
        P(),
        P(),
        P("wt", None),
        P("wt", None),
        P("wt", None),
        P("wt", None),
        P(),
        P(),
        P(),
        P(),
        P(),
        P(),
        P(),
        P(),
        P(),
        P(),
        P(),
        P(),
    )
    return jax.shard_map(
        body,
        mesh=mesh,
        in_specs=placed,
        out_specs=(
            P("wt", "ctx", None),
            P("wt", "ctx", None),
            P(None, "wt", None),
            P(None, None, "wt"),
            P(None, "wt", None),
            P(None, None, "wt"),
            P(None, "wt", None),
            P(None, None, "wt"),
            P(None, "wt", None),
            P(None, None, "wt"),
            P(None, "wt", None),
            P(None, None, "wt"),
            P(None, "wt", None),
            P(None, None, "wt"),
        ),
        check_vma=False,
    )
```

```python
import functools
import math

import jax
import jax.numpy as jnp
from jax import lax
from jax.experimental import pallas as pl
from jax.experimental.pallas import tpu as pltpu
from jax.sharding import PartitionSpec as P

EPSILON = 1e-05
LOWEST = -1e30

MESH = pl.DeviceIdType.MESH
GELU_SCALE = 0.7978845608


def dot_nn(left, right):
    return lax.dot_general(
        left, right, (((1,), (0,)), ((), ())), preferred_element_type=jnp.float32
    )


def dot_nt(left, right):
    return lax.dot_general(
        left, right, (((1,), (1,)), ((), ())), preferred_element_type=jnp.float32
    )


def dot_tn(left, right):
    return lax.dot_general(
        left, right, (((0,), (0,)), ((), ())), preferred_element_type=jnp.float32
    )


NORM_ROWS = 32


def norm_rows(values, gain, offset):
    mean = jnp.mean(values, -1, keepdims=True)
    centre = values - mean
    scale_inv = lax.rsqrt(jnp.mean(centre * centre, -1, keepdims=True) + EPSILON)
    normed = centre * scale_inv
    return normed * gain + offset, normed, scale_inv


def mask_fill(bias, seg_win, seg_own, window, tok):
    keys_at = lax.broadcasted_iota(jnp.int32, (tok, tok), 0)
    tokens_at = lax.broadcasted_iota(jnp.int32, (tok, tok), 1)
    own = seg_own[0:1, :].astype(jnp.float32)
    for block in range(window):
        same = seg_win[block].astype(jnp.float32).T[:, 0:1] == own
        if block == window - 1:
            same = same & (keys_at <= tokens_at)
        bias[block * tok : (block + 1) * tok, :] = jnp.where(
            same, 0.0, LOWEST
        ).astype(bias.dtype)


def turned(values):
    return values.astype(jnp.float32).T.astype(jnp.bfloat16)


def pick_kernel(
    index_ref,
    q_a,
    q_b,
    k_a,
    k_b,
    v_a,
    v_b,
    o_a,
    o_b,
    e_a,
    e_b,
    s_a,
    s_b,
    attn_a,
    attn_b,
    out_a,
    out_b,
    exp_a,
    shr_b,
    ext,
    mark,
):
    rank, width = q_a.shape[1:]
    head = k_b.shape[2]
    units = ext.shape[3]
    for table in (attn_a, attn_b):
        table[...] = jnp.zeros_like(table)
    attn_a[0:rank, :] = q_a[0]
    attn_a[rank : 2 * rank, :] = k_a[0]
    attn_a[2 * rank : 3 * rank, :] = v_a[0]
    attn_b[0:rank, 0:width] = q_b[0]
    attn_b[rank : 2 * rank, width : width + head] = k_b[0]
    attn_b[2 * rank : 3 * rank, width + head : width + 2 * head] = v_b[0]
    out_a[0:rank, :] = o_a[0]
    out_b[0:rank, :] = o_b[0]
    exp_a[0:rank, :] = e_a[0]
    shr_b[0:rank, :] = s_b[0]
    for part in range(ext.shape[0]):
        span = slice(part * units, (part + 1) * units)
        ext[part, 0] = e_b[0, :, span]
        ext[part, 1] = s_a[0, :, span]
    lane = lax.broadcasted_iota(jnp.int32, mark.shape, 1)
    mark[...] = jnp.where(lane < 64, 0.0, index_ref[0].astype(jnp.float32))


def pick_call(adapter_index, tables, members):
    adapters, rank, width = tables[0].shape
    head = tables[3].shape[2]
    units = tables[10].shape[2] // members
    bf = jnp.bfloat16
    shapes = [
        ((128, width), bf),
        ((128, width + 2 * head), bf),
        ((rank, width), bf),
        ((rank, width), bf),
        ((rank, width), bf),
        ((rank, width), bf),
        ((members, 2, rank, units), bf),
        ((8, 128), jnp.float32),
    ]
    return pl.pallas_call(
        pick_kernel,
        grid_spec=pltpu.PrefetchScalarGridSpec(
            num_scalar_prefetch=1,
            grid=(1,),
            in_specs=[
                pl.BlockSpec((1,) + table.shape[1:], lambda i, index: (index[0], 0, 0))
                for table in tables
            ],
            out_specs=[
                pl.BlockSpec(shape, lambda i, index, r=len(shape): (0,) * r) for shape, _ in shapes
            ],
        ),
        out_shape=[jax.ShapeDtypeStruct(shape, kind) for shape, kind in shapes],
        name="pick",
    )(adapter_index, *tables)


def core_kernel(
    dims,
    tokens_ref,
    seg_ref,
    gain1,
    bias1,
    gain2,
    bias2,
    attn_a,
    attn_b,
    out_a,
    out_b,
    exp_a,
    shr_b,
    mark,
    grad_hbm,
    ext_hbm,
    qkv_hbm,
    out_hbm,
    exp_hbm,
    ws_hbm,
    kv_win,
    seg_win,
    lse_ref,
    mid_ref,
    low1_ref,
    low_o_ref,
    out_ref,
    dh_ref,
    lows_ref,
    table_ref,
    ids_ref,
    q_out,
    o_out,
    h2_out,
    out_far,
    wq_out,
    wo_out,
    q_ref,
    o_ref,
    h1,
    bias,
    flipped,
    wq,
    wo,
    we,
    land,
    h2_all,
    dy_all,
    lowt_all,
    ext_all,
    sis_send,
    sis_recv,
    own_recv,
    low_keep,
    low_send,
    low_recv,
    link_send,
    link_recv,
    pass_send,
    pass_recv,
    shard_send,
    shard_recv,
    kv_send,
    kv_recv,
    seg_send,
    seg_recv,
    side_send,
    side_recv,
    sis_ssem,
    sis_rsem,
    own_ssem,
    own_rsem,
    far_ssem,
    far_rsem,
    low_ssem,
    low_rsem,
    local_sem,
    spill_sem,
):
    tok, width, units, rows, count, window, heads, head, rank = dims
    bf = jnp.bfloat16
    me = lax.axis_index("wt")
    ctx = lax.axis_index("ctx")
    core = lax.rem(me, 2)
    side = lax.div(me, 2)
    sister = me + 1 - 2 * core
    across = me + 2 - 4 * side
    diagonal = sister + 2 - 4 * side
    stride = count // 4
    bit_y = lax.rem(ctx, 2)
    bit_z = lax.rem(lax.div(ctx, stride), 2)
    next_y = ctx + 1 - 2 * bit_y
    next_z = ctx + stride - 2 * stride * bit_z
    reach = window - 1
    own_block = window - 1

    def remote(src, dst, send, recv, peer):
        return pltpu.make_async_remote_copy(
            src_ref=src, dst_ref=dst, send_sem=send, recv_sem=recv, device_id=peer,
            device_id_type=MESH,
        )

    my_rows = pl.ds(pl.multiple_of(me * rows, rows), rows)
    quarter = pl.ds(pl.multiple_of(me * units, units), units)
    local = [
        pltpu.make_async_copy(qkv_hbm, wq.at[my_rows], local_sem.at[0]),
        pltpu.make_async_copy(out_hbm, wo.at[my_rows], local_sem.at[1]),
        pltpu.make_async_copy(exp_hbm.at[:, quarter], we.at[my_rows], local_sem.at[2]),
        pltpu.make_async_copy(seg_ref, seg_win.at[own_block], local_sem.at[3]),
        pltpu.make_async_copy(grad_hbm, dy_all.at[pl.ds(0, tok)], local_sem.at[4]),
        pltpu.make_async_copy(ext_hbm.at[me], ext_all.at[0], local_sem.at[5]),
    ]
    for copy in local:
        copy.start()
    for step in range(1, window):

        @pl.when(ctx < step)
        def _(step=step):
            slot = own_block - step
            kv_win[slot * tok : (slot + 1) * tok, :] = jnp.zeros((tok, 2 * head), jnp.bfloat16)
            seg_win[slot] = jnp.full(seg_ref.shape, -1, jnp.int32)

    barrier = pltpu.get_barrier_semaphore()
    for peer in (sister, across, diagonal):
        pl.semaphore_signal(barrier, inc=1, device_id={"wt": peer}, device_id_type=MESH)
    for other in range(count):

        @pl.when(ctx != other)
        def _(other=other):
            pl.semaphore_signal(barrier, inc=1, device_id={"ctx": other}, device_id_type=MESH)

    pl.semaphore_wait(barrier, 3 + count - 1)

    def part_rows(first, flip_y, flip_z, skip, length):
        turn_y = 1 - bit_y if flip_y else bit_y
        turn_z = 1 - bit_z if flip_z else bit_z
        start = first + (turn_y + 2 * turn_z) * (rows // 4) + skip
        return pl.ds(pl.multiple_of(start, 16), length)

    piece = rows // 4
    splits = {0: (80, 32, 16)}
    wide = width // 2
    slim = width // 4
    chunks = [(0, width, 2 * head)]
    chunks += [(0, i * slim, slim) for i in range(4)]
    chunks += [(1, i * wide, wide) for i in range(2)]
    for i in range(2):
        chunks += [(kind, i * (units // 2), units // 2) for kind in (2, 3)]

    def chunk_copies(number):
        kind, start, span = chunks[number]
        cut_x, cut_y, cut_z = (n * piece // 128 for n in splits.get(kind, (0, 64, 64)))
        cols = pl.ds(start, span)
        if kind < 2:
            source = (qkv_hbm, out_hbm)[kind]
            source_cols = cols
        else:
            source = exp_hbm
            target = across if kind == 2 else sister + 2 - 4 * side
            source_cols = pl.ds(pl.multiple_of(target * units + start, 128), span)
        home = (wq, wo, we, land)[kind]
        base = 0 if kind == 3 else across * rows
        home_base = 0 if kind == 3 else me * rows
        full = (False, False)
        sems = lambda way: (link_send.at[number, way], link_recv.at[number, way])

        def from_source(parity, skip, length):
            return (
                source.at[part_rows(0, *parity, skip, length), source_cols],
                home.at[part_rows(home_base, *parity, skip, length), cols],
            )

        def passing(parity, skip, length):
            at = home.at[part_rows(base, *parity, skip, length), cols]
            return (at, at)

        return [
            remote(*from_source(full, 0, piece), *sems(0), {"wt": across}),
            None if cut_x == 0 else
            remote(*from_source((True, True), 0, cut_x), *sems(5), {"wt": across}),
            remote(*passing(full, 0, piece), *sems(1), {"ctx": next_y}),
            remote(*passing(full, 0, piece), *sems(2), {"ctx": next_z}),
            remote(*passing((False, True), cut_x, cut_y), *sems(3), {"ctx": next_y}),
            remote(*passing((True, False), cut_x + cut_y, cut_z), *sems(4), {"ctx": next_z}),
        ]

    def sister_copy(number):
        kind, start, span = chunks[number]
        cols = pl.ds(start, span)
        far_rows = pl.ds(pl.multiple_of(across * rows, rows), rows)
        if kind == 3:
            src, dst = land.at[:, cols], we.at[far_rows, cols]
        else:
            home = (wq, wo)[kind]
            src = home.at[far_rows, cols]
            dst = src
        return remote(src, dst, pass_send.at[number], pass_recv.at[number], {"wt": sister})

    links = [chunk_copies(number) for number in range(len(chunks))]
    forwards = [None if chunks[n][0] == 2 else sister_copy(n) for n in range(len(chunks))]
    sister_quarter = pl.ds(pl.multiple_of(sister * units, units), units)
    own = [
        remote(qkv_hbm, wq.at[my_rows], shard_send.at[0], shard_recv.at[0], {"wt": sister}),
        remote(out_hbm, wo.at[my_rows], shard_send.at[1], shard_recv.at[1], {"wt": sister}),
        remote(
            exp_hbm.at[:, sister_quarter], we.at[my_rows], shard_send.at[2], shard_recv.at[2],
            {"wt": sister},
        ),
    ]

    def arrive(number):
        links[number][0].wait_recv()
        links[number][2].start()
        links[number][3].start()

    def turn(number):
        links[number][2].wait_recv()
        links[number][5].start()
        links[number][3].wait_recv()
        links[number][4].start()

    def finish(number):
        for way in (1, 4, 5):
            if links[number][way] is not None:
                links[number][way].wait_recv()
        if forwards[number] is not None:
            forwards[number].start()

    def ready(number):
        if forwards[number] is not None:
            forwards[number].wait_recv()

    def side_copy(number, src, dst, peer):
        return remote(src, dst, side_send.at[number], side_recv.at[number], {"wt": peer})

    def sent(number):
        for copy in links[number]:
            if copy is not None:
                copy.wait_send()
        if forwards[number] is not None:
            forwards[number].wait_send()

    half = tok // 2

    def far_rows(slot, part):
        return pl.ds(2 * tok + part * tok + (slot - 2) * half, half)

    near = [
        side_copy(0, ext_hbm.at[sister], ext_all.at[1], sister),
        side_copy(1, grad_hbm, dy_all.at[pl.ds(tok, tok)], sister),
    ]
    distant = [
        side_copy(2, ext_hbm.at[across], ext_all.at[2], across),
        side_copy(3, ext_hbm.at[diagonal], ext_all.at[3], diagonal),
    ]
    far_dy = [
        side_copy(
            4 + i, grad_hbm.at[pl.ds(i * half, half)], dy_all.at[far_rows(2, i)], across
        )
        for i in range(2)
    ]
    relay_dy = [
        side_copy(6 + i, dy_all.at[far_rows(2, i)], dy_all.at[far_rows(3, i)], sister)
        for i in range(2)
    ]
    near_h2 = side_copy(8, h2_all.at[pl.ds(0, tok)], h2_all.at[pl.ds(tok, tok)], sister)
    far_h2 = [
        side_copy(
            9 + i, h2_all.at[pl.ds(i * half, half)], h2_all.at[far_rows(2, i)], across
        )
        for i in range(2)
    ]
    relay_h2 = [
        side_copy(11 + i, h2_all.at[far_rows(2, i)], h2_all.at[far_rows(3, i)], sister)
        for i in range(2)
    ]
    send_low = [
        side_copy(12 + slot, lowt_all.at[0], lowt_all.at[slot], peer)
        for slot, peer in ((1, sister), (2, across), (3, diagonal))
    ]

    for number in range(len(chunks)):
        links[number][0].start()
        if links[number][1] is not None:
            links[number][1].start()
        if number == 0:
            own[0].start()
    own[1].start()
    own[2].start()
    for copy in near + distant + far_dy:
        copy.start()

    def seg_copy(step):
        return remote(
            seg_ref, seg_win.at[own_block - step], seg_send.at[step - 1], seg_recv.at[step - 1],
            {"ctx": ctx + step},
        )

    def kv_rows(distance):
        slot = own_block - distance
        return pl.ds(slot * tok if isinstance(slot, int) else pl.multiple_of(slot * tok, tok), tok)

    def kv_copy(held, send, distance, peer):
        return remote(
            kv_win.at[kv_rows(held)],
            kv_win.at[kv_rows(distance)],
            kv_send.at[send],
            kv_recv.at[distance - 1],
            {"ctx": peer},
        )

    place = lax.rem(ctx, stride)

    def kv_pass(level, act):
        if level < 2:

            @pl.when((ctx >= level * stride) & (ctx + stride < count))
            def _():
                far = (level + 1) * stride
                act(kv_copy(level * stride, (level, stride), far, ctx + stride))

        for other in range(stride):
            wanted = (other > place, other != place, other < place)[level]

            @pl.when(wanted & (ctx >= level * stride))
            def _(other=other):
                distance = other - place + level * stride
                act(kv_copy(level * stride, (level, other), distance, ctx - place + other))

    def kv_wait(distance):
        @pl.when(ctx >= distance)
        def _():
            kv_copy(0, (0, 0), distance, ctx).wait_recv()

    def kv_relay(level):
        kv_wait(level * stride)
        kv_pass(level, lambda copy: copy.start())

    def each_sent(make, act):
        for step in range(1, window):

            @pl.when(ctx + step < count)
            def _(step=step):
                act(make(step))

    def each_received(make):
        for step in range(1, window):

            @pl.when(ctx >= step)
            def _(step=step):
                make(step).wait_recv()

    each_sent(seg_copy, lambda copy: copy.start())

    def first_norm(number, carry):
        at = pl.ds(pl.multiple_of(number * NORM_ROWS, NORM_ROWS), NORM_ROWS)
        out, _, _ = norm_rows(tokens_ref[at, :].astype(jnp.float32), gain1[...], bias1[...])
        h1[at, :] = out.astype(jnp.bfloat16)
        return carry

    lax.fori_loop(0, tok // NORM_ROWS, first_norm, 0)
    low1_ref[...] = dot_nt(h1[...], attn_a[...]).astype(jnp.bfloat16)
    local[4].wait()
    lowt_all[0, rank : 2 * rank, :] = dot_nt(shr_b[...], dy_all[0:tok, :]).astype(bf)
    lowt_all[0, 2 * rank : 3 * rank, :] = jnp.broadcast_to(mark[0:1, 64:65], (rank, tok)).astype(
        bf
    )

    arrive(0)
    turn(0)
    arrive(1)
    finish(0)
    local[0].wait()
    own[0].wait_recv()
    ready(0)
    last = pl.ds(width, 2 * head)
    kv_win[own_block * tok : (own_block + 1) * tok, :] = (
        dot_nn(h1[...], wq[:, last]) + dot_nn(low1_ref[...], attn_b[:, last])
    ).astype(jnp.bfloat16)
    kv_pass(0, lambda copy: copy.start())
    turn(1)
    arrive(2)
    finish(1)
    kv_relay(1)
    turn(2)
    arrive(3)
    finish(2)
    kv_relay(2)
    turn(3)
    arrive(4)
    finish(3)
    local[3].wait()
    each_received(seg_copy)
    mask_fill(bias, seg_win, seg_ref, window, tok)
    turn(4)
    arrive(5)
    finish(4)
    for number in range(1, 5):
        ready(number)

    def query_tile(number, carry):
        cols = pl.ds(pl.multiple_of(number * 256, 256), 256)
        q_ref[:, cols] = (
            dot_nn(h1[...], wq[:, cols]) + dot_nn(low1_ref[...], attn_b[:, cols])
        ).astype(jnp.bfloat16)
        return carry

    lax.fori_loop(0, width // 256, query_tile, 0)
    spill_q = pltpu.make_async_copy(wq, wq_out, spill_sem.at[0])
    spill_q.start()
    turn(5)
    arrive(6)
    finish(5)
    for distance in range(1, window):
        if distance % stride:
            kv_wait(distance)
    scale = 1.0 / math.sqrt(head)

    for block in range(window):
        span = slice(block * tok, (block + 1) * tok)
        flipped[:, span] = turned(kv_win[span, head : 2 * head])
    span_q = tok if window * tok <= 2048 else 128

    def one_head(number, carry):
        cols = pl.ds(pl.multiple_of(number * head, head), head)
        for first in range(0, tok, span_q):
            at = slice(first, first + span_q)
            scores = dot_nt(kv_win[:, 0:head], q_ref[at, cols]) * scale + bias[:, at]
            highest = jnp.max(scores, 0, keepdims=True)
            weights = jnp.exp(scores - highest)
            total = jnp.sum(weights, 0, keepdims=True)
            probs = (weights * (1.0 / total)).astype(jnp.bfloat16)
            o_ref[at, cols] = dot_nn(flipped[...], probs).T.astype(jnp.bfloat16)
            lse_ref[number, :, at] = jnp.broadcast_to(highest + jnp.log(total), (8, span_q))
        return carry

    group = heads // 4
    lax.fori_loop(0, group, one_head, 0)
    arrive(7)
    lax.fori_loop(group, 2 * group, one_head, 0)
    turn(6)
    arrive(8)
    lax.fori_loop(2 * group, 3 * group, one_head, 0)
    finish(6)
    arrive(9)
    lax.fori_loop(3 * group, heads, one_head, 0)
    turn(7)
    arrive(10)
    spill_query = pltpu.make_async_copy(q_ref, q_out, spill_sem.at[5])
    spill_query.start()
    local[1].wait()
    own[1].wait_recv()
    ready(5)
    ready(6)
    spill_q.wait()
    for number in range(5):
        sent(number)
    own[0].wait_send()
    ws = wq.at[:, 0:width]
    load_ws = pltpu.make_async_copy(ws_hbm, ws, spill_sem.at[2])
    load_ws.start()
    low_o_ref[...] = dot_nt(o_ref[...], out_a[...]).astype(jnp.bfloat16)

    def out_tile(number, carry):
        cols = pl.ds(pl.multiple_of(number * 256, 256), 256)
        mid_ref[:, cols] = (
            tokens_ref[:, cols].astype(jnp.float32)
            + dot_nn(o_ref[...], wo[:, cols])
            + dot_nn(low_o_ref[...], out_b[:, cols])
        )
        return carry

    lax.fori_loop(0, width // 256, out_tile, 0)
    spill_o = pltpu.make_async_copy(wo, wo_out, spill_sem.at[1])
    spill_o.start()
    spill_mixed = pltpu.make_async_copy(o_ref, o_out, spill_sem.at[6])
    spill_mixed.start()

    def second_norm(number, carry):
        at = pl.ds(pl.multiple_of(number * NORM_ROWS, NORM_ROWS), NORM_ROWS)
        out, _, _ = norm_rows(mid_ref[at, :], gain2[...], bias2[...])
        h2_all[at, :] = out.astype(bf)
        return carry

    spill_mixed.wait()
    for part in range(2):
        steps = half // NORM_ROWS
        lax.fori_loop(part * steps, (part + 1) * steps, second_norm, 0)
        far_h2[part].start()
    near_h2.start()
    lowt_all[0, 0:rank, :] = dot_nt(exp_a[...], h2_all[0:tok, :]).astype(bf)
    for copy in send_low:
        copy.start()
    spill_h2 = pltpu.make_async_copy(h2_all.at[pl.ds(0, tok)], h2_out, spill_sem.at[3])
    spill_h2.start()
    spill_query.wait()
    spill_o.wait()
    for number in (5, 6):
        sent(number)
    own[1].wait_send()

    tile_a = 256
    tile_b = 512
    tiles_a = units // tile_a
    tiles_b = width // tile_b
    act_base = 0
    dup_base = 4 * tok
    units_of_work = [
        (0, 2 * tok, [(0, 0, tok, 0), (1, 0, tok, tok)]),
        (2 * tok, tok, [(2, 0, half, 0), (3, 0, half, half)]),
        (3 * tok, tok, [(2, half, half, 0), (3, half, half, half)]),
    ]

    def low_ready(slot):
        at = slice(slot * tok, (slot + 1) * tok)
        wq[at, width : width + rank] = turned(lowt_all[slot, 0:rank, :])
        wq[at, width + 128 : width + 128 + rank] = turned(lowt_all[slot, rank : 2 * rank, :])

    def forward(work, first, last):
        base, span, parts = units_of_work[work]

        def step(number, carry):
            cols = pl.ds(pl.multiple_of(number * tile_a, tile_a), tile_a)

            def with_low(kind):
                pieces = []
                for slot, skip, size, _ in parts:
                    at = slice(slot * tok + skip, slot * tok + skip + size)
                    small = wq[at, width + kind * 128 : width + kind * 128 + rank]
                    pieces.append(dot_nn(small, ext_all[slot, kind, :, cols]))
                return jnp.concatenate(pieces, 0)

            upward = dot_nn(h2_all[base : base + span, :], we[:, cols]) + with_low(0)
            square = upward * upward
            bend = jnp.tanh(GELU_SCALE * (upward + 0.044715 * (square * upward)))
            active = (0.5 * upward * (1.0 + bend)).astype(bf)
            slope = 0.5 * (1.0 + bend) + 0.5 * upward * (1.0 - bend * bend) * GELU_SCALE * (
                1.0 + 3.0 * 0.044715 * square
            )
            grad = (dot_nt(dy_all[base : base + span, :], wq[cols, 0:width]) + with_low(1)).astype(
                bf
            )
            grad_up = (grad.astype(jnp.float32) * slope).astype(bf)
            wo[act_base + base : act_base + base + span, cols] = active
            wo[dup_base + base : dup_base + base + span, cols] = grad_up
            for slot, skip, size, row in parts:
                for kind, right in enumerate((grad_up, active)):
                    left = lowt_all[slot, kind * rank : (kind + 1) * rank, skip : skip + size]
                    at = pl.ds((2 * slot + kind) * rank, rank)
                    value = dot_nn(left, right[row : row + size])
                    if work == 2:
                        value = value + table_ref[at, cols].astype(jnp.float32)
                    table_ref[at, cols] = value.astype(bf)
            return carry

        lax.fori_loop(first, last, step, 0)

    def low_sums(work):
        base, _, parts = units_of_work[work]
        for slot, skip, size, row in parts:
            at = slice(dup_base + base + row, dup_base + base + row + size)
            grad_low = dot_nt(wo[at, :], ext_all[slot, 0])
            at = slice(act_base + base + row, act_base + base + row + size)
            act_low = dot_nt(wo[at, :], ext_all[slot, 1])
            for start, value in ((0, grad_low), (128, act_low)):
                to = (slice(skip, skip + size), slice(start, start + rank))
                if slot == 0:
                    lows_ref[to] = value
                elif slot == 2:
                    low_keep[to] = value
                else:
                    low_send[(0 if slot == 1 else 1,) + to] = value.astype(bf)

    def back_tile(work, kind, number):
        base, span, _ = units_of_work[work]
        cols = pl.ds(pl.multiple_of(number * tile_b, tile_b), tile_b)
        if kind == 0:
            return dot_nt(wo[dup_base + base : dup_base + base + span, :], we[cols, :])
        return dot_nn(wo[act_base + base : act_base + base + span, :], wq[:, cols])

    def sis_copy(kind, part, number):
        at = (kind, part, number)
        return remote(
            sis_send.at[at], sis_recv.at[at], sis_ssem.at[at], sis_rsem.at[at], {"wt": sister}
        )

    def tile_cols(number):
        return pl.ds(pl.multiple_of(number * tile_b, tile_b), tile_b)

    def own_at(kind, number):
        return (pl.ds(kind * tok, tok), tile_cols(number))

    def far_at(part, number):
        return (pl.ds(part * half, half), tile_cols(number))

    def part_at(number):
        return (pl.ds(pl.multiple_of(lax.rem(number, 2) * half, half), half), pl.ds(0, tile_b))

    def own_copy(kind, number):
        at = (kind, number)
        return remote(
            land.at[own_at(kind, number)], own_recv.at[at], own_ssem.at[at], own_rsem.at[at],
            {"wt": sister},
        )

    def far_copy(part, number):
        at = (part, number)
        return remote(
            q_ref.at[far_at(part, number)], o_ref.at[far_at(part, number)], far_ssem.at[at],
            far_rsem.at[at], {"wt": across},
        )

    def low_copy(number, peer):
        return remote(
            low_send.at[number],
            low_recv.at[number],
            low_ssem.at[number],
            low_rsem.at[number],
            {"wt": peer},
        )

    def join(kind, part, number):
        sis_copy(kind, part, number).wait_recv()
        total = (
            dh_ref[part_at(number)] + sis_recv[kind, part, number].astype(jnp.float32)
        ).astype(bf)
        if kind == 0:
            q_ref[far_at(part, number)] = total
            far_copy(part, number).start()
        else:
            cols = pl.ds(pl.multiple_of(number * tile_b, tile_b), tile_b)
            h1[part * half : (part + 1) * half, cols] = total

    def far_tiles(kind, part):
        def step(number, carry):
            both = back_tile(1 + part, kind, number)
            sis_send[kind, part, number] = both[half:].astype(bf)
            sis_copy(kind, part, number).start()

            @pl.when(number > 0)
            def _():
                join(kind, part, number - 1)

            dh_ref[part_at(number)] = both[:half]
            return carry

        lax.fori_loop(0, tiles_b, step, 0)
        join(kind, part, tiles_b - 1)

    def near_tiles(kind, target):
        def step(number, carry):
            cols = pl.ds(pl.multiple_of(number * tile_b, tile_b), tile_b)
            both = back_tile(0, kind, number)
            target[:, cols] = both[:tok].astype(target.dtype)
            land[own_at(kind, number)] = both[tok:].astype(bf)
            own_copy(kind, number).start()
            return carry

        lax.fori_loop(0, tiles_b, step, 0)

    lows_ref[...] = jnp.zeros_like(lows_ref)
    low_send[...] = jnp.zeros_like(low_send)
    low_ready(0)
    finish(7)
    turn(8)
    finish(8)
    turn(9)
    local[2].wait()
    local[5].wait()
    own[2].wait_recv()
    ready(8)
    load_ws.wait()
    near[0].wait_recv()
    near[1].wait_recv()
    send_low[0].wait_recv()
    low_ready(1)
    near_h2.wait_recv()
    forward(0, 0, tiles_a // 2)
    finish(9)
    turn(10)
    finish(10)
    for index in range(2):
        far_dy[index].wait_recv()
        relay_dy[index].start()
    ready(10)
    forward(0, tiles_a // 2, tiles_a)
    low_sums(0)
    low_own = low_copy(0, sister)
    low_own.start()
    for slot in (2, 3):
        distant[slot - 2].wait_recv()
        send_low[slot - 1].wait_recv()
        low_ready(slot)
    for slot in range(4):
        ids_ref[slot] = lowt_all[slot, 2 * rank : 3 * rank, 0:128].astype(jnp.float32)
    for part in range(2):
        if part == 0:
            for index in range(2):
                far_h2[index].wait_recv()
                relay_h2[index].start()
        relay_dy[part].wait_recv()
        relay_h2[part].wait_recv()
        forward(1 + part, 0, tiles_a)
        far_tiles(0, part)
        low_sums(1 + part)
    low_sis = low_copy(1, sister)
    low_sis.start()
    far_tiles(1, 0)
    far_tiles(1, 1)
    spill_far = pltpu.make_async_copy(h1, out_far, spill_sem.at[4])
    spill_far.start()
    low_sis.wait_recv()
    for start in (0, 128):
        to = (slice(None), slice(start, start + rank))
        low_send[(2,) + to] = (low_keep[to] + low_recv[(1,) + to].astype(jnp.float32)).astype(bf)
    low_far = low_copy(2, across)
    low_far.start()
    for number in range(7, len(chunks)):
        sent(number)
    near_tiles(0, dh_ref)
    near_tiles(1, out_ref)

    def end_step(number, carry):
        cols = pl.ds(pl.multiple_of(number * tile_b, tile_b), tile_b)
        own_copy(0, number).wait_recv()
        own_copy(1, number).wait_recv()
        for part in range(2):
            at = slice(part * half, (part + 1) * half)
            far_copy(part, number).wait_recv()
            dh_ref[at, cols] = (
                dh_ref[at, cols]
                + own_recv[0, number, at, :].astype(jnp.float32)
                + o_ref[far_at(part, number)].astype(jnp.float32)
            )
        out_ref[:, cols] = (
            out_ref[:, cols].astype(jnp.float32) + own_recv[1, number].astype(jnp.float32)
        ).astype(bf)
        for kind in range(2):
            own_copy(kind, number).wait_send()
            for part in range(2):
                sis_copy(kind, part, number).wait_send()
        for part in range(2):
            far_copy(part, number).wait_send()
        return carry

    lax.fori_loop(0, tiles_b, end_step, 0)
    low_own.wait_recv()
    low_far.wait_recv()
    lows_ref[...] = (
        lows_ref[...] + low_recv[0].astype(jnp.float32) + low_recv[2].astype(jnp.float32)
    )
    own[2].wait_send()
    for copy in near + distant + far_dy + relay_dy + [near_h2] + far_h2 + relay_h2 + send_low:
        copy.wait_send()
    for copy in (low_own, low_sis, low_far):
        copy.wait_send()
    each_sent(seg_copy, lambda copy: copy.wait_send())
    for level in range(3):
        kv_pass(level, lambda copy: copy.wait_send())
    spill_h2.wait()
    spill_far.wait()


def core_call(tokens, grad_top, segments, vectors, picked, weights, count):
    tok, width = tokens.shape
    qkv_weight, out_weight, expand_weight, shrink_weight = weights
    rows = qkv_weight.shape[0]
    head = (qkv_weight.shape[1] - width) // 2
    heads = width // head
    units = shrink_weight.shape[0]
    window = count // 2 + 1
    bf = jnp.bfloat16
    f32 = jnp.float32
    seg_rows = jnp.broadcast_to(segments[None, :], (8, tok))
    attn_a, attn_b, out_a, out_b, exp_a, shr_b, ext, mark = picked
    rank = ext.shape[2]
    half, tiles = tok // 2, width // 512
    vmem = lambda: pl.BlockSpec(memory_space=pltpu.VMEM)
    hbm = lambda: pl.BlockSpec(memory_space=pl.ANY)
    dma = pltpu.SemaphoreType.DMA
    dims = (tok, width, units, rows, count, window, heads, head, rank)
    shape = jax.ShapeDtypeStruct
    inputs = [
        tokens, seg_rows, *vectors, attn_a, attn_b, out_a, out_b, exp_a, shr_b, mark,
    ]
    outs = [
        shape((window * tok, 2 * head), bf),
        shape((window, 8, tok), jnp.int32),
        shape((heads, 8, tok), f32),
        shape((tok, width), f32),
        shape((tok, 128), bf),
        shape((tok, rank), bf),
        shape((tok, width), bf),
        shape((tok, width), f32),
        shape((tok, 256), f32),
        shape((8 * rank, units), bf),
        shape((4, rank, 128), f32),
    ]
    spilled = [
        shape((tok, width), bf),
        shape((tok, width), bf),
        shape((tok, width), bf),
        shape((tok, width), bf),
        shape((width, width + 2 * head), bf),
        shape((width, width), bf),
    ]
    return pl.pallas_call(
        functools.partial(core_kernel, dims),
        out_shape=tuple(outs + spilled),
        in_specs=[vmem() for _ in inputs] + [hbm() for _ in range(6)],
        out_specs=tuple([vmem() for _ in outs] + [hbm() for _ in spilled]),
        scratch_shapes=[
            pltpu.VMEM((tok, width), bf),
            pltpu.VMEM((tok, width), bf),
            pltpu.VMEM((tok, width), bf),
            pltpu.VMEM((window * tok, tok), bf),
            pltpu.VMEM((head, window * tok), bf),
            pltpu.VMEM((width, width + 2 * head), bf),
            pltpu.VMEM((width, width), bf),
            pltpu.VMEM((width, units), bf),
            pltpu.VMEM((rows, units), bf),
            pltpu.VMEM((4 * tok, width), bf),
            pltpu.VMEM((4 * tok, width), bf),
            pltpu.VMEM((4, 3 * rank, tok), bf),
            pltpu.VMEM((4, 2, rank, units), bf),
            pltpu.VMEM((2, 2, tiles, half, 512), bf),
            pltpu.VMEM((2, 2, tiles, half, 512), bf),
            pltpu.VMEM((2, tiles, tok, 512), bf),
            pltpu.VMEM((tok, 256), f32),
            pltpu.VMEM((3, tok, 256), bf),
            pltpu.VMEM((3, tok, 256), bf),
            dma((11, 6)),
            dma((11, 6)),
            dma((11,)),
            dma((11,)),
            dma((3,)),
            dma((3,)),
            dma((3, count // 4 + 1)),
            dma((window - 1,)),
            dma((window - 1,)),
            dma((window - 1,)),
            dma((16,)),
            dma((16,)),
            dma((2, 2, tiles)),
            dma((2, 2, tiles)),
            dma((2, tiles)),
            dma((2, tiles)),
            dma((2, tiles)),
            dma((2, tiles)),
            dma((3,)),
            dma((3,)),
            dma((6,)),
            dma((7,)),
        ],
        compiler_params=pltpu.CompilerParams(
            collective_id=2, has_side_effects=True, vmem_limit_bytes=67043328
        ),
        name="core",
    )(
        *inputs, grad_top, ext, qkv_weight, out_weight, expand_weight, shrink_weight,
    )


def norm_pull(grad_out, gain, normed, scale_inv):
    grad_norm = grad_out * gain
    return scale_inv * (
        grad_norm
        - jnp.mean(grad_norm, -1, keepdims=True)
        - normed * jnp.mean(grad_norm * normed, -1, keepdims=True)
    )


def back_kernel(
    dims,
    tokens_ref,
    grad_ref,
    seg_ref,
    gain1,
    bias1,
    gain2,
    bias2,
    attn_a,
    attn_b,
    out_a,
    out_b,
    exp_a,
    shr_b,
    q_ref,
    kv_win,
    seg_win,
    lse_ref,
    o_ref,
    mid_ref,
    h2_ref,
    low1_ref,
    low_o_ref,
    shrunk_ref,
    dh_ref,
    lows_ref,
    ids_ref,
    wq_hbm,
    wo_hbm,
    out_far,
    mlp_tab,
    layer_ref,
    tgrad_ref,
    q_a,
    q_b,
    k_a,
    v_a,
    o_a,
    o_b,
    e_a,
    s_b,
    k_b,
    v_b,
    e_b,
    s_a,
    wq,
    bias,
    flipped,
    dmid,
    dacc,
    db,
    dout,
    dqkv,
    h1,
    dkv,
    dkv_send,
    dkv_recv,
    share,
    land,
    rs_a,
    ag_a,
    rs_b,
    ag_b,
    out_recv,
    out_ssem,
    out_rsem,
    local_sem,
    kv_ssem,
    kv_rsem,
    share_ssem,
    share_rsem,
    red_ssem,
    red_rsem,
):
    tok, width, rank, count, members, window, heads, head = dims
    me = lax.axis_index("wt")
    ctx = lax.axis_index("ctx")
    core = lax.rem(me, 2)
    side = lax.div(me, 2)
    sister = me + 1 - 2 * core
    across = me + 2 - 4 * side
    diagonal = sister + 2 - 4 * side
    own_block = window - 1
    part = width // members
    bf = jnp.bfloat16

    wo = wq.at[:, 0:width]
    local = [
        pltpu.make_async_copy(wo_hbm, wo, local_sem.at[0]),
        pltpu.make_async_copy(wq_hbm, wq, local_sem.at[1]),
    ]
    local[0].start()

    barrier = pltpu.get_barrier_semaphore()
    for peer in (sister, across, diagonal):
        pl.semaphore_signal(barrier, inc=1, device_id={"wt": peer}, device_id_type=MESH)
    for other in range(count):

        @pl.when(ctx != other)
        def _(other=other):
            pl.semaphore_signal(barrier, inc=1, device_id={"ctx": other}, device_id_type=MESH)

    def remote(src, dst, send, recv, peer):
        return pltpu.make_async_remote_copy(
            src_ref=src, dst_ref=dst, send_sem=send, recv_sem=recv, device_id=peer,
            device_id_type=MESH,
        )

    def each_other(act):
        for other in range(count):

            @pl.when(ctx != other)
            def _(other=other):
                act(other)

    def scatter_copy(lane, table, piece, landing, other):
        return remote(
            table.at[piece(other)],
            landing.at[ctx],
            red_ssem.at[lane, 0, other],
            red_rsem.at[lane, 0, ctx],
            {"ctx": other},
        )

    def scatter_wait(lane, table, piece, landing, other):
        remote(
            table.at[piece(other)],
            landing.at[other],
            red_ssem.at[lane, 0, other],
            red_rsem.at[lane, 0, other],
            {"ctx": other},
        ).wait_recv()

    def gather_copy(lane, result, other):
        return remote(
            result.at[ctx],
            result.at[ctx],
            red_ssem.at[lane, 1, other],
            red_rsem.at[lane, 1, ctx],
            {"ctx": other},
        )

    def gather_wait(lane, result, other):
        remote(
            result.at[other],
            result.at[other],
            red_ssem.at[lane, 1, other],
            red_rsem.at[lane, 1, other],
            {"ctx": other},
        ).wait_recv()

    def scatter_start(lane, table, piece, landing):
        each_other(lambda other: scatter_copy(lane, table, piece, landing, other).start())
        mine = pltpu.make_async_copy(
            table.at[piece(ctx)], landing.at[ctx], local_sem.at[2 + lane]
        )
        mine.start()
        return mine

    def reduce_gather(lane, table, piece, landing, result, mine):
        mine.wait()
        each_other(lambda other: scatter_wait(lane, table, piece, landing, other))
        total = landing[0].astype(jnp.float32)
        for other in range(1, count):
            total = total + landing[other].astype(jnp.float32)
        result[ctx] = total.astype(bf)
        each_other(lambda other: gather_copy(lane, result, other).start())

    def reduce_end(lane, table, piece, landing, result):
        each_other(lambda other: gather_wait(lane, result, other))
        each_other(lambda other: scatter_copy(lane, table, piece, landing, other).wait_send())
        each_other(lambda other: gather_copy(lane, result, other).wait_send())

    lanes_b = min(16, count)
    rows_b = count // lanes_b
    high_b, wide_b = rs_b.shape[1:]
    high_a, wide_a = rs_a.shape[1:]

    def piece_b(other):
        down = lax.div(other, lanes_b) if not isinstance(other, int) else other // lanes_b
        along = lax.rem(other, lanes_b) if not isinstance(other, int) else other % lanes_b
        return (
            pl.ds(pl.multiple_of(down * high_b, 16), high_b),
            pl.ds(pl.multiple_of(along * wide_b, 128), wide_b),
        )

    def piece_a(other):
        down = lax.div(other, 4) if not isinstance(other, int) else other // 4
        along = lax.rem(other, 4) if not isinstance(other, int) else other % 4
        return (
            pl.ds(pl.multiple_of(down * high_a, 16), high_a),
            pl.ds(pl.multiple_of(along * wide_a, 128), wide_a),
        )

    pl.semaphore_wait(barrier, 3 + count - 1)
    mine_b = scatter_start(1, mlp_tab, piece_b, rs_b)
    out_copy = remote(out_far, out_recv, out_ssem.at[0], out_rsem.at[0], {"wt": across})
    out_copy.start()

    grad_low = lows_ref[:, 0:rank].astype(bf)
    shrink_low = lows_ref[:, 128 : 128 + rank].astype(bf)
    lows_tile = 512

    def low_step(number, carry):
        cols = pl.ds(pl.multiple_of(number * lows_tile, lows_tile), lows_tile)
        dmid[:, cols] = dh_ref[:, cols] + dot_nn(grad_low, exp_a[:, cols])
        return carry

    lax.fori_loop(0, width // lows_tile, low_step, 0)

    def second_pull(number, carry):
        at = pl.ds(pl.multiple_of(number * NORM_ROWS, NORM_ROWS), NORM_ROWS)
        _, normed, scale_inv = norm_rows(mid_ref[at, :], gain2[...], bias2[...])
        value = grad_ref[at, :].astype(jnp.float32) + norm_pull(
            dmid[at, :], gain2[...], normed, scale_inv
        )
        dmid[at, :] = value
        db[at, :] = value.astype(bf)
        return carry

    lax.fori_loop(0, tok // NORM_ROWS, second_pull, 0)
    grad_out_low = dot_nt(db[...], out_b[...]).astype(bf)
    local[0].wait()

    def out_pull(number, carry):
        cols = pl.ds(pl.multiple_of(number * 256, 256), 256)
        dout[:, cols] = (
            dot_nt(db[...], wq[cols, 0:width]) + dot_nn(grad_out_low, out_a[:, cols])
        ).astype(bf)
        return carry

    lax.fori_loop(0, width // 256, out_pull, 0)
    local[1].start()
    reduce_gather(1, mlp_tab, piece_b, rs_b, ag_b, mine_b)

    mask_fill(bias, seg_win, seg_ref, window, tok)
    for block in range(window):
        span = slice(block * tok, (block + 1) * tok)
        flipped[:, span] = turned(kv_win[span, 0:head])
    dkv[...] = jnp.zeros_like(dkv)
    scale = 1.0 / math.sqrt(head)
    span_q = tok if window * tok <= 2048 else 128

    def one_head(number, carry):
        cols = pl.ds(pl.multiple_of(number * head, head), head)
        for first in range(0, tok, span_q):
            at = slice(first, first + span_q)
            query = q_ref[at, cols]
            grad = dout[at, cols]
            scores = dot_nt(kv_win[:, 0:head], query) * scale + bias[:, at]
            probs = jnp.exp(scores - lse_ref[number, 0:1, at])
            grad_probs = dot_nt(kv_win[:, head : 2 * head], grad)
            delta = jnp.sum(probs * grad_probs, 0, keepdims=True)
            grad_scores = (probs * (grad_probs - delta)).astype(bf)
            dqkv[at, cols] = (dot_nn(flipped[...], grad_scores).T * scale).astype(bf)
            dkv[:, 0:head] = dkv[:, 0:head] + dot_nn(grad_scores, query)
            dkv[:, head : 2 * head] = dkv[:, head : 2 * head] + dot_nn(probs.astype(bf), grad)
        return carry

    lax.fori_loop(0, heads, one_head, 0)

    out_copy.wait_recv()

    def layer_step(number, carry):
        cols = pl.ds(pl.multiple_of(number * lows_tile, lows_tile), lows_tile)
        layer_ref[:, cols] = (
            mid_ref[:, cols]
            + shrunk_ref[:, cols].astype(jnp.float32)
            + out_recv[:, cols].astype(jnp.float32)
            + dot_nn(shrink_low, shr_b[:, cols])
        ).astype(bf)
        return carry

    def kv_copy(step):
        return remote(
            dkv_send.at[step - 1],
            dkv_recv.at[step - 1],
            kv_ssem.at[step - 1],
            kv_rsem.at[step - 1],
            {"ctx": ctx - step},
        )

    for step in range(1, window):

        @pl.when(ctx >= step)
        def _(step=step):
            at = slice((own_block - step) * tok, (own_block - step + 1) * tok)
            dkv_send[step - 1, :, 0:head] = (dkv[at, 0:head] * scale).astype(bf)
            dkv_send[step - 1, :, head : 2 * head] = dkv[at, head : 2 * head].astype(bf)
            kv_copy(step).start()

    local[1].wait()

    def first_norm(number, carry):
        at = pl.ds(pl.multiple_of(number * NORM_ROWS, NORM_ROWS), NORM_ROWS)
        out, _, _ = norm_rows(tokens_ref[at, :].astype(jnp.float32), gain1[...], bias1[...])
        h1[at, :] = out.astype(bf)
        return carry

    lax.fori_loop(0, tok // NORM_ROWS, first_norm, 0)
    lax.fori_loop(0, width // lows_tile, layer_step, 0)

    def put(group, value):
        for other in range(members):
            span = slice(other * part, (other + 1) * part)
            share[other, group * rank : (group + 1) * rank, :] = value[:, span].astype(bf)

    query_grad = dqkv[:, 0:width]
    put(1, dot_tn(low1_ref[:, 0:rank], query_grad))
    put(4, dot_tn(grad_out_low[:, 0:rank], o_ref[...]))
    put(5, dot_tn(low_o_ref[:, 0:rank], db[...]))
    put(6, dot_tn(grad_low[:, 0:rank], h2_ref[...]))
    put(7, dot_tn(shrink_low[:, 0:rank], grad_ref[...]))

    def first_half(number, carry):
        cols = pl.ds(pl.multiple_of(number * 256, 256), 256)
        dacc[:, cols] = dot_nt(dqkv[:, 0:width], wq[cols, 0:width])
        return carry

    lax.fori_loop(0, width // 256, first_half, 0)

    own_at = slice(own_block * tok, (own_block + 1) * tok)
    dkv[own_at, 0:head] = dkv[own_at, 0:head] * scale
    for step in range(1, window):

        @pl.when(ctx + step < count)
        def _(step=step):
            kv_copy(step).wait_recv()
            dkv[own_at, :] = dkv[own_at, :] + dkv_recv[step - 1].astype(jnp.float32)

    last = slice(width, width + 2 * head)
    dqkv[:, last] = dkv[own_at, :].astype(bf)
    grad_rank = dot_nt(dqkv[...], attn_b[...]).astype(bf)
    first_grads = dot_tn(grad_rank[:, 0 : 3 * rank], h1[...])
    put(0, first_grads[0:rank])
    put(2, first_grads[rank : 2 * rank])
    put(3, first_grads[2 * rank : 3 * rank])
    small = dot_tn(low1_ref[...], dqkv[:, last])
    thin = head // members
    share[:, 8 * rank : 10 * rank, :] = jnp.zeros((members, 2 * rank, part), bf)
    for other in range(members):
        span = slice(other * thin, (other + 1) * thin)
        share[other, 8 * rank : 9 * rank, 0:thin] = small[rank : 2 * rank, span].astype(bf)
        span = slice(head + other * thin, head + (other + 1) * thin)
        share[other, 9 * rank : 10 * rank, 0:thin] = small[2 * rank : 3 * rank, span].astype(bf)

    deep = 10 * rank

    def slot_rows(slot):
        return pl.ds(slot * deep, deep)

    exchange = [
        remote(
            share.at[peer],
            land.at[slot_rows(slot)],
            share_ssem.at[slot - 1],
            share_rsem.at[slot - 1],
            {"wt": peer},
        )
        for slot, peer in ((1, sister), (2, across), (3, diagonal))
    ]
    for copy in exchange:
        copy.start()
    mine_share = pltpu.make_async_copy(share.at[me], land.at[slot_rows(0)], local_sem.at[4])
    mine_share.start()

    def second_half(number, carry):
        cols = pl.ds(pl.multiple_of(number * 256, 256), 256)
        dacc[:, cols] = (
            dacc[:, cols]
            + dot_nt(dqkv[:, last], wq[cols, last])
            + dot_nn(grad_rank, attn_a[:, cols])
        )
        return carry

    lax.fori_loop(0, width // 256, second_half, 0)

    mine_share.wait()
    for copy in exchange:
        copy.wait_recv()
    mine_a = scatter_start(0, land, piece_a, rs_a)

    def first_pull(number, carry):
        at = pl.ds(pl.multiple_of(number * NORM_ROWS, NORM_ROWS), NORM_ROWS)
        _, normed, scale_inv = norm_rows(
            tokens_ref[at, :].astype(jnp.float32), gain1[...], bias1[...]
        )
        tgrad_ref[at, :] = (
            dmid[at, :] + norm_pull(dacc[at, :], gain1[...], normed, scale_inv)
        ).astype(bf)
        return carry

    lax.fori_loop(0, tok // NORM_ROWS, first_pull, 0)
    reduce_gather(0, land, piece_a, rs_a, ag_a, mine_a)
    reduce_end(1, mlp_tab, piece_b, rs_b, ag_b)

    adapters = q_a.shape[0]
    marks = [ids_ref[slot, 0:1, 64:65] for slot in range(members)]

    def spread(targets, sources):
        for number in range(adapters):
            total = 0.0
            for slot in range(members):
                hot = jnp.where(marks[slot] == float(number), 1.0, 0.0)
                total = total + hot * sources[slot]
            targets(number, total)

    for group, target in ((0, e_b), (1, s_a)):
        for other in range(count):
            along = (other % lanes_b) * wide_b
            down = other // lanes_b
            sources = []
            for slot in range(members):
                top = (2 * slot + group) * rank - down * high_b
                if 0 <= top < high_b:
                    sources.append((slot, ag_b[other, top : top + rank, :].astype(jnp.float32)))
            for number in range(adapters):
                total = None
                for slot, value in sources:
                    hot = jnp.where(marks[slot] == float(number), 1.0, 0.0) * value
                    total = hot if total is None else total + hot
                at = (number, slice(None), slice(along, along + wide_b))
                if down == 0:
                    target[at] = total
                else:
                    target[at] = target[at] + total

    reduce_end(0, land, piece_a, rs_a, ag_a)
    for group, target in enumerate((q_a, q_b, k_a, v_a, o_a, o_b, e_a, s_b, k_b, v_b)):
        for along in range(4):
            sources = []
            for slot in range(members):
                top = slot * deep + group * rank
                down = top // high_a
                low = top - down * high_a
                sources.append(ag_a[down * 4 + along, low : low + rank, :].astype(jnp.float32))
            for number in range(adapters):
                total = 0.0
                for slot in range(members):
                    hot = jnp.where(marks[slot] == float(number), 1.0, 0.0)
                    total = total + hot * sources[slot]
                if group < 8:
                    target[number, :, along * wide_a : (along + 1) * wide_a] = total
                elif along == 0:
                    target[number] = total[:, 0:thin]
    for copy in exchange:
        copy.wait_send()
    out_copy.wait_send()
    for step in range(1, window):

        @pl.when(ctx >= step)
        def _(step=step):
            kv_copy(step).wait_send()


def back_call(tokens, grad_top, segments, vectors, picked, core, count, members):
    tok, width = tokens.shape
    kv_win, seg_win, lse, mid, low1, low_o, shrunk, grad_second, lows = core[:9]
    mlp_tab, ids, q, o, h2, out_far, wq, wo = core[9:]
    attn_a, attn_b, out_a, out_b, exp_a, shr_b, _, _ = picked
    head = kv_win.shape[1] // 2
    heads = width // head
    rank, units = ids.shape[1], mlp_tab.shape[1]
    window = count // 2 + 1
    part = width // members
    adapters = 8
    lanes_b = min(16, count)
    high_b, wide_b = 2 * rank * members * lanes_b // count, units // lanes_b
    high_a, wide_a = 10 * rank * members * 4 // count, part // 4
    bf = jnp.bfloat16
    seg_rows = jnp.broadcast_to(segments[None, :], (8, tok))
    vmem = lambda: pl.BlockSpec(memory_space=pltpu.VMEM)
    hbm = lambda: pl.BlockSpec(memory_space=pl.ANY)
    dma = pltpu.SemaphoreType.DMA
    shape = jax.ShapeDtypeStruct
    dims = (tok, width, rank, count, members, window, heads, head)
    inputs = [
        tokens, grad_top, seg_rows, *vectors, attn_a, attn_b, out_a, out_b, exp_a, shr_b,
        q, kv_win, seg_win, lse, o, mid, h2, low1, low_o, shrunk, grad_second, lows, ids,
    ]
    outs = [shape((tok, width), bf), shape((tok, width), bf)]
    outs += [shape((adapters, rank, part), jnp.float32) for _ in range(8)]
    outs += [shape((adapters, rank, head // members), jnp.float32) for _ in range(2)]
    outs += [shape((adapters, rank, units), jnp.float32) for _ in range(2)]
    return pl.pallas_call(
        functools.partial(back_kernel, dims),
        out_shape=tuple(outs),
        in_specs=[vmem() for _ in inputs] + [hbm() for _ in range(4)],
        out_specs=tuple(vmem() for _ in outs),
        scratch_shapes=[
            pltpu.VMEM((width, width + 2 * head), bf),
            pltpu.VMEM((window * tok, tok), jnp.float32 if window * tok <= 2048 else bf),
            pltpu.VMEM((head, window * tok), bf),
            pltpu.VMEM((tok, width), jnp.float32),
            pltpu.VMEM((tok, width), jnp.float32),
            pltpu.VMEM((tok, width), bf),
            pltpu.VMEM((tok, width), bf),
            pltpu.VMEM((tok, width + 2 * head), bf),
            pltpu.VMEM((tok, width), bf),
            pltpu.VMEM((window * tok, 2 * head), jnp.float32),
            pltpu.VMEM((window - 1, tok, 2 * head), bf),
            pltpu.VMEM((window - 1, tok, 2 * head), bf),
            pltpu.VMEM((members, 10 * rank, part), bf),
            pltpu.VMEM((members * 10 * rank, part), bf),
            pltpu.VMEM((count, high_a, wide_a), bf),
            pltpu.VMEM((count, high_a, wide_a), bf),
            pltpu.VMEM((count, high_b, wide_b), bf),
            pltpu.VMEM((count, high_b, wide_b), bf),
            pltpu.VMEM((tok, width), bf),
            dma((1,)),
            dma((1,)),
            dma((5,)),
            dma((window - 1,)),
            dma((window - 1,)),
            dma((3,)),
            dma((3,)),
            dma((2, 2, count)),
            dma((2, 2, count)),
        ],
        compiler_params=pltpu.CompilerParams(
            collective_id=3, has_side_effects=True, vmem_limit_bytes=63 * 1024 * 1024
        ),
        name="back",
    )(*inputs, wq, wo, out_far, mlp_tab)


def body(
    tokens,
    out_grad,
    segments,
    adapter_index,
    first_gain,
    first_bias,
    second_gain,
    second_bias,
    qkv_weight,
    out_weight,
    expand_weight,
    shrink_weight,
    query_first,
    query_second,
    key_first,
    key_second,
    value_first,
    value_second,
    output_first,
    output_second,
    expand_first,
    expand_second,
    shrink_first,
    shrink_second,
):
    count = lax.axis_size("ctx")
    members = lax.axis_size("wt")
    rank = query_second.shape[1]
    flip = lambda table: table.transpose(0, 2, 1)
    row = lambda vector: vector[None, :]
    tables = [
        flip(query_first),
        query_second,
        flip(key_first),
        key_second,
        flip(value_first),
        value_second,
        flip(output_first),
        output_second,
        flip(expand_first),
        expand_second,
        flip(shrink_first),
        shrink_second,
    ]
    picked = pick_call(adapter_index, tables, members)
    vectors = [row(first_gain), row(first_bias), row(second_gain), row(second_bias)]
    weights = (qkv_weight, out_weight, expand_weight, shrink_weight)
    core = core_call(tokens[0], out_grad[0], segments[0], vectors, picked, weights, count)
    results = back_call(
        tokens[0], out_grad[0], segments[0], vectors, picked, core, count, members
    )
    layer_out, tokens_grad = results[0][None], results[1][None]
    q_a, q_b, k_a, v_a, o_a, o_b, e_a, s_b, k_b, v_b, e_b, s_a = results[2:]
    return (
        layer_out,
        tokens_grad,
        flip(q_a),
        q_b,
        flip(k_a),
        k_b,
        flip(v_a),
        v_b,
        flip(o_a),
        o_b,
        flip(e_a),
        e_b,
        flip(s_a),
        s_b,
    )


def solution(mesh):
    placed = (
        P("wt", "ctx", None),
        P("wt", "ctx", None),
        P("wt", "ctx"),
        P("wt"),
        P(),
        P(),
        P(),
        P(),
        P("wt", None),
        P("wt", None),
        P("wt", None),
        P("wt", None),
        P(),
        P(),
        P(),
        P(),
        P(),
        P(),
        P(),
        P(),
        P(),
        P(),
        P(),
        P(),
    )
    return jax.shard_map(
        body,
        mesh=mesh,
        in_specs=placed,
        out_specs=(
            P("wt", "ctx", None),
            P("wt", "ctx", None),
            P(None, "wt", None),
            P(None, None, "wt"),
            P(None, "wt", None),
            P(None, None, "wt"),
            P(None, "wt", None),
            P(None, None, "wt"),
            P(None, "wt", None),
            P(None, None, "wt"),
            P(None, "wt", None),
            P(None, None, "wt"),
            P(None, "wt", None),
            P(None, None, "wt"),
        ),
        check_vma=False,
    )
```

```python
import functools
import math

import jax
import jax.numpy as jnp
from jax import lax
from jax.experimental import pallas as pl
from jax.experimental.pallas import tpu as pltpu
from jax.sharding import PartitionSpec as P

EPSILON = 1e-05
LOWEST = -1e30

MESH = pl.DeviceIdType.MESH
GELU_SCALE = 0.7978845608


def dot_nn(left, right):
    return lax.dot_general(
        left, right, (((1,), (0,)), ((), ())), preferred_element_type=jnp.float32
    )


def dot_nt(left, right):
    return lax.dot_general(
        left, right, (((1,), (1,)), ((), ())), preferred_element_type=jnp.float32
    )


def dot_tn(left, right):
    return lax.dot_general(
        left, right, (((0,), (0,)), ((), ())), preferred_element_type=jnp.float32
    )


NORM_ROWS = 32


def norm_rows(values, gain, offset):
    mean = jnp.mean(values, -1, keepdims=True)
    centre = values - mean
    scale_inv = lax.rsqrt(jnp.mean(centre * centre, -1, keepdims=True) + EPSILON)
    normed = centre * scale_inv
    return normed * gain + offset, normed, scale_inv


def mask_fill(bias, seg_win, seg_own, window, tok):
    keys_at = lax.broadcasted_iota(jnp.int32, (tok, tok), 0)
    tokens_at = lax.broadcasted_iota(jnp.int32, (tok, tok), 1)
    own = seg_own[0:1, :].astype(jnp.float32)
    for block in range(window):
        same = seg_win[block].astype(jnp.float32).T[:, 0:1] == own
        if block == window - 1:
            same = same & (keys_at <= tokens_at)
        bias[block * tok : (block + 1) * tok, :] = jnp.where(
            same, 0.0, LOWEST
        ).astype(bias.dtype)


def turned(values):
    return values.astype(jnp.float32).T.astype(jnp.bfloat16)


def pick_kernel(
    index_ref,
    q_a,
    q_b,
    k_a,
    k_b,
    v_a,
    v_b,
    o_a,
    o_b,
    e_a,
    e_b,
    s_a,
    s_b,
    attn_a,
    attn_b,
    out_a,
    out_b,
    exp_a,
    shr_b,
    ext,
    mark,
):
    rank, width = q_a.shape[1:]
    head = k_b.shape[2]
    units = ext.shape[3]
    for table in (attn_a, attn_b):
        table[...] = jnp.zeros_like(table)
    attn_a[0:rank, :] = q_a[0]
    attn_a[rank : 2 * rank, :] = k_a[0]
    attn_a[2 * rank : 3 * rank, :] = v_a[0]
    attn_b[0:rank, 0:width] = q_b[0]
    attn_b[rank : 2 * rank, width : width + head] = k_b[0]
    attn_b[2 * rank : 3 * rank, width + head : width + 2 * head] = v_b[0]
    out_a[0:rank, :] = o_a[0]
    out_b[0:rank, :] = o_b[0]
    exp_a[0:rank, :] = e_a[0]
    shr_b[0:rank, :] = s_b[0]
    for part in range(ext.shape[0]):
        span = slice(part * units, (part + 1) * units)
        ext[part, 0] = e_b[0, :, span]
        ext[part, 1] = s_a[0, :, span]
    lane = lax.broadcasted_iota(jnp.int32, mark.shape, 1)
    mark[...] = jnp.where(lane < 64, 0.0, index_ref[0].astype(jnp.float32))


def pick_call(adapter_index, tables, members):
    adapters, rank, width = tables[0].shape
    head = tables[3].shape[2]
    units = tables[10].shape[2] // members
    bf = jnp.bfloat16
    shapes = [
        ((128, width), bf),
        ((128, width + 2 * head), bf),
        ((rank, width), bf),
        ((rank, width), bf),
        ((rank, width), bf),
        ((rank, width), bf),
        ((members, 2, rank, units), bf),
        ((8, 128), jnp.float32),
    ]
    return pl.pallas_call(
        pick_kernel,
        grid_spec=pltpu.PrefetchScalarGridSpec(
            num_scalar_prefetch=1,
            grid=(1,),
            in_specs=[
                pl.BlockSpec((1,) + table.shape[1:], lambda i, index: (index[0], 0, 0))
                for table in tables
            ],
            out_specs=[
                pl.BlockSpec(shape, lambda i, index, r=len(shape): (0,) * r) for shape, _ in shapes
            ],
        ),
        out_shape=[jax.ShapeDtypeStruct(shape, kind) for shape, kind in shapes],
        name="pick",
    )(adapter_index, *tables)


def core_kernel(
    dims,
    tokens_ref,
    seg_ref,
    gain1,
    bias1,
    gain2,
    bias2,
    attn_a,
    attn_b,
    out_a,
    out_b,
    exp_a,
    shr_b,
    mark,
    grad_hbm,
    ext_hbm,
    qkv_hbm,
    out_hbm,
    exp_hbm,
    ws_hbm,
    kv_win,
    seg_win,
    lse_ref,
    mid_ref,
    low1_ref,
    low_o_ref,
    out_ref,
    dh_ref,
    lows_ref,
    ids_ref,
    ag_b,
    q_out,
    o_out,
    h2_out,
    out_far,
    wq_out,
    wo_out,
    q_ref,
    o_ref,
    h1,
    bias,
    flipped,
    wq,
    wo,
    we,
    land,
    h2_all,
    dy_all,
    lowt_all,
    ext_all,
    sis_send,
    sis_recv,
    own_recv,
    table_ref,
    rs_b,
    low_keep,
    low_send,
    low_recv,
    link_send,
    link_recv,
    pass_send,
    pass_recv,
    shard_send,
    shard_recv,
    kv_send,
    kv_recv,
    seg_send,
    seg_recv,
    side_send,
    side_recv,
    sis_ssem,
    sis_rsem,
    own_ssem,
    own_rsem,
    far_ssem,
    far_rsem,
    low_ssem,
    low_rsem,
    red_ssem,
    red_rsem,
    local_sem,
    spill_sem,
):
    tok, width, units, rows, count, window, heads, head, rank = dims
    bf = jnp.bfloat16
    strip = 512 if window * tok <= 2048 else 256
    me = lax.axis_index("wt")
    ctx = lax.axis_index("ctx")
    core = lax.rem(me, 2)
    side = lax.div(me, 2)
    sister = me + 1 - 2 * core
    across = me + 2 - 4 * side
    diagonal = sister + 2 - 4 * side
    stride = count // 4
    bit_y = lax.rem(ctx, 2)
    bit_z = lax.rem(lax.div(ctx, stride), 2)
    next_y = ctx + 1 - 2 * bit_y
    next_z = ctx + stride - 2 * stride * bit_z
    reach = window - 1
    own_block = window - 1

    def remote(src, dst, send, recv, peer):
        return pltpu.make_async_remote_copy(
            src_ref=src, dst_ref=dst, send_sem=send, recv_sem=recv, device_id=peer,
            device_id_type=MESH,
        )

    my_rows = pl.ds(pl.multiple_of(me * rows, rows), rows)
    quarter = pl.ds(pl.multiple_of(me * units, units), units)
    local = [
        pltpu.make_async_copy(qkv_hbm, wq.at[my_rows], local_sem.at[0]),
        pltpu.make_async_copy(out_hbm, wo.at[my_rows], local_sem.at[1]),
        pltpu.make_async_copy(exp_hbm.at[:, quarter], we.at[my_rows], local_sem.at[2]),
        pltpu.make_async_copy(seg_ref, seg_win.at[own_block], local_sem.at[3]),
        pltpu.make_async_copy(grad_hbm, dy_all.at[pl.ds(0, tok)], local_sem.at[4]),
        pltpu.make_async_copy(ext_hbm.at[me], ext_all.at[0], local_sem.at[5]),
    ]
    for copy in local:
        copy.start()
    for step in range(1, window):

        @pl.when(ctx < step)
        def _(step=step):
            slot = own_block - step
            kv_win[slot * tok : (slot + 1) * tok, :] = jnp.zeros((tok, 2 * head), jnp.bfloat16)
            seg_win[slot] = jnp.full(seg_ref.shape, -1, jnp.int32)

    barrier = pltpu.get_barrier_semaphore()
    for peer in (sister, across, diagonal):
        pl.semaphore_signal(barrier, inc=1, device_id={"wt": peer}, device_id_type=MESH)
    for other in range(count):

        @pl.when(ctx != other)
        def _(other=other):
            pl.semaphore_signal(barrier, inc=1, device_id={"ctx": other}, device_id_type=MESH)

    pl.semaphore_wait(barrier, 3 + count - 1)

    def part_rows(first, flip_y, flip_z, skip, length):
        turn_y = 1 - bit_y if flip_y else bit_y
        turn_z = 1 - bit_z if flip_z else bit_z
        start = first + (turn_y + 2 * turn_z) * (rows // 4) + skip
        return pl.ds(pl.multiple_of(start, 16), length)

    piece = rows // 4
    splits = {0: (80, 32, 16)}
    wide = width // 2
    slim = width // 4
    chunks = [(0, width, 2 * head)]
    chunks += [(0, i * slim, slim) for i in range(4)]
    chunks += [(1, i * wide, wide) for i in range(2)]
    for i in range(2):
        chunks += [(kind, i * (units // 2), units // 2) for kind in (2, 3)]

    def chunk_copies(number):
        kind, start, span = chunks[number]
        cut_x, cut_y, cut_z = (n * piece // 128 for n in splits.get(kind, (0, 64, 64)))
        cols = pl.ds(start, span)
        if kind < 2:
            source = (qkv_hbm, out_hbm)[kind]
            source_cols = cols
        else:
            source = exp_hbm
            target = across if kind == 2 else sister + 2 - 4 * side
            source_cols = pl.ds(pl.multiple_of(target * units + start, 128), span)
        home = (wq, wo, we, land)[kind]
        base = 0 if kind == 3 else across * rows
        home_base = 0 if kind == 3 else me * rows
        full = (False, False)
        sems = lambda way: (link_send.at[number, way], link_recv.at[number, way])

        def from_source(parity, skip, length):
            return (
                source.at[part_rows(0, *parity, skip, length), source_cols],
                home.at[part_rows(home_base, *parity, skip, length), cols],
            )

        def passing(parity, skip, length):
            at = home.at[part_rows(base, *parity, skip, length), cols]
            return (at, at)

        return [
            remote(*from_source(full, 0, piece), *sems(0), {"wt": across}),
            None if cut_x == 0 else
            remote(*from_source((True, True), 0, cut_x), *sems(5), {"wt": across}),
            remote(*passing(full, 0, piece), *sems(1), {"ctx": next_y}),
            remote(*passing(full, 0, piece), *sems(2), {"ctx": next_z}),
            remote(*passing((False, True), cut_x, cut_y), *sems(3), {"ctx": next_y}),
            remote(*passing((True, False), cut_x + cut_y, cut_z), *sems(4), {"ctx": next_z}),
        ]

    def sister_copy(number):
        kind, start, span = chunks[number]
        cols = pl.ds(start, span)
        far_rows = pl.ds(pl.multiple_of(across * rows, rows), rows)
        if kind == 3:
            src, dst = land.at[:, cols], we.at[far_rows, cols]
        else:
            home = (wq, wo)[kind]
            src = home.at[far_rows, cols]
            dst = src
        return remote(src, dst, pass_send.at[number], pass_recv.at[number], {"wt": sister})

    links = [chunk_copies(number) for number in range(len(chunks))]
    forwards = [None if chunks[n][0] == 2 else sister_copy(n) for n in range(len(chunks))]
    sister_quarter = pl.ds(pl.multiple_of(sister * units, units), units)
    own = [
        remote(qkv_hbm, wq.at[my_rows], shard_send.at[0], shard_recv.at[0], {"wt": sister}),
        remote(out_hbm, wo.at[my_rows], shard_send.at[1], shard_recv.at[1], {"wt": sister}),
        remote(
            exp_hbm.at[:, sister_quarter], we.at[my_rows], shard_send.at[2], shard_recv.at[2],
            {"wt": sister},
        ),
    ]

    def arrive(number):
        links[number][0].wait_recv()
        links[number][2].start()
        links[number][3].start()

    def turn(number):
        links[number][2].wait_recv()
        links[number][5].start()
        links[number][3].wait_recv()
        links[number][4].start()

    def finish(number):
        for way in (1, 4, 5):
            if links[number][way] is not None:
                links[number][way].wait_recv()
        if forwards[number] is not None:
            forwards[number].start()

    def ready(number):
        if forwards[number] is not None:
            forwards[number].wait_recv()

    def side_copy(number, src, dst, peer):
        return remote(src, dst, side_send.at[number], side_recv.at[number], {"wt": peer})

    def sent(number):
        for copy in links[number]:
            if copy is not None:
                copy.wait_send()
        if forwards[number] is not None:
            forwards[number].wait_send()

    half = tok // 2

    def far_rows(slot, part):
        return pl.ds(2 * tok + part * tok + (slot - 2) * half, half)

    near = [
        side_copy(0, ext_hbm.at[sister], ext_all.at[1], sister),
        side_copy(1, grad_hbm, dy_all.at[pl.ds(tok, tok)], sister),
    ]
    distant = [
        side_copy(2, ext_hbm.at[across], ext_all.at[2], across),
        side_copy(3, ext_hbm.at[diagonal], ext_all.at[3], diagonal),
    ]
    far_dy = [
        side_copy(
            4 + i, grad_hbm.at[pl.ds(i * half, half)], dy_all.at[far_rows(2, i)], across
        )
        for i in range(2)
    ]
    relay_dy = [
        side_copy(6 + i, dy_all.at[far_rows(2, i)], dy_all.at[far_rows(3, i)], sister)
        for i in range(2)
    ]
    near_h2 = side_copy(8, h2_all.at[pl.ds(0, tok)], h2_all.at[pl.ds(tok, tok)], sister)
    far_h2 = [
        side_copy(
            9 + i, h2_all.at[pl.ds(i * half, half)], h2_all.at[far_rows(2, i)], across
        )
        for i in range(2)
    ]
    relay_h2 = [
        side_copy(11 + i, h2_all.at[far_rows(2, i)], h2_all.at[far_rows(3, i)], sister)
        for i in range(2)
    ]
    send_low = [
        side_copy(12 + slot, lowt_all.at[0], lowt_all.at[slot], peer)
        for slot, peer in ((1, sister), (2, across), (3, diagonal))
    ]

    for number in range(len(chunks)):
        links[number][0].start()
        if links[number][1] is not None:
            links[number][1].start()
        if number == 0:
            own[0].start()
    own[1].start()
    own[2].start()
    for copy in near + distant + far_dy:
        copy.start()

    def seg_copy(step):
        return remote(
            seg_ref, seg_win.at[own_block - step], seg_send.at[step - 1], seg_recv.at[step - 1],
            {"ctx": ctx + step},
        )

    def kv_rows(distance):
        slot = own_block - distance
        return pl.ds(slot * tok if isinstance(slot, int) else pl.multiple_of(slot * tok, tok), tok)

    def kv_copy(held, send, distance, peer):
        return remote(
            kv_win.at[kv_rows(held)],
            kv_win.at[kv_rows(distance)],
            kv_send.at[send],
            kv_recv.at[distance - 1],
            {"ctx": peer},
        )

    place = lax.rem(ctx, stride)

    def kv_pass(level, act):
        if level < 2:

            @pl.when((ctx >= level * stride) & (ctx + stride < count))
            def _():
                far = (level + 1) * stride
                act(kv_copy(level * stride, (level, stride), far, ctx + stride))

        for other in range(stride):
            wanted = (other > place, other != place, other < place)[level]

            @pl.when(wanted & (ctx >= level * stride))
            def _(other=other):
                distance = other - place + level * stride
                act(kv_copy(level * stride, (level, other), distance, ctx - place + other))

    def kv_wait(distance):
        @pl.when(ctx >= distance)
        def _():
            kv_copy(0, (0, 0), distance, ctx).wait_recv()

    def kv_relay(level):
        kv_wait(level * stride)
        kv_pass(level, lambda copy: copy.start())

    def each_sent(make, act):
        for step in range(1, window):

            @pl.when(ctx + step < count)
            def _(step=step):
                act(make(step))

    def each_received(make):
        for step in range(1, window):

            @pl.when(ctx >= step)
            def _(step=step):
                make(step).wait_recv()

    each_sent(seg_copy, lambda copy: copy.start())

    def first_norm(number, carry):
        at = pl.ds(pl.multiple_of(number * NORM_ROWS, NORM_ROWS), NORM_ROWS)
        out, _, _ = norm_rows(tokens_ref[at, :].astype(jnp.float32), gain1[...], bias1[...])
        h1[at, :] = out.astype(jnp.bfloat16)
        return carry

    lax.fori_loop(0, tok // NORM_ROWS, first_norm, 0)
    low1_ref[...] = dot_nt(h1[...], attn_a[...]).astype(jnp.bfloat16)
    local[4].wait()
    lowt_all[0, rank : 2 * rank, :] = dot_nt(shr_b[...], dy_all[0:tok, :]).astype(bf)
    lowt_all[0, 2 * rank : 3 * rank, :] = jnp.broadcast_to(mark[0:1, 64:65], (rank, tok)).astype(
        bf
    )

    arrive(0)
    turn(0)
    arrive(1)
    finish(0)
    local[0].wait()
    own[0].wait_recv()
    ready(0)
    last = pl.ds(width, 2 * head)
    kv_win[own_block * tok : (own_block + 1) * tok, :] = (
        dot_nn(h1[...], wq[:, last]) + dot_nn(low1_ref[...], attn_b[:, last])
    ).astype(jnp.bfloat16)
    kv_pass(0, lambda copy: copy.start())
    turn(1)
    arrive(2)
    finish(1)
    kv_relay(1)
    turn(2)
    arrive(3)
    finish(2)
    kv_relay(2)
    turn(3)
    arrive(4)
    finish(3)
    local[3].wait()
    each_received(seg_copy)
    mask_fill(bias, seg_win, seg_ref, window, tok)
    turn(4)
    arrive(5)
    finish(4)
    for number in range(1, 5):
        ready(number)

    def query_tile(number, carry):
        cols = pl.ds(pl.multiple_of(number * strip, strip), strip)
        q_ref[:, cols] = (
            dot_nn(h1[...], wq[:, cols]) + dot_nn(low1_ref[...], attn_b[:, cols])
        ).astype(jnp.bfloat16)
        return carry

    lax.fori_loop(0, width // strip, query_tile, 0)
    spill_q = pltpu.make_async_copy(wq, wq_out, spill_sem.at[0])
    spill_q.start()
    turn(5)
    arrive(6)
    finish(5)
    for distance in range(1, window):
        if distance % stride:
            kv_wait(distance)
    scale = 1.0 / math.sqrt(head)

    for block in range(window):
        span = slice(block * tok, (block + 1) * tok)
        flipped[:, span] = turned(kv_win[span, head : 2 * head])
    span_q = tok if window * tok <= 2048 else 128

    def one_head(number, carry):
        cols = pl.ds(pl.multiple_of(number * head, head), head)
        for first in range(0, tok, span_q):
            at = slice(first, first + span_q)
            scores = dot_nt(kv_win[:, 0:head], q_ref[at, cols]) * scale + bias[:, at]
            highest = jnp.max(scores, 0, keepdims=True)
            weights = jnp.exp(scores - highest)
            total = jnp.sum(weights, 0, keepdims=True)
            probs = (weights * (1.0 / total)).astype(jnp.bfloat16)
            o_ref[at, cols] = dot_nn(flipped[...], probs).T.astype(jnp.bfloat16)
            lse_ref[number, :, at] = jnp.broadcast_to(highest + jnp.log(total), (8, span_q))
        return carry

    group = heads // 4
    lax.fori_loop(0, group, one_head, 0)
    arrive(7)
    lax.fori_loop(group, 2 * group, one_head, 0)
    turn(6)
    arrive(8)
    lax.fori_loop(2 * group, 3 * group, one_head, 0)
    finish(6)
    arrive(9)
    lax.fori_loop(3 * group, heads, one_head, 0)
    turn(7)
    arrive(10)
    spill_query = pltpu.make_async_copy(q_ref, q_out, spill_sem.at[5])
    spill_query.start()
    local[1].wait()
    own[1].wait_recv()
    ready(5)
    ready(6)
    spill_q.wait()
    for number in range(5):
        sent(number)
    own[0].wait_send()
    ws = wq.at[:, 0:width]
    load_ws = pltpu.make_async_copy(ws_hbm, ws, spill_sem.at[2])
    load_ws.start()
    low_o_ref[...] = dot_nt(o_ref[...], out_a[...]).astype(jnp.bfloat16)

    def out_tile(number, carry):
        cols = pl.ds(pl.multiple_of(number * strip, strip), strip)
        mid_ref[:, cols] = (
            tokens_ref[:, cols].astype(jnp.float32)
            + dot_nn(o_ref[...], wo[:, cols])
            + dot_nn(low_o_ref[...], out_b[:, cols])
        )
        return carry

    lax.fori_loop(0, width // strip, out_tile, 0)
    spill_o = pltpu.make_async_copy(wo, wo_out, spill_sem.at[1])
    spill_o.start()
    spill_mixed = pltpu.make_async_copy(o_ref, o_out, spill_sem.at[6])
    spill_mixed.start()

    def second_norm(number, carry):
        at = pl.ds(pl.multiple_of(number * NORM_ROWS, NORM_ROWS), NORM_ROWS)
        out, _, _ = norm_rows(mid_ref[at, :], gain2[...], bias2[...])
        h2_all[at, :] = out.astype(bf)
        return carry

    spill_mixed.wait()
    for part in range(2):
        steps = half // NORM_ROWS
        lax.fori_loop(part * steps, (part + 1) * steps, second_norm, 0)
        far_h2[part].start()
    near_h2.start()
    lowt_all[0, 0:rank, :] = dot_nt(exp_a[...], h2_all[0:tok, :]).astype(bf)
    for copy in send_low:
        copy.start()
    spill_h2 = pltpu.make_async_copy(h2_all.at[pl.ds(0, tok)], h2_out, spill_sem.at[3])
    spill_h2.start()
    spill_query.wait()
    spill_o.wait()
    for number in (5, 6):
        sent(number)
    own[1].wait_send()

    tile_a = 512 if window * tok <= 2048 else 256
    tile_b = 512
    tiles_a = units // tile_a
    tiles_b = width // tile_b
    act_base = 0
    dup_base = 4 * tok
    units_of_work = [
        (0, 2 * tok, [(0, 0, tok, 0), (1, 0, tok, tok)]),
        (2 * tok, tok, [(2, 0, half, 0), (3, 0, half, half)]),
        (3 * tok, tok, [(2, half, half, 0), (3, half, half, half)]),
    ]

    def low_ready(slot):
        at = slice(slot * tok, (slot + 1) * tok)
        wq[at, width : width + rank] = turned(lowt_all[slot, 0:rank, :])
        wq[at, width + 128 : width + 128 + rank] = turned(lowt_all[slot, rank : 2 * rank, :])

    def forward(work, first, last):
        base, span, parts = units_of_work[work]

        def step(number, carry):
            cols = pl.ds(pl.multiple_of(number * tile_a, tile_a), tile_a)

            def with_low(kind):
                pieces = []
                for slot, skip, size, _ in parts:
                    at = slice(slot * tok + skip, slot * tok + skip + size)
                    small = wq[at, width + kind * 128 : width + kind * 128 + rank]
                    pieces.append(dot_nn(small, ext_all[slot, kind, :, cols]))
                return jnp.concatenate(pieces, 0)

            upward = dot_nn(h2_all[base : base + span, :], we[:, cols]) + with_low(0)
            square = upward * upward
            bend = jnp.tanh(GELU_SCALE * (upward + 0.044715 * (square * upward)))
            active = (0.5 * upward * (1.0 + bend)).astype(bf)
            slope = 0.5 * (1.0 + bend) + 0.5 * upward * (1.0 - bend * bend) * GELU_SCALE * (
                1.0 + 3.0 * 0.044715 * square
            )
            grad = (dot_nt(dy_all[base : base + span, :], wq[cols, 0:width]) + with_low(1)).astype(
                bf
            )
            grad_up = (grad.astype(jnp.float32) * slope).astype(bf)
            wo[act_base + base : act_base + base + span, cols] = active
            wo[dup_base + base : dup_base + base + span, cols] = grad_up
            for slot, skip, size, row in parts:
                for kind, right in enumerate((grad_up, active)):
                    left = lowt_all[slot, kind * rank : (kind + 1) * rank, skip : skip + size]
                    at = pl.ds((2 * slot + kind) * rank, rank)
                    value = dot_nn(left, right[row : row + size])
                    if work == 2:
                        value = value + table_ref[at, cols].astype(jnp.float32)
                    table_ref[at, cols] = value.astype(bf)
            return carry

        lax.fori_loop(first, last, step, 0)

    def low_sums(work):
        base, _, parts = units_of_work[work]
        for slot, skip, size, row in parts:
            at = slice(dup_base + base + row, dup_base + base + row + size)
            grad_low = dot_nt(wo[at, :], ext_all[slot, 0])
            at = slice(act_base + base + row, act_base + base + row + size)
            act_low = dot_nt(wo[at, :], ext_all[slot, 1])
            for start, value in ((0, grad_low), (128, act_low)):
                to = (slice(skip, skip + size), slice(start, start + rank))
                if slot == 0:
                    lows_ref[to] = value
                elif slot == 2:
                    low_keep[to] = value
                else:
                    low_send[(0 if slot == 1 else 1,) + to] = value.astype(bf)

    def back_tile(work, kind, number):
        base, span, _ = units_of_work[work]
        cols = pl.ds(pl.multiple_of(number * tile_b, tile_b), tile_b)
        if kind == 0:
            return dot_nt(wo[dup_base + base : dup_base + base + span, :], we[cols, :])
        return dot_nn(wo[act_base + base : act_base + base + span, :], wq[:, cols])

    def sis_copy(kind, part, number):
        at = (kind, part, number)
        return remote(
            sis_send.at[at], sis_recv.at[at], sis_ssem.at[at], sis_rsem.at[at], {"wt": sister}
        )

    def tile_cols(number):
        return pl.ds(pl.multiple_of(number * tile_b, tile_b), tile_b)

    def own_at(kind, number):
        return (pl.ds(kind * tok, tok), tile_cols(number))

    def far_at(part, number):
        return (pl.ds(part * half, half), tile_cols(number))

    def part_at(number):
        return (pl.ds(pl.multiple_of(lax.rem(number, 2) * half, half), half), pl.ds(0, tile_b))

    def own_copy(kind, number):
        at = (kind, number)
        return remote(
            land.at[own_at(kind, number)], own_recv.at[at], own_ssem.at[at], own_rsem.at[at],
            {"wt": sister},
        )

    def far_copy(part, number):
        at = (part, number)
        return remote(
            q_ref.at[far_at(part, number)], o_ref.at[far_at(part, number)], far_ssem.at[at],
            far_rsem.at[at], {"wt": across},
        )

    def low_copy(number, peer):
        return remote(
            low_send.at[number],
            low_recv.at[number],
            low_ssem.at[number],
            low_rsem.at[number],
            {"wt": peer},
        )

    def join(kind, part, number):
        sis_copy(kind, part, number).wait_recv()
        total = (
            dh_ref[part_at(number)] + sis_recv[kind, part, number].astype(jnp.float32)
        ).astype(bf)
        if kind == 0:
            q_ref[far_at(part, number)] = total
            far_copy(part, number).start()
        else:
            cols = pl.ds(pl.multiple_of(number * tile_b, tile_b), tile_b)
            h1[part * half : (part + 1) * half, cols] = total

    def far_tiles(kind, part):
        def step(number, carry):
            both = back_tile(1 + part, kind, number)
            sis_send[kind, part, number] = both[half:].astype(bf)
            sis_copy(kind, part, number).start()

            @pl.when(number > 0)
            def _():
                join(kind, part, number - 1)

            dh_ref[part_at(number)] = both[:half]
            return carry

        lax.fori_loop(0, tiles_b, step, 0)
        join(kind, part, tiles_b - 1)

    def near_tiles(kind, target):
        def step(number, carry):
            cols = pl.ds(pl.multiple_of(number * tile_b, tile_b), tile_b)
            both = back_tile(0, kind, number)
            target[:, cols] = both[:tok].astype(target.dtype)
            land[own_at(kind, number)] = both[tok:].astype(bf)
            own_copy(kind, number).start()
            return carry

        lax.fori_loop(0, tiles_b, step, 0)

    high_b, wide_b = rs_b.shape[1:]
    lanes_b = min(16, count)

    def piece_b(other):
        return (
            pl.ds(pl.multiple_of(lax.div(other, lanes_b) * high_b, 16), high_b),
            pl.ds(pl.multiple_of(lax.rem(other, lanes_b) * wide_b, 128), wide_b),
        )

    def each_other(act):
        for other in range(count):

            @pl.when(ctx != other)
            def _(other=other):
                act(jnp.int32(other))

    def scatter_copy(other, origin):
        return remote(
            table_ref.at[piece_b(other)], rs_b.at[origin], red_ssem.at[0, other],
            red_rsem.at[0, origin], {"ctx": other},
        )

    def gather_copy(other, origin):
        return remote(
            rs_b.at[origin], ag_b.at[origin], red_ssem.at[1, other], red_rsem.at[1, origin],
            {"ctx": other},
        )

    mine = pltpu.make_async_copy(table_ref.at[piece_b(ctx)], rs_b.at[ctx], local_sem.at[6])
    kept = pltpu.make_async_copy(rs_b.at[ctx], ag_b.at[ctx], local_sem.at[7])
    lows_ref[...] = jnp.zeros_like(lows_ref)
    low_send[...] = jnp.zeros_like(low_send)
    low_ready(0)
    finish(7)
    turn(8)
    finish(8)
    turn(9)
    local[2].wait()
    local[5].wait()
    own[2].wait_recv()
    ready(8)
    load_ws.wait()
    near[0].wait_recv()
    near[1].wait_recv()
    send_low[0].wait_recv()
    low_ready(1)
    near_h2.wait_recv()
    forward(0, 0, tiles_a // 2)
    finish(9)
    turn(10)
    finish(10)
    for index in range(2):
        far_dy[index].wait_recv()
        relay_dy[index].start()
    ready(10)
    forward(0, tiles_a // 2, tiles_a)
    low_sums(0)
    low_own = low_copy(0, sister)
    low_own.start()
    for slot in (2, 3):
        distant[slot - 2].wait_recv()
        send_low[slot - 1].wait_recv()
        low_ready(slot)
    for slot in range(4):
        ids_ref[slot] = lowt_all[slot, 2 * rank : 3 * rank, 0:128].astype(jnp.float32)
    for part in range(2):
        if part == 0:
            for index in range(2):
                far_h2[index].wait_recv()
                relay_h2[index].start()
        relay_dy[part].wait_recv()
        relay_h2[part].wait_recv()
        forward(1 + part, 0, tiles_a)
        if part == 1:
            each_other(lambda other: scatter_copy(other, ctx).start())
            mine.start()
        far_tiles(0, part)
        low_sums(1 + part)
    low_sis = low_copy(1, sister)
    low_sis.start()
    far_tiles(1, 0)
    far_tiles(1, 1)
    spill_far = pltpu.make_async_copy(h1, out_far, spill_sem.at[4])
    spill_far.start()
    mine.wait()
    each_other(lambda other: scatter_copy(ctx, other).wait_recv())
    sums = rs_b[0].astype(jnp.float32)
    for other in range(1, count):
        sums = sums + rs_b[other].astype(jnp.float32)
    rs_b[ctx] = sums.astype(bf)
    each_other(lambda other: gather_copy(other, ctx).start())
    kept.start()
    low_sis.wait_recv()
    for start in (0, 128):
        to = (slice(None), slice(start, start + rank))
        low_send[(2,) + to] = (low_keep[to] + low_recv[(1,) + to].astype(jnp.float32)).astype(bf)
    low_far = low_copy(2, across)
    low_far.start()
    for number in range(7, len(chunks)):
        sent(number)
    near_tiles(0, dh_ref)
    near_tiles(1, out_ref)

    each_other(lambda other: scatter_copy(other, ctx).wait_send())
    each_other(lambda other: gather_copy(other, ctx).wait_send())

    def end_step(number, carry):
        cols = pl.ds(pl.multiple_of(number * tile_b, tile_b), tile_b)
        own_copy(0, number).wait_recv()
        own_copy(1, number).wait_recv()
        for part in range(2):
            at = slice(part * half, (part + 1) * half)
            far_copy(part, number).wait_recv()
            dh_ref[at, cols] = (
                dh_ref[at, cols]
                + own_recv[0, number, at, :].astype(jnp.float32)
                + o_ref[far_at(part, number)].astype(jnp.float32)
            )
        out_ref[:, cols] = (
            out_ref[:, cols].astype(jnp.float32) + own_recv[1, number].astype(jnp.float32)
        ).astype(bf)
        for kind in range(2):
            own_copy(kind, number).wait_send()
            for part in range(2):
                sis_copy(kind, part, number).wait_send()
        for part in range(2):
            far_copy(part, number).wait_send()
        return carry

    lax.fori_loop(0, tiles_b, end_step, 0)
    low_own.wait_recv()
    low_far.wait_recv()
    lows_ref[...] = (
        lows_ref[...] + low_recv[0].astype(jnp.float32) + low_recv[2].astype(jnp.float32)
    )
    own[2].wait_send()
    for copy in near + distant + far_dy + relay_dy + [near_h2] + far_h2 + relay_h2 + send_low:
        copy.wait_send()
    for copy in (low_own, low_sis, low_far):
        copy.wait_send()
    each_sent(seg_copy, lambda copy: copy.wait_send())
    for level in range(3):
        kv_pass(level, lambda copy: copy.wait_send())
    spill_h2.wait()
    spill_far.wait()
    kept.wait()
    each_other(lambda other: gather_copy(ctx, other).wait_recv())


def core_call(tokens, grad_top, segments, vectors, picked, weights, count):
    tok, width = tokens.shape
    qkv_weight, out_weight, expand_weight, shrink_weight = weights
    rows = qkv_weight.shape[0]
    head = (qkv_weight.shape[1] - width) // 2
    heads = width // head
    units = shrink_weight.shape[0]
    window = count // 2 + 1
    bf = jnp.bfloat16
    f32 = jnp.float32
    seg_rows = jnp.broadcast_to(segments[None, :], (8, tok))
    attn_a, attn_b, out_a, out_b, exp_a, shr_b, ext, mark = picked
    rank = ext.shape[2]
    half, tiles = tok // 2, width // 512
    vmem = lambda: pl.BlockSpec(memory_space=pltpu.VMEM)
    hbm = lambda: pl.BlockSpec(memory_space=pl.ANY)
    dma = pltpu.SemaphoreType.DMA
    dims = (tok, width, units, rows, count, window, heads, head, rank)
    shape = jax.ShapeDtypeStruct
    inputs = [
        tokens, seg_rows, *vectors, attn_a, attn_b, out_a, out_b, exp_a, shr_b, mark,
    ]
    outs = [
        shape((window * tok, 2 * head), bf),
        shape((window, 8, tok), jnp.int32),
        shape((heads, 8, tok), f32),
        shape((tok, width), f32),
        shape((tok, 128), bf),
        shape((tok, rank), bf),
        shape((tok, width), bf),
        shape((tok, width), f32),
        shape((tok, 256), f32),
        shape((4, rank, 128), f32),
    ]
    lanes_b = min(16, count)
    sums = (count, 8 * rank * lanes_b // count, units // lanes_b)
    spilled = [
        shape(sums, bf),
        shape((tok, width), bf),
        shape((tok, width), bf),
        shape((tok, width), bf),
        shape((tok, width), bf),
        shape((width, width + 2 * head), bf),
        shape((width, width), bf),
    ]
    return pl.pallas_call(
        functools.partial(core_kernel, dims),
        out_shape=tuple(outs + spilled),
        in_specs=[vmem() for _ in inputs] + [hbm() for _ in range(6)],
        out_specs=tuple([vmem() for _ in outs] + [hbm() for _ in spilled]),
        scratch_shapes=[
            pltpu.VMEM((tok, width), bf),
            pltpu.VMEM((tok, width), bf),
            pltpu.VMEM((tok, width), bf),
            pltpu.VMEM((window * tok, tok), bf),
            pltpu.VMEM((head, window * tok), bf),
            pltpu.VMEM((width, width + 2 * head), bf),
            pltpu.VMEM((width, width), bf),
            pltpu.VMEM((width, units), bf),
            pltpu.VMEM((rows, units), bf),
            pltpu.VMEM((4 * tok, width), bf),
            pltpu.VMEM((4 * tok, width), bf),
            pltpu.VMEM((4, 3 * rank, tok), bf),
            pltpu.VMEM((4, 2, rank, units), bf),
            pltpu.VMEM((2, 2, tiles, half, 512), bf),
            pltpu.VMEM((2, 2, tiles, half, 512), bf),
            pltpu.VMEM((2, tiles, tok, 512), bf),
            pltpu.VMEM((8 * rank, units), bf),
            pltpu.VMEM(sums, bf),
            pltpu.VMEM((tok, 256), f32),
            pltpu.VMEM((3, tok, 256), bf),
            pltpu.VMEM((3, tok, 256), bf),
            dma((11, 6)),
            dma((11, 6)),
            dma((11,)),
            dma((11,)),
            dma((3,)),
            dma((3,)),
            dma((3, count // 4 + 1)),
            dma((window - 1,)),
            dma((window - 1,)),
            dma((window - 1,)),
            dma((16,)),
            dma((16,)),
            dma((2, 2, tiles)),
            dma((2, 2, tiles)),
            dma((2, tiles)),
            dma((2, tiles)),
            dma((2, tiles)),
            dma((2, tiles)),
            dma((3,)),
            dma((3,)),
            dma((2, count)),
            dma((2, count)),
            dma((8,)),
            dma((7,)),
        ],
        compiler_params=pltpu.CompilerParams(
            collective_id=2, has_side_effects=True, vmem_limit_bytes=67043328
        ),
        name="core",
    )(
        *inputs, grad_top, ext, qkv_weight, out_weight, expand_weight, shrink_weight,
    )


def norm_pull(grad_out, gain, normed, scale_inv):
    grad_norm = grad_out * gain
    return scale_inv * (
        grad_norm
        - jnp.mean(grad_norm, -1, keepdims=True)
        - normed * jnp.mean(grad_norm * normed, -1, keepdims=True)
    )


def back_kernel(
    dims,
    tokens_ref,
    grad_ref,
    seg_ref,
    gain1,
    bias1,
    gain2,
    bias2,
    attn_a,
    attn_b,
    out_a,
    out_b,
    exp_a,
    shr_b,
    q_ref,
    kv_win,
    seg_win,
    lse_ref,
    o_ref,
    mid_ref,
    h2_ref,
    low1_ref,
    low_o_ref,
    shrunk_ref,
    dh_ref,
    lows_ref,
    ids_ref,
    wq_hbm,
    wo_hbm,
    out_far,
    layer_ref,
    tgrad_ref,
    ag_a,
    ag_q,
    ag_e,
    wq,
    bias,
    flipped,
    dmid,
    dacc,
    db,
    dout,
    dqkv,
    h1,
    dkv,
    dkv_send,
    dkv_recv,
    share,
    land,
    rs_a,
    share_q,
    land_q,
    rs_q,
    share_e,
    land_e,
    rs_e,
    out_recv,
    out_ssem,
    out_rsem,
    local_sem,
    kv_ssem,
    kv_rsem,
    share_ssem,
    share_rsem,
    red_ssem,
    red_rsem,
):
    tok, width, rank, count, members, window, heads, head = dims
    strip = 512 if window * tok <= 2048 else 256
    me = lax.axis_index("wt")
    ctx = lax.axis_index("ctx")
    core = lax.rem(me, 2)
    side = lax.div(me, 2)
    sister = me + 1 - 2 * core
    across = me + 2 - 4 * side
    diagonal = sister + 2 - 4 * side
    own_block = window - 1
    part = width // members
    bf = jnp.bfloat16

    wo = wq.at[:, 0:width]
    local = [
        pltpu.make_async_copy(wo_hbm, wo, local_sem.at[0]),
        pltpu.make_async_copy(wq_hbm, wq, local_sem.at[1]),
    ]
    local[0].start()

    barrier = pltpu.get_barrier_semaphore()
    for peer in (sister, across, diagonal):
        pl.semaphore_signal(barrier, inc=1, device_id={"wt": peer}, device_id_type=MESH)
    for other in range(count):

        @pl.when(ctx != other)
        def _(other=other):
            pl.semaphore_signal(barrier, inc=1, device_id={"ctx": other}, device_id_type=MESH)

    def remote(src, dst, send, recv, peer):
        return pltpu.make_async_remote_copy(
            src_ref=src, dst_ref=dst, send_sem=send, recv_sem=recv, device_id=peer,
            device_id_type=MESH,
        )

    def each_other(act):
        for other in range(count):

            @pl.when(ctx != other)
            def _(other=other):
                act(other)

    def scatter_copy(lane, table, piece, landing, other):
        return remote(
            table.at[piece(other)],
            landing.at[ctx],
            red_ssem.at[lane, 0, other],
            red_rsem.at[lane, 0, ctx],
            {"ctx": other},
        )

    def scatter_wait(lane, table, piece, landing, other):
        remote(
            table.at[piece(other)],
            landing.at[other],
            red_ssem.at[lane, 0, other],
            red_rsem.at[lane, 0, other],
            {"ctx": other},
        ).wait_recv()

    def gather_copy(lane, result, other):
        return remote(
            result.at[ctx],
            result.at[ctx],
            red_ssem.at[lane, 1, other],
            red_rsem.at[lane, 1, ctx],
            {"ctx": other},
        )

    def gather_wait(lane, result, other):
        remote(
            result.at[other],
            result.at[other],
            red_ssem.at[lane, 1, other],
            red_rsem.at[lane, 1, other],
            {"ctx": other},
        ).wait_recv()

    def scatter_start(lane, table, piece, landing):
        each_other(lambda other: scatter_copy(lane, table, piece, landing, other).start())
        mine = pltpu.make_async_copy(
            table.at[piece(ctx)], landing.at[ctx], local_sem.at[2 + lane]
        )
        mine.start()
        return mine

    def reduce_gather(lane, table, piece, landing, result, mine):
        mine.wait()
        each_other(lambda other: scatter_wait(lane, table, piece, landing, other))
        total = landing[0].astype(jnp.float32)
        for other in range(1, count):
            total = total + landing[other].astype(jnp.float32)
        result[ctx] = total.astype(bf)
        each_other(lambda other: gather_copy(lane, result, other).start())

    def reduce_end(lane, table, piece, landing, result):
        each_other(lambda other: gather_wait(lane, result, other))
        each_other(lambda other: scatter_copy(lane, table, piece, landing, other).wait_send())
        each_other(lambda other: gather_copy(lane, result, other).wait_send())

    high_a, wide_a = rs_a.shape[1:]
    high_e = rs_e.shape[1]

    def quarter_piece(high):
        def piece(other):
            down = lax.div(other, 4) if not isinstance(other, int) else other // 4
            along = lax.rem(other, 4) if not isinstance(other, int) else other % 4
            return (
                pl.ds(pl.multiple_of(down * high, 8), high),
                pl.ds(pl.multiple_of(along * wide_a, 128), wide_a),
            )

        return piece

    piece_a, piece_e = quarter_piece(high_a), quarter_piece(high_e)
    piece_q = quarter_piece(rs_q.shape[1])

    pl.semaphore_wait(barrier, 3 + count - 1)
    out_copy = remote(out_far, out_recv, out_ssem.at[0], out_rsem.at[0], {"wt": across})

    grad_low = lows_ref[:, 0:rank].astype(bf)
    shrink_low = lows_ref[:, 128 : 128 + rank].astype(bf)
    lows_tile = 512

    def low_step(number, carry):
        cols = pl.ds(pl.multiple_of(number * lows_tile, lows_tile), lows_tile)
        dmid[:, cols] = dh_ref[:, cols] + dot_nn(grad_low, exp_a[:, cols])
        return carry

    lax.fori_loop(0, width // lows_tile, low_step, 0)

    def second_pull(number, carry):
        at = pl.ds(pl.multiple_of(number * NORM_ROWS, NORM_ROWS), NORM_ROWS)
        _, normed, scale_inv = norm_rows(mid_ref[at, :], gain2[...], bias2[...])
        value = grad_ref[at, :].astype(jnp.float32) + norm_pull(
            dmid[at, :], gain2[...], normed, scale_inv
        )
        dmid[at, :] = value
        db[at, :] = value.astype(bf)
        return carry

    lax.fori_loop(0, tok // NORM_ROWS, second_pull, 0)
    grad_out_low = dot_nt(db[...], out_b[...]).astype(bf)
    local[0].wait()

    def out_pull(number, carry):
        cols = pl.ds(pl.multiple_of(number * strip, strip), strip)
        dout[:, cols] = (
            dot_nt(db[...], wq[cols, 0:width]) + dot_nn(grad_out_low, out_a[:, cols])
        ).astype(bf)
        return carry

    lax.fori_loop(0, width // strip, out_pull, 0)
    local[1].start()

    def put(table, group, value):
        for other in range(members):
            span = slice(other * part, (other + 1) * part)
            table[other, group * rank : (group + 1) * rank, :] = value[:, span].astype(bf)

    def exchange_of(first, table, landing):
        deep = table.shape[1]
        return [
            remote(
                table.at[peer],
                landing.at[pl.ds(slot * deep, deep)],
                share_ssem.at[first + slot - 1],
                share_rsem.at[first + slot - 1],
                {"wt": peer},
            )
            for slot, peer in ((1, sister), (2, across), (3, diagonal))
        ]

    put(share_e, 0, dot_tn(grad_out_low[:, 0:rank], o_ref[...]))
    put(share_e, 1, dot_tn(low_o_ref[:, 0:rank], db[...]))
    put(share_e, 2, dot_tn(grad_low[:, 0:rank], h2_ref[...]))
    put(share_e, 3, dot_tn(shrink_low[:, 0:rank], grad_ref[...]))
    exchange_e = exchange_of(3, share_e, land_e)
    for copy in exchange_e:
        copy.start()
    mine_share_e = pltpu.make_async_copy(
        share_e.at[me], land_e.at[pl.ds(0, 4 * rank)], local_sem.at[5]
    )
    mine_share_e.start()
    out_copy.start()

    mask_fill(bias, seg_win, seg_ref, window, tok)
    for block in range(window):
        span = slice(block * tok, (block + 1) * tok)
        flipped[:, span] = turned(kv_win[span, 0:head])
    dkv[...] = jnp.zeros_like(dkv)
    scale = 1.0 / math.sqrt(head)
    span_q = tok if window * tok <= 2048 else 128

    def one_head(number, carry):
        cols = pl.ds(pl.multiple_of(number * head, head), head)
        for first in range(0, tok, span_q):
            at = slice(first, first + span_q)
            query = q_ref[at, cols]
            grad = dout[at, cols]
            scores = dot_nt(kv_win[:, 0:head], query) * scale + bias[:, at]
            probs = jnp.exp(scores - lse_ref[number, 0:1, at])
            grad_probs = dot_nt(kv_win[:, head : 2 * head], grad)
            delta = jnp.sum(probs * grad_probs, 0, keepdims=True)
            grad_scores = (probs * (grad_probs - delta)).astype(bf)
            dqkv[at, cols] = (dot_nn(flipped[...], grad_scores).T * scale).astype(bf)
            dkv[:, 0:head] = dkv[:, 0:head] + dot_nn(grad_scores, query)
            dkv[:, head : 2 * head] = dkv[:, head : 2 * head] + dot_nn(probs.astype(bf), grad)
        return carry

    lax.fori_loop(0, heads // 4, one_head, 0)
    mine_share_e.wait()
    for copy in exchange_e:
        copy.wait_recv()
    mine_e = scatter_start(2, land_e, piece_e, rs_e)
    lax.fori_loop(heads // 4, 3 * heads // 4, one_head, 0)
    reduce_gather(2, land_e, piece_e, rs_e, ag_e, mine_e)
    lax.fori_loop(3 * heads // 4, heads, one_head, 0)

    out_copy.wait_recv()

    def layer_step(number, carry):
        cols = pl.ds(pl.multiple_of(number * lows_tile, lows_tile), lows_tile)
        layer_ref[:, cols] = (
            mid_ref[:, cols]
            + shrunk_ref[:, cols].astype(jnp.float32)
            + out_recv[:, cols].astype(jnp.float32)
            + dot_nn(shrink_low, shr_b[:, cols])
        ).astype(bf)
        return carry

    def kv_copy(step):
        return remote(
            dkv_send.at[step - 1],
            dkv_recv.at[step - 1],
            kv_ssem.at[step - 1],
            kv_rsem.at[step - 1],
            {"ctx": ctx - step},
        )

    for step in range(1, window):

        @pl.when(ctx >= step)
        def _(step=step):
            at = slice((own_block - step) * tok, (own_block - step + 1) * tok)
            dkv_send[step - 1, :, 0:head] = (dkv[at, 0:head] * scale).astype(bf)
            dkv_send[step - 1, :, head : 2 * head] = dkv[at, head : 2 * head].astype(bf)
            kv_copy(step).start()

    local[1].wait()

    def first_norm(number, carry):
        at = pl.ds(pl.multiple_of(number * NORM_ROWS, NORM_ROWS), NORM_ROWS)
        out, _, _ = norm_rows(tokens_ref[at, :].astype(jnp.float32), gain1[...], bias1[...])
        h1[at, :] = out.astype(bf)
        return carry

    lax.fori_loop(0, tok // NORM_ROWS, first_norm, 0)
    lax.fori_loop(0, width // lows_tile, layer_step, 0)

    rank_part = dot_nt(dqkv[:, 0:width], attn_b[:, 0:width])
    put(share_q, 0, dot_tn(rank_part[:, 0:rank].astype(bf), h1[...]))
    put(share_q, 1, dot_tn(low1_ref[:, 0:rank], dqkv[:, 0:width]))
    exchange_q = exchange_of(6, share_q, land_q)
    for copy in exchange_q:
        copy.start()
    mine_share_q = pltpu.make_async_copy(
        share_q.at[me], land_q.at[pl.ds(0, 2 * rank)], local_sem.at[4]
    )
    mine_share_q.start()

    def first_half(number, carry):
        cols = pl.ds(pl.multiple_of(number * strip, strip), strip)
        dacc[:, cols] = dot_nt(dqkv[:, 0:width], wq[cols, 0:width])
        return carry

    lax.fori_loop(0, width // strip, first_half, 0)
    mine_share_q.wait()
    for copy in exchange_q:
        copy.wait_recv()
    mine_q = scatter_start(1, land_q, piece_q, rs_q)

    own_at = slice(own_block * tok, (own_block + 1) * tok)
    dkv[own_at, 0:head] = dkv[own_at, 0:head] * scale
    for step in range(1, window):

        @pl.when(ctx + step < count)
        def _(step=step):
            kv_copy(step).wait_recv()
            dkv[own_at, :] = dkv[own_at, :] + dkv_recv[step - 1].astype(jnp.float32)

    last = slice(width, width + 2 * head)
    dqkv[:, last] = dkv[own_at, :].astype(bf)
    grad_rank = (rank_part + dot_nt(dqkv[:, last], attn_b[:, last])).astype(bf)
    first_grads = dot_tn(grad_rank[:, 0 : 3 * rank], h1[...])
    put(share, 0, first_grads[rank : 2 * rank])
    put(share, 1, first_grads[2 * rank : 3 * rank])
    small = dot_tn(low1_ref[...], dqkv[:, last])
    thin = head // members
    tail = slice(2 * rank, 3 * rank)
    share[:, tail, :] = jnp.zeros((members, rank, part), bf)
    for other in range(members):
        span = slice(other * thin, (other + 1) * thin)
        share[other, tail, 0:thin] = small[rank : 2 * rank, span].astype(bf)
        span = slice(head + other * thin, head + (other + 1) * thin)
        share[other, tail, 128 : 128 + thin] = small[2 * rank : 3 * rank, span].astype(bf)

    exchange = exchange_of(0, share, land)
    for copy in exchange:
        copy.start()
    mine_share = pltpu.make_async_copy(
        share.at[me], land.at[pl.ds(0, 3 * rank)], local_sem.at[6]
    )
    mine_share.start()

    def second_half(number, carry):
        cols = pl.ds(pl.multiple_of(number * strip, strip), strip)
        dacc[:, cols] = (
            dacc[:, cols]
            + dot_nt(dqkv[:, last], wq[cols, last])
            + dot_nn(grad_rank, attn_a[:, cols])
        )
        return carry

    lax.fori_loop(0, width // strip, second_half, 0)
    reduce_gather(1, land_q, piece_q, rs_q, ag_q, mine_q)
    mine_share.wait()
    for copy in exchange:
        copy.wait_recv()
    mine_a = scatter_start(0, land, piece_a, rs_a)

    def first_pull(number, carry):
        at = pl.ds(pl.multiple_of(number * NORM_ROWS, NORM_ROWS), NORM_ROWS)
        _, normed, scale_inv = norm_rows(
            tokens_ref[at, :].astype(jnp.float32), gain1[...], bias1[...]
        )
        tgrad_ref[at, :] = (
            dmid[at, :] + norm_pull(dacc[at, :], gain1[...], normed, scale_inv)
        ).astype(bf)
        return carry

    lax.fori_loop(0, tok // NORM_ROWS, first_pull, 0)
    reduce_gather(0, land, piece_a, rs_a, ag_a, mine_a)

    reduce_end(2, land_e, piece_e, rs_e, ag_e)
    reduce_end(1, land_q, piece_q, rs_q, ag_q)
    for copy in exchange_q:
        copy.wait_send()
    reduce_end(0, land, piece_a, rs_a, ag_a)
    for copy in exchange_e:
        copy.wait_send()
    for copy in exchange:
        copy.wait_send()
    out_copy.wait_send()
    for step in range(1, window):

        @pl.when(ctx >= step)
        def _(step=step):
            kv_copy(step).wait_send()


def finish_kernel(
    dims,
    layer_ref,
    tgrad_ref,
    late,
    middle,
    mlp,
    early,
    ids_ref,
    layer_out,
    tgrad_out,
    q_a,
    q_b,
    k_a,
    v_a,
    o_a,
    o_b,
    e_a,
    s_b,
    k_b,
    v_b,
    e_b,
    s_a,
):
    rank, members = dims
    count, high_b, wide_b = mlp.shape
    lanes_b = min(16, count)
    thin = k_b.shape[2]
    wide = late.shape[2]
    own = pl.program_id(0).astype(jnp.float32)
    layer_out[...] = layer_ref[...]
    tgrad_out[...] = tgrad_ref[...]
    hot = [jnp.where(ids_ref[slot, 0:1, 64:65] == own, 1.0, 0.0) for slot in range(members)]

    def mixed(read):
        total = hot[0] * read(0).astype(jnp.float32)
        for slot in range(1, members):
            total = total + hot[slot] * read(slot).astype(jnp.float32)
        return total

    for group, target in ((0, e_b), (1, s_a)):
        for along in range(lanes_b):

            def read(slot, group=group, along=along):
                down, low = divmod((2 * slot + group) * rank, high_b)
                return mlp[down * lanes_b + along, low : low + rank, :]

            target[0, :, along * wide_b : (along + 1) * wide_b] = mixed(read)
    plans = (
        (late, 3, (k_a, v_a)),
        (middle, 2, (q_a, q_b)),
        (early, 4, (o_a, o_b, e_a, s_b)),
    )
    for table, groups, targets in plans:
        high = table.shape[1]
        for group in range(groups):
            for along in range(4):
                for row in range(0, rank, 8):

                    def read(slot, group=group, along=along, row=row, groups=groups, table=table):
                        down, low = divmod((slot * groups + group) * rank + row, high)
                        return table[down * 4 + along, low : low + 8, :]

                    if group < len(targets):
                        targets[group][0, row : row + 8, along * wide : (along + 1) * wide] = (
                            mixed(read)
                        )
                    elif along < 2:
                        (k_b, v_b)[along][0, row : row + 8, :] = mixed(read)[:, 0:thin]


def finish_call(back, mlp, ids, adapters, members, head):
    layer, tgrad, late, middle, early = back
    tok, width = layer.shape
    rank = ids.shape[1]
    part = width // members
    units = mlp.shape[2] * min(16, mlp.shape[0])
    rows = tok // adapters
    f32 = jnp.float32
    whole = lambda array: pl.BlockSpec(array.shape, lambda i: (0,) * array.ndim)
    strip = lambda: pl.BlockSpec((rows, width), lambda i: (i, 0))
    shapes = [(adapters, rank, part)] * 8 + [(adapters, rank, head // members)] * 2
    shapes += [(adapters, rank, units)] * 2
    return pl.pallas_call(
        functools.partial(finish_kernel, (rank, members)),
        grid=(adapters,),
        in_specs=[strip(), strip()]
        + [whole(table) for table in (late, middle, mlp, early, ids)],
        out_specs=[strip(), strip()]
        + [pl.BlockSpec((1,) + shape[1:], lambda i: (i, 0, 0)) for shape in shapes],
        out_shape=[
            jax.ShapeDtypeStruct(layer.shape, layer.dtype),
            jax.ShapeDtypeStruct(tgrad.shape, tgrad.dtype),
        ]
        + [jax.ShapeDtypeStruct(shape, f32) for shape in shapes],
        name="finish",
    )(layer, tgrad, late, middle, mlp, early, ids)


def back_call(tokens, grad_top, segments, vectors, picked, core, count, members):
    tok, width = tokens.shape
    kv_win, seg_win, lse, mid, low1, low_o, shrunk, grad_second, lows = core[:9]
    ids, _, q, o, h2, out_far, wq, wo = core[9:]
    attn_a, attn_b, out_a, out_b, exp_a, shr_b, _, _ = picked
    head = kv_win.shape[1] // 2
    heads = width // head
    rank = ids.shape[1]
    window = count // 2 + 1
    part = width // members
    high_a, wide_a = 3 * rank * members * 4 // count, part // 4
    high_q = 2 * rank * members * 4 // count
    high_e = 4 * rank * members * 4 // count
    bf = jnp.bfloat16
    seg_rows = jnp.broadcast_to(segments[None, :], (8, tok))
    vmem = lambda: pl.BlockSpec(memory_space=pltpu.VMEM)
    hbm = lambda: pl.BlockSpec(memory_space=pl.ANY)
    dma = pltpu.SemaphoreType.DMA
    shape = jax.ShapeDtypeStruct
    dims = (tok, width, rank, count, members, window, heads, head)
    inputs = [
        tokens, grad_top, seg_rows, *vectors, attn_a, attn_b, out_a, out_b, exp_a, shr_b,
        q, kv_win, seg_win, lse, o, mid, h2, low1, low_o, shrunk, grad_second, lows, ids,
    ]
    outs = [shape((tok, width), bf), shape((tok, width), bf)]
    outs += [
        shape((count, high_a, wide_a), bf),
        shape((count, high_q, wide_a), bf),
        shape((count, high_e, wide_a), bf),
    ]
    return pl.pallas_call(
        functools.partial(back_kernel, dims),
        out_shape=tuple(outs),
        in_specs=[vmem() for _ in inputs] + [hbm() for _ in range(3)],
        out_specs=tuple(vmem() for _ in outs),
        scratch_shapes=[
            pltpu.VMEM((width, width + 2 * head), bf),
            pltpu.VMEM((window * tok, tok), jnp.float32 if window * tok <= 2048 else bf),
            pltpu.VMEM((head, window * tok), bf),
            pltpu.VMEM((tok, width), jnp.float32),
            pltpu.VMEM((tok, width), jnp.float32),
            pltpu.VMEM((tok, width), bf),
            pltpu.VMEM((tok, width), bf),
            pltpu.VMEM((tok, width + 2 * head), bf),
            pltpu.VMEM((tok, width), bf),
            pltpu.VMEM((window * tok, 2 * head), jnp.float32),
            pltpu.VMEM((window - 1, tok, 2 * head), bf),
            pltpu.VMEM((window - 1, tok, 2 * head), bf),
            pltpu.VMEM((members, 3 * rank, part), bf),
            pltpu.VMEM((members * 3 * rank, part), bf),
            pltpu.VMEM((count, high_a, wide_a), bf),
            pltpu.VMEM((members, 2 * rank, part), bf),
            pltpu.VMEM((members * 2 * rank, part), bf),
            pltpu.VMEM((count, high_q, wide_a), bf),
            pltpu.VMEM((members, 4 * rank, part), bf),
            pltpu.VMEM((members * 4 * rank, part), bf),
            pltpu.VMEM((count, high_e, wide_a), bf),
            pltpu.VMEM((tok, width), bf),
            dma((1,)),
            dma((1,)),
            dma((7,)),
            dma((window - 1,)),
            dma((window - 1,)),
            dma((9,)),
            dma((9,)),
            dma((3, 2, count)),
            dma((3, 2, count)),
        ],
        compiler_params=pltpu.CompilerParams(
            collective_id=3, has_side_effects=True, vmem_limit_bytes=63 * 1024 * 1024
        ),
        name="back",
    )(*inputs, wq, wo, out_far)


def body(
    tokens,
    out_grad,
    segments,
    adapter_index,
    first_gain,
    first_bias,
    second_gain,
    second_bias,
    qkv_weight,
    out_weight,
    expand_weight,
    shrink_weight,
    query_first,
    query_second,
    key_first,
    key_second,
    value_first,
    value_second,
    output_first,
    output_second,
    expand_first,
    expand_second,
    shrink_first,
    shrink_second,
):
    count = lax.axis_size("ctx")
    members = lax.axis_size("wt")
    rank = query_second.shape[1]
    flip = lambda table: table.transpose(0, 2, 1)
    row = lambda vector: vector[None, :]
    tables = [
        flip(query_first),
        query_second,
        flip(key_first),
        key_second,
        flip(value_first),
        value_second,
        flip(output_first),
        output_second,
        flip(expand_first),
        expand_second,
        flip(shrink_first),
        shrink_second,
    ]
    picked = pick_call(adapter_index, tables, members)
    vectors = [row(first_gain), row(first_bias), row(second_gain), row(second_bias)]
    weights = (qkv_weight, out_weight, expand_weight, shrink_weight)
    core = core_call(tokens[0], out_grad[0], segments[0], vectors, picked, weights, count)
    back = back_call(
        tokens[0], out_grad[0], segments[0], vectors, picked, core, count, members
    )
    results = finish_call(
        back, core[10], core[9], query_first.shape[0], members, key_second.shape[2]
    )
    layer_out, tokens_grad = results[0][None], results[1][None]
    q_a, q_b, k_a, v_a, o_a, o_b, e_a, s_b, k_b, v_b, e_b, s_a = results[2:]
    return (
        layer_out,
        tokens_grad,
        flip(q_a),
        q_b,
        flip(k_a),
        k_b,
        flip(v_a),
        v_b,
        flip(o_a),
        o_b,
        flip(e_a),
        e_b,
        flip(s_a),
        s_b,
    )


def solution(mesh):
    placed = (
        P("wt", "ctx", None),
        P("wt", "ctx", None),
        P("wt", "ctx"),
        P("wt"),
        P(),
        P(),
        P(),
        P(),
        P("wt", None),
        P("wt", None),
        P("wt", None),
        P("wt", None),
        P(),
        P(),
        P(),
        P(),
        P(),
        P(),
        P(),
        P(),
        P(),
        P(),
        P(),
        P(),
    )
    return jax.shard_map(
        body,
        mesh=mesh,
        in_specs=placed,
        out_specs=(
            P("wt", "ctx", None),
            P("wt", "ctx", None),
            P(None, "wt", None),
            P(None, None, "wt"),
            P(None, "wt", None),
            P(None, None, "wt"),
            P(None, "wt", None),
            P(None, None, "wt"),
            P(None, "wt", None),
            P(None, None, "wt"),
            P(None, "wt", None),
            P(None, None, "wt"),
            P(None, "wt", None),
            P(None, None, "wt"),
        ),
        check_vma=False,
    )
```

```python
import functools
import math

import jax
import jax.numpy as jnp
from jax import lax
from jax.experimental import pallas as pl
from jax.experimental.pallas import tpu as pltpu
from jax.sharding import PartitionSpec as P

EPSILON = 1e-05
LOWEST = -1e30

MESH = pl.DeviceIdType.MESH
GELU_SCALE = 0.7978845608


def dot_nn(left, right):
    return lax.dot_general(
        left, right, (((1,), (0,)), ((), ())), preferred_element_type=jnp.float32
    )


def dot_nt(left, right):
    return lax.dot_general(
        left, right, (((1,), (1,)), ((), ())), preferred_element_type=jnp.float32
    )


def dot_tn(left, right):
    return lax.dot_general(
        left, right, (((0,), (0,)), ((), ())), preferred_element_type=jnp.float32
    )


NORM_ROWS = 32


def norm_rows(values, gain, offset):
    mean = jnp.mean(values, -1, keepdims=True)
    centre = values - mean
    scale_inv = lax.rsqrt(jnp.mean(centre * centre, -1, keepdims=True) + EPSILON)
    normed = centre * scale_inv
    return normed * gain + offset, normed, scale_inv


def mask_fill(bias, seg_win, seg_own, window, tok):
    keys_at = lax.broadcasted_iota(jnp.int32, (tok, tok), 0)
    tokens_at = lax.broadcasted_iota(jnp.int32, (tok, tok), 1)
    own = seg_own[0:1, :].astype(jnp.float32)
    for block in range(window):
        same = seg_win[block].astype(jnp.float32).T[:, 0:1] == own
        if block == window - 1:
            same = same & (keys_at <= tokens_at)
        bias[block * tok : (block + 1) * tok, :] = jnp.where(
            same, 0.0, LOWEST
        ).astype(bias.dtype)


def turned(values):
    return values.astype(jnp.float32).T.astype(jnp.bfloat16)


def pick_kernel(
    index_ref,
    q_a,
    q_b,
    k_a,
    k_b,
    v_a,
    v_b,
    o_a,
    o_b,
    e_a,
    e_b,
    s_a,
    s_b,
    attn_a,
    attn_b,
    out_a,
    out_b,
    exp_a,
    shr_b,
    ext,
    mark,
):
    rank, width = q_a.shape[1:]
    head = k_b.shape[2]
    units = ext.shape[3]
    for table in (attn_a, attn_b):
        table[...] = jnp.zeros_like(table)
    attn_a[0:rank, :] = q_a[0]
    attn_a[rank : 2 * rank, :] = k_a[0]
    attn_a[2 * rank : 3 * rank, :] = v_a[0]
    attn_b[0:rank, 0:width] = q_b[0]
    attn_b[rank : 2 * rank, width : width + head] = k_b[0]
    attn_b[2 * rank : 3 * rank, width + head : width + 2 * head] = v_b[0]
    out_a[0:rank, :] = o_a[0]
    out_b[0:rank, :] = o_b[0]
    exp_a[0:rank, :] = e_a[0]
    shr_b[0:rank, :] = s_b[0]
    for part in range(ext.shape[0]):
        span = slice(part * units, (part + 1) * units)
        ext[part, 0] = e_b[0, :, span]
        ext[part, 1] = s_a[0, :, span]
    lane = lax.broadcasted_iota(jnp.int32, mark.shape, 1)
    mark[...] = jnp.where(lane < 64, 0.0, index_ref[0].astype(jnp.float32))


def pick_call(adapter_index, tables, members):
    adapters, rank, width = tables[0].shape
    head = tables[3].shape[2]
    units = tables[10].shape[2] // members
    bf = jnp.bfloat16
    shapes = [
        ((128, width), bf),
        ((128, width + 2 * head), bf),
        ((rank, width), bf),
        ((rank, width), bf),
        ((rank, width), bf),
        ((rank, width), bf),
        ((members, 2, rank, units), bf),
        ((8, 128), jnp.float32),
    ]
    return pl.pallas_call(
        pick_kernel,
        grid_spec=pltpu.PrefetchScalarGridSpec(
            num_scalar_prefetch=1,
            grid=(1,),
            in_specs=[
                pl.BlockSpec((1,) + table.shape[1:], lambda i, index: (index[0], 0, 0))
                for table in tables
            ],
            out_specs=[
                pl.BlockSpec(shape, lambda i, index, r=len(shape): (0,) * r) for shape, _ in shapes
            ],
        ),
        out_shape=[jax.ShapeDtypeStruct(shape, kind) for shape, kind in shapes],
        name="pick",
    )(adapter_index, *tables)


def core_kernel(
    dims,
    tokens_ref,
    seg_ref,
    gain1,
    bias1,
    gain2,
    bias2,
    attn_a,
    attn_b,
    out_a,
    out_b,
    exp_a,
    shr_b,
    mark,
    grad_hbm,
    ext_hbm,
    qkv_hbm,
    out_hbm,
    exp_hbm,
    ws_hbm,
    kv_win,
    seg_win,
    lse_ref,
    mid_ref,
    low1_ref,
    low_o_ref,
    out_ref,
    dh_ref,
    lows_ref,
    ids_ref,
    ag_b,
    q_out,
    o_out,
    h2_out,
    out_far,
    wq_out,
    wo_out,
    q_ref,
    o_ref,
    h1,
    bias,
    flipped,
    wq,
    wo,
    we,
    land,
    h2_all,
    dy_all,
    lowt_all,
    ext_all,
    sis_send,
    sis_recv,
    own_recv,
    table_ref,
    rs_b,
    low_keep,
    low_send,
    low_recv,
    link_send,
    link_recv,
    pass_send,
    pass_recv,
    shard_send,
    shard_recv,
    kv_send,
    kv_recv,
    seg_send,
    seg_recv,
    side_send,
    side_recv,
    sis_ssem,
    sis_rsem,
    own_ssem,
    own_rsem,
    far_ssem,
    far_rsem,
    low_ssem,
    low_rsem,
    red_ssem,
    red_rsem,
    local_sem,
    spill_sem,
):
    tok, width, units, rows, count, window, heads, head, rank = dims
    bf = jnp.bfloat16
    strip = 512 if window * tok <= 2048 else 256
    me = lax.axis_index("wt")
    ctx = lax.axis_index("ctx")
    core = lax.rem(me, 2)
    side = lax.div(me, 2)
    sister = me + 1 - 2 * core
    across = me + 2 - 4 * side
    diagonal = sister + 2 - 4 * side
    stride = count // 4
    bit_y = lax.rem(ctx, 2)
    bit_z = lax.rem(lax.div(ctx, stride), 2)
    next_y = ctx + 1 - 2 * bit_y
    next_z = ctx + stride - 2 * stride * bit_z
    reach = window - 1
    own_block = window - 1

    def remote(src, dst, send, recv, peer):
        return pltpu.make_async_remote_copy(
            src_ref=src, dst_ref=dst, send_sem=send, recv_sem=recv, device_id=peer,
            device_id_type=MESH,
        )

    my_rows = pl.ds(pl.multiple_of(me * rows, rows), rows)
    quarter = pl.ds(pl.multiple_of(me * units, units), units)
    local = [
        pltpu.make_async_copy(qkv_hbm, wq.at[my_rows], local_sem.at[0]),
        pltpu.make_async_copy(out_hbm, wo.at[my_rows], local_sem.at[1]),
        pltpu.make_async_copy(exp_hbm.at[:, quarter], we.at[my_rows], local_sem.at[2]),
        pltpu.make_async_copy(seg_ref, seg_win.at[own_block], local_sem.at[3]),
        pltpu.make_async_copy(grad_hbm, dy_all.at[pl.ds(0, tok)], local_sem.at[4]),
        pltpu.make_async_copy(ext_hbm.at[me], ext_all.at[0], local_sem.at[5]),
    ]
    for copy in local:
        copy.start()
    for step in range(1, window):

        @pl.when(ctx < step)
        def _(step=step):
            slot = own_block - step
            kv_win[slot * tok : (slot + 1) * tok, :] = jnp.zeros((tok, 2 * head), jnp.bfloat16)
            seg_win[slot] = jnp.full(seg_ref.shape, -1, jnp.int32)

    barrier = pltpu.get_barrier_semaphore()
    for peer in (sister, across, diagonal):
        pl.semaphore_signal(barrier, inc=1, device_id={"wt": peer}, device_id_type=MESH)
    for other in range(count):

        @pl.when(ctx != other)
        def _(other=other):
            pl.semaphore_signal(barrier, inc=1, device_id={"ctx": other}, device_id_type=MESH)

    pl.semaphore_wait(barrier, 3 + count - 1)

    def part_rows(first, flip_y, flip_z, skip, length):
        turn_y = 1 - bit_y if flip_y else bit_y
        turn_z = 1 - bit_z if flip_z else bit_z
        start = first + (turn_y + 2 * turn_z) * (rows // 4) + skip
        return pl.ds(pl.multiple_of(start, 16), length)

    piece = rows // 4
    splits = {0: (80, 32, 16)}
    wide = width // 2
    slim = width // 4
    chunks = [(0, width, 2 * head)]
    chunks += [(0, i * slim, slim) for i in range(4)]
    chunks += [(1, i * wide, wide) for i in range(2)]
    for i in range(2):
        chunks += [(kind, i * (units // 2), units // 2) for kind in (2, 3)]

    def chunk_copies(number):
        kind, start, span = chunks[number]
        cut_x, cut_y, cut_z = (n * piece // 128 for n in splits.get(kind, (0, 64, 64)))
        cols = pl.ds(start, span)
        if kind < 2:
            source = (qkv_hbm, out_hbm)[kind]
            source_cols = cols
        else:
            source = exp_hbm
            target = across if kind == 2 else sister + 2 - 4 * side
            source_cols = pl.ds(pl.multiple_of(target * units + start, 128), span)
        home = (wq, wo, we, land)[kind]
        base = 0 if kind == 3 else across * rows
        home_base = 0 if kind == 3 else me * rows
        full = (False, False)
        sems = lambda way: (link_send.at[number, way], link_recv.at[number, way])

        def from_source(parity, skip, length):
            return (
                source.at[part_rows(0, *parity, skip, length), source_cols],
                home.at[part_rows(home_base, *parity, skip, length), cols],
            )

        def passing(parity, skip, length):
            at = home.at[part_rows(base, *parity, skip, length), cols]
            return (at, at)

        return [
            remote(*from_source(full, 0, piece), *sems(0), {"wt": across}),
            None if cut_x == 0 else
            remote(*from_source((True, True), 0, cut_x), *sems(5), {"wt": across}),
            remote(*passing(full, 0, piece), *sems(1), {"ctx": next_y}),
            remote(*passing(full, 0, piece), *sems(2), {"ctx": next_z}),
            remote(*passing((False, True), cut_x, cut_y), *sems(3), {"ctx": next_y}),
            remote(*passing((True, False), cut_x + cut_y, cut_z), *sems(4), {"ctx": next_z}),
        ]

    def sister_copy(number):
        kind, start, span = chunks[number]
        cols = pl.ds(start, span)
        far_rows = pl.ds(pl.multiple_of(across * rows, rows), rows)
        if kind == 3:
            src, dst = land.at[:, cols], we.at[far_rows, cols]
        else:
            home = (wq, wo)[kind]
            src = home.at[far_rows, cols]
            dst = src
        return remote(src, dst, pass_send.at[number], pass_recv.at[number], {"wt": sister})

    links = [chunk_copies(number) for number in range(len(chunks))]
    forwards = [None if chunks[n][0] == 2 else sister_copy(n) for n in range(len(chunks))]
    sister_quarter = pl.ds(pl.multiple_of(sister * units, units), units)
    own = [
        remote(qkv_hbm, wq.at[my_rows], shard_send.at[0], shard_recv.at[0], {"wt": sister}),
        remote(out_hbm, wo.at[my_rows], shard_send.at[1], shard_recv.at[1], {"wt": sister}),
        remote(
            exp_hbm.at[:, sister_quarter], we.at[my_rows], shard_send.at[2], shard_recv.at[2],
            {"wt": sister},
        ),
    ]

    def arrive(number):
        links[number][0].wait_recv()
        links[number][2].start()
        links[number][3].start()

    def turn(number):
        links[number][2].wait_recv()
        links[number][5].start()
        links[number][3].wait_recv()
        links[number][4].start()

    def finish(number):
        for way in (1, 4, 5):
            if links[number][way] is not None:
                links[number][way].wait_recv()
        if forwards[number] is not None:
            forwards[number].start()

    def ready(number):
        if forwards[number] is not None:
            forwards[number].wait_recv()

    def side_copy(number, src, dst, peer):
        return remote(src, dst, side_send.at[number], side_recv.at[number], {"wt": peer})

    def sent(number):
        for copy in links[number]:
            if copy is not None:
                copy.wait_send()
        if forwards[number] is not None:
            forwards[number].wait_send()

    half = tok // 2

    def far_rows(slot, part):
        return pl.ds(2 * tok + part * tok + (slot - 2) * half, half)

    near = [
        side_copy(0, ext_hbm.at[sister], ext_all.at[1], sister),
        side_copy(1, grad_hbm, dy_all.at[pl.ds(tok, tok)], sister),
    ]
    distant = [
        side_copy(2, ext_hbm.at[across], ext_all.at[2], across),
        side_copy(3, ext_hbm.at[diagonal], ext_all.at[3], diagonal),
    ]
    far_dy = [
        side_copy(
            4 + i, grad_hbm.at[pl.ds(i * half, half)], dy_all.at[far_rows(2, i)], across
        )
        for i in range(2)
    ]
    relay_dy = [
        side_copy(6 + i, dy_all.at[far_rows(2, i)], dy_all.at[far_rows(3, i)], sister)
        for i in range(2)
    ]
    near_h2 = side_copy(8, h2_all.at[pl.ds(0, tok)], h2_all.at[pl.ds(tok, tok)], sister)
    far_h2 = [
        side_copy(
            9 + i, h2_all.at[pl.ds(i * half, half)], h2_all.at[far_rows(2, i)], across
        )
        for i in range(2)
    ]
    relay_h2 = [
        side_copy(11 + i, h2_all.at[far_rows(2, i)], h2_all.at[far_rows(3, i)], sister)
        for i in range(2)
    ]
    send_low = [
        side_copy(12 + slot, lowt_all.at[0], lowt_all.at[slot], peer)
        for slot, peer in ((1, sister), (2, across), (3, diagonal))
    ]

    for number in range(len(chunks)):
        links[number][0].start()
        if links[number][1] is not None:
            links[number][1].start()
        if number == 0:
            own[0].start()
    own[1].start()
    own[2].start()
    for copy in near + distant + far_dy:
        copy.start()

    def seg_copy(step):
        return remote(
            seg_ref, seg_win.at[own_block - step], seg_send.at[step - 1], seg_recv.at[step - 1],
            {"ctx": ctx + step},
        )

    def kv_rows(distance):
        slot = own_block - distance
        return pl.ds(slot * tok if isinstance(slot, int) else pl.multiple_of(slot * tok, tok), tok)

    def kv_copy(held, send, distance, peer):
        return remote(
            kv_win.at[kv_rows(held)],
            kv_win.at[kv_rows(distance)],
            kv_send.at[send],
            kv_recv.at[distance - 1],
            {"ctx": peer},
        )

    place = lax.rem(ctx, stride)

    def kv_pass(level, act):
        if level < 2:

            @pl.when((ctx >= level * stride) & (ctx + stride < count))
            def _():
                far = (level + 1) * stride
                act(kv_copy(level * stride, (level, stride), far, ctx + stride))

        for other in range(stride):
            wanted = (other > place, other != place, other < place)[level]

            @pl.when(wanted & (ctx >= level * stride))
            def _(other=other):
                distance = other - place + level * stride
                act(kv_copy(level * stride, (level, other), distance, ctx - place + other))

    def kv_wait(distance):
        @pl.when(ctx >= distance)
        def _():
            kv_copy(0, (0, 0), distance, ctx).wait_recv()

    def kv_relay(level):
        kv_wait(level * stride)
        kv_pass(level, lambda copy: copy.start())

    def each_sent(make, act):
        for step in range(1, window):

            @pl.when(ctx + step < count)
            def _(step=step):
                act(make(step))

    def each_received(make):
        for step in range(1, window):

            @pl.when(ctx >= step)
            def _(step=step):
                make(step).wait_recv()

    each_sent(seg_copy, lambda copy: copy.start())

    def first_norm(number, carry):
        at = pl.ds(pl.multiple_of(number * NORM_ROWS, NORM_ROWS), NORM_ROWS)
        out, _, _ = norm_rows(tokens_ref[at, :].astype(jnp.float32), gain1[...], bias1[...])
        h1[at, :] = out.astype(jnp.bfloat16)
        return carry

    lax.fori_loop(0, tok // NORM_ROWS, first_norm, 0)
    low1_ref[...] = dot_nt(h1[...], attn_a[...]).astype(jnp.bfloat16)
    local[4].wait()
    lowt_all[0, rank : 2 * rank, :] = dot_nt(shr_b[...], dy_all[0:tok, :]).astype(bf)
    lowt_all[0, 2 * rank : 3 * rank, :] = jnp.broadcast_to(mark[0:1, 64:65], (rank, tok)).astype(
        bf
    )

    arrive(0)
    turn(0)
    arrive(1)
    finish(0)
    local[0].wait()
    own[0].wait_recv()
    ready(0)
    last = pl.ds(width, 2 * head)
    kv_win[own_block * tok : (own_block + 1) * tok, :] = (
        dot_nn(h1[...], wq[:, last]) + dot_nn(low1_ref[...], attn_b[:, last])
    ).astype(jnp.bfloat16)
    kv_pass(0, lambda copy: copy.start())
    turn(1)
    arrive(2)
    finish(1)
    kv_relay(1)
    turn(2)
    arrive(3)
    finish(2)
    kv_relay(2)
    turn(3)
    arrive(4)
    finish(3)
    local[3].wait()
    each_received(seg_copy)
    mask_fill(bias, seg_win, seg_ref, window, tok)
    turn(4)
    arrive(5)
    finish(4)
    for number in range(1, 5):
        ready(number)

    def query_tile(number, carry):
        cols = pl.ds(pl.multiple_of(number * strip, strip), strip)
        q_ref[:, cols] = (
            dot_nn(h1[...], wq[:, cols]) + dot_nn(low1_ref[...], attn_b[:, cols])
        ).astype(jnp.bfloat16)
        return carry

    lax.fori_loop(0, width // strip, query_tile, 0)
    spill_q = pltpu.make_async_copy(wq, wq_out, spill_sem.at[0])
    spill_q.start()
    turn(5)
    arrive(6)
    finish(5)
    for distance in range(1, window):
        if distance % stride:
            kv_wait(distance)
    scale = 1.0 / math.sqrt(head)

    for block in range(window):
        span = slice(block * tok, (block + 1) * tok)
        flipped[:, span] = turned(kv_win[span, head : 2 * head])
    span_q = tok if window * tok <= 2048 else 128

    def one_head(number, carry):
        cols = pl.ds(pl.multiple_of(number * head, head), head)
        for first in range(0, tok, span_q):
            at = slice(first, first + span_q)
            scores = dot_nt(kv_win[:, 0:head], q_ref[at, cols]) * scale + bias[:, at]
            highest = jnp.max(scores, 0, keepdims=True)
            weights = jnp.exp(scores - highest)
            total = jnp.sum(weights, 0, keepdims=True)
            probs = (weights * (1.0 / total)).astype(jnp.bfloat16)
            o_ref[at, cols] = dot_nn(flipped[...], probs).T.astype(jnp.bfloat16)
            lse_ref[number, :, at] = jnp.broadcast_to(highest + jnp.log(total), (8, span_q))
        return carry

    group = heads // 4
    lax.fori_loop(0, group, one_head, 0)
    arrive(7)
    lax.fori_loop(group, 2 * group, one_head, 0)
    turn(6)
    arrive(8)
    lax.fori_loop(2 * group, 3 * group, one_head, 0)
    finish(6)
    arrive(9)
    lax.fori_loop(3 * group, heads, one_head, 0)
    turn(7)
    arrive(10)
    spill_query = pltpu.make_async_copy(q_ref, q_out, spill_sem.at[5])
    spill_query.start()
    local[1].wait()
    own[1].wait_recv()
    ready(5)
    ready(6)
    spill_q.wait()
    for number in range(5):
        sent(number)
    own[0].wait_send()
    ws = wq.at[:, 0:width]
    load_ws = pltpu.make_async_copy(ws_hbm, ws, spill_sem.at[2])
    load_ws.start()
    low_o_ref[...] = dot_nt(o_ref[...], out_a[...]).astype(jnp.bfloat16)

    def out_tile(number, carry):
        cols = pl.ds(pl.multiple_of(number * strip, strip), strip)
        mid_ref[:, cols] = (
            tokens_ref[:, cols].astype(jnp.float32)
            + dot_nn(o_ref[...], wo[:, cols])
            + dot_nn(low_o_ref[...], out_b[:, cols])
        )
        return carry

    lax.fori_loop(0, width // strip, out_tile, 0)
    spill_o = pltpu.make_async_copy(wo, wo_out, spill_sem.at[1])
    spill_o.start()
    spill_mixed = pltpu.make_async_copy(o_ref, o_out, spill_sem.at[6])
    spill_mixed.start()

    def second_norm(number, carry):
        at = pl.ds(pl.multiple_of(number * NORM_ROWS, NORM_ROWS), NORM_ROWS)
        out, _, _ = norm_rows(mid_ref[at, :], gain2[...], bias2[...])
        h2_all[at, :] = out.astype(bf)
        return carry

    spill_mixed.wait()
    for part in range(2):
        steps = half // NORM_ROWS
        lax.fori_loop(part * steps, (part + 1) * steps, second_norm, 0)
        far_h2[part].start()
    near_h2.start()
    lowt_all[0, 0:rank, :] = dot_nt(exp_a[...], h2_all[0:tok, :]).astype(bf)
    for copy in send_low:
        copy.start()
    spill_h2 = pltpu.make_async_copy(h2_all.at[pl.ds(0, tok)], h2_out, spill_sem.at[3])
    spill_h2.start()
    spill_query.wait()
    spill_o.wait()
    for number in (5, 6):
        sent(number)
    own[1].wait_send()

    tile_a = 512 if window * tok <= 2048 else 256
    tile_b = 512
    tiles_a = units // tile_a
    tiles_b = width // tile_b
    act_base = 0
    dup_base = 4 * tok
    units_of_work = [
        (0, 2 * tok, [(0, 0, tok, 0), (1, 0, tok, tok)]),
        (2 * tok, tok, [(2, 0, half, 0), (3, 0, half, half)]),
        (3 * tok, tok, [(2, half, half, 0), (3, half, half, half)]),
    ]

    def low_ready(slot):
        at = slice(slot * tok, (slot + 1) * tok)
        wq[at, width : width + rank] = turned(lowt_all[slot, 0:rank, :])
        wq[at, width + 128 : width + 128 + rank] = turned(lowt_all[slot, rank : 2 * rank, :])

    def forward(work, first, last):
        base, span, parts = units_of_work[work]

        def step(number, carry):
            cols = pl.ds(pl.multiple_of(number * tile_a, tile_a), tile_a)

            def with_low(kind):
                pieces = []
                for slot, skip, size, _ in parts:
                    at = slice(slot * tok + skip, slot * tok + skip + size)
                    small = wq[at, width + kind * 128 : width + kind * 128 + rank]
                    pieces.append(dot_nn(small, ext_all[slot, kind, :, cols]))
                return jnp.concatenate(pieces, 0)

            upward = dot_nn(h2_all[base : base + span, :], we[:, cols]) + with_low(0)
            square = upward * upward
            bend = jnp.tanh(GELU_SCALE * (upward + 0.044715 * (square * upward)))
            active = (0.5 * upward * (1.0 + bend)).astype(bf)
            slope = 0.5 * (1.0 + bend) + 0.5 * upward * (1.0 - bend * bend) * GELU_SCALE * (
                1.0 + 3.0 * 0.044715 * square
            )
            grad = (dot_nt(dy_all[base : base + span, :], wq[cols, 0:width]) + with_low(1)).astype(
                bf
            )
            grad_up = (grad.astype(jnp.float32) * slope).astype(bf)
            wo[act_base + base : act_base + base + span, cols] = active
            wo[dup_base + base : dup_base + base + span, cols] = grad_up
            for slot, skip, size, row in parts:
                for kind, right in enumerate((grad_up, active)):
                    left = lowt_all[slot, kind * rank : (kind + 1) * rank, skip : skip + size]
                    at = pl.ds((2 * slot + kind) * rank, rank)
                    value = dot_nn(left, right[row : row + size])
                    if work == 2:
                        value = value + table_ref[at, cols].astype(jnp.float32)
                    table_ref[at, cols] = value.astype(bf)
            return carry

        lax.fori_loop(first, last, step, 0)

    def low_sums(work):
        base, _, parts = units_of_work[work]
        for slot, skip, size, row in parts:
            at = slice(dup_base + base + row, dup_base + base + row + size)
            grad_low = dot_nt(wo[at, :], ext_all[slot, 0])
            at = slice(act_base + base + row, act_base + base + row + size)
            act_low = dot_nt(wo[at, :], ext_all[slot, 1])
            for start, value in ((0, grad_low), (128, act_low)):
                to = (slice(skip, skip + size), slice(start, start + rank))
                if slot == 0:
                    lows_ref[to] = value
                elif slot == 2:
                    low_keep[to] = value
                else:
                    low_send[(0 if slot == 1 else 1,) + to] = value.astype(bf)

    def back_tile(work, kind, number):
        base, span, _ = units_of_work[work]
        cols = pl.ds(pl.multiple_of(number * tile_b, tile_b), tile_b)
        if kind == 0:
            return dot_nt(wo[dup_base + base : dup_base + base + span, :], we[cols, :])
        return dot_nn(wo[act_base + base : act_base + base + span, :], wq[:, cols])

    def sis_copy(kind, part, number):
        at = (kind, part, number)
        return remote(
            sis_send.at[at], sis_recv.at[at], sis_ssem.at[at], sis_rsem.at[at], {"wt": sister}
        )

    def tile_cols(number):
        return pl.ds(pl.multiple_of(number * tile_b, tile_b), tile_b)

    def own_at(kind, number):
        return (pl.ds(kind * tok, tok), tile_cols(number))

    def far_at(part, number):
        return (pl.ds(part * half, half), tile_cols(number))

    def part_at(number):
        return (pl.ds(pl.multiple_of(lax.rem(number, 2) * half, half), half), pl.ds(0, tile_b))

    def own_copy(kind, number):
        at = (kind, number)
        return remote(
            land.at[own_at(kind, number)], own_recv.at[at], own_ssem.at[at], own_rsem.at[at],
            {"wt": sister},
        )

    def far_copy(part, number):
        at = (part, number)
        return remote(
            q_ref.at[far_at(part, number)], o_ref.at[far_at(part, number)], far_ssem.at[at],
            far_rsem.at[at], {"wt": across},
        )

    def low_copy(number, peer):
        return remote(
            low_send.at[number],
            low_recv.at[number],
            low_ssem.at[number],
            low_rsem.at[number],
            {"wt": peer},
        )

    def join(kind, part, number):
        sis_copy(kind, part, number).wait_recv()
        total = (
            dh_ref[part_at(number)] + sis_recv[kind, part, number].astype(jnp.float32)
        ).astype(bf)
        if kind == 0:
            q_ref[far_at(part, number)] = total
            far_copy(part, number).start()
        else:
            cols = pl.ds(pl.multiple_of(number * tile_b, tile_b), tile_b)
            h1[part * half : (part + 1) * half, cols] = total

    def far_tiles(kind, part):
        def step(number, carry):
            both = back_tile(1 + part, kind, number)
            sis_send[kind, part, number] = both[half:].astype(bf)
            sis_copy(kind, part, number).start()

            @pl.when(number > 0)
            def _():
                join(kind, part, number - 1)

            dh_ref[part_at(number)] = both[:half]
            return carry

        lax.fori_loop(0, tiles_b, step, 0)
        join(kind, part, tiles_b - 1)

    def near_tiles(kind, target):
        def step(number, carry):
            cols = pl.ds(pl.multiple_of(number * tile_b, tile_b), tile_b)
            both = back_tile(0, kind, number)
            target[:, cols] = both[:tok].astype(target.dtype)
            land[own_at(kind, number)] = both[tok:].astype(bf)
            own_copy(kind, number).start()
            return carry

        lax.fori_loop(0, tiles_b, step, 0)

    high_b, wide_b = rs_b.shape[1:]
    lanes_b = min(16, count)

    def piece_b(other):
        return (
            pl.ds(pl.multiple_of(lax.div(other, lanes_b) * high_b, 16), high_b),
            pl.ds(pl.multiple_of(lax.rem(other, lanes_b) * wide_b, 128), wide_b),
        )

    def each_other(act):
        for other in range(count):

            @pl.when(ctx != other)
            def _(other=other):
                act(jnp.int32(other))

    def scatter_copy(other, origin):
        return remote(
            table_ref.at[piece_b(other)], rs_b.at[origin], red_ssem.at[0, other],
            red_rsem.at[0, origin], {"ctx": other},
        )

    def gather_copy(other, origin):
        return remote(
            rs_b.at[origin], ag_b.at[origin], red_ssem.at[1, other], red_rsem.at[1, origin],
            {"ctx": other},
        )

    mine = pltpu.make_async_copy(table_ref.at[piece_b(ctx)], rs_b.at[ctx], local_sem.at[6])
    kept = pltpu.make_async_copy(rs_b.at[ctx], ag_b.at[ctx], local_sem.at[7])
    lows_ref[...] = jnp.zeros_like(lows_ref)
    low_send[...] = jnp.zeros_like(low_send)
    low_ready(0)
    finish(7)
    turn(8)
    finish(8)
    turn(9)
    local[2].wait()
    local[5].wait()
    own[2].wait_recv()
    ready(8)
    load_ws.wait()
    near[0].wait_recv()
    near[1].wait_recv()
    send_low[0].wait_recv()
    low_ready(1)
    near_h2.wait_recv()
    forward(0, 0, tiles_a // 2)
    finish(9)
    turn(10)
    finish(10)
    for index in range(2):
        far_dy[index].wait_recv()
        relay_dy[index].start()
    ready(10)
    forward(0, tiles_a // 2, tiles_a)
    low_sums(0)
    low_own = low_copy(0, sister)
    low_own.start()
    for slot in (2, 3):
        distant[slot - 2].wait_recv()
        send_low[slot - 1].wait_recv()
        low_ready(slot)
    for slot in range(4):
        ids_ref[slot] = lowt_all[slot, 2 * rank : 3 * rank, 0:128].astype(jnp.float32)
    for part in range(2):
        if part == 0:
            for index in range(2):
                far_h2[index].wait_recv()
                relay_h2[index].start()
        relay_dy[part].wait_recv()
        relay_h2[part].wait_recv()
        forward(1 + part, 0, tiles_a)
        if part == 1:
            each_other(lambda other: scatter_copy(other, ctx).start())
            mine.start()
        far_tiles(0, part)
        low_sums(1 + part)
    low_sis = low_copy(1, sister)
    low_sis.start()
    far_tiles(1, 0)
    far_tiles(1, 1)
    spill_far = pltpu.make_async_copy(h1, out_far, spill_sem.at[4])
    spill_far.start()
    mine.wait()
    each_other(lambda other: scatter_copy(ctx, other).wait_recv())
    sums = rs_b[0].astype(jnp.float32)
    for other in range(1, count):
        sums = sums + rs_b[other].astype(jnp.float32)
    rs_b[ctx] = sums.astype(bf)
    each_other(lambda other: gather_copy(other, ctx).start())
    kept.start()
    low_sis.wait_recv()
    for start in (0, 128):
        to = (slice(None), slice(start, start + rank))
        low_send[(2,) + to] = (low_keep[to] + low_recv[(1,) + to].astype(jnp.float32)).astype(bf)
    low_far = low_copy(2, across)
    low_far.start()
    for number in range(7, len(chunks)):
        sent(number)
    near_tiles(0, dh_ref)
    near_tiles(1, out_ref)

    each_other(lambda other: scatter_copy(other, ctx).wait_send())
    each_other(lambda other: gather_copy(other, ctx).wait_send())

    def end_step(number, carry):
        cols = pl.ds(pl.multiple_of(number * tile_b, tile_b), tile_b)
        own_copy(0, number).wait_recv()
        own_copy(1, number).wait_recv()
        for part in range(2):
            at = slice(part * half, (part + 1) * half)
            far_copy(part, number).wait_recv()
            dh_ref[at, cols] = (
                dh_ref[at, cols]
                + own_recv[0, number, at, :].astype(jnp.float32)
                + o_ref[far_at(part, number)].astype(jnp.float32)
            )
        out_ref[:, cols] = (
            out_ref[:, cols].astype(jnp.float32) + own_recv[1, number].astype(jnp.float32)
        ).astype(bf)
        for kind in range(2):
            own_copy(kind, number).wait_send()
            for part in range(2):
                sis_copy(kind, part, number).wait_send()
        for part in range(2):
            far_copy(part, number).wait_send()
        return carry

    lax.fori_loop(0, tiles_b, end_step, 0)
    low_own.wait_recv()
    low_far.wait_recv()
    lows_ref[...] = (
        lows_ref[...] + low_recv[0].astype(jnp.float32) + low_recv[2].astype(jnp.float32)
    )
    own[2].wait_send()
    for copy in near + distant + far_dy + relay_dy + [near_h2] + far_h2 + relay_h2 + send_low:
        copy.wait_send()
    for copy in (low_own, low_sis, low_far):
        copy.wait_send()
    each_sent(seg_copy, lambda copy: copy.wait_send())
    for level in range(3):
        kv_pass(level, lambda copy: copy.wait_send())
    spill_h2.wait()
    spill_far.wait()
    kept.wait()
    each_other(lambda other: gather_copy(ctx, other).wait_recv())


def core_call(tokens, grad_top, segments, vectors, picked, weights, count):
    tok, width = tokens.shape
    qkv_weight, out_weight, expand_weight, shrink_weight = weights
    rows = qkv_weight.shape[0]
    head = (qkv_weight.shape[1] - width) // 2
    heads = width // head
    units = shrink_weight.shape[0]
    window = count // 2 + 1
    bf = jnp.bfloat16
    f32 = jnp.float32
    seg_rows = jnp.broadcast_to(segments[None, :], (8, tok))
    attn_a, attn_b, out_a, out_b, exp_a, shr_b, ext, mark = picked
    rank = ext.shape[2]
    half, tiles = tok // 2, width // 512
    vmem = lambda: pl.BlockSpec(memory_space=pltpu.VMEM)
    hbm = lambda: pl.BlockSpec(memory_space=pl.ANY)
    dma = pltpu.SemaphoreType.DMA
    dims = (tok, width, units, rows, count, window, heads, head, rank)
    shape = jax.ShapeDtypeStruct
    inputs = [
        tokens, seg_rows, *vectors, attn_a, attn_b, out_a, out_b, exp_a, shr_b, mark,
    ]
    outs = [
        shape((window * tok, 2 * head), bf),
        shape((window, 8, tok), jnp.int32),
        shape((heads, 8, tok), f32),
        shape((tok, width), f32),
        shape((tok, 128), bf),
        shape((tok, rank), bf),
        shape((tok, width), bf),
        shape((tok, width), f32),
        shape((tok, 256), f32),
        shape((4, rank, 128), f32),
    ]
    lanes_b = min(16, count)
    sums = (count, 8 * rank * lanes_b // count, units // lanes_b)
    spilled = [
        shape(sums, bf),
        shape((tok, width), bf),
        shape((tok, width), bf),
        shape((tok, width), bf),
        shape((tok, width), bf),
        shape((width, width + 2 * head), bf),
        shape((width, width), bf),
    ]
    return pl.pallas_call(
        functools.partial(core_kernel, dims),
        out_shape=tuple(outs + spilled),
        in_specs=[vmem() for _ in inputs] + [hbm() for _ in range(6)],
        out_specs=tuple([vmem() for _ in outs] + [hbm() for _ in spilled]),
        scratch_shapes=[
            pltpu.VMEM((tok, width), bf),
            pltpu.VMEM((tok, width), bf),
            pltpu.VMEM((tok, width), bf),
            pltpu.VMEM((window * tok, tok), bf),
            pltpu.VMEM((head, window * tok), bf),
            pltpu.VMEM((width, width + 2 * head), bf),
            pltpu.VMEM((width, width), bf),
            pltpu.VMEM((width, units), bf),
            pltpu.VMEM((rows, units), bf),
            pltpu.VMEM((4 * tok, width), bf),
            pltpu.VMEM((4 * tok, width), bf),
            pltpu.VMEM((4, 3 * rank, tok), bf),
            pltpu.VMEM((4, 2, rank, units), bf),
            pltpu.VMEM((2, 2, tiles, half, 512), bf),
            pltpu.VMEM((2, 2, tiles, half, 512), bf),
            pltpu.VMEM((2, tiles, tok, 512), bf),
            pltpu.VMEM((8 * rank, units), bf),
            pltpu.VMEM(sums, bf),
            pltpu.VMEM((tok, 256), f32),
            pltpu.VMEM((3, tok, 256), bf),
            pltpu.VMEM((3, tok, 256), bf),
            dma((11, 6)),
            dma((11, 6)),
            dma((11,)),
            dma((11,)),
            dma((3,)),
            dma((3,)),
            dma((3, count // 4 + 1)),
            dma((window - 1,)),
            dma((window - 1,)),
            dma((window - 1,)),
            dma((16,)),
            dma((16,)),
            dma((2, 2, tiles)),
            dma((2, 2, tiles)),
            dma((2, tiles)),
            dma((2, tiles)),
            dma((2, tiles)),
            dma((2, tiles)),
            dma((3,)),
            dma((3,)),
            dma((2, count)),
            dma((2, count)),
            dma((8,)),
            dma((7,)),
        ],
        compiler_params=pltpu.CompilerParams(
            collective_id=2, has_side_effects=True, vmem_limit_bytes=67043328
        ),
        name="core",
    )(
        *inputs, grad_top, ext, qkv_weight, out_weight, expand_weight, shrink_weight,
    )


def norm_pull(grad_out, gain, normed, scale_inv):
    grad_norm = grad_out * gain
    return scale_inv * (
        grad_norm
        - jnp.mean(grad_norm, -1, keepdims=True)
        - normed * jnp.mean(grad_norm * normed, -1, keepdims=True)
    )


def back_kernel(
    dims,
    tokens_ref,
    grad_ref,
    seg_ref,
    gain1,
    bias1,
    gain2,
    bias2,
    attn_a,
    attn_b,
    out_a,
    out_b,
    exp_a,
    shr_b,
    q_ref,
    kv_win,
    seg_win,
    lse_ref,
    o_ref,
    mid_ref,
    h2_ref,
    low1_ref,
    low_o_ref,
    shrunk_ref,
    dh_ref,
    lows_ref,
    ids_ref,
    wq_hbm,
    wo_hbm,
    out_far,
    layer_ref,
    tgrad_ref,
    ag_a,
    ag_q,
    ag_e,
    wq,
    bias,
    flipped,
    dmid,
    dacc,
    db,
    dout,
    dqkv,
    h1,
    dkv,
    dkv_send,
    dkv_recv,
    share,
    land,
    rs_a,
    share_q,
    land_q,
    rs_q,
    share_e,
    land_e,
    rs_e,
    out_recv,
    out_ssem,
    out_rsem,
    local_sem,
    kv_ssem,
    kv_rsem,
    share_ssem,
    share_rsem,
    red_ssem,
    red_rsem,
):
    tok, width, rank, count, members, window, heads, head = dims
    strip = 512 if window * tok <= 2048 else 256
    me = lax.axis_index("wt")
    ctx = lax.axis_index("ctx")
    core = lax.rem(me, 2)
    side = lax.div(me, 2)
    sister = me + 1 - 2 * core
    across = me + 2 - 4 * side
    diagonal = sister + 2 - 4 * side
    own_block = window - 1
    part = width // members
    bf = jnp.bfloat16

    wo = wq.at[:, 0:width]
    local = [
        pltpu.make_async_copy(wo_hbm, wo, local_sem.at[0]),
        pltpu.make_async_copy(wq_hbm, wq, local_sem.at[1]),
    ]
    local[0].start()

    barrier = pltpu.get_barrier_semaphore()
    for peer in (sister, across, diagonal):
        pl.semaphore_signal(barrier, inc=1, device_id={"wt": peer}, device_id_type=MESH)
    for other in range(count):

        @pl.when(ctx != other)
        def _(other=other):
            pl.semaphore_signal(barrier, inc=1, device_id={"ctx": other}, device_id_type=MESH)

    def remote(src, dst, send, recv, peer):
        return pltpu.make_async_remote_copy(
            src_ref=src, dst_ref=dst, send_sem=send, recv_sem=recv, device_id=peer,
            device_id_type=MESH,
        )

    def each_other(act):
        for other in range(count):

            @pl.when(ctx != other)
            def _(other=other):
                act(other)

    def scatter_copy(lane, table, piece, landing, other):
        return remote(
            table.at[piece(other)],
            landing.at[ctx],
            red_ssem.at[lane, 0, other],
            red_rsem.at[lane, 0, ctx],
            {"ctx": other},
        )

    def scatter_wait(lane, table, piece, landing, other):
        remote(
            table.at[piece(other)],
            landing.at[other],
            red_ssem.at[lane, 0, other],
            red_rsem.at[lane, 0, other],
            {"ctx": other},
        ).wait_recv()

    def gather_copy(lane, result, other):
        return remote(
            result.at[ctx],
            result.at[ctx],
            red_ssem.at[lane, 1, other],
            red_rsem.at[lane, 1, ctx],
            {"ctx": other},
        )

    def gather_wait(lane, result, other):
        remote(
            result.at[other],
            result.at[other],
            red_ssem.at[lane, 1, other],
            red_rsem.at[lane, 1, other],
            {"ctx": other},
        ).wait_recv()

    def scatter_start(lane, table, piece, landing):
        each_other(lambda other: scatter_copy(lane, table, piece, landing, other).start())
        mine = pltpu.make_async_copy(
            table.at[piece(ctx)], landing.at[ctx], local_sem.at[2 + lane]
        )
        mine.start()
        return mine

    def reduce_gather(lane, table, piece, landing, result, mine):
        mine.wait()
        each_other(lambda other: scatter_wait(lane, table, piece, landing, other))
        total = landing[0].astype(jnp.float32)
        for other in range(1, count):
            total = total + landing[other].astype(jnp.float32)
        result[ctx] = total.astype(bf)
        each_other(lambda other: gather_copy(lane, result, other).start())

    def reduce_end(lane, table, piece, landing, result):
        each_other(lambda other: gather_wait(lane, result, other))
        each_other(lambda other: scatter_copy(lane, table, piece, landing, other).wait_send())
        each_other(lambda other: gather_copy(lane, result, other).wait_send())

    high_a, wide_a = rs_a.shape[1:]
    high_e = rs_e.shape[1]

    def quarter_piece(high):
        def piece(other):
            down = lax.div(other, 4) if not isinstance(other, int) else other // 4
            along = lax.rem(other, 4) if not isinstance(other, int) else other % 4
            return (
                pl.ds(pl.multiple_of(down * high, 8), high),
                pl.ds(pl.multiple_of(along * wide_a, 128), wide_a),
            )

        return piece

    piece_a, piece_e = quarter_piece(high_a), quarter_piece(high_e)
    piece_q = quarter_piece(rs_q.shape[1])

    pl.semaphore_wait(barrier, 3 + count - 1)
    out_copy = remote(out_far, out_recv, out_ssem.at[0], out_rsem.at[0], {"wt": across})

    grad_low = lows_ref[:, 0:rank].astype(bf)
    shrink_low = lows_ref[:, 128 : 128 + rank].astype(bf)
    lows_tile = 512

    def low_step(number, carry):
        cols = pl.ds(pl.multiple_of(number * lows_tile, lows_tile), lows_tile)
        dmid[:, cols] = dh_ref[:, cols] + dot_nn(grad_low, exp_a[:, cols])
        return carry

    lax.fori_loop(0, width // lows_tile, low_step, 0)

    def second_pull(number, carry):
        at = pl.ds(pl.multiple_of(number * NORM_ROWS, NORM_ROWS), NORM_ROWS)
        _, normed, scale_inv = norm_rows(mid_ref[at, :], gain2[...], bias2[...])
        value = grad_ref[at, :].astype(jnp.float32) + norm_pull(
            dmid[at, :], gain2[...], normed, scale_inv
        )
        dmid[at, :] = value
        db[at, :] = value.astype(bf)
        return carry

    lax.fori_loop(0, tok // NORM_ROWS, second_pull, 0)
    grad_out_low = dot_nt(db[...], out_b[...]).astype(bf)
    local[0].wait()

    def out_pull(number, carry):
        cols = pl.ds(pl.multiple_of(number * strip, strip), strip)
        dout[:, cols] = (
            dot_nt(db[...], wq[cols, 0:width]) + dot_nn(grad_out_low, out_a[:, cols])
        ).astype(bf)
        return carry

    lax.fori_loop(0, width // strip, out_pull, 0)
    local[1].start()

    def put(table, group, value):
        for other in range(members):
            span = slice(other * part, (other + 1) * part)
            table[other, group * rank : (group + 1) * rank, :] = value[:, span].astype(bf)

    def exchange_of(first, table, landing):
        deep = table.shape[1]
        return [
            remote(
                table.at[peer],
                landing.at[pl.ds(slot * deep, deep)],
                share_ssem.at[first + slot - 1],
                share_rsem.at[first + slot - 1],
                {"wt": peer},
            )
            for slot, peer in ((1, sister), (2, across), (3, diagonal))
        ]

    put(share_e, 0, dot_tn(grad_out_low[:, 0:rank], o_ref[...]))
    put(share_e, 1, dot_tn(low_o_ref[:, 0:rank], db[...]))
    put(share_e, 2, dot_tn(grad_low[:, 0:rank], h2_ref[...]))
    put(share_e, 3, dot_tn(shrink_low[:, 0:rank], grad_ref[...]))
    exchange_e = exchange_of(3, share_e, land_e)
    for copy in exchange_e:
        copy.start()
    mine_share_e = pltpu.make_async_copy(
        share_e.at[me], land_e.at[pl.ds(0, 4 * rank)], local_sem.at[5]
    )
    mine_share_e.start()
    out_copy.start()

    mask_fill(bias, seg_win, seg_ref, window, tok)
    for block in range(window):
        span = slice(block * tok, (block + 1) * tok)
        flipped[:, span] = turned(kv_win[span, 0:head])
    dkv[...] = jnp.zeros_like(dkv)
    scale = 1.0 / math.sqrt(head)
    span_q = tok if window * tok <= 2048 else 128

    pack = 2 if window * tok <= 2048 else 1

    def one_head(number, carry):
        for first in range(0, tok, span_q):
            at = slice(first, first + span_q)
            queries, grads, changes, masses = [], [], [], []
            for own in range(pack):
                head_at = number * pack + own
                cols = pl.ds(pl.multiple_of(head_at * head, head), head)
                query = q_ref[at, cols]
                grad = dout[at, cols]
                scores = dot_nt(kv_win[:, 0:head], query) * scale + bias[:, at]
                probs = jnp.exp(scores - lse_ref[head_at, 0:1, at])
                grad_probs = dot_nt(kv_win[:, head : 2 * head], grad)
                delta = jnp.sum(probs * grad_probs, 0, keepdims=True)
                grad_scores = (probs * (grad_probs - delta)).astype(bf)
                dqkv[at, cols] = (dot_nn(flipped[...], grad_scores).T * scale).astype(bf)
                queries.append(query)
                grads.append(grad)
                changes.append(grad_scores)
                masses.append(probs.astype(bf))
            joined = lambda parts, axis: parts[0] if pack == 1 else jnp.concatenate(parts, axis)
            dkv[:, 0:head] = dkv[:, 0:head] + dot_nn(joined(changes, 1), joined(queries, 0))
            dkv[:, head : 2 * head] = dkv[:, head : 2 * head] + dot_nn(
                joined(masses, 1), joined(grads, 0)
            )
        return carry

    turns = heads // pack
    lax.fori_loop(0, turns // 4, one_head, 0)
    mine_share_e.wait()
    for copy in exchange_e:
        copy.wait_recv()
    mine_e = scatter_start(2, land_e, piece_e, rs_e)
    lax.fori_loop(turns // 4, 3 * turns // 4, one_head, 0)
    reduce_gather(2, land_e, piece_e, rs_e, ag_e, mine_e)
    lax.fori_loop(3 * turns // 4, turns, one_head, 0)

    out_copy.wait_recv()

    def layer_step(number, carry):
        cols = pl.ds(pl.multiple_of(number * lows_tile, lows_tile), lows_tile)
        layer_ref[:, cols] = (
            mid_ref[:, cols]
            + shrunk_ref[:, cols].astype(jnp.float32)
            + out_recv[:, cols].astype(jnp.float32)
            + dot_nn(shrink_low, shr_b[:, cols])
        ).astype(bf)
        return carry

    def kv_copy(step):
        return remote(
            dkv_send.at[step - 1],
            dkv_recv.at[step - 1],
            kv_ssem.at[step - 1],
            kv_rsem.at[step - 1],
            {"ctx": ctx - step},
        )

    for step in range(1, window):

        @pl.when(ctx >= step)
        def _(step=step):
            at = slice((own_block - step) * tok, (own_block - step + 1) * tok)
            dkv_send[step - 1, :, 0:head] = (dkv[at, 0:head] * scale).astype(bf)
            dkv_send[step - 1, :, head : 2 * head] = dkv[at, head : 2 * head].astype(bf)
            kv_copy(step).start()

    local[1].wait()

    def first_norm(number, carry):
        at = pl.ds(pl.multiple_of(number * NORM_ROWS, NORM_ROWS), NORM_ROWS)
        out, _, _ = norm_rows(tokens_ref[at, :].astype(jnp.float32), gain1[...], bias1[...])
        h1[at, :] = out.astype(bf)
        return carry

    lax.fori_loop(0, tok // NORM_ROWS, first_norm, 0)
    lax.fori_loop(0, width // lows_tile, layer_step, 0)

    rank_part = dot_nt(dqkv[:, 0:width], attn_b[:, 0:width])
    put(share_q, 0, dot_tn(rank_part[:, 0:rank].astype(bf), h1[...]))
    put(share_q, 1, dot_tn(low1_ref[:, 0:rank], dqkv[:, 0:width]))
    exchange_q = exchange_of(6, share_q, land_q)
    for copy in exchange_q:
        copy.start()
    mine_share_q = pltpu.make_async_copy(
        share_q.at[me], land_q.at[pl.ds(0, 2 * rank)], local_sem.at[4]
    )
    mine_share_q.start()

    def first_half(number, carry):
        cols = pl.ds(pl.multiple_of(number * strip, strip), strip)
        dacc[:, cols] = dot_nt(dqkv[:, 0:width], wq[cols, 0:width])
        return carry

    lax.fori_loop(0, width // strip, first_half, 0)
    mine_share_q.wait()
    for copy in exchange_q:
        copy.wait_recv()
    mine_q = scatter_start(1, land_q, piece_q, rs_q)

    own_at = slice(own_block * tok, (own_block + 1) * tok)
    dkv[own_at, 0:head] = dkv[own_at, 0:head] * scale
    for step in range(1, window):

        @pl.when(ctx + step < count)
        def _(step=step):
            kv_copy(step).wait_recv()
            dkv[own_at, :] = dkv[own_at, :] + dkv_recv[step - 1].astype(jnp.float32)

    last = slice(width, width + 2 * head)
    dqkv[:, last] = dkv[own_at, :].astype(bf)
    grad_rank = (rank_part + dot_nt(dqkv[:, last], attn_b[:, last])).astype(bf)
    first_grads = dot_tn(grad_rank[:, 0 : 3 * rank], h1[...])
    put(share, 0, first_grads[rank : 2 * rank])
    put(share, 1, first_grads[2 * rank : 3 * rank])
    small = dot_tn(low1_ref[...], dqkv[:, last])
    thin = head // members
    tail = slice(2 * rank, 3 * rank)
    share[:, tail, :] = jnp.zeros((members, rank, part), bf)
    for other in range(members):
        span = slice(other * thin, (other + 1) * thin)
        share[other, tail, 0:thin] = small[rank : 2 * rank, span].astype(bf)
        span = slice(head + other * thin, head + (other + 1) * thin)
        share[other, tail, 128 : 128 + thin] = small[2 * rank : 3 * rank, span].astype(bf)

    exchange = exchange_of(0, share, land)
    for copy in exchange:
        copy.start()
    mine_share = pltpu.make_async_copy(
        share.at[me], land.at[pl.ds(0, 3 * rank)], local_sem.at[6]
    )
    mine_share.start()

    def second_half(number, carry):
        cols = pl.ds(pl.multiple_of(number * strip, strip), strip)
        dacc[:, cols] = (
            dacc[:, cols]
            + dot_nt(dqkv[:, last], wq[cols, last])
            + dot_nn(grad_rank, attn_a[:, cols])
        )
        return carry

    lax.fori_loop(0, width // strip, second_half, 0)
    reduce_gather(1, land_q, piece_q, rs_q, ag_q, mine_q)
    mine_share.wait()
    for copy in exchange:
        copy.wait_recv()
    mine_a = scatter_start(0, land, piece_a, rs_a)

    def first_pull(number, carry):
        at = pl.ds(pl.multiple_of(number * NORM_ROWS, NORM_ROWS), NORM_ROWS)
        _, normed, scale_inv = norm_rows(
            tokens_ref[at, :].astype(jnp.float32), gain1[...], bias1[...]
        )
        tgrad_ref[at, :] = (
            dmid[at, :] + norm_pull(dacc[at, :], gain1[...], normed, scale_inv)
        ).astype(bf)
        return carry

    lax.fori_loop(0, tok // NORM_ROWS, first_pull, 0)
    reduce_gather(0, land, piece_a, rs_a, ag_a, mine_a)

    reduce_end(2, land_e, piece_e, rs_e, ag_e)
    reduce_end(1, land_q, piece_q, rs_q, ag_q)
    for copy in exchange_q:
        copy.wait_send()
    reduce_end(0, land, piece_a, rs_a, ag_a)
    for copy in exchange_e:
        copy.wait_send()
    for copy in exchange:
        copy.wait_send()
    out_copy.wait_send()
    for step in range(1, window):

        @pl.when(ctx >= step)
        def _(step=step):
            kv_copy(step).wait_send()


def finish_kernel(
    dims,
    layer_ref,
    tgrad_ref,
    late,
    middle,
    mlp,
    early,
    ids_ref,
    layer_out,
    tgrad_out,
    q_a,
    q_b,
    k_a,
    v_a,
    o_a,
    o_b,
    e_a,
    s_b,
    k_b,
    v_b,
    e_b,
    s_a,
):
    rank, members = dims
    count, high_b, wide_b = mlp.shape
    lanes_b = min(16, count)
    thin = k_b.shape[2]
    wide = late.shape[2]
    batch = q_a.shape[0]
    first = pl.program_id(0) * batch
    layer_out[...] = layer_ref[...]
    tgrad_out[...] = tgrad_ref[...]
    hot = [
        [
            jnp.where(
                ids_ref[slot, 0:1, 64:65] == (first + own).astype(jnp.float32), 1.0, 0.0
            )
            for slot in range(members)
        ]
        for own in range(batch)
    ]

    def mixed(read, store):
        values = [read(slot).astype(jnp.float32) for slot in range(members)]
        for own in range(batch):
            total = hot[own][0] * values[0]
            for slot in range(1, members):
                total = total + hot[own][slot] * values[slot]
            store(own, total)

    for group, target in ((0, e_b), (1, s_a)):
        for along in range(lanes_b):

            def read(slot, group=group, along=along):
                down, low = divmod((2 * slot + group) * rank, high_b)
                return mlp[down * lanes_b + along, low : low + rank, :]

            def store(own, total, along=along, target=target):
                target[own, :, along * wide_b : (along + 1) * wide_b] = total

            mixed(read, store)
    plans = (
        (late, 3, (k_a, v_a)),
        (middle, 2, (q_a, q_b)),
        (early, 4, (o_a, o_b, e_a, s_b)),
    )
    for table, groups, targets in plans:
        high = table.shape[1]
        for group in range(groups):
            for along in range(4):
                for row in range(0, rank, 8):

                    def read(slot, group=group, along=along, row=row, groups=groups, table=table):
                        down, low = divmod((slot * groups + group) * rank + row, high)
                        return table[down * 4 + along, low : low + 8, :]

                    def store(own, total, group=group, along=along, row=row, targets=targets):
                        if group < len(targets):
                            span = slice(along * wide, (along + 1) * wide)
                            targets[group][own, row : row + 8, span] = total
                        else:
                            (k_b, v_b)[along][own, row : row + 8, :] = total[:, 0:thin]

                    if group < len(targets) or along < 2:
                        mixed(read, store)


def finish_call(back, mlp, ids, adapters, members, head):
    layer, tgrad, late, middle, early = back
    tok, width = layer.shape
    rank = ids.shape[1]
    part = width // members
    units = mlp.shape[2] * min(16, mlp.shape[0])
    batch = 2
    rows = tok * batch // adapters
    f32 = jnp.float32
    whole = lambda array: pl.BlockSpec(array.shape, lambda i: (0,) * array.ndim)
    strip = lambda: pl.BlockSpec((rows, width), lambda i: (i, 0))
    shapes = [(adapters, rank, part)] * 8 + [(adapters, rank, head // members)] * 2
    shapes += [(adapters, rank, units)] * 2
    return pl.pallas_call(
        functools.partial(finish_kernel, (rank, members)),
        grid=(adapters // batch,),
        in_specs=[strip(), strip()]
        + [whole(table) for table in (late, middle, mlp, early, ids)],
        out_specs=[strip(), strip()]
        + [pl.BlockSpec((batch,) + shape[1:], lambda i: (i, 0, 0)) for shape in shapes],
        out_shape=[
            jax.ShapeDtypeStruct(layer.shape, layer.dtype),
            jax.ShapeDtypeStruct(tgrad.shape, tgrad.dtype),
        ]
        + [jax.ShapeDtypeStruct(shape, f32) for shape in shapes],
        name="finish",
    )(layer, tgrad, late, middle, mlp, early, ids)


def back_call(tokens, grad_top, segments, vectors, picked, core, count, members):
    tok, width = tokens.shape
    kv_win, seg_win, lse, mid, low1, low_o, shrunk, grad_second, lows = core[:9]
    ids, _, q, o, h2, out_far, wq, wo = core[9:]
    attn_a, attn_b, out_a, out_b, exp_a, shr_b, _, _ = picked
    head = kv_win.shape[1] // 2
    heads = width // head
    rank = ids.shape[1]
    window = count // 2 + 1
    part = width // members
    high_a, wide_a = 3 * rank * members * 4 // count, part // 4
    high_q = 2 * rank * members * 4 // count
    high_e = 4 * rank * members * 4 // count
    bf = jnp.bfloat16
    seg_rows = jnp.broadcast_to(segments[None, :], (8, tok))
    vmem = lambda: pl.BlockSpec(memory_space=pltpu.VMEM)
    hbm = lambda: pl.BlockSpec(memory_space=pl.ANY)
    dma = pltpu.SemaphoreType.DMA
    shape = jax.ShapeDtypeStruct
    dims = (tok, width, rank, count, members, window, heads, head)
    inputs = [
        tokens, grad_top, seg_rows, *vectors, attn_a, attn_b, out_a, out_b, exp_a, shr_b,
        q, kv_win, seg_win, lse, o, mid, h2, low1, low_o, shrunk, grad_second, lows, ids,
    ]
    outs = [shape((tok, width), bf), shape((tok, width), bf)]
    outs += [
        shape((count, high_a, wide_a), bf),
        shape((count, high_q, wide_a), bf),
        shape((count, high_e, wide_a), bf),
    ]
    return pl.pallas_call(
        functools.partial(back_kernel, dims),
        out_shape=tuple(outs),
        in_specs=[vmem() for _ in inputs] + [hbm() for _ in range(3)],
        out_specs=tuple(vmem() for _ in outs),
        scratch_shapes=[
            pltpu.VMEM((width, width + 2 * head), bf),
            pltpu.VMEM((window * tok, tok), jnp.float32 if window * tok <= 2048 else bf),
            pltpu.VMEM((head, window * tok), bf),
            pltpu.VMEM((tok, width), jnp.float32),
            pltpu.VMEM((tok, width), jnp.float32),
            pltpu.VMEM((tok, width), bf),
            pltpu.VMEM((tok, width), bf),
            pltpu.VMEM((tok, width + 2 * head), bf),
            pltpu.VMEM((tok, width), bf),
            pltpu.VMEM((window * tok, 2 * head), jnp.float32),
            pltpu.VMEM((window - 1, tok, 2 * head), bf),
            pltpu.VMEM((window - 1, tok, 2 * head), bf),
            pltpu.VMEM((members, 3 * rank, part), bf),
            pltpu.VMEM((members * 3 * rank, part), bf),
            pltpu.VMEM((count, high_a, wide_a), bf),
            pltpu.VMEM((members, 2 * rank, part), bf),
            pltpu.VMEM((members * 2 * rank, part), bf),
            pltpu.VMEM((count, high_q, wide_a), bf),
            pltpu.VMEM((members, 4 * rank, part), bf),
            pltpu.VMEM((members * 4 * rank, part), bf),
            pltpu.VMEM((count, high_e, wide_a), bf),
            pltpu.VMEM((tok, width), bf),
            dma((1,)),
            dma((1,)),
            dma((7,)),
            dma((window - 1,)),
            dma((window - 1,)),
            dma((9,)),
            dma((9,)),
            dma((3, 2, count)),
            dma((3, 2, count)),
        ],
        compiler_params=pltpu.CompilerParams(
            collective_id=3, has_side_effects=True, vmem_limit_bytes=63 * 1024 * 1024
        ),
        name="back",
    )(*inputs, wq, wo, out_far)


def body(
    tokens,
    out_grad,
    segments,
    adapter_index,
    first_gain,
    first_bias,
    second_gain,
    second_bias,
    qkv_weight,
    out_weight,
    expand_weight,
    shrink_weight,
    query_first,
    query_second,
    key_first,
    key_second,
    value_first,
    value_second,
    output_first,
    output_second,
    expand_first,
    expand_second,
    shrink_first,
    shrink_second,
):
    count = lax.axis_size("ctx")
    members = lax.axis_size("wt")
    rank = query_second.shape[1]
    flip = lambda table: table.transpose(0, 2, 1)
    row = lambda vector: vector[None, :]
    tables = [
        flip(query_first),
        query_second,
        flip(key_first),
        key_second,
        flip(value_first),
        value_second,
        flip(output_first),
        output_second,
        flip(expand_first),
        expand_second,
        flip(shrink_first),
        shrink_second,
    ]
    picked = pick_call(adapter_index, tables, members)
    vectors = [row(first_gain), row(first_bias), row(second_gain), row(second_bias)]
    weights = (qkv_weight, out_weight, expand_weight, shrink_weight)
    core = core_call(tokens[0], out_grad[0], segments[0], vectors, picked, weights, count)
    back = back_call(
        tokens[0], out_grad[0], segments[0], vectors, picked, core, count, members
    )
    results = finish_call(
        back, core[10], core[9], query_first.shape[0], members, key_second.shape[2]
    )
    layer_out, tokens_grad = results[0][None], results[1][None]
    q_a, q_b, k_a, v_a, o_a, o_b, e_a, s_b, k_b, v_b, e_b, s_a = results[2:]
    return (
        layer_out,
        tokens_grad,
        flip(q_a),
        q_b,
        flip(k_a),
        k_b,
        flip(v_a),
        v_b,
        flip(o_a),
        o_b,
        flip(e_a),
        e_b,
        flip(s_a),
        s_b,
    )


def solution(mesh):
    placed = (
        P("wt", "ctx", None),
        P("wt", "ctx", None),
        P("wt", "ctx"),
        P("wt"),
        P(),
        P(),
        P(),
        P(),
        P("wt", None),
        P("wt", None),
        P("wt", None),
        P("wt", None),
        P(),
        P(),
        P(),
        P(),
        P(),
        P(),
        P(),
        P(),
        P(),
        P(),
        P(),
        P(),
    )
    return jax.shard_map(
        body,
        mesh=mesh,
        in_specs=placed,
        out_specs=(
            P("wt", "ctx", None),
            P("wt", "ctx", None),
            P(None, "wt", None),
            P(None, None, "wt"),
            P(None, "wt", None),
            P(None, None, "wt"),
            P(None, "wt", None),
            P(None, None, "wt"),
            P(None, "wt", None),
            P(None, None, "wt"),
            P(None, "wt", None),
            P(None, None, "wt"),
            P(None, "wt", None),
            P(None, None, "wt"),
        ),
        check_vma=False,
    )
```

```python
import functools
import math

import jax
import jax.numpy as jnp
from jax import lax
from jax.experimental import pallas as pl
from jax.experimental.pallas import tpu as pltpu
from jax.sharding import PartitionSpec as P

EPSILON = 1e-05
LOWEST = -1e30

MESH = pl.DeviceIdType.MESH
GELU_SCALE = 0.7978845608


def dot_nn(left, right):
    return lax.dot_general(
        left, right, (((1,), (0,)), ((), ())), preferred_element_type=jnp.float32
    )


def dot_nt(left, right):
    return lax.dot_general(
        left, right, (((1,), (1,)), ((), ())), preferred_element_type=jnp.float32
    )


def dot_tn(left, right):
    return lax.dot_general(
        left, right, (((0,), (0,)), ((), ())), preferred_element_type=jnp.float32
    )


NORM_ROWS = 32


def norm_rows(values, gain, offset):
    mean = jnp.mean(values, -1, keepdims=True)
    centre = values - mean
    scale_inv = lax.rsqrt(jnp.mean(centre * centre, -1, keepdims=True) + EPSILON)
    normed = centre * scale_inv
    return normed * gain + offset, normed, scale_inv


def mask_fill(bias, seg_win, seg_own, window, tok):
    keys_at = lax.broadcasted_iota(jnp.int32, (tok, tok), 0)
    tokens_at = lax.broadcasted_iota(jnp.int32, (tok, tok), 1)
    own = seg_own[0:1, :].astype(jnp.float32)
    for block in range(window):
        same = seg_win[block].astype(jnp.float32).T[:, 0:1] == own
        if block == window - 1:
            same = same & (keys_at <= tokens_at)
        bias[block * tok : (block + 1) * tok, :] = jnp.where(
            same, 0.0, LOWEST
        ).astype(bias.dtype)


def turned(values):
    return values.astype(jnp.float32).T.astype(jnp.bfloat16)


def pick_kernel(
    index_ref,
    q_a,
    q_b,
    k_a,
    k_b,
    v_a,
    v_b,
    o_a,
    o_b,
    e_a,
    e_b,
    s_a,
    s_b,
    attn_a,
    attn_b,
    out_a,
    out_b,
    exp_a,
    shr_b,
    ext,
    mark,
):
    rank, width = q_a.shape[1:]
    head = k_b.shape[2]
    units = ext.shape[3]
    for table in (attn_a, attn_b):
        table[...] = jnp.zeros_like(table)
    attn_a[0:rank, :] = q_a[0]
    attn_a[rank : 2 * rank, :] = k_a[0]
    attn_a[2 * rank : 3 * rank, :] = v_a[0]
    attn_b[0:rank, 0:width] = q_b[0]
    attn_b[rank : 2 * rank, width : width + head] = k_b[0]
    attn_b[2 * rank : 3 * rank, width + head : width + 2 * head] = v_b[0]
    out_a[0:rank, :] = o_a[0]
    out_b[0:rank, :] = o_b[0]
    exp_a[0:rank, :] = e_a[0]
    shr_b[0:rank, :] = s_b[0]
    for part in range(ext.shape[0]):
        span = slice(part * units, (part + 1) * units)
        ext[part, 0] = e_b[0, :, span]
        ext[part, 1] = s_a[0, :, span]
    lane = lax.broadcasted_iota(jnp.int32, mark.shape, 1)
    mark[...] = jnp.where(lane < 64, 0.0, index_ref[0].astype(jnp.float32))


def pick_call(adapter_index, tables, members):
    adapters, rank, width = tables[0].shape
    head = tables[3].shape[2]
    units = tables[10].shape[2] // members
    bf = jnp.bfloat16
    shapes = [
        ((128, width), bf),
        ((128, width + 2 * head), bf),
        ((rank, width), bf),
        ((rank, width), bf),
        ((rank, width), bf),
        ((rank, width), bf),
        ((members, 2, rank, units), bf),
        ((8, 128), jnp.float32),
    ]
    return pl.pallas_call(
        pick_kernel,
        grid_spec=pltpu.PrefetchScalarGridSpec(
            num_scalar_prefetch=1,
            grid=(1,),
            in_specs=[
                pl.BlockSpec((1,) + table.shape[1:], lambda i, index: (index[0], 0, 0))
                for table in tables
            ],
            out_specs=[
                pl.BlockSpec(shape, lambda i, index, r=len(shape): (0,) * r) for shape, _ in shapes
            ],
        ),
        out_shape=[jax.ShapeDtypeStruct(shape, kind) for shape, kind in shapes],
        name="pick",
    )(adapter_index, *tables)


def core_kernel(
    dims,
    tokens_ref,
    seg_ref,
    gain1,
    bias1,
    gain2,
    bias2,
    attn_a,
    attn_b,
    out_a,
    out_b,
    exp_a,
    shr_b,
    mark,
    grad_hbm,
    ext_hbm,
    qkv_hbm,
    out_hbm,
    exp_hbm,
    ws_hbm,
    kv_win,
    seg_win,
    lse_ref,
    mid_ref,
    low1_ref,
    low_o_ref,
    out_ref,
    dh_ref,
    lows_ref,
    ids_ref,
    ag_b,
    q_out,
    o_out,
    h2_out,
    out_far,
    wq_out,
    wo_out,
    q_ref,
    o_ref,
    h1,
    bias,
    flipped,
    wq,
    wo,
    we,
    land,
    h2_all,
    dy_all,
    lowt_all,
    ext_all,
    sis_send,
    sis_recv,
    own_recv,
    table_ref,
    rs_b,
    low_keep,
    low_send,
    low_recv,
    link_send,
    link_recv,
    pass_send,
    pass_recv,
    shard_send,
    shard_recv,
    kv_send,
    kv_recv,
    seg_send,
    seg_recv,
    side_send,
    side_recv,
    sis_ssem,
    sis_rsem,
    own_ssem,
    own_rsem,
    far_ssem,
    far_rsem,
    low_ssem,
    low_rsem,
    red_ssem,
    red_rsem,
    local_sem,
    spill_sem,
):
    tok, width, units, rows, count, window, heads, head, rank = dims
    bf = jnp.bfloat16
    strip = 512 if window * tok <= 2048 else 256
    me = lax.axis_index("wt")
    ctx = lax.axis_index("ctx")
    core = lax.rem(me, 2)
    side = lax.div(me, 2)
    sister = me + 1 - 2 * core
    across = me + 2 - 4 * side
    diagonal = sister + 2 - 4 * side
    stride = count // 4
    bit_y = lax.rem(ctx, 2)
    bit_z = lax.rem(lax.div(ctx, stride), 2)
    next_y = ctx + 1 - 2 * bit_y
    next_z = ctx + stride - 2 * stride * bit_z
    reach = window - 1
    own_block = window - 1

    def remote(src, dst, send, recv, peer):
        return pltpu.make_async_remote_copy(
            src_ref=src, dst_ref=dst, send_sem=send, recv_sem=recv, device_id=peer,
            device_id_type=MESH,
        )

    my_rows = pl.ds(pl.multiple_of(me * rows, rows), rows)
    quarter = pl.ds(pl.multiple_of(me * units, units), units)
    local = [
        pltpu.make_async_copy(qkv_hbm, wq.at[my_rows], local_sem.at[0]),
        pltpu.make_async_copy(out_hbm, wo.at[my_rows], local_sem.at[1]),
        pltpu.make_async_copy(exp_hbm.at[:, quarter], we.at[my_rows], local_sem.at[2]),
        pltpu.make_async_copy(seg_ref, seg_win.at[own_block], local_sem.at[3]),
        pltpu.make_async_copy(grad_hbm, dy_all.at[pl.ds(0, tok)], local_sem.at[4]),
        pltpu.make_async_copy(ext_hbm.at[me], ext_all.at[0], local_sem.at[5]),
    ]
    for copy in local:
        copy.start()
    for step in range(1, window):

        @pl.when(ctx < step)
        def _(step=step):
            slot = own_block - step
            kv_win[slot * tok : (slot + 1) * tok, :] = jnp.zeros((tok, 2 * head), jnp.bfloat16)
            seg_win[slot] = jnp.full(seg_ref.shape, -1, jnp.int32)

    barrier = pltpu.get_barrier_semaphore()
    for peer in (sister, across, diagonal):
        pl.semaphore_signal(barrier, inc=1, device_id={"wt": peer}, device_id_type=MESH)
    for other in range(count):

        @pl.when(ctx != other)
        def _(other=other):
            pl.semaphore_signal(barrier, inc=1, device_id={"ctx": other}, device_id_type=MESH)

    pl.semaphore_wait(barrier, 3 + count - 1)

    def part_rows(first, flip_y, flip_z, skip, length):
        turn_y = 1 - bit_y if flip_y else bit_y
        turn_z = 1 - bit_z if flip_z else bit_z
        start = first + (turn_y + 2 * turn_z) * (rows // 4) + skip
        return pl.ds(pl.multiple_of(start, 16), length)

    piece = rows // 4
    splits = {0: (80, 32, 16)}
    wide = width // 2
    slim = width // 4
    chunks = [(0, width, 2 * head)]
    chunks += [(0, i * slim, slim) for i in range(4)]
    chunks += [(1, i * wide, wide) for i in range(2)]
    for i in range(2):
        chunks += [(kind, i * (units // 2), units // 2) for kind in (2, 3)]

    def chunk_copies(number):
        kind, start, span = chunks[number]
        cut_x, cut_y, cut_z = (n * piece // 128 for n in splits.get(kind, (0, 64, 64)))
        cols = pl.ds(start, span)
        if kind < 2:
            source = (qkv_hbm, out_hbm)[kind]
            source_cols = cols
        else:
            source = exp_hbm
            target = across if kind == 2 else sister + 2 - 4 * side
            source_cols = pl.ds(pl.multiple_of(target * units + start, 128), span)
        home = (wq, wo, we, land)[kind]
        base = 0 if kind == 3 else across * rows
        home_base = 0 if kind == 3 else me * rows
        full = (False, False)
        sems = lambda way: (link_send.at[number, way], link_recv.at[number, way])

        def from_source(parity, skip, length):
            return (
                source.at[part_rows(0, *parity, skip, length), source_cols],
                home.at[part_rows(home_base, *parity, skip, length), cols],
            )

        def passing(parity, skip, length):
            at = home.at[part_rows(base, *parity, skip, length), cols]
            return (at, at)

        return [
            remote(*from_source(full, 0, piece), *sems(0), {"wt": across}),
            None if cut_x == 0 else
            remote(*from_source((True, True), 0, cut_x), *sems(5), {"wt": across}),
            remote(*passing(full, 0, piece), *sems(1), {"ctx": next_y}),
            remote(*passing(full, 0, piece), *sems(2), {"ctx": next_z}),
            remote(*passing((False, True), cut_x, cut_y), *sems(3), {"ctx": next_y}),
            remote(*passing((True, False), cut_x + cut_y, cut_z), *sems(4), {"ctx": next_z}),
        ]

    def sister_copy(number):
        kind, start, span = chunks[number]
        cols = pl.ds(start, span)
        far_rows = pl.ds(pl.multiple_of(across * rows, rows), rows)
        if kind == 3:
            src, dst = land.at[:, cols], we.at[far_rows, cols]
        else:
            home = (wq, wo)[kind]
            src = home.at[far_rows, cols]
            dst = src
        return remote(src, dst, pass_send.at[number], pass_recv.at[number], {"wt": sister})

    links = [chunk_copies(number) for number in range(len(chunks))]
    forwards = [None if chunks[n][0] == 2 else sister_copy(n) for n in range(len(chunks))]
    sister_quarter = pl.ds(pl.multiple_of(sister * units, units), units)
    own = [
        remote(qkv_hbm, wq.at[my_rows], shard_send.at[0], shard_recv.at[0], {"wt": sister}),
        remote(out_hbm, wo.at[my_rows], shard_send.at[1], shard_recv.at[1], {"wt": sister}),
        remote(
            exp_hbm.at[:, sister_quarter], we.at[my_rows], shard_send.at[2], shard_recv.at[2],
            {"wt": sister},
        ),
    ]

    def arrive(number):
        links[number][0].wait_recv()
        links[number][2].start()
        links[number][3].start()

    def turn(number):
        links[number][2].wait_recv()
        links[number][5].start()
        links[number][3].wait_recv()
        links[number][4].start()

    def finish(number):
        for way in (1, 4, 5):
            if links[number][way] is not None:
                links[number][way].wait_recv()
        if forwards[number] is not None:
            forwards[number].start()

    def ready(number):
        if forwards[number] is not None:
            forwards[number].wait_recv()

    def side_copy(number, src, dst, peer):
        return remote(src, dst, side_send.at[number], side_recv.at[number], {"wt": peer})

    def sent(number):
        for copy in links[number]:
            if copy is not None:
                copy.wait_send()
        if forwards[number] is not None:
            forwards[number].wait_send()

    half = tok // 2

    def far_rows(slot, part):
        return pl.ds(2 * tok + part * tok + (slot - 2) * half, half)

    near = [
        side_copy(0, ext_hbm.at[sister], ext_all.at[1], sister),
        side_copy(1, grad_hbm, dy_all.at[pl.ds(tok, tok)], sister),
    ]
    distant = [
        side_copy(2, ext_hbm.at[across], ext_all.at[2], across),
        side_copy(3, ext_hbm.at[diagonal], ext_all.at[3], diagonal),
    ]
    far_dy = [
        side_copy(
            4 + i, grad_hbm.at[pl.ds(i * half, half)], dy_all.at[far_rows(2, i)], across
        )
        for i in range(2)
    ]
    relay_dy = [
        side_copy(6 + i, dy_all.at[far_rows(2, i)], dy_all.at[far_rows(3, i)], sister)
        for i in range(2)
    ]
    near_h2 = side_copy(8, h2_all.at[pl.ds(0, tok)], h2_all.at[pl.ds(tok, tok)], sister)
    far_h2 = [
        side_copy(
            9 + i, h2_all.at[pl.ds(i * half, half)], h2_all.at[far_rows(2, i)], across
        )
        for i in range(2)
    ]
    relay_h2 = [
        side_copy(11 + i, h2_all.at[far_rows(2, i)], h2_all.at[far_rows(3, i)], sister)
        for i in range(2)
    ]
    send_low = [
        side_copy(12 + slot, lowt_all.at[0], lowt_all.at[slot], peer)
        for slot, peer in ((1, sister), (2, across), (3, diagonal))
    ]

    for number in range(len(chunks)):
        links[number][0].start()
        if links[number][1] is not None:
            links[number][1].start()
        if number == 0:
            own[0].start()
    own[1].start()
    own[2].start()
    for copy in near + distant + far_dy:
        copy.start()

    def seg_copy(step):
        return remote(
            seg_ref, seg_win.at[own_block - step], seg_send.at[step - 1], seg_recv.at[step - 1],
            {"ctx": ctx + step},
        )

    def kv_rows(distance):
        slot = own_block - distance
        return pl.ds(slot * tok if isinstance(slot, int) else pl.multiple_of(slot * tok, tok), tok)

    def kv_copy(held, send, distance, peer):
        return remote(
            kv_win.at[kv_rows(held)],
            kv_win.at[kv_rows(distance)],
            kv_send.at[send],
            kv_recv.at[distance - 1],
            {"ctx": peer},
        )

    place = lax.rem(ctx, stride)

    def kv_pass(level, act):
        if level < 2:

            @pl.when((ctx >= level * stride) & (ctx + stride < count))
            def _():
                far = (level + 1) * stride
                act(kv_copy(level * stride, (level, stride), far, ctx + stride))

        for other in range(stride):
            wanted = (other > place, other != place, other < place)[level]

            @pl.when(wanted & (ctx >= level * stride))
            def _(other=other):
                distance = other - place + level * stride
                act(kv_copy(level * stride, (level, other), distance, ctx - place + other))

    def kv_wait(distance):
        @pl.when(ctx >= distance)
        def _():
            kv_copy(0, (0, 0), distance, ctx).wait_recv()

    def kv_relay(level):
        kv_wait(level * stride)
        kv_pass(level, lambda copy: copy.start())

    def each_sent(make, act):
        for step in range(1, window):

            @pl.when(ctx + step < count)
            def _(step=step):
                act(make(step))

    def each_received(make):
        for step in range(1, window):

            @pl.when(ctx >= step)
            def _(step=step):
                make(step).wait_recv()

    each_sent(seg_copy, lambda copy: copy.start())

    def first_norm(number, carry):
        at = pl.ds(pl.multiple_of(number * NORM_ROWS, NORM_ROWS), NORM_ROWS)
        out, _, _ = norm_rows(tokens_ref[at, :].astype(jnp.float32), gain1[...], bias1[...])
        h1[at, :] = out.astype(jnp.bfloat16)
        return carry

    lax.fori_loop(0, tok // NORM_ROWS, first_norm, 0)
    low1_ref[...] = dot_nt(h1[...], attn_a[...]).astype(jnp.bfloat16)
    local[4].wait()
    lowt_all[0, rank : 2 * rank, :] = dot_nt(shr_b[...], dy_all[0:tok, :]).astype(bf)
    lowt_all[0, 2 * rank : 3 * rank, :] = jnp.broadcast_to(mark[0:1, 64:65], (rank, tok)).astype(
        bf
    )

    arrive(0)
    turn(0)
    arrive(1)
    finish(0)
    local[0].wait()
    own[0].wait_recv()
    ready(0)
    last = pl.ds(width, 2 * head)
    kv_win[own_block * tok : (own_block + 1) * tok, :] = (
        dot_nn(h1[...], wq[:, last]) + dot_nn(low1_ref[...], attn_b[:, last])
    ).astype(jnp.bfloat16)
    kv_pass(0, lambda copy: copy.start())
    turn(1)
    arrive(2)
    finish(1)
    kv_relay(1)
    turn(2)
    arrive(3)
    finish(2)
    kv_relay(2)
    turn(3)
    arrive(4)
    finish(3)
    local[3].wait()
    each_received(seg_copy)
    mask_fill(bias, seg_win, seg_ref, window, tok)
    turn(4)
    arrive(5)
    finish(4)
    for number in range(1, 5):
        ready(number)

    def query_tile(number, carry):
        cols = pl.ds(pl.multiple_of(number * strip, strip), strip)
        q_ref[:, cols] = (
            dot_nn(h1[...], wq[:, cols]) + dot_nn(low1_ref[...], attn_b[:, cols])
        ).astype(jnp.bfloat16)
        return carry

    lax.fori_loop(0, width // strip, query_tile, 0)
    spill_q = pltpu.make_async_copy(wq, wq_out, spill_sem.at[0])
    spill_q.start()
    turn(5)
    arrive(6)
    finish(5)
    for distance in range(1, window):
        if distance % stride:
            kv_wait(distance)
    scale = 1.0 / math.sqrt(head)

    for block in range(window):
        span = slice(block * tok, (block + 1) * tok)
        flipped[:, span] = turned(kv_win[span, head : 2 * head])
    span_q = tok if window * tok <= 2048 else 128

    def one_head(number, carry):
        cols = pl.ds(pl.multiple_of(number * head, head), head)
        for first in range(0, tok, span_q):
            at = slice(first, first + span_q)
            scores = dot_nt(kv_win[:, 0:head], q_ref[at, cols]) * scale + bias[:, at]
            highest = jnp.max(scores, 0, keepdims=True)
            weights = jnp.exp(scores - highest)
            total = jnp.sum(weights, 0, keepdims=True)
            probs = (weights * (1.0 / total)).astype(jnp.bfloat16)
            o_ref[at, cols] = dot_nn(flipped[...], probs).T.astype(jnp.bfloat16)
            lse_ref[number, :, at] = jnp.broadcast_to(highest + jnp.log(total), (8, span_q))
        return carry

    group = heads // 4
    lax.fori_loop(0, group, one_head, 0)
    arrive(7)
    lax.fori_loop(group, 2 * group, one_head, 0)
    turn(6)
    arrive(8)
    lax.fori_loop(2 * group, 3 * group, one_head, 0)
    finish(6)
    arrive(9)
    lax.fori_loop(3 * group, heads, one_head, 0)
    turn(7)
    arrive(10)
    spill_query = pltpu.make_async_copy(q_ref, q_out, spill_sem.at[5])
    spill_query.start()
    local[1].wait()
    own[1].wait_recv()
    ready(5)
    ready(6)
    spill_q.wait()
    for number in range(5):
        sent(number)
    own[0].wait_send()
    ws = wq.at[:, 0:width]
    load_ws = pltpu.make_async_copy(ws_hbm, ws, spill_sem.at[2])
    load_ws.start()
    low_o_ref[...] = dot_nt(o_ref[...], out_a[...]).astype(jnp.bfloat16)

    def out_tile(number, carry):
        cols = pl.ds(pl.multiple_of(number * strip, strip), strip)
        mid_ref[:, cols] = (
            tokens_ref[:, cols].astype(jnp.float32)
            + dot_nn(o_ref[...], wo[:, cols])
            + dot_nn(low_o_ref[...], out_b[:, cols])
        )
        return carry

    lax.fori_loop(0, width // strip, out_tile, 0)
    spill_o = pltpu.make_async_copy(wo, wo_out, spill_sem.at[1])
    spill_o.start()
    spill_mixed = pltpu.make_async_copy(o_ref, o_out, spill_sem.at[6])
    spill_mixed.start()

    def second_norm(number, carry):
        at = pl.ds(pl.multiple_of(number * NORM_ROWS, NORM_ROWS), NORM_ROWS)
        out, _, _ = norm_rows(mid_ref[at, :], gain2[...], bias2[...])
        h2_all[at, :] = out.astype(bf)
        return carry

    spill_mixed.wait()
    for part in range(2):
        steps = half // NORM_ROWS
        lax.fori_loop(part * steps, (part + 1) * steps, second_norm, 0)
        far_h2[part].start()
    near_h2.start()
    lowt_all[0, 0:rank, :] = dot_nt(exp_a[...], h2_all[0:tok, :]).astype(bf)
    for copy in send_low:
        copy.start()
    spill_h2 = pltpu.make_async_copy(h2_all.at[pl.ds(0, tok)], h2_out, spill_sem.at[3])
    spill_h2.start()
    spill_query.wait()
    spill_o.wait()
    for number in (5, 6):
        sent(number)
    own[1].wait_send()

    tile_a = 512 if window * tok <= 2048 else 256
    tile_b = 512
    tiles_a = units // tile_a
    tiles_b = width // tile_b
    act_base = 0
    dup_base = 4 * tok
    units_of_work = [
        (0, 2 * tok, [(0, 0, tok, 0), (1, 0, tok, tok)]),
        (2 * tok, tok, [(2, 0, half, 0), (3, 0, half, half)]),
        (3 * tok, tok, [(2, half, half, 0), (3, half, half, half)]),
    ]

    def low_ready(slot):
        at = slice(slot * tok, (slot + 1) * tok)
        wq[at, width : width + rank] = turned(lowt_all[slot, 0:rank, :])
        wq[at, width + 128 : width + 128 + rank] = turned(lowt_all[slot, rank : 2 * rank, :])

    def forward(work, first, last):
        base, span, parts = units_of_work[work]

        def step(number, carry):
            cols = pl.ds(pl.multiple_of(number * tile_a, tile_a), tile_a)

            def with_low(kind):
                pieces = []
                for slot, skip, size, _ in parts:
                    at = slice(slot * tok + skip, slot * tok + skip + size)
                    small = wq[at, width + kind * 128 : width + kind * 128 + rank]
                    pieces.append(dot_nn(small, ext_all[slot, kind, :, cols]))
                return jnp.concatenate(pieces, 0)

            upward = dot_nn(h2_all[base : base + span, :], we[:, cols]) + with_low(0)
            square = upward * upward
            bend = jnp.tanh(GELU_SCALE * (upward + 0.044715 * (square * upward)))
            active = (0.5 * upward * (1.0 + bend)).astype(bf)
            slope = 0.5 * (1.0 + bend) + 0.5 * upward * (1.0 - bend * bend) * GELU_SCALE * (
                1.0 + 3.0 * 0.044715 * square
            )
            grad = (dot_nt(dy_all[base : base + span, :], wq[cols, 0:width]) + with_low(1)).astype(
                bf
            )
            grad_up = (grad.astype(jnp.float32) * slope).astype(bf)
            wo[act_base + base : act_base + base + span, cols] = active
            wo[dup_base + base : dup_base + base + span, cols] = grad_up
            for slot, skip, size, row in parts:
                for kind, right in enumerate((grad_up, active)):
                    left = lowt_all[slot, kind * rank : (kind + 1) * rank, skip : skip + size]
                    at = pl.ds((2 * slot + kind) * rank, rank)
                    value = dot_nn(left, right[row : row + size])
                    if work == 2:
                        value = value + table_ref[at, cols].astype(jnp.float32)
                    table_ref[at, cols] = value.astype(bf)
            return carry

        lax.fori_loop(first, last, step, 0)

    def low_sums(work):
        base, _, parts = units_of_work[work]
        for slot, skip, size, row in parts:
            at = slice(dup_base + base + row, dup_base + base + row + size)
            grad_low = dot_nt(wo[at, :], ext_all[slot, 0])
            at = slice(act_base + base + row, act_base + base + row + size)
            act_low = dot_nt(wo[at, :], ext_all[slot, 1])
            for start, value in ((0, grad_low), (128, act_low)):
                to = (slice(skip, skip + size), slice(start, start + rank))
                if slot == 0:
                    lows_ref[to] = value
                elif slot == 2:
                    low_keep[to] = value
                else:
                    low_send[(0 if slot == 1 else 1,) + to] = value.astype(bf)

    def back_tile(work, kind, number):
        base, span, _ = units_of_work[work]
        cols = pl.ds(pl.multiple_of(number * tile_b, tile_b), tile_b)
        if kind == 0:
            return dot_nt(wo[dup_base + base : dup_base + base + span, :], we[cols, :])
        return dot_nn(wo[act_base + base : act_base + base + span, :], wq[:, cols])

    def sis_copy(kind, part, number):
        at = (kind, part, number)
        return remote(
            sis_send.at[at], sis_recv.at[at], sis_ssem.at[at], sis_rsem.at[at], {"wt": sister}
        )

    def tile_cols(number):
        return pl.ds(pl.multiple_of(number * tile_b, tile_b), tile_b)

    def own_at(kind, number):
        return (pl.ds(kind * tok, tok), tile_cols(number))

    def far_at(part, number):
        return (pl.ds(part * half, half), tile_cols(number))

    def part_at(number):
        return (pl.ds(pl.multiple_of(lax.rem(number, 2) * half, half), half), pl.ds(0, tile_b))

    def own_copy(kind, number):
        at = (kind, number)
        return remote(
            land.at[own_at(kind, number)], own_recv.at[at], own_ssem.at[at], own_rsem.at[at],
            {"wt": sister},
        )

    def far_copy(part, number):
        at = (part, number)
        return remote(
            q_ref.at[far_at(part, number)], o_ref.at[far_at(part, number)], far_ssem.at[at],
            far_rsem.at[at], {"wt": across},
        )

    def low_copy(number, peer):
        return remote(
            low_send.at[number],
            low_recv.at[number],
            low_ssem.at[number],
            low_rsem.at[number],
            {"wt": peer},
        )

    def join(kind, part, number):
        sis_copy(kind, part, number).wait_recv()
        total = (
            dh_ref[part_at(number)] + sis_recv[kind, part, number].astype(jnp.float32)
        ).astype(bf)
        if kind == 0:
            q_ref[far_at(part, number)] = total
            far_copy(part, number).start()
        else:
            cols = pl.ds(pl.multiple_of(number * tile_b, tile_b), tile_b)
            h1[part * half : (part + 1) * half, cols] = total

    def far_tiles(kind, part):
        def step(number, carry):
            both = back_tile(1 + part, kind, number)
            sis_send[kind, part, number] = both[half:].astype(bf)
            sis_copy(kind, part, number).start()

            @pl.when(number > 0)
            def _():
                join(kind, part, number - 1)

            dh_ref[part_at(number)] = both[:half]
            return carry

        lax.fori_loop(0, tiles_b, step, 0)
        join(kind, part, tiles_b - 1)

    def near_tiles(kind, target):
        def step(number, carry):
            cols = pl.ds(pl.multiple_of(number * tile_b, tile_b), tile_b)
            both = back_tile(0, kind, number)
            target[:, cols] = both[:tok].astype(target.dtype)
            land[own_at(kind, number)] = both[tok:].astype(bf)
            own_copy(kind, number).start()
            return carry

        lax.fori_loop(0, tiles_b, step, 0)

    high_b, wide_b = rs_b.shape[1:]
    lanes_b = min(16, count)

    def piece_b(other):
        return (
            pl.ds(pl.multiple_of(lax.div(other, lanes_b) * high_b, 16), high_b),
            pl.ds(pl.multiple_of(lax.rem(other, lanes_b) * wide_b, 128), wide_b),
        )

    def each_other(act):
        for other in range(count):

            @pl.when(ctx != other)
            def _(other=other):
                act(jnp.int32(other))

    def scatter_copy(other, origin):
        return remote(
            table_ref.at[piece_b(other)], rs_b.at[origin], red_ssem.at[0, other],
            red_rsem.at[0, origin], {"ctx": other},
        )

    def gather_copy(other, origin):
        return remote(
            rs_b.at[origin], ag_b.at[origin], red_ssem.at[1, other], red_rsem.at[1, origin],
            {"ctx": other},
        )

    mine = pltpu.make_async_copy(table_ref.at[piece_b(ctx)], rs_b.at[ctx], local_sem.at[6])
    kept = pltpu.make_async_copy(rs_b.at[ctx], ag_b.at[ctx], local_sem.at[7])
    lows_ref[...] = jnp.zeros_like(lows_ref)
    low_send[...] = jnp.zeros_like(low_send)
    low_ready(0)
    finish(7)
    turn(8)
    finish(8)
    turn(9)
    local[2].wait()
    local[5].wait()
    own[2].wait_recv()
    ready(8)
    load_ws.wait()
    near[0].wait_recv()
    near[1].wait_recv()
    send_low[0].wait_recv()
    low_ready(1)
    near_h2.wait_recv()
    forward(0, 0, tiles_a // 2)
    finish(9)
    turn(10)
    finish(10)
    for index in range(2):
        far_dy[index].wait_recv()
        relay_dy[index].start()
    ready(10)
    forward(0, tiles_a // 2, tiles_a)
    low_sums(0)
    low_own = low_copy(0, sister)
    low_own.start()
    for slot in (2, 3):
        distant[slot - 2].wait_recv()
        send_low[slot - 1].wait_recv()
        low_ready(slot)
    for slot in range(4):
        ids_ref[slot] = lowt_all[slot, 2 * rank : 3 * rank, 0:128].astype(jnp.float32)
    for part in range(2):
        if part == 0:
            far_h2[0].wait_recv()
            relay_h2[0].start()
        relay_dy[part].wait_recv()
        relay_h2[part].wait_recv()
        forward(1 + part, 0, tiles_a)
        if part == 0:
            far_h2[1].wait_recv()
            relay_h2[1].start()
        else:
            each_other(lambda other: scatter_copy(other, ctx).start())
            mine.start()
        far_tiles(0, part)
        low_sums(1 + part)
    low_sis = low_copy(1, sister)
    low_sis.start()
    far_tiles(1, 0)
    far_tiles(1, 1)
    spill_far = pltpu.make_async_copy(h1, out_far, spill_sem.at[4])
    spill_far.start()
    mine.wait()
    each_other(lambda other: scatter_copy(ctx, other).wait_recv())
    sums = rs_b[0].astype(jnp.float32)
    for other in range(1, count):
        sums = sums + rs_b[other].astype(jnp.float32)
    rs_b[ctx] = sums.astype(bf)
    each_other(lambda other: gather_copy(other, ctx).start())
    kept.start()
    low_sis.wait_recv()
    for start in (0, 128):
        to = (slice(None), slice(start, start + rank))
        low_send[(2,) + to] = (low_keep[to] + low_recv[(1,) + to].astype(jnp.float32)).astype(bf)
    low_far = low_copy(2, across)
    low_far.start()
    for number in range(7, len(chunks)):
        sent(number)
    near_tiles(0, dh_ref)
    near_tiles(1, out_ref)

    each_other(lambda other: scatter_copy(other, ctx).wait_send())
    each_other(lambda other: gather_copy(other, ctx).wait_send())

    def end_step(number, carry):
        cols = pl.ds(pl.multiple_of(number * tile_b, tile_b), tile_b)
        own_copy(0, number).wait_recv()
        own_copy(1, number).wait_recv()
        for part in range(2):
            at = slice(part * half, (part + 1) * half)
            far_copy(part, number).wait_recv()
            dh_ref[at, cols] = (
                dh_ref[at, cols]
                + own_recv[0, number, at, :].astype(jnp.float32)
                + o_ref[far_at(part, number)].astype(jnp.float32)
            )
        out_ref[:, cols] = (
            out_ref[:, cols].astype(jnp.float32) + own_recv[1, number].astype(jnp.float32)
        ).astype(bf)
        for kind in range(2):
            own_copy(kind, number).wait_send()
            for part in range(2):
                sis_copy(kind, part, number).wait_send()
        for part in range(2):
            far_copy(part, number).wait_send()
        return carry

    lax.fori_loop(0, tiles_b, end_step, 0)
    low_own.wait_recv()
    low_far.wait_recv()
    lows_ref[...] = (
        lows_ref[...] + low_recv[0].astype(jnp.float32) + low_recv[2].astype(jnp.float32)
    )
    own[2].wait_send()
    for copy in near + distant + far_dy + relay_dy + [near_h2] + far_h2 + relay_h2 + send_low:
        copy.wait_send()
    for copy in (low_own, low_sis, low_far):
        copy.wait_send()
    each_sent(seg_copy, lambda copy: copy.wait_send())
    for level in range(3):
        kv_pass(level, lambda copy: copy.wait_send())
    spill_h2.wait()
    spill_far.wait()
    kept.wait()
    each_other(lambda other: gather_copy(ctx, other).wait_recv())


def core_call(tokens, grad_top, segments, vectors, picked, weights, count):
    tok, width = tokens.shape
    qkv_weight, out_weight, expand_weight, shrink_weight = weights
    rows = qkv_weight.shape[0]
    head = (qkv_weight.shape[1] - width) // 2
    heads = width // head
    units = shrink_weight.shape[0]
    window = count // 2 + 1
    bf = jnp.bfloat16
    f32 = jnp.float32
    seg_rows = jnp.broadcast_to(segments[None, :], (8, tok))
    attn_a, attn_b, out_a, out_b, exp_a, shr_b, ext, mark = picked
    rank = ext.shape[2]
    half, tiles = tok // 2, width // 512
    vmem = lambda: pl.BlockSpec(memory_space=pltpu.VMEM)
    hbm = lambda: pl.BlockSpec(memory_space=pl.ANY)
    dma = pltpu.SemaphoreType.DMA
    dims = (tok, width, units, rows, count, window, heads, head, rank)
    shape = jax.ShapeDtypeStruct
    inputs = [
        tokens, seg_rows, *vectors, attn_a, attn_b, out_a, out_b, exp_a, shr_b, mark,
    ]
    outs = [
        shape((window * tok, 2 * head), bf),
        shape((window, 8, tok), jnp.int32),
        shape((heads, 8, tok), f32),
        shape((tok, width), f32),
        shape((tok, 128), bf),
        shape((tok, rank), bf),
        shape((tok, width), bf),
        shape((tok, width), f32),
        shape((tok, 256), f32),
        shape((4, rank, 128), f32),
    ]
    lanes_b = min(16, count)
    sums = (count, 8 * rank * lanes_b // count, units // lanes_b)
    spilled = [
        shape(sums, bf),
        shape((tok, width), bf),
        shape((tok, width), bf),
        shape((tok, width), bf),
        shape((tok, width), bf),
        shape((width, width + 2 * head), bf),
        shape((width, width), bf),
    ]
    return pl.pallas_call(
        functools.partial(core_kernel, dims),
        out_shape=tuple(outs + spilled),
        in_specs=[vmem() for _ in inputs] + [hbm() for _ in range(6)],
        out_specs=tuple([vmem() for _ in outs] + [hbm() for _ in spilled]),
        scratch_shapes=[
            pltpu.VMEM((tok, width), bf),
            pltpu.VMEM((tok, width), bf),
            pltpu.VMEM((tok, width), bf),
            pltpu.VMEM((window * tok, tok), bf),
            pltpu.VMEM((head, window * tok), bf),
            pltpu.VMEM((width, width + 2 * head), bf),
            pltpu.VMEM((width, width), bf),
            pltpu.VMEM((width, units), bf),
            pltpu.VMEM((rows, units), bf),
            pltpu.VMEM((4 * tok, width), bf),
            pltpu.VMEM((4 * tok, width), bf),
            pltpu.VMEM((4, 3 * rank, tok), bf),
            pltpu.VMEM((4, 2, rank, units), bf),
            pltpu.VMEM((2, 2, tiles, half, 512), bf),
            pltpu.VMEM((2, 2, tiles, half, 512), bf),
            pltpu.VMEM((2, tiles, tok, 512), bf),
            pltpu.VMEM((8 * rank, units), bf),
            pltpu.VMEM(sums, bf),
            pltpu.VMEM((tok, 256), f32),
            pltpu.VMEM((3, tok, 256), bf),
            pltpu.VMEM((3, tok, 256), bf),
            dma((11, 6)),
            dma((11, 6)),
            dma((11,)),
            dma((11,)),
            dma((3,)),
            dma((3,)),
            dma((3, count // 4 + 1)),
            dma((window - 1,)),
            dma((window - 1,)),
            dma((window - 1,)),
            dma((16,)),
            dma((16,)),
            dma((2, 2, tiles)),
            dma((2, 2, tiles)),
            dma((2, tiles)),
            dma((2, tiles)),
            dma((2, tiles)),
            dma((2, tiles)),
            dma((3,)),
            dma((3,)),
            dma((2, count)),
            dma((2, count)),
            dma((8,)),
            dma((7,)),
        ],
        compiler_params=pltpu.CompilerParams(
            collective_id=2, has_side_effects=True, vmem_limit_bytes=67043328
        ),
        name="core",
    )(
        *inputs, grad_top, ext, qkv_weight, out_weight, expand_weight, shrink_weight,
    )


def norm_pull(grad_out, gain, normed, scale_inv):
    grad_norm = grad_out * gain
    return scale_inv * (
        grad_norm
        - jnp.mean(grad_norm, -1, keepdims=True)
        - normed * jnp.mean(grad_norm * normed, -1, keepdims=True)
    )


def back_kernel(
    dims,
    tokens_ref,
    grad_ref,
    seg_ref,
    gain1,
    bias1,
    gain2,
    bias2,
    attn_a,
    attn_b,
    out_a,
    out_b,
    exp_a,
    shr_b,
    q_ref,
    kv_win,
    seg_win,
    lse_ref,
    o_ref,
    mid_ref,
    h2_ref,
    low1_ref,
    low_o_ref,
    shrunk_ref,
    dh_ref,
    lows_ref,
    ids_ref,
    wq_hbm,
    wo_hbm,
    out_far,
    layer_ref,
    tgrad_ref,
    ag_a,
    ag_q,
    ag_e,
    wq,
    bias,
    flipped,
    dmid,
    dacc,
    db,
    dout,
    dqkv,
    h1,
    dkv,
    dkv_send,
    dkv_recv,
    share,
    land,
    rs_a,
    share_q,
    land_q,
    rs_q,
    share_e,
    land_e,
    rs_e,
    out_recv,
    out_ssem,
    out_rsem,
    local_sem,
    kv_ssem,
    kv_rsem,
    share_ssem,
    share_rsem,
    red_ssem,
    red_rsem,
):
    tok, width, rank, count, members, window, heads, head = dims
    strip = 512 if window * tok <= 2048 else 256
    me = lax.axis_index("wt")
    ctx = lax.axis_index("ctx")
    core = lax.rem(me, 2)
    side = lax.div(me, 2)
    sister = me + 1 - 2 * core
    across = me + 2 - 4 * side
    diagonal = sister + 2 - 4 * side
    own_block = window - 1
    part = width // members
    bf = jnp.bfloat16

    wo = wq.at[:, 0:width]
    local = [
        pltpu.make_async_copy(wo_hbm, wo, local_sem.at[0]),
        pltpu.make_async_copy(wq_hbm, wq, local_sem.at[1]),
    ]
    local[0].start()

    barrier = pltpu.get_barrier_semaphore()
    for peer in (sister, across, diagonal):
        pl.semaphore_signal(barrier, inc=1, device_id={"wt": peer}, device_id_type=MESH)
    for other in range(count):

        @pl.when(ctx != other)
        def _(other=other):
            pl.semaphore_signal(barrier, inc=1, device_id={"ctx": other}, device_id_type=MESH)

    def remote(src, dst, send, recv, peer):
        return pltpu.make_async_remote_copy(
            src_ref=src, dst_ref=dst, send_sem=send, recv_sem=recv, device_id=peer,
            device_id_type=MESH,
        )

    def each_other(act):
        for other in range(count):

            @pl.when(ctx != other)
            def _(other=other):
                act(other)

    def scatter_copy(lane, table, piece, landing, other):
        return remote(
            table.at[piece(other)],
            landing.at[ctx],
            red_ssem.at[lane, 0, other],
            red_rsem.at[lane, 0, ctx],
            {"ctx": other},
        )

    def scatter_wait(lane, table, piece, landing, other):
        remote(
            table.at[piece(other)],
            landing.at[other],
            red_ssem.at[lane, 0, other],
            red_rsem.at[lane, 0, other],
            {"ctx": other},
        ).wait_recv()

    def gather_copy(lane, result, other):
        return remote(
            result.at[ctx],
            result.at[ctx],
            red_ssem.at[lane, 1, other],
            red_rsem.at[lane, 1, ctx],
            {"ctx": other},
        )

    def gather_wait(lane, result, other):
        remote(
            result.at[other],
            result.at[other],
            red_ssem.at[lane, 1, other],
            red_rsem.at[lane, 1, other],
            {"ctx": other},
        ).wait_recv()

    def scatter_start(lane, table, piece, landing):
        each_other(lambda other: scatter_copy(lane, table, piece, landing, other).start())
        mine = pltpu.make_async_copy(
            table.at[piece(ctx)], landing.at[ctx], local_sem.at[2 + lane]
        )
        mine.start()
        return mine

    def reduce_gather(lane, table, piece, landing, result, mine):
        mine.wait()
        each_other(lambda other: scatter_wait(lane, table, piece, landing, other))
        total = landing[0].astype(jnp.float32)
        for other in range(1, count):
            total = total + landing[other].astype(jnp.float32)
        result[ctx] = total.astype(bf)
        each_other(lambda other: gather_copy(lane, result, other).start())

    def reduce_end(lane, table, piece, landing, result):
        each_other(lambda other: gather_wait(lane, result, other))
        each_other(lambda other: scatter_copy(lane, table, piece, landing, other).wait_send())
        each_other(lambda other: gather_copy(lane, result, other).wait_send())

    high_a, wide_a = rs_a.shape[1:]
    high_e = rs_e.shape[1]

    def quarter_piece(high):
        def piece(other):
            down = lax.div(other, 4) if not isinstance(other, int) else other // 4
            along = lax.rem(other, 4) if not isinstance(other, int) else other % 4
            return (
                pl.ds(pl.multiple_of(down * high, 8), high),
                pl.ds(pl.multiple_of(along * wide_a, 128), wide_a),
            )

        return piece

    piece_a, piece_e = quarter_piece(high_a), quarter_piece(high_e)
    piece_q = quarter_piece(rs_q.shape[1])

    pl.semaphore_wait(barrier, 3 + count - 1)
    out_copy = remote(out_far, out_recv, out_ssem.at[0], out_rsem.at[0], {"wt": across})

    grad_low = lows_ref[:, 0:rank].astype(bf)
    shrink_low = lows_ref[:, 128 : 128 + rank].astype(bf)
    lows_tile = 512

    def low_step(number, carry):
        cols = pl.ds(pl.multiple_of(number * lows_tile, lows_tile), lows_tile)
        dmid[:, cols] = dh_ref[:, cols] + dot_nn(grad_low, exp_a[:, cols])
        return carry

    lax.fori_loop(0, width // lows_tile, low_step, 0)

    def second_pull(number, carry):
        at = pl.ds(pl.multiple_of(number * NORM_ROWS, NORM_ROWS), NORM_ROWS)
        _, normed, scale_inv = norm_rows(mid_ref[at, :], gain2[...], bias2[...])
        value = grad_ref[at, :].astype(jnp.float32) + norm_pull(
            dmid[at, :], gain2[...], normed, scale_inv
        )
        dmid[at, :] = value
        db[at, :] = value.astype(bf)
        return carry

    lax.fori_loop(0, tok // NORM_ROWS, second_pull, 0)
    grad_out_low = dot_nt(db[...], out_b[...]).astype(bf)
    local[0].wait()

    def out_pull(number, carry):
        cols = pl.ds(pl.multiple_of(number * strip, strip), strip)
        dout[:, cols] = (
            dot_nt(db[...], wq[cols, 0:width]) + dot_nn(grad_out_low, out_a[:, cols])
        ).astype(bf)
        return carry

    lax.fori_loop(0, width // strip, out_pull, 0)
    local[1].start()

    def put(table, group, value):
        for other in range(members):
            span = slice(other * part, (other + 1) * part)
            table[other, group * rank : (group + 1) * rank, :] = value[:, span].astype(bf)

    def exchange_of(first, table, landing):
        deep = table.shape[1]
        return [
            remote(
                table.at[peer],
                landing.at[pl.ds(slot * deep, deep)],
                share_ssem.at[first + slot - 1],
                share_rsem.at[first + slot - 1],
                {"wt": peer},
            )
            for slot, peer in ((1, sister), (2, across), (3, diagonal))
        ]

    put(share_e, 0, dot_tn(grad_out_low[:, 0:rank], o_ref[...]))
    put(share_e, 1, dot_tn(low_o_ref[:, 0:rank], db[...]))
    put(share_e, 2, dot_tn(grad_low[:, 0:rank], h2_ref[...]))
    put(share_e, 3, dot_tn(shrink_low[:, 0:rank], grad_ref[...]))
    exchange_e = exchange_of(3, share_e, land_e)
    for copy in exchange_e:
        copy.start()
    mine_share_e = pltpu.make_async_copy(
        share_e.at[me], land_e.at[pl.ds(0, 4 * rank)], local_sem.at[5]
    )
    mine_share_e.start()
    out_copy.start()

    mask_fill(bias, seg_win, seg_ref, window, tok)
    for block in range(window):
        span = slice(block * tok, (block + 1) * tok)
        flipped[:, span] = turned(kv_win[span, 0:head])
    dkv[...] = jnp.zeros_like(dkv)
    scale = 1.0 / math.sqrt(head)
    span_q = tok if window * tok <= 2048 else 128

    pack = 2 if window * tok <= 2048 else 1

    def one_head(number, carry):
        for first in range(0, tok, span_q):
            at = slice(first, first + span_q)
            queries, grads, changes, masses = [], [], [], []
            for own in range(pack):
                head_at = number * pack + own
                cols = pl.ds(pl.multiple_of(head_at * head, head), head)
                query = q_ref[at, cols]
                grad = dout[at, cols]
                scores = dot_nt(kv_win[:, 0:head], query) * scale + bias[:, at]
                probs = jnp.exp(scores - lse_ref[head_at, 0:1, at])
                grad_probs = dot_nt(kv_win[:, head : 2 * head], grad)
                delta = jnp.sum(probs * grad_probs, 0, keepdims=True)
                grad_scores = (probs * (grad_probs - delta)).astype(bf)
                dqkv[at, cols] = (dot_nn(flipped[...], grad_scores).T * scale).astype(bf)
                queries.append(query)
                grads.append(grad)
                changes.append(grad_scores)
                masses.append(probs.astype(bf))
            joined = lambda parts, axis: parts[0] if pack == 1 else jnp.concatenate(parts, axis)
            dkv[:, 0:head] = dkv[:, 0:head] + dot_nn(joined(changes, 1), joined(queries, 0))
            dkv[:, head : 2 * head] = dkv[:, head : 2 * head] + dot_nn(
                joined(masses, 1), joined(grads, 0)
            )
        return carry

    turns = heads // pack
    lax.fori_loop(0, turns // 4, one_head, 0)
    mine_share_e.wait()
    for copy in exchange_e:
        copy.wait_recv()
    mine_e = scatter_start(2, land_e, piece_e, rs_e)
    lax.fori_loop(turns // 4, 3 * turns // 4, one_head, 0)
    reduce_gather(2, land_e, piece_e, rs_e, ag_e, mine_e)
    lax.fori_loop(3 * turns // 4, turns, one_head, 0)

    out_copy.wait_recv()

    def layer_step(number, carry):
        cols = pl.ds(pl.multiple_of(number * lows_tile, lows_tile), lows_tile)
        layer_ref[:, cols] = (
            mid_ref[:, cols]
            + shrunk_ref[:, cols].astype(jnp.float32)
            + out_recv[:, cols].astype(jnp.float32)
            + dot_nn(shrink_low, shr_b[:, cols])
        ).astype(bf)
        return carry

    def kv_copy(step):
        return remote(
            dkv_send.at[step - 1],
            dkv_recv.at[step - 1],
            kv_ssem.at[step - 1],
            kv_rsem.at[step - 1],
            {"ctx": ctx - step},
        )

    for step in range(1, window):

        @pl.when(ctx >= step)
        def _(step=step):
            at = slice((own_block - step) * tok, (own_block - step + 1) * tok)
            dkv_send[step - 1, :, 0:head] = (dkv[at, 0:head] * scale).astype(bf)
            dkv_send[step - 1, :, head : 2 * head] = dkv[at, head : 2 * head].astype(bf)
            kv_copy(step).start()

    local[1].wait()

    def first_norm(number, carry):
        at = pl.ds(pl.multiple_of(number * NORM_ROWS, NORM_ROWS), NORM_ROWS)
        out, _, _ = norm_rows(tokens_ref[at, :].astype(jnp.float32), gain1[...], bias1[...])
        h1[at, :] = out.astype(bf)
        return carry

    lax.fori_loop(0, tok // NORM_ROWS, first_norm, 0)
    lax.fori_loop(0, width // lows_tile, layer_step, 0)

    rank_part = dot_nt(dqkv[:, 0:width], attn_b[:, 0:width])
    put(share_q, 0, dot_tn(rank_part[:, 0:rank].astype(bf), h1[...]))
    put(share_q, 1, dot_tn(low1_ref[:, 0:rank], dqkv[:, 0:width]))
    exchange_q = exchange_of(6, share_q, land_q)
    for copy in exchange_q:
        copy.start()
    mine_share_q = pltpu.make_async_copy(
        share_q.at[me], land_q.at[pl.ds(0, 2 * rank)], local_sem.at[4]
    )
    mine_share_q.start()

    def first_half(number, carry):
        cols = pl.ds(pl.multiple_of(number * strip, strip), strip)
        dacc[:, cols] = dot_nt(dqkv[:, 0:width], wq[cols, 0:width])
        return carry

    lax.fori_loop(0, width // strip, first_half, 0)
    mine_share_q.wait()
    for copy in exchange_q:
        copy.wait_recv()
    mine_q = scatter_start(1, land_q, piece_q, rs_q)

    own_at = slice(own_block * tok, (own_block + 1) * tok)
    dkv[own_at, 0:head] = dkv[own_at, 0:head] * scale
    for step in range(1, window):

        @pl.when(ctx + step < count)
        def _(step=step):
            kv_copy(step).wait_recv()
            dkv[own_at, :] = dkv[own_at, :] + dkv_recv[step - 1].astype(jnp.float32)

    last = slice(width, width + 2 * head)
    dqkv[:, last] = dkv[own_at, :].astype(bf)
    grad_rank = (rank_part + dot_nt(dqkv[:, last], attn_b[:, last])).astype(bf)
    first_grads = dot_tn(grad_rank[:, 0 : 3 * rank], h1[...])
    put(share, 0, first_grads[rank : 2 * rank])
    put(share, 1, first_grads[2 * rank : 3 * rank])
    small = dot_tn(low1_ref[...], dqkv[:, last])
    thin = head // members
    tail = slice(2 * rank, 3 * rank)
    share[:, tail, :] = jnp.zeros((members, rank, part), bf)
    for other in range(members):
        span = slice(other * thin, (other + 1) * thin)
        share[other, tail, 0:thin] = small[rank : 2 * rank, span].astype(bf)
        span = slice(head + other * thin, head + (other + 1) * thin)
        share[other, tail, 128 : 128 + thin] = small[2 * rank : 3 * rank, span].astype(bf)

    exchange = exchange_of(0, share, land)
    for copy in exchange:
        copy.start()
    mine_share = pltpu.make_async_copy(
        share.at[me], land.at[pl.ds(0, 3 * rank)], local_sem.at[6]
    )
    mine_share.start()

    def second_half(number, carry):
        cols = pl.ds(pl.multiple_of(number * strip, strip), strip)
        dacc[:, cols] = (
            dacc[:, cols]
            + dot_nt(dqkv[:, last], wq[cols, last])
            + dot_nn(grad_rank, attn_a[:, cols])
        )
        return carry

    lax.fori_loop(0, width // strip, second_half, 0)
    reduce_gather(1, land_q, piece_q, rs_q, ag_q, mine_q)
    mine_share.wait()
    for copy in exchange:
        copy.wait_recv()
    mine_a = scatter_start(0, land, piece_a, rs_a)

    def first_pull(number, carry):
        at = pl.ds(pl.multiple_of(number * NORM_ROWS, NORM_ROWS), NORM_ROWS)
        _, normed, scale_inv = norm_rows(
            tokens_ref[at, :].astype(jnp.float32), gain1[...], bias1[...]
        )
        tgrad_ref[at, :] = (
            dmid[at, :] + norm_pull(dacc[at, :], gain1[...], normed, scale_inv)
        ).astype(bf)
        return carry

    lax.fori_loop(0, tok // NORM_ROWS, first_pull, 0)
    reduce_gather(0, land, piece_a, rs_a, ag_a, mine_a)

    reduce_end(2, land_e, piece_e, rs_e, ag_e)
    reduce_end(1, land_q, piece_q, rs_q, ag_q)
    for copy in exchange_q:
        copy.wait_send()
    reduce_end(0, land, piece_a, rs_a, ag_a)
    for copy in exchange_e:
        copy.wait_send()
    for copy in exchange:
        copy.wait_send()
    out_copy.wait_send()
    for step in range(1, window):

        @pl.when(ctx >= step)
        def _(step=step):
            kv_copy(step).wait_send()


def finish_kernel(
    dims,
    layer_ref,
    tgrad_ref,
    late,
    middle,
    mlp,
    early,
    ids_ref,
    layer_out,
    tgrad_out,
    q_a,
    q_b,
    k_a,
    v_a,
    o_a,
    o_b,
    e_a,
    s_b,
    k_b,
    v_b,
    e_b,
    s_a,
):
    rank, members = dims
    count, high_b, wide_b = mlp.shape
    lanes_b = min(16, count)
    thin = k_b.shape[2]
    wide = late.shape[2]
    batch = q_a.shape[0]
    first = pl.program_id(0) * batch
    layer_out[...] = layer_ref[...]
    tgrad_out[...] = tgrad_ref[...]
    hot = [
        [
            jnp.where(
                ids_ref[slot, 0:1, 64:65] == (first + own).astype(jnp.float32), 1.0, 0.0
            )
            for slot in range(members)
        ]
        for own in range(batch)
    ]

    def mixed(read, store):
        values = [read(slot).astype(jnp.float32) for slot in range(members)]
        for own in range(batch):
            total = hot[own][0] * values[0]
            for slot in range(1, members):
                total = total + hot[own][slot] * values[slot]
            store(own, total)

    for group, target in ((0, e_b), (1, s_a)):
        for along in range(lanes_b):

            def read(slot, group=group, along=along):
                down, low = divmod((2 * slot + group) * rank, high_b)
                return mlp[down * lanes_b + along, low : low + rank, :]

            def store(own, total, along=along, target=target):
                target[own, :, along * wide_b : (along + 1) * wide_b] = total

            mixed(read, store)
    plans = (
        (late, 3, (k_a, v_a)),
        (middle, 2, (q_a, q_b)),
        (early, 4, (o_a, o_b, e_a, s_b)),
    )
    for table, groups, targets in plans:
        high = table.shape[1]
        for group in range(groups):
            for along in range(4):
                for row in range(0, rank, 8):

                    def read(slot, group=group, along=along, row=row, groups=groups, table=table):
                        down, low = divmod((slot * groups + group) * rank + row, high)
                        return table[down * 4 + along, low : low + 8, :]

                    def store(own, total, group=group, along=along, row=row, targets=targets):
                        if group < len(targets):
                            span = slice(along * wide, (along + 1) * wide)
                            targets[group][own, row : row + 8, span] = total
                        else:
                            (k_b, v_b)[along][own, row : row + 8, :] = total[:, 0:thin]

                    if group < len(targets) or along < 2:
                        mixed(read, store)


def finish_call(back, mlp, ids, adapters, members, head):
    layer, tgrad, late, middle, early = back
    tok, width = layer.shape
    rank = ids.shape[1]
    part = width // members
    units = mlp.shape[2] * min(16, mlp.shape[0])
    batch = 2
    rows = tok * batch // adapters
    f32 = jnp.float32
    whole = lambda array: pl.BlockSpec(array.shape, lambda i: (0,) * array.ndim)
    strip = lambda: pl.BlockSpec((rows, width), lambda i: (i, 0))
    shapes = [(adapters, rank, part)] * 8 + [(adapters, rank, head // members)] * 2
    shapes += [(adapters, rank, units)] * 2
    return pl.pallas_call(
        functools.partial(finish_kernel, (rank, members)),
        grid=(adapters // batch,),
        in_specs=[strip(), strip()]
        + [whole(table) for table in (late, middle, mlp, early, ids)],
        out_specs=[strip(), strip()]
        + [pl.BlockSpec((batch,) + shape[1:], lambda i: (i, 0, 0)) for shape in shapes],
        out_shape=[
            jax.ShapeDtypeStruct(layer.shape, layer.dtype),
            jax.ShapeDtypeStruct(tgrad.shape, tgrad.dtype),
        ]
        + [jax.ShapeDtypeStruct(shape, f32) for shape in shapes],
        name="finish",
    )(layer, tgrad, late, middle, mlp, early, ids)


def back_call(tokens, grad_top, segments, vectors, picked, core, count, members):
    tok, width = tokens.shape
    kv_win, seg_win, lse, mid, low1, low_o, shrunk, grad_second, lows = core[:9]
    ids, _, q, o, h2, out_far, wq, wo = core[9:]
    attn_a, attn_b, out_a, out_b, exp_a, shr_b, _, _ = picked
    head = kv_win.shape[1] // 2
    heads = width // head
    rank = ids.shape[1]
    window = count // 2 + 1
    part = width // members
    high_a, wide_a = 3 * rank * members * 4 // count, part // 4
    high_q = 2 * rank * members * 4 // count
    high_e = 4 * rank * members * 4 // count
    bf = jnp.bfloat16
    seg_rows = jnp.broadcast_to(segments[None, :], (8, tok))
    vmem = lambda: pl.BlockSpec(memory_space=pltpu.VMEM)
    hbm = lambda: pl.BlockSpec(memory_space=pl.ANY)
    dma = pltpu.SemaphoreType.DMA
    shape = jax.ShapeDtypeStruct
    dims = (tok, width, rank, count, members, window, heads, head)
    inputs = [
        tokens, grad_top, seg_rows, *vectors, attn_a, attn_b, out_a, out_b, exp_a, shr_b,
        q, kv_win, seg_win, lse, o, mid, h2, low1, low_o, shrunk, grad_second, lows, ids,
    ]
    outs = [shape((tok, width), bf), shape((tok, width), bf)]
    outs += [
        shape((count, high_a, wide_a), bf),
        shape((count, high_q, wide_a), bf),
        shape((count, high_e, wide_a), bf),
    ]
    return pl.pallas_call(
        functools.partial(back_kernel, dims),
        out_shape=tuple(outs),
        in_specs=[vmem() for _ in inputs] + [hbm() for _ in range(3)],
        out_specs=tuple(vmem() for _ in outs),
        scratch_shapes=[
            pltpu.VMEM((width, width + 2 * head), bf),
            pltpu.VMEM((window * tok, tok), jnp.float32 if window * tok <= 2048 else bf),
            pltpu.VMEM((head, window * tok), bf),
            pltpu.VMEM((tok, width), jnp.float32),
            pltpu.VMEM((tok, width), jnp.float32),
            pltpu.VMEM((tok, width), bf),
            pltpu.VMEM((tok, width), bf),
            pltpu.VMEM((tok, width + 2 * head), bf),
            pltpu.VMEM((tok, width), bf),
            pltpu.VMEM((window * tok, 2 * head), jnp.float32),
            pltpu.VMEM((window - 1, tok, 2 * head), bf),
            pltpu.VMEM((window - 1, tok, 2 * head), bf),
            pltpu.VMEM((members, 3 * rank, part), bf),
            pltpu.VMEM((members * 3 * rank, part), bf),
            pltpu.VMEM((count, high_a, wide_a), bf),
            pltpu.VMEM((members, 2 * rank, part), bf),
            pltpu.VMEM((members * 2 * rank, part), bf),
            pltpu.VMEM((count, high_q, wide_a), bf),
            pltpu.VMEM((members, 4 * rank, part), bf),
            pltpu.VMEM((members * 4 * rank, part), bf),
            pltpu.VMEM((count, high_e, wide_a), bf),
            pltpu.VMEM((tok, width), bf),
            dma((1,)),
            dma((1,)),
            dma((7,)),
            dma((window - 1,)),
            dma((window - 1,)),
            dma((9,)),
            dma((9,)),
            dma((3, 2, count)),
            dma((3, 2, count)),
        ],
        compiler_params=pltpu.CompilerParams(
            collective_id=3, has_side_effects=True, vmem_limit_bytes=63 * 1024 * 1024
        ),
        name="back",
    )(*inputs, wq, wo, out_far)


def body(
    tokens,
    out_grad,
    segments,
    adapter_index,
    first_gain,
    first_bias,
    second_gain,
    second_bias,
    qkv_weight,
    out_weight,
    expand_weight,
    shrink_weight,
    query_first,
    query_second,
    key_first,
    key_second,
    value_first,
    value_second,
    output_first,
    output_second,
    expand_first,
    expand_second,
    shrink_first,
    shrink_second,
):
    count = lax.axis_size("ctx")
    members = lax.axis_size("wt")
    rank = query_second.shape[1]
    flip = lambda table: table.transpose(0, 2, 1)
    row = lambda vector: vector[None, :]
    tables = [
        flip(query_first),
        query_second,
        flip(key_first),
        key_second,
        flip(value_first),
        value_second,
        flip(output_first),
        output_second,
        flip(expand_first),
        expand_second,
        flip(shrink_first),
        shrink_second,
    ]
    picked = pick_call(adapter_index, tables, members)
    vectors = [row(first_gain), row(first_bias), row(second_gain), row(second_bias)]
    weights = (qkv_weight, out_weight, expand_weight, shrink_weight)
    core = core_call(tokens[0], out_grad[0], segments[0], vectors, picked, weights, count)
    back = back_call(
        tokens[0], out_grad[0], segments[0], vectors, picked, core, count, members
    )
    results = finish_call(
        back, core[10], core[9], query_first.shape[0], members, key_second.shape[2]
    )
    layer_out, tokens_grad = results[0][None], results[1][None]
    q_a, q_b, k_a, v_a, o_a, o_b, e_a, s_b, k_b, v_b, e_b, s_a = results[2:]
    return (
        layer_out,
        tokens_grad,
        flip(q_a),
        q_b,
        flip(k_a),
        k_b,
        flip(v_a),
        v_b,
        flip(o_a),
        o_b,
        flip(e_a),
        e_b,
        flip(s_a),
        s_b,
    )


def solution(mesh):
    placed = (
        P("wt", "ctx", None),
        P("wt", "ctx", None),
        P("wt", "ctx"),
        P("wt"),
        P(),
        P(),
        P(),
        P(),
        P("wt", None),
        P("wt", None),
        P("wt", None),
        P("wt", None),
        P(),
        P(),
        P(),
        P(),
        P(),
        P(),
        P(),
        P(),
        P(),
        P(),
        P(),
        P(),
    )
    return jax.shard_map(
        body,
        mesh=mesh,
        in_specs=placed,
        out_specs=(
            P("wt", "ctx", None),
            P("wt", "ctx", None),
            P(None, "wt", None),
            P(None, None, "wt"),
            P(None, "wt", None),
            P(None, None, "wt"),
            P(None, "wt", None),
            P(None, None, "wt"),
            P(None, "wt", None),
            P(None, None, "wt"),
            P(None, "wt", None),
            P(None, None, "wt"),
            P(None, "wt", None),
            P(None, None, "wt"),
        ),
        check_vma=False,
    )
```
